32 devices in a mesh: fsdp: 8 (over y, x, core), tensor: 4 (over z).
Axes of the slice: x: 2, y: 2, z: 4, core: 2. Of those that a mesh axis runs over, the one named last changes fastest.
Arguments:
- tokens: bfloat16 [16384, 1024], P(('fsdp', 'tensor')), may hold values from -6 to 6
- cotangent: bfloat16 [16384, 1024], P(('fsdp', 'tensor')), may hold values from -6 to 6
- qkv_weight: float32 [1024, 3, 1024], P('fsdp', None, 'tensor'), may hold values from -0.1875 to 0.1875
- qkv_bias: float32 [3, 1024], P(None, 'tensor'), may hold values from -3 to 3
- proj_weight: float32 [1024, 1024], P('fsdp', 'tensor'), may hold values from -0.1875 to 0.1875
- fc1_weight: float32 [1024, 4096], P('fsdp', 'tensor'), may hold values from -0.1875 to 0.1875
- fc1_bias: float32 [4096], P('tensor'), may hold values from -3 to 3
- fc2_weight: float32 [1024, 4096], P('fsdp', 'tensor'), may hold values from -0.09375 to 0.09375
- vectors: float32 [1024, 6], P('fsdp'), may hold values from -2 to 2, as said below
- row_state: float32 [4, 1024], P(None, 'fsdp'), may hold values from 802.816 to 83558.4, as said below
- qkv_cols: float32 [3, 1024], P(None, 'tensor'), may hold values from 802.816 to 83558.4, as said below
- proj_cols: float32 [1024], P('tensor'), may hold values from 802.816 to 83558.4, as said below
- fc1_cols: float32 [4096], P('tensor'), may hold values from 802.816 to 83558.4, as said below
- fc2_cols: float32 [4096], P('tensor'), may hold values from 802.816 to 83558.4, as said below
- vector_state: float32 [1024, 6], P('fsdp'), may hold values from 802.816 to 83558.4, as said below
- qkv_bias_state: float32 [3, 1024], P(None, 'tensor'), may hold values from 802.816 to 83558.4, as said below
- fc1_bias_state: float32 [4096], P('tensor'), may hold values from 802.816 to 83558.4, as said below
Outputs:
- layer_out: float32 [16384, 1024], P(('fsdp', 'tensor'))
- input_grad: float32 [16384, 1024], P(('fsdp', 'tensor'))
- qkv_weight_grad: float32 [1024, 3, 1024], P('fsdp', None, 'tensor')
- qkv_bias_grad: float32 [3, 1024], P(None, 'tensor')
- proj_weight_grad: float32 [1024, 1024], P('fsdp', 'tensor')
- fc1_weight_grad: float32 [1024, 4096], P('fsdp', 'tensor')
- fc1_bias_grad: float32 [4096], P('tensor')
- fc2_weight_grad: float32 [1024, 4096], P('fsdp', 'tensor')
- vectors_grad: float32 [1024, 6], P('fsdp')
- row_state_new: float32 [4, 1024], P(None, 'fsdp')
- qkv_cols_new: float32 [3, 1024], P(None, 'tensor')
- proj_cols_new: float32 [1024], P('tensor')
- fc1_cols_new: float32 [4096], P('tensor')
- fc2_cols_new: float32 [4096], P('tensor')
- vector_state_new: float32 [1024, 6], P('fsdp')
- qkv_bias_state_new: float32 [3, 1024], P(None, 'tensor')
- fc1_bias_state_new: float32 [4096], P('tensor')
- qkv_weight_new: float32 [1024, 3, 1024], P('fsdp', None, 'tensor')
- qkv_bias_new: float32 [3, 1024], P(None, 'tensor')
- proj_weight_new: float32 [1024, 1024], P('fsdp', 'tensor')
- fc1_weight_new: float32 [1024, 4096], P('fsdp', 'tensor')
- fc1_bias_new: float32 [4096], P('tensor')
- fc2_weight_new: float32 [1024, 4096], P('fsdp', 'tensor')
- vectors_new: float32 [1024, 6], P('fsdp')
- update_rms: float32 [4], replicated
The draws below stay inside these ranges and needn't reach their ends.
Inputs may be any that keep to these rules, and one draw needn't show every extreme that they name: `vectors`: columns 0 and 3 are gains between 0.5 and 1.5; the other columns are shifts. `row_state`: Positive. `qkv_cols`: Positive. `proj_cols`: Positive. `fc1_cols`: Positive. `fc2_cols`: Positive. `vector_state`: Positive. `qkv_bias_state`: Positive. `fc1_bias_state`: Positive.
All inputs are finite; a program needn't handle non-finite values.
Results may differ from the reference program's by a relative error of at most 0.0078.
Values may be sent and summed in bfloat16 or wider, within the bound.
A program may use at most 192 MiB of HBM per device.

```python
import math
import jax
import jax.numpy as jnp
from jax import lax

D = 1024
H = 16
HD = 64
FF = 4096
GH = 16
GW = 16
CLIPS = 2
LENGTH = 1024
TOKENS = 16384


def positive_state(key, extent):
    lowest = math.log(0.05)
    highest = math.log(5.0)
    spread = jax.random.uniform(key, extent, jnp.float32, lowest, highest)
    return jnp.exp(spread) * TOKENS


def draw_row_state(key, part):
    return positive_state(jax.random.fold_in(key, 11), (4, D))


def draw_qkv_cols(key, part):
    return positive_state(jax.random.fold_in(key, 12), (3, D))


def draw_proj_cols(key, part):
    return positive_state(jax.random.fold_in(key, 13), (D,))


def draw_fc1_cols(key, part):
    return positive_state(jax.random.fold_in(key, 14), (FF,))


def draw_fc2_cols(key, part):
    return positive_state(jax.random.fold_in(key, 15), (FF,))


def draw_vector_state(key, part):
    return positive_state(jax.random.fold_in(key, 16), (D, 6))


def draw_qkv_bias_state(key, part):
    return positive_state(jax.random.fold_in(key, 17), (3, D))


def draw_fc1_bias_state(key, part):
    return positive_state(jax.random.fold_in(key, 18), (FF,))


def draw_vectors(key, part):
    gain_key = jax.random.fold_in(key, 21)
    shift_key = jax.random.fold_in(key, 22)
    gain_draw = jnp.clip(1.0 + 0.2 * jax.random.normal(gain_key, (D, 6), jnp.float32), 0.5, 1.5)
    shifts = jnp.clip(0.5 * jax.random.normal(shift_key, (D, 6), jnp.float32), -2.0, 2.0)
    column = jnp.arange(6, dtype=jnp.int32)
    gain_column = (column == 0) | (column == 3)
    return jnp.where(gain_column[None, :], gain_draw, shifts)


def block_scale(own_key, shape, shards, low, top_value):
    level = 1.0
    for position, shards_of in shards:
        steps = jax.random.uniform(jax.random.fold_in(jax.random.fold_in(own_key, 6), position), (shards_of,), jnp.float32, low / len(shards), top_value / len(shards))
        level = level * jnp.repeat(jnp.exp(steps), shape[position] // shards_of).reshape((-1,) + (1,) * (len(shape) - 1 - position))
    return level


def normal_values(rng, dims, scale, bound, pieces=(), kind=jnp.bfloat16):
    loudness = block_scale(rng, dims, pieces, -0.22, 0.18) if pieces else 1.0
    result = jax.random.normal(rng, dims, jnp.float32) * scale * loudness
    return jnp.minimum(jnp.maximum(result, -bound), bound).astype(kind)


def setup_inputs(seed: int = 0) -> dict:
    seeds = jax.random.split(jax.random.key(seed), 18)
    tokens = normal_values(seeds[0], (TOKENS, D), 1.0, 6.0, ((0, 32),))
    cotangent = normal_values(seeds[1], (TOKENS, D), 1.0, 6.0, ((0, 32),))
    qkv_weight = normal_values(seeds[2], (D, 3, D), D ** -0.5, 0.1875, ((0, 8), (2, 4)), jnp.float32)
    qkv_bias = normal_values(seeds[3], (3, D), 0.5, 3.0, ((1, 4),), jnp.float32)
    proj_weight = normal_values(seeds[4], (D, D), D ** -0.5, 0.1875, ((0, 8), (1, 4)), jnp.float32)
    fc1_weight = normal_values(seeds[5], (D, FF), D ** -0.5, 0.1875, ((0, 8), (1, 4)), jnp.float32)
    fc1_bias = normal_values(seeds[6], (FF,), 0.5, 3.0, ((0, 4),), jnp.float32)
    fc2_weight = normal_values(seeds[7], (D, FF), FF ** -0.5, 0.09375, ((0, 8), (1, 4)), jnp.float32)
    vectors = draw_vectors(jax.random.fold_in(seeds[17], 71), 0)
    row_state = draw_row_state(jax.random.fold_in(seeds[17], 71), 0)
    qkv_cols = draw_qkv_cols(jax.random.fold_in(seeds[17], 71), 0)
    proj_cols = draw_proj_cols(jax.random.fold_in(seeds[17], 71), 0)
    fc1_cols = draw_fc1_cols(jax.random.fold_in(seeds[17], 71), 0)
    fc2_cols = draw_fc2_cols(jax.random.fold_in(seeds[17], 71), 0)
    vector_state = draw_vector_state(jax.random.fold_in(seeds[17], 71), 0)
    qkv_bias_state = draw_qkv_bias_state(jax.random.fold_in(seeds[17], 71), 0)
    fc1_bias_state = draw_fc1_bias_state(jax.random.fold_in(seeds[17], 71), 0)
    return dict(tokens=tokens, cotangent=cotangent, qkv_weight=qkv_weight, qkv_bias=qkv_bias, proj_weight=proj_weight, fc1_weight=fc1_weight, fc1_bias=fc1_bias, fc2_weight=fc2_weight, vectors=vectors, row_state=row_state, qkv_cols=qkv_cols, proj_cols=proj_cols, fc1_cols=fc1_cols, fc2_cols=fc2_cols, vector_state=vector_state, qkv_bias_state=qkv_bias_state, fc1_bias_state=fc1_bias_state)


NORM_EPS = 1e-06
DECAY = 0.5
CLIP_LEVEL = 1.0
RATE = 0.3
TINY = 1e-30
BASE = 10000.0

@jax.custom_vjp
def low(v):
    return lax.optimization_barrier(v.astype(jnp.bfloat16)).astype(jnp.float32)

@jax.custom_vjp
def low_back(v):
    return v

def low_keep(v):
    return (low(v), None)

def low_pass(kept, grad):
    return (grad,)

def back_keep(v):
    return (v, None)

def back_low(kept, grad):
    return (low(grad),)
low.defvjp(low_keep, low_pass)
low_back.defvjp(back_keep, back_low)

def dot_high(left, right):
    return jnp.dot(left, right, precision=lax.Precision.HIGHEST, preferred_element_type=jnp.float32)

def layer_norm(values, gain_row, shift_row):
    center = values - lax.optimization_barrier(jnp.mean(values, axis=-1, keepdims=True))
    variance = lax.optimization_barrier(jnp.mean(center * center, axis=-1, keepdims=True))
    return center * lax.rsqrt(variance + NORM_EPS) * gain_row + shift_row

def rope_tables(length, half_width):
    token_index = jnp.arange(length, dtype=jnp.int32)
    coordinates = jnp.stack([token_index // (GH * GW), token_index // GW % GH, token_index % GW], axis=1).astype(jnp.float32)
    frequency = BASE ** (-jnp.arange(half_width, dtype=jnp.float32) / half_width)
    angles = coordinates[:, :, None] * frequency[None, None, :]
    return (jnp.cos(angles), jnp.sin(angles))

def rotate(values, cosine_table, sine_table):
    half_width = cosine_table.shape[-1]
    rotated_width = 6 * half_width
    leading = values.shape[:-1]
    pair_rows = values[..., :rotated_width].reshape(leading + (3, 2, half_width))
    first_half = pair_rows[..., 0, :]
    second_half = pair_rows[..., 1, :]
    cosine_wide = cosine_table[:, None]
    sine_wide = sine_table[:, None]
    turned = jnp.stack([first_half * cosine_wide - second_half * sine_wide, second_half * cosine_wide + first_half * sine_wide], axis=-2)
    return jnp.concatenate([turned.reshape(leading + (rotated_width,)), values[..., rotated_width:]], axis=-1)

def attend_block(query_block, key_rows, value_rows):
    scores = jnp.einsum('qhd,khd->hqk', query_block, key_rows, precision=lax.Precision.HIGHEST) * HD ** (-0.5)
    scores = low_back(scores)
    row_peak = lax.optimization_barrier(jnp.max(scores, axis=-1, keepdims=True))
    raised = jnp.exp(scores - row_peak)
    attention = low(raised / lax.optimization_barrier(jnp.sum(raised, axis=-1, keepdims=True)))
    return jnp.einsum('hqk,khd->qhd', attention, value_rows, precision=lax.Precision.HIGHEST)

def attend_clip(clip_item):
    query_rows, key_rows, value_rows = clip_item
    length = query_rows.shape[0]
    block_rows = min(512, length)
    blocks = query_rows.reshape((length // block_rows, block_rows) + query_rows.shape[1:])
    block_step = jax.checkpoint(lambda query_block: attend_block(query_block, key_rows, value_rows))
    return lax.map(block_step, blocks).reshape(query_rows.shape)

def group_forward(inputs, qkv_weight, qkv_bias, proj_weight, fc1_weight, fc1_bias, fc2_weight, vectors):
    weight_qkv = low(qkv_weight)
    bias_qkv = low(qkv_bias)
    weight_proj = low(proj_weight)
    weight_up = low(fc1_weight)
    bias_up = low(fc1_bias)
    weight_down = low(fc2_weight)
    vector_low = low(vectors)
    gain_one = vector_low[:, 0]
    shift_one = vector_low[:, 1]
    proj_shift = vector_low[:, 2]
    gain_two = vector_low[:, 3]
    shift_two = vector_low[:, 4]
    down_shift = vector_low[:, 5]
    normed_one = low(layer_norm(inputs, gain_one, shift_one))
    projected = dot_high(normed_one, weight_qkv.reshape(D, 3 * D)) + bias_qkv.reshape(3 * D)
    projected = low_back(projected).reshape(CLIPS, LENGTH, 3, H, HD)
    cosine_table, sine_table = rope_tables(LENGTH, HD // 3 // 2)
    queries = low(rotate(projected[:, :, 0], cosine_table, sine_table))
    key_rows = low(rotate(projected[:, :, 1], cosine_table, sine_table))
    value_rows = low(projected[:, :, 2])
    mixed_rows = lax.map(attend_clip, (queries, key_rows, value_rows))
    mixed_rows = low(low_back(mixed_rows.reshape(CLIPS * LENGTH, D)))
    branch = low_back(dot_high(mixed_rows, weight_proj.T) + proj_shift)
    middle = inputs + branch
    normed_two = low(layer_norm(middle, gain_two, shift_two))
    hidden = low_back(dot_high(normed_two, weight_up) + bias_up)
    active = low(jax.nn.gelu(hidden, approximate=False))
    return middle + low_back(dot_high(active, weight_down.T) + down_shift)

def factored_update(grad, weight, rows_old, cols_old):
    squares = grad * grad + TINY
    rows_new = DECAY * rows_old + (1.0 - DECAY) * lax.optimization_barrier(jnp.mean(squares, axis=1))
    cols_new = DECAY * cols_old + (1.0 - DECAY) * lax.optimization_barrier(jnp.mean(squares, axis=0))
    second = rows_new[:, None] * cols_new[None, :] / jnp.mean(rows_new)
    direction = grad * lax.rsqrt(second)
    spread = jnp.sqrt(jnp.mean(direction * direction))
    weight_scale = jnp.sqrt(jnp.mean(weight * weight))
    new_weight = weight - RATE * weight_scale * direction / jnp.maximum(1.0, spread / CLIP_LEVEL)
    return (rows_new, cols_new, new_weight, spread)

def vector_update(grad, weight, state_old):
    state_new = DECAY * state_old + (1.0 - DECAY) * (grad * grad + TINY)
    direction = grad * lax.rsqrt(state_new)
    spread = jnp.sqrt(lax.optimization_barrier(jnp.mean(direction * direction, axis=0)))
    weight_scale = jnp.sqrt(lax.optimization_barrier(jnp.mean(weight * weight, axis=0)))
    return (state_new, weight - RATE * weight_scale * direction / jnp.maximum(1.0, spread / CLIP_LEVEL))

def reference(tokens, cotangent, qkv_weight, qkv_bias, proj_weight, fc1_weight, fc1_bias, fc2_weight, vectors, row_state, qkv_cols, proj_cols, fc1_cols, fc2_cols, vector_state, qkv_bias_state, fc1_bias_state):
    group_rows = CLIPS * LENGTH
    inputs = tokens.astype(jnp.float32).reshape(-1, group_rows, D)
    upstream = cotangent.astype(jnp.float32).reshape(-1, group_rows, D)
    parameters = (qkv_weight, qkv_bias, proj_weight, fc1_weight, fc1_bias, fc2_weight, vectors)

    def one_group(running, group_pair):
        outputs, pullback = jax.vjp(group_forward, group_pair[0], *parameters)
        gradients = pullback(group_pair[1])
        return (tuple((total + extra for total, extra in zip(running, gradients[1:]))), (outputs, gradients[0]))
    starts = tuple((jnp.zeros(entry.shape, jnp.float32) for entry in parameters))
    gradients, (outputs, input_grads) = lax.scan(one_group, starts, (inputs, upstream))
    grad_qkv, grad_qkv_bias, grad_proj, grad_up, grad_up_bias, grad_down, grad_vectors = gradients
    rows_qkv, cols_qkv, new_qkv, spread_qkv = factored_update(grad_qkv.reshape(D, 3 * D), qkv_weight.reshape(D, 3 * D), row_state[0], qkv_cols.reshape(3 * D))
    rows_proj, cols_proj, new_proj, spread_proj = factored_update(grad_proj, proj_weight, row_state[1], proj_cols)
    rows_up, cols_up, new_up, spread_up = factored_update(grad_up, fc1_weight, row_state[2], fc1_cols)
    rows_down, cols_down, new_down, spread_down = factored_update(grad_down, fc2_weight, row_state[3], fc2_cols)
    vector_state_new, vectors_new = vector_update(grad_vectors, vectors, vector_state)
    qkv_state_new, qkv_bias_new = vector_update(grad_qkv_bias.reshape(3 * D), qkv_bias.reshape(3 * D), qkv_bias_state.reshape(3 * D))
    up_state_new, up_bias_new = vector_update(grad_up_bias, fc1_bias, fc1_bias_state)
    return (outputs.reshape(-1, D), input_grads.reshape(-1, D), grad_qkv, grad_qkv_bias, grad_proj, grad_up, grad_up_bias, grad_down, grad_vectors, jnp.stack([rows_qkv, rows_proj, rows_up, rows_down]), cols_qkv.reshape(3, D), cols_proj, cols_up, cols_down, vector_state_new, qkv_state_new.reshape(3, D), up_state_new, new_qkv.reshape(D, 3, D), qkv_bias_new.reshape(3, D), new_proj, new_up, up_bias_new, new_down, vectors_new, jnp.stack([spread_qkv, spread_proj, spread_up, spread_down]))
```

```python
import functools

import jax
import jax.numpy as jnp
from jax import lax
from jax.experimental import pallas as pl
from jax.experimental.pallas import tpu as pltpu
from jax.sharding import PartitionSpec as P

D = 1024
HD = 64
FF = 4096
GT = 4
GH = 16
GW = 16


NORM_EPS = 1e-06
DECAY = 0.5
CLIP_LEVEL = 1.0
RATE = 0.3
TINY = 1e-30
BASE = 10000.0


def layer_norm(values, gain_row, shift_row):
    center = values - jnp.mean(values, axis=-1, keepdims=True)
    variance = jnp.mean(center * center, axis=-1, keepdims=True)
    return center * lax.rsqrt(variance + NORM_EPS) * gain_row + shift_row


def exact_gelu(values):
    return jax.nn.gelu(values, approximate=False)


def rope_tables(length, half_width):
    token_index = jnp.arange(length, dtype=jnp.int32)
    coordinates = jnp.stack(
        [token_index // (GH * GW), token_index // GW % GH, token_index % GW], axis=1
    ).astype(jnp.float32)
    frequency = BASE ** (-jnp.arange(half_width, dtype=jnp.float32) / half_width)
    angles = coordinates[:, :, None] * frequency[None, None, :]
    return (jnp.cos(angles), jnp.sin(angles))


def rotate(values, cosine_table, sine_table):
    half_width = cosine_table.shape[-1]
    rotated_width = 6 * half_width
    leading = values.shape[:-1]
    pair_rows = values[..., :rotated_width].reshape(leading + (3, 2, half_width))
    first_half = pair_rows[..., 0, :]
    second_half = pair_rows[..., 1, :]
    cosine_wide = cosine_table[:, None]
    sine_wide = sine_table[:, None]
    turned = jnp.stack(
        [
            first_half * cosine_wide - second_half * sine_wide,
            second_half * cosine_wide + first_half * sine_wide,
        ],
        axis=-2,
    )
    return jnp.concatenate(
        [turned.reshape(leading + (rotated_width,)), values[..., rotated_width:]], axis=-1
    )


def contract_rows(left, right):
    return lax.dot_general(
        left, right, (((0,), (0,)), ((), ())), preferred_element_type=jnp.float32
    )


def times_transposed(left, right):
    return lax.dot_general(
        left, right, (((1,), (1,)), ((), ())), preferred_element_type=jnp.float32
    )


def forward_block(query_rows, key_rows, value_rows):
    score_scale = query_rows.shape[-1] ** (-0.5)
    scores = (
        jnp.einsum("qhd,khd->hqk", query_rows, key_rows, preferred_element_type=jnp.float32)
        * score_scale
    )
    row_peak = jnp.max(scores, axis=-1, keepdims=True)
    raised = jnp.exp(scores - row_peak)
    totals = jnp.sum(raised, axis=-1, keepdims=True)
    attention = (raised / totals).astype(jnp.bfloat16)
    mixed_rows = jnp.einsum(
        "hqk,khd->qhd", attention, value_rows, preferred_element_type=jnp.float32
    )
    return (mixed_rows, (row_peak + jnp.log(totals))[..., 0])


def backward_block(running, block_item, key_rows, value_rows):
    query_rows, log_totals, grad_mixed = block_item
    score_scale = query_rows.shape[-1] ** (-0.5)
    scores = (
        jnp.einsum("qhd,khd->hqk", query_rows, key_rows, preferred_element_type=jnp.float32)
        * score_scale
    )
    attention = jnp.exp(scores - log_totals[..., None])
    grad_attention = jnp.einsum(
        "qhd,khd->hqk", grad_mixed, value_rows, preferred_element_type=jnp.float32
    )
    grad_scores = attention * (
        grad_attention - jnp.sum(attention * grad_attention, axis=-1, keepdims=True)
    )
    grad_low = grad_scores.astype(jnp.bfloat16)
    grad_queries = (
        jnp.einsum("hqk,khd->qhd", grad_low, key_rows, preferred_element_type=jnp.float32)
        * score_scale
    )
    key_total = (
        running[0]
        + jnp.einsum("hqk,qhd->khd", grad_low, query_rows, preferred_element_type=jnp.float32)
        * score_scale
    )
    value_total = running[1] + jnp.einsum(
        "hqk,qhd->khd",
        attention.astype(jnp.bfloat16),
        grad_mixed,
        preferred_element_type=jnp.float32,
    )
    return ((key_total, value_total), grad_queries)


def on_device(
    tokens,
    cotangent,
    qkv_weight,
    qkv_bias,
    proj_weight,
    fc1_weight,
    fc1_bias,
    fc2_weight,
    vectors,
    row_state,
    qkv_cols,
    proj_cols,
    fc1_cols,
    fc2_cols,
    vector_state,
    qkv_bias_state,
    fc1_bias_state,
):
    low_type = jnp.bfloat16
    lane_count = lax.axis_size("tensor")
    local_rows = tokens.shape[0]
    group_rows = local_rows * lane_count
    length = GT * GH * GW
    clip_count = group_rows // length
    block_rows = min(512, length)
    block_count = length // block_rows
    head_width = qkv_weight.shape[2]
    head_count = head_width // HD
    hidden_width = fc1_weight.shape[1]
    shard_rows = qkv_weight.shape[0]
    cosine_table, sine_table = rope_tables(length, HD // 3 // 2)
    weight_qkv, weight_proj, weight_up, weight_down, vector_low = (
        lax.all_gather(qkv_weight.astype(low_type), "fsdp", axis=0, tiled=True),
        lax.all_gather(proj_weight.astype(low_type), "fsdp", axis=0, tiled=True),
        lax.all_gather(fc1_weight.astype(low_type), "fsdp", axis=0, tiled=True),
        lax.all_gather(fc2_weight.astype(low_type), "fsdp", axis=0, tiled=True),
        lax.all_gather(vectors.astype(low_type), "fsdp", axis=0, tiled=True),
    )
    weight_qkv = weight_qkv.reshape(D, 3 * head_width)
    vector_full = vector_low.astype(jnp.float32)
    gain_one = vector_full[:, 0]
    shift_one = vector_full[:, 1]
    proj_shift = vector_full[:, 2]
    gain_two = vector_full[:, 3]
    shift_two = vector_full[:, 4]
    down_shift = vector_full[:, 5]
    bias_qkv = (
        lax.optimization_barrier(qkv_bias.astype(low_type))
        .astype(jnp.float32)
        .reshape(3 * head_width)
    )
    bias_up = lax.optimization_barrier(fc1_bias.astype(low_type)).astype(jnp.float32)
    inputs = tokens.astype(jnp.float32)
    normed_one = layer_norm(inputs, gain_one, shift_one).astype(low_type)
    gathered_one = lax.all_gather(normed_one, "tensor", axis=0, tiled=True)
    projected = jnp.dot(gathered_one, weight_qkv, preferred_element_type=jnp.float32) + bias_qkv
    projected = projected.reshape(clip_count, length, 3, head_count, HD)
    queries = rotate(projected[:, :, 0], cosine_table, sine_table).astype(low_type)
    key_rows = rotate(projected[:, :, 1], cosine_table, sine_table).astype(low_type)
    value_rows = projected[:, :, 2].astype(low_type)

    def clip_forward(clip_item):
        query_rows, clip_keys, clip_values = clip_item
        blocks = query_rows.reshape(block_count, block_rows, head_count, HD)
        return lax.map(
            lambda query_block: forward_block(query_block, clip_keys, clip_values), blocks
        )

    mixed_rows, log_totals = lax.map(clip_forward, (queries, key_rows, value_rows))
    mixed_low = mixed_rows.reshape(group_rows, head_width).astype(low_type)
    attn_sum = lax.psum_scatter(
        times_transposed(mixed_low, weight_proj), "tensor", scatter_dimension=0, tiled=True
    )
    middle = inputs + attn_sum + proj_shift
    normed_two = layer_norm(middle, gain_two, shift_two).astype(low_type)
    gathered_two = lax.all_gather(normed_two, "tensor", axis=0, tiled=True)
    hidden = jnp.dot(gathered_two, weight_up, preferred_element_type=jnp.float32) + bias_up
    active = exact_gelu(hidden).astype(low_type)
    layer_out = (
        middle
        + lax.psum_scatter(
            times_transposed(active, weight_down), "tensor", scatter_dimension=0, tiled=True
        )
        + down_shift
    )
    upstream = cotangent.astype(jnp.float32)
    grad_out_all, normed_two_all = (
        lax.all_gather(cotangent, "tensor", axis=0, tiled=True),
        lax.all_gather(normed_two, "tensor", axis=0, tiled=True),
    )
    grad_down = contract_rows(grad_out_all, active)
    grad_active = jnp.dot(grad_out_all, weight_down, preferred_element_type=jnp.float32)
    gelu_pull = jax.vjp(exact_gelu, hidden)[1]
    grad_hidden = gelu_pull(grad_active)[0].astype(low_type)
    grad_up = contract_rows(normed_two_all, grad_hidden)
    grad_bias_up = jnp.sum(grad_hidden.astype(jnp.float32), axis=0)
    grad_normed_two = lax.psum_scatter(
        times_transposed(grad_hidden, weight_up), "tensor", scatter_dimension=0, tiled=True
    )
    middle_part, grad_gain_two, grad_shift_two = jax.vjp(layer_norm, middle, gain_two, shift_two)[
        1
    ](grad_normed_two)
    grad_middle = upstream + middle_part
    grad_branch = grad_middle.astype(low_type)
    grad_proj_shift = jnp.sum(grad_branch.astype(jnp.float32), axis=0)
    grad_down_shift = jnp.sum(upstream, axis=0)
    grad_branch_all, normed_one_all = (
        lax.all_gather(grad_branch, "tensor", axis=0, tiled=True),
        lax.all_gather(normed_one, "tensor", axis=0, tiled=True),
    )
    grad_proj = contract_rows(grad_branch_all, mixed_low)
    grad_mixed = jnp.dot(grad_branch_all, weight_proj, preferred_element_type=jnp.float32).astype(
        low_type
    )
    grad_mixed = grad_mixed.reshape(clip_count, length, head_count, HD)

    def clip_backward(clip_item):
        query_rows, clip_keys, clip_values, clip_totals, clip_grads = clip_item
        starts = (jnp.zeros(clip_keys.shape, jnp.float32), jnp.zeros(clip_keys.shape, jnp.float32))
        block_items = (
            query_rows.reshape(block_count, block_rows, head_count, HD),
            clip_totals,
            clip_grads.reshape(block_count, block_rows, head_count, HD),
        )
        sums, grad_queries = lax.scan(
            lambda running, block_item: backward_block(running, block_item, clip_keys, clip_values),
            starts,
            block_items,
        )
        return (grad_queries.reshape(query_rows.shape), sums[0], sums[1])

    grad_queries, grad_keys, grad_values = lax.map(
        clip_backward, (queries, key_rows, value_rows, log_totals, grad_mixed)
    )
    grad_projected = jnp.stack(
        [
            rotate(grad_queries, cosine_table, -sine_table),
            rotate(grad_keys, cosine_table, -sine_table),
            grad_values,
        ],
        axis=2,
    )
    grad_projected = grad_projected.reshape(group_rows, 3 * head_width).astype(low_type)
    grad_qkv = contract_rows(normed_one_all, grad_projected).reshape(D, 3, head_width)
    grad_bias_qkv = jnp.sum(grad_projected.astype(jnp.float32), axis=0)
    grad_normed_one = lax.psum_scatter(
        times_transposed(grad_projected, weight_qkv), "tensor", scatter_dimension=0, tiled=True
    )
    input_part, grad_gain_one, grad_shift_one = jax.vjp(layer_norm, inputs, gain_one, shift_one)[1](
        grad_normed_one
    )
    input_grad = grad_middle + input_part
    grad_qkv, grad_proj, grad_up, grad_down = (
        lax.psum_scatter(grad_qkv, "fsdp", scatter_dimension=0, tiled=True),
        lax.psum_scatter(grad_proj, "fsdp", scatter_dimension=0, tiled=True),
        lax.psum_scatter(grad_up, "fsdp", scatter_dimension=0, tiled=True),
        lax.psum_scatter(grad_down, "fsdp", scatter_dimension=0, tiled=True),
    )
    lane_index = lax.axis_index("tensor")
    vector_part = jnp.stack(
        [
            grad_gain_one,
            grad_shift_one,
            grad_proj_shift,
            grad_gain_two,
            grad_shift_two,
            grad_down_shift,
        ],
        axis=1,
    )
    qkv_placed = lax.dynamic_update_slice(
        jnp.zeros((3, D), jnp.float32),
        grad_bias_qkv.reshape(3, head_width),
        (jnp.int32(0), lane_index * head_width),
    )
    up_placed = lax.dynamic_update_slice(
        jnp.zeros((FF,), jnp.float32), grad_bias_up, (lane_index * hidden_width,)
    )
    vector_total, qkv_total, up_total = lax.psum(
        (vector_part, qkv_placed, up_placed), ("fsdp", "tensor")
    )
    grad_vectors = lax.dynamic_slice_in_dim(
        vector_total, lax.axis_index("fsdp") * shard_rows, shard_rows, 0
    )
    grad_qkv_bias = lax.dynamic_slice_in_dim(qkv_total, lane_index * head_width, head_width, 1)
    grad_up_bias = lax.dynamic_slice_in_dim(up_total, lane_index * hidden_width, hidden_width, 0)
    matrices = [
        (
            grad_qkv.reshape(shard_rows, 3 * head_width),
            qkv_weight.reshape(shard_rows, 3 * head_width),
            qkv_cols.reshape(3 * head_width),
        ),
        (grad_proj, proj_weight, proj_cols),
        (grad_up, fc1_weight, fc1_cols),
        (grad_down, fc2_weight, fc2_cols),
    ]
    column_counts = [3 * D, D, FF, FF]
    column_weights = jnp.array(column_counts, jnp.float32)
    qkv_state_new = DECAY * qkv_bias_state + (1.0 - DECAY) * (grad_qkv_bias * grad_qkv_bias + TINY)
    qkv_direction = grad_qkv_bias * lax.rsqrt(qkv_state_new)
    up_state_new = DECAY * fc1_bias_state + (1.0 - DECAY) * (grad_up_bias * grad_up_bias + TINY)
    up_direction = grad_up_bias * lax.rsqrt(up_state_new)
    row_squares = jnp.stack(
        [jnp.sum(matrix_entry[0] * matrix_entry[0], axis=1) for matrix_entry in matrices]
    )
    weight_squares = jnp.stack(
        [jnp.sum(matrix_entry[1] * matrix_entry[1]) for matrix_entry in matrices]
    )
    bias_terms = jnp.stack(
        [
            jnp.sum(qkv_direction * qkv_direction),
            jnp.sum(up_direction * up_direction),
            jnp.sum(qkv_bias * qkv_bias),
            jnp.sum(fc1_bias * fc1_bias),
        ]
    )
    row_total, weight_partial, bias_total = lax.psum(
        (row_squares, weight_squares, bias_terms), "tensor"
    )
    rows_new = DECAY * row_state + (1.0 - DECAY) * (row_total / column_weights[:, None] + TINY)
    vector_state_new = DECAY * vector_state + (1.0 - DECAY) * (grad_vectors * grad_vectors + TINY)
    vector_direction = grad_vectors * lax.rsqrt(vector_state_new)
    vector_terms = jnp.stack(
        [jnp.sum(vector_direction * vector_direction, axis=0), jnp.sum(vectors * vectors, axis=0)]
    )
    col_squares = jnp.concatenate(
        [jnp.sum(matrix_entry[0] * matrix_entry[0], axis=0) for matrix_entry in matrices]
    )
    row_new_sums = jnp.sum(rows_new, axis=1)
    col_total, row_new_total, weight_total, vector_sums = lax.psum(
        (col_squares, row_new_sums, weight_partial, vector_terms), "fsdp"
    )
    mean_rows = row_new_total / D
    offsets = [0]
    for matrix_entry in matrices:
        offsets.append(offsets[-1] + matrix_entry[0].shape[1])
    cols_list = []
    direction_list = []
    square_list = []
    for position, matrix_entry in enumerate(matrices):
        col_slice = col_total[offsets[position] : offsets[position + 1]]
        cols_new = DECAY * matrix_entry[2] + (1.0 - DECAY) * (col_slice / D + TINY)
        direction = matrix_entry[0] * lax.rsqrt(
            rows_new[position][:, None] * cols_new[None, :] / mean_rows[position]
        )
        cols_list.append(cols_new)
        direction_list.append(direction)
        square_list.append(jnp.sum(direction * direction))
    square_total = lax.psum(jnp.stack(square_list), ("fsdp", "tensor"))
    matrix_count = D * column_weights
    update_rms = jnp.sqrt(square_total / matrix_count)
    weight_scale = jnp.sqrt(weight_total / matrix_count)
    new_weights = []
    for position, matrix_entry in enumerate(matrices):
        new_weights.append(
            matrix_entry[1]
            - RATE
            * weight_scale[position]
            * direction_list[position]
            / jnp.maximum(1.0, update_rms[position] / CLIP_LEVEL)
        )
    vector_rms = jnp.sqrt(vector_sums[0] / D)
    vector_scale = jnp.sqrt(vector_sums[1] / D)
    vectors_new = vectors - RATE * vector_scale * vector_direction / jnp.maximum(
        1.0, vector_rms / CLIP_LEVEL
    )
    qkv_rms = jnp.sqrt(bias_total[0] / (3 * D))
    qkv_scale = jnp.sqrt(bias_total[2] / (3 * D))
    qkv_bias_new = qkv_bias - RATE * qkv_scale * qkv_direction / jnp.maximum(
        1.0, qkv_rms / CLIP_LEVEL
    )
    up_rms = jnp.sqrt(bias_total[1] / FF)
    up_scale = jnp.sqrt(bias_total[3] / FF)
    up_bias_new = fc1_bias - RATE * up_scale * up_direction / jnp.maximum(1.0, up_rms / CLIP_LEVEL)
    return (
        layer_out,
        input_grad,
        grad_qkv,
        grad_qkv_bias,
        grad_proj,
        grad_up,
        grad_up_bias,
        grad_down,
        grad_vectors,
        rows_new,
        cols_list[0].reshape(3, head_width),
        cols_list[1],
        cols_list[2],
        cols_list[3],
        vector_state_new,
        qkv_state_new,
        up_state_new,
        new_weights[0].reshape(shard_rows, 3, head_width),
        qkv_bias_new,
        new_weights[1],
        new_weights[2],
        up_bias_new,
        new_weights[3],
        vectors_new,
        update_rms,
    )


SCALE = HD**-0.5
LENGTH = GT * GH * GW
ROLL = HD // 3 // 2
CORE_SWAP = [(i, i ^ 1) for i in range(8)]
LOW = jnp.bfloat16
QB = 256


def chip_tables(core):
    rows = lax.broadcasted_iota(jnp.int32, (LENGTH, 2 * HD), 0)
    token = (rows + core * (LENGTH // 2)) % LENGTH
    lane = lax.broadcasted_iota(jnp.int32, (LENGTH, 2 * HD), 1) % HD
    axis = lane // (2 * ROLL)
    within = lane % (2 * ROLL)
    coordinate = jnp.where(
        axis == 0, token // (GH * GW), jnp.where(axis == 1, token // GW % GH, token % GW)
    ).astype(jnp.float32)
    step = (within % ROLL).astype(jnp.float32)
    frequency = BASE ** (-step / ROLL)
    live = lane < 6 * ROLL
    angle = jnp.where(live, coordinate * frequency, 0.0)
    cosine = jnp.cos(angle)
    sine = jnp.sin(angle)
    second = within >= ROLL
    from_first = jnp.where(live & second, sine, 0.0)
    from_second = jnp.where(live & ~second, -sine, 0.0)
    return cosine, from_first, from_second


def turn(v, c, s1, s2, sign):
    return v * c + sign * (pltpu.roll(v, ROLL, 1) * s1 + pltpu.roll(v, 2 * HD - ROLL, 1) * s2)


def dot_nt(a, b):
    return lax.dot_general(a, b, (((1,), (1,)), ((), ())), preferred_element_type=jnp.float32)


def dot_tn(a, b):
    return lax.dot_general(a, b, (((0,), (0,)), ((), ())), preferred_element_type=jnp.float32)


def dot_nn(a, b):
    return lax.dot_general(a, b, (((1,), (0,)), ((), ())), preferred_element_type=jnp.float32)


def attend_kernel(x_ref, c_ref, s1_ref, s2_ref, low_ref, o_ref, lse_ref, kh_ref, vh_ref):
    width = 2 * HD
    c, s1, s2 = c_ref[...], s1_ref[...], s2_ref[...]
    lane = lax.broadcasted_iota(jnp.int32, (LENGTH, width), 1)
    low_ref[:, :width] = turn(x_ref[:, :width], c, s1, s2, 1.0).astype(LOW)
    k = turn(x_ref[:, width : 2 * width], c, s1, s2, 1.0)
    v = x_ref[:, 2 * width :]
    low_ref[:, width : 2 * width] = k.astype(LOW)
    low_ref[:, 2 * width :] = v.astype(LOW)
    for h in range(2):
        mine = (lane < HD) if h == 0 else (lane >= HD)
        kh_ref[h] = jnp.where(mine, k, 0.0).astype(LOW)
        vh_ref[h] = jnp.where(mine, v, 0.0).astype(LOW)

    def block(j, carry):
        rows = pl.ds(pl.multiple_of(j * QB, QB), QB)
        q = (low_ref[rows, :width].astype(jnp.float32) * SCALE).astype(LOW)
        total = jnp.zeros((width, QB), jnp.float32)
        for h in range(2):
            s = dot_nt(kh_ref[h], q)
            peak = jnp.max(s, axis=0, keepdims=True)
            e = jnp.exp(s - peak)
            mass = jnp.sum(e, axis=0, keepdims=True)
            p = (e * (1.0 / mass)).astype(LOW)
            total += dot_tn(vh_ref[h], p)
            lse_ref[0, h : h + 1, rows] = peak + jnp.log(mass)
        o_ref[rows, :] = total.T.astype(LOW)
        return carry

    lax.fori_loop(0, LENGTH // QB, block, 0)


def attend(projected, tables):
    lanes = projected.shape[1] // (6 * HD)
    table = pl.BlockSpec((LENGTH, 2 * HD), lambda z: (0, 0))
    return pl.pallas_call(
        attend_kernel,
        grid=(lanes,),
        in_specs=[pl.BlockSpec((LENGTH, 6 * HD), lambda z: (0, z)), table, table, table],
        out_specs=[
            pl.BlockSpec((LENGTH, 6 * HD), lambda z: (0, z)),
            pl.BlockSpec((LENGTH, 2 * HD), lambda z: (0, z)),
            pl.BlockSpec((1, 2, LENGTH), lambda z: (z, 0, 0)),
        ],
        out_shape=[
            jax.ShapeDtypeStruct((LENGTH, lanes * 6 * HD), LOW),
            jax.ShapeDtypeStruct((LENGTH, lanes * 2 * HD), LOW),
            jax.ShapeDtypeStruct((lanes, 2, LENGTH), jnp.float32),
        ],
        scratch_shapes=[pltpu.VMEM((2, LENGTH, 2 * HD), LOW), pltpu.VMEM((2, LENGTH, 2 * HD), LOW)],
        compiler_params=pltpu.CompilerParams(vmem_limit_bytes=40 * 1024 * 1024),
        cost_estimate=pl.CostEstimate(
            flops=16 * LENGTH * LENGTH * HD * lanes,
            bytes_accessed=20 * LENGTH * HD * lanes,
            transcendentals=2 * lanes * LENGTH * LENGTH,
        ),
        name="attend",
    )(projected, *tables)


def attend_back_kernel(
    low_ref, go_ref, lse_ref, c_ref, s1_ref, s2_ref, g_ref, sum_ref, kh_ref, vh_ref, gk_ref, gv_ref
):
    width = 2 * HD
    lane = lax.broadcasted_iota(jnp.int32, (LENGTH, width), 1)
    lane_q = lax.broadcasted_iota(jnp.int32, (QB, width), 1)
    k = low_ref[:, width : 2 * width].astype(jnp.float32)
    v = low_ref[:, 2 * width :].astype(jnp.float32)
    for h in range(2):
        mine = (lane < HD) if h == 0 else (lane >= HD)
        kh_ref[h] = jnp.where(mine, k, 0.0).astype(LOW)
        vh_ref[h] = jnp.where(mine, v, 0.0).astype(LOW)
    gk_ref[...] = jnp.zeros_like(gk_ref)
    gv_ref[...] = jnp.zeros_like(gv_ref)

    def block(j, carry):
        rows = pl.ds(pl.multiple_of(j * QB, QB), QB)
        q = low_ref[rows, :width].astype(jnp.float32) * SCALE
        go = go_ref[rows, :].astype(jnp.float32)
        total = jnp.zeros((width, QB), jnp.float32)
        for h in range(2):
            mine = (lane_q < HD) if h == 0 else (lane_q >= HD)
            qh = jnp.where(mine, q, 0.0).astype(LOW)
            gh = jnp.where(mine, go, 0.0).astype(LOW)
            p = jnp.exp(dot_nt(kh_ref[h], qh) - lse_ref[0, h : h + 1, rows])
            dp = dot_nt(vh_ref[h], gh)
            pd = jnp.sum(p * dp, axis=0, keepdims=True)
            ds = (p * (dp - pd)).astype(LOW)
            gv_ref[...] += dot_nn(p.astype(LOW), gh)
            gk_ref[...] += dot_nn(ds, qh)
            total += dot_tn(kh_ref[h], ds)
        gq = turn(total.T * SCALE, c_ref[rows, :], s1_ref[rows, :], s2_ref[rows, :], -1.0)
        g_ref[rows, :width] = gq.astype(LOW)
        return carry

    lax.fori_loop(0, LENGTH // QB, block, 0)
    gk = turn(gk_ref[...], c_ref[...], s1_ref[...], s2_ref[...], -1.0)
    g_ref[:, width : 2 * width] = gk.astype(LOW)
    g_ref[:, 2 * width :] = gv_ref[...].astype(LOW)
    sum_ref[...] = jnp.sum(g_ref[...].astype(jnp.float32), axis=0, keepdims=True)


def attend_back(low, go, lse, tables):
    lanes = low.shape[1] // (6 * HD)
    table = pl.BlockSpec((LENGTH, 2 * HD), lambda z: (0, 0))
    wide = pl.BlockSpec((LENGTH, 6 * HD), lambda z: (0, z))
    return pl.pallas_call(
        attend_back_kernel,
        grid=(lanes,),
        in_specs=[
            wide,
            pl.BlockSpec((LENGTH, 2 * HD), lambda z: (0, z)),
            pl.BlockSpec((1, 2, LENGTH), lambda z: (z, 0, 0)),
            table,
            table,
            table,
        ],
        out_specs=[wide, pl.BlockSpec((1, 6 * HD), lambda z: (0, z))],
        out_shape=[
            jax.ShapeDtypeStruct((LENGTH, lanes * 6 * HD), LOW),
            jax.ShapeDtypeStruct((1, lanes * 6 * HD), jnp.float32),
        ],
        scratch_shapes=[
            pltpu.VMEM((2, LENGTH, 2 * HD), LOW),
            pltpu.VMEM((2, LENGTH, 2 * HD), LOW),
            pltpu.VMEM((LENGTH, 2 * HD), jnp.float32),
            pltpu.VMEM((LENGTH, 2 * HD), jnp.float32),
        ],
        compiler_params=pltpu.CompilerParams(vmem_limit_bytes=40 * 1024 * 1024),
        cost_estimate=pl.CostEstimate(
            flops=40 * LENGTH * LENGTH * HD * lanes,
            bytes_accessed=26 * LENGTH * HD * lanes,
            transcendentals=2 * lanes * LENGTH * LENGTH,
        ),
        name="attend_back",
    )(low, go, lse, *tables)


MESH = pl.DeviceIdType.MESH
PIECES = ((0, 0, 384, 0), (1, 384, 128, 0), (2, 512, 256, 0), (2, 768, 256, 1024), (3, 1024, 256, 0), (3, 1280, 256, 1024))
SHARD = 128


def remote(src, dst, send, recv, target):
    return pltpu.make_async_remote_copy(
        src_ref=src, dst_ref=dst, send_sem=send, recv_sem=recv, device_id=target, device_id_type=MESH
    )


def flip(index, bit):
    return index + bit - 2 * bit * ((index // bit) % 2)


def peers():
    lane = lax.axis_index("tensor")
    shard = lax.axis_index("fsdp")
    is_mid = (lane == 1) | (lane == 2)
    pair = {"tensor": flip(lane, 1)}
    across = {"tensor": 3 - lane}
    x_peer = {"fsdp": flip(shard, 2)}
    y_peer = {"fsdp": flip(shard, 4)}
    return lane, shard, is_mid, pair, across, x_peer, y_peer


def meet(targets):
    barrier = pltpu.get_barrier_semaphore()
    for target in targets:
        pl.semaphore_signal(barrier, inc=1, device_id=target, device_id_type=MESH)
    pl.semaphore_wait(barrier, len(targets))


def gather_kernel(
    pack_ref, vec_ref, bias_ref, qkv_ref, proj_ref, up_ref, down_ref, vec_all, bias_all,
    local_sem, send_sem, recv_sem, small_send, small_recv,
):
    lane, shard, is_mid, pair, across, x_peer, y_peer = peers()
    core = shard % 2
    outs = (qkv_ref, proj_ref, up_ref, down_ref)
    shard_peers = [
        (q, dc, {"fsdp": flip_place(shard, q, dc)})
        for q in range(4)
        for dc in range(2)
        if (q, dc) != (0, 0)
    ]
    lane_peers = [pair, {"tensor": (lane + 2) % 4}, across]
    meet([t for _, _, t in shard_peers] + lane_peers)

    chunks = [(piece, r) for piece in PIECES for r in range(2)]

    def window(c, row0, row_count, col0, col_count):
        (m, _, width, base), r = chunks[c]
        return outs[m].at[
            pl.ds(r * 4 * SHARD + row0, row_count), pl.ds(base + col0 * width, col_count * width)
        ]

    def own(c):
        (_, first, width, _), r = chunks[c]
        return pack_ref.at[r, :, pl.ds(first, width)]

    def local(c):
        return pltpu.make_async_copy(own(c), window(c, 0, SHARD, 0, 1), local_sem.at[c])

    def hop_pair(c):
        return remote(own(c), window(c, 0, SHARD, 1, 1), send_sem.at[c, 0], recv_sem.at[c, 0], pair)

    def hop_across(c):
        return remote(
            window(c, 0, SHARD, 0, 2), window(c, 0, SHARD, 2, 2), send_sem.at[c, 1], recv_sem.at[c, 1], across
        )

    def hop_out(c):
        far = window(c, 0, SHARD, 2, 2)
        return remote(far, far, send_sem.at[c, 2], recv_sem.at[c, 1], pair)

    def hop_first(c):
        src = window(c, 0, SHARD, 0, 4)
        if chunks[c][1] == 0:
            return remote(src, window(c, SHARD, SHARD, 0, 4), send_sem.at[c, 3], recv_sem.at[c, 2], x_peer)
        return remote(src, window(c, 2 * SHARD, SHARD, 0, 4), send_sem.at[c, 3], recv_sem.at[c, 2], y_peer)

    def hop_second(c):
        if chunks[c][1] == 0:
            return [
                remote(
                    window(c, 0, 2 * SHARD, 0, 4), window(c, 2 * SHARD, 2 * SHARD, 0, 4),
                    send_sem.at[c, 4], recv_sem.at[c, 3], y_peer,
                )
            ]
        return [
            remote(
                window(c, k * 2 * SHARD, SHARD, 0, 4), window(c, (2 * k + 1) * SHARD, SHARD, 0, 4),
                send_sem.at[c, 4 + k], recv_sem.at[c, 3 + k], x_peer,
            )
            for k in range(2)
        ]

    count = len(chunks)
    small = []
    slot = core * 4
    vec_all[pl.ds(slot, 1)] = vec_ref[...][None]
    bias_all[0] = bias_ref[...]
    for i, (q, _, target) in enumerate(shard_peers):
        small.append(remote(vec_ref, vec_all.at[slot + q], small_send.at[i], small_recv.at[i], target))
    far_slot = 3 - is_mid.astype(jnp.int32)
    for i, target in enumerate(lane_peers):
        to = bias_all.at[1] if i == 0 else bias_all.at[far_slot]
        small.append(remote(bias_ref, to, small_send.at[7 + i], small_recv.at[7 + i], target))
    for c in range(count):
        local(c).start()
    hop_pair(0).start()
    hop_pair(1).start()
    for copy in small:
        copy.start()
    for tick in range(count + 5):
        if 2 <= tick < count:
            hop_pair(tick).start()
        c = tick - 1
        if 0 <= c < count:
            local(c).wait()
            hop_pair(c).wait_recv()

            @pl.when(is_mid)
            def _():
                hop_across(c).start()

        c = tick - 2
        if 0 <= c < count:
            hop_across(c).wait_recv()

            @pl.when(is_mid)
            def _():
                hop_out(c).start()

            hop_first(c).start()
        c = tick - 4
        if 0 <= c < count:
            hop_first(c).wait_recv()
            for copy in hop_second(c):
                copy.start()
    for copy in small:
        copy.wait()
    for c in range(count):
        for copy in hop_second(c):
            copy.wait()
        hop_pair(c).wait_send()
        hop_first(c).wait_send()

        @pl.when(is_mid)
        def _():
            hop_across(c).wait_send()
            hop_out(c).wait_send()


def flip_place(shard, q, dc):
    target = shard
    for bit, on in ((1, dc), (2, q & 1), (4, q >> 1)):
        if on:
            target = flip(target, bit)
    return target


def gather_all(pack, vec, bias):
    count = 2 * len(PIECES)
    width = pack.shape[2]
    rows = 8 * SHARD
    any_space = pl.BlockSpec(memory_space=pl.ANY)
    vmem = pl.BlockSpec(memory_space=pltpu.VMEM)
    return pl.pallas_call(
        gather_kernel,
        in_specs=[vmem] * 3,
        out_specs=[any_space] * 4 + [vmem] * 2,
        out_shape=[
            jax.ShapeDtypeStruct((rows, 1536), LOW),
            jax.ShapeDtypeStruct((rows, 512), LOW),
            jax.ShapeDtypeStruct((rows, 2048), LOW),
            jax.ShapeDtypeStruct((rows, 2048), LOW),
            jax.ShapeDtypeStruct((8,) + vec.shape, jnp.float32),
            jax.ShapeDtypeStruct((4,) + bias.shape, jnp.float32),
        ],
        scratch_shapes=[
            pltpu.SemaphoreType.DMA((count,)),
            pltpu.SemaphoreType.DMA((count, 6)),
            pltpu.SemaphoreType.DMA((count, 5)),
            pltpu.SemaphoreType.DMA((10,)),
            pltpu.SemaphoreType.DMA((10,)),
        ],
        compiler_params=pltpu.CompilerParams(collective_id=1, has_side_effects=True),
        name="gather_all",
    )(pack, vec, bias)


def scatter_kernel(arrays, chunks, *refs):
    grads = refs[:arrays]
    out_ref, own_ref, first_ref, second_ref, in_ref, mid_ref, near_ref = refs[arrays : arrays + 7]
    local_sem, send_sem, recv_sem = refs[arrays + 7 :]
    lane, shard, is_mid, pair, across, x_peer, y_peer = peers()
    barrier = pltpu.get_barrier_semaphore()
    for target in (pair, x_peer, y_peer):
        pl.semaphore_signal(barrier, inc=1, device_id=target, device_id_type=MESH)

    @pl.when(is_mid)
    def _():
        pl.semaphore_signal(barrier, inc=1, device_id=across, device_id_type=MESH)

    pl.semaphore_wait(barrier, 3 + is_mid.astype(jnp.int32))

    def source(c, row0, row_count):
        (a, _, width, base), r = chunks[c]
        return grads[a].at[pl.ds(r * 4 * SHARD + row0, row_count), pl.ds(base, 4 * width)]

    def part(ref, c, row0, row_count, lo, hi, each):
        (_, first, width, _), r = chunks[c]
        return ref.at[r, pl.ds(row0, row_count), pl.ds(first * each + lo * width, (hi - lo) * width)]

    def keep(c):
        if chunks[c][1] == 0:
            return [
                pltpu.make_async_copy(
                    source(c, 0, 2 * SHARD), part(own_ref, c, 0, 2 * SHARD, 0, 4, 4), local_sem.at[c, 0]
                )
            ]
        return [
            pltpu.make_async_copy(
                source(c, k * 2 * SHARD, SHARD), part(own_ref, c, k * SHARD, SHARD, 0, 4, 4), local_sem.at[c, k]
            )
            for k in range(2)
        ]

    def hop_first(c):
        if chunks[c][1] == 0:
            return [
                remote(
                    source(c, 2 * SHARD, 2 * SHARD), part(first_ref, c, 0, 2 * SHARD, 0, 4, 4),
                    send_sem.at[c, 0], recv_sem.at[c, 0], y_peer,
                )
            ]
        return [
            remote(
                source(c, (2 * k + 1) * SHARD, SHARD), part(first_ref, c, k * SHARD, SHARD, 0, 4, 4),
                send_sem.at[c, k], recv_sem.at[c, k], x_peer,
            )
            for k in range(2)
        ]

    def hop_second(c):
        return remote(
            part(own_ref, c, SHARD, SHARD, 0, 4, 4), part(second_ref, c, 0, SHARD, 0, 4, 4),
            send_sem.at[c, 2], recv_sem.at[c, 2], x_peer if chunks[c][1] == 0 else y_peer,
        )

    def hop_in(c):
        return remote(
            part(own_ref, c, 0, SHARD, 2, 4, 4), part(in_ref, c, 0, SHARD, 0, 2, 2),
            send_sem.at[c, 3], recv_sem.at[c, 3], pair,
        )

    def hop_across(c):
        return remote(
            part(own_ref, c, 0, SHARD, 2, 4, 4), part(mid_ref, c, 0, SHARD, 0, 2, 2),
            send_sem.at[c, 3], recv_sem.at[c, 4], across,
        )

    def hop_pair(c):
        return remote(
            part(own_ref, c, 0, SHARD, 1, 2, 4), part(near_ref, c, 0, SHARD, 0, 1, 1),
            send_sem.at[c, 4], recv_sem.at[c, 5], pair,
        )

    def add(dst, left, right, rows):
        step = 16

        @pl.loop(0, rows // step)
        def _(i):
            at = pl.ds(pl.multiple_of(i * step, step), step)
            total = left[at, :].astype(jnp.float32) + right[at, :].astype(jnp.float32)
            dst[at, :] = total.astype(dst.dtype)

    count = len(chunks)
    lead = 4
    for c in range(count):
        for copy in keep(c):
            copy.start()
    for c in range(min(lead, count)):
        for copy in hop_first(c):
            copy.start()
    for tick in range(count + 5):
        c = tick
        if c < count:
            for copy in keep(c):
                copy.wait()
            for copy in hop_first(c):
                copy.wait_recv()
            if c + lead < count:
                for copy in hop_first(c + lead):
                    copy.start()
            mine = part(own_ref, c, SHARD, SHARD, 0, 4, 4)
            add(mine, mine, part(first_ref, c, SHARD, SHARD, 0, 4, 4), SHARD)
            hop_second(c).start()
            mine = part(own_ref, c, 0, SHARD, 0, 4, 4)
            add(mine, mine, part(first_ref, c, 0, SHARD, 0, 4, 4), SHARD)
        c = tick - 2
        if 0 <= c < count:
            hop_second(c).wait_recv()
            mine = part(own_ref, c, 0, SHARD, 0, 4, 4)
            add(mine, mine, part(second_ref, c, 0, SHARD, 0, 4, 4), SHARD)

            @pl.when(jnp.logical_not(is_mid))
            def _():
                hop_in(c).start()

        c = tick - 3
        if 0 <= c < count:

            @pl.when(is_mid)
            def _():
                hop_in(c).wait_recv()
                far = part(own_ref, c, 0, SHARD, 2, 4, 4)
                add(far, far, part(in_ref, c, 0, SHARD, 0, 2, 2), SHARD)
                hop_across(c).start()

        c = tick - 4
        if 0 <= c < count:

            @pl.when(is_mid)
            def _():
                hop_across(c).wait_recv()
                near = part(own_ref, c, 0, SHARD, 0, 2, 4)
                add(near, near, part(mid_ref, c, 0, SHARD, 0, 2, 2), SHARD)

            hop_pair(c).start()
        c = tick - 5
        if 0 <= c < count:
            hop_pair(c).wait_recv()
            add(
                part(out_ref, c, 0, SHARD, 0, 1, 1), part(own_ref, c, 0, SHARD, 0, 1, 4),
                part(near_ref, c, 0, SHARD, 0, 1, 1), SHARD,
            )
    for c in range(count):
        for copy in hop_first(c):
            copy.wait_send()
        hop_second(c).wait_send()
        hop_pair(c).wait_send()

        @pl.when(is_mid)
        def _():
            hop_across(c).wait_send()

        @pl.when(jnp.logical_not(is_mid))
        def _():
            hop_in(c).wait_send()


def scatter_all(grads, pieces, collective_id):
    chunks = [(piece, r) for piece in pieces for r in range(2)]
    count = len(chunks)
    width = sum(piece[2] for piece in pieces)
    vmem = pl.BlockSpec(memory_space=pltpu.VMEM)
    return pl.pallas_call(
        functools.partial(scatter_kernel, len(grads), chunks),
        in_specs=[pl.BlockSpec(memory_space=pl.ANY)] * len(grads),
        out_specs=vmem,
        out_shape=jax.ShapeDtypeStruct((2, SHARD, width), jnp.float32),
        scratch_shapes=[
            pltpu.VMEM((2, 2 * SHARD, 4 * width), LOW),
            pltpu.VMEM((2, 2 * SHARD, 4 * width), LOW),
            pltpu.VMEM((2, SHARD, 4 * width), LOW),
            pltpu.VMEM((2, SHARD, 2 * width), LOW),
            pltpu.VMEM((2, SHARD, 2 * width), LOW),
            pltpu.VMEM((2, SHARD, width), LOW),
            pltpu.SemaphoreType.DMA((count, 2)),
            pltpu.SemaphoreType.DMA((count, 5)),
            pltpu.SemaphoreType.DMA((count, 6)),
        ],
        compiler_params=pltpu.CompilerParams(collective_id=collective_id, has_side_effects=True, vmem_limit_bytes=48 * 1024 * 1024),
        name="scatter_all",
    )(*grads)


def by_core(core, mine, theirs):
    return jnp.where(core == 0, mine, theirs), jnp.where(core == 0, theirs, mine)


def gelu_parts(u):
    cdf = 0.5 * (1.0 + lax.erf(u * (0.5**0.5)))
    density = jnp.exp(-0.5 * u * u) * ((2.0 * jnp.pi) ** -0.5)
    return u * cdf, cdf + u * density


def norm_parts(values):
    center = values - jnp.mean(values, axis=-1, keepdims=True)
    scale = lax.rsqrt(jnp.mean(center * center, axis=-1, keepdims=True) + NORM_EPS)
    return center * scale, scale


def norm_back(grad, unit, scale, gain):
    c = grad * gain
    return scale * (
        c
        - jnp.mean(c, axis=-1, keepdims=True)
        - unit * jnp.mean(c * unit, axis=-1, keepdims=True)
    )


def on_chip(
    tokens,
    cotangent,
    qkv_weight,
    qkv_bias,
    proj_weight,
    fc1_weight,
    fc1_bias,
    fc2_weight,
    vectors,
    row_state,
    qkv_cols,
    proj_cols,
    fc1_cols,
    fc2_cols,
    vector_state,
    qkv_bias_state,
    fc1_bias_state,
):
    shard = lax.axis_index("fsdp")
    lane = lax.axis_index("tensor")
    core = shard % 2
    place = shard // 2
    rows = tokens.shape[0]
    head_width = qkv_weight.shape[2]
    hidden_width = fc1_weight.shape[1]
    hw, fw = head_width // 2, hidden_width // 2
    shard_rows = qkv_weight.shape[0]
    swap_tokens = []
    for k in range(4):
        for p in range(2):
            a, b = (2 * k + 1) * 4 + 2 * p, 2 * k * 4 + 2 * p + 1
            swap_tokens += [(a, b), (b, a)]
    moved = (core ^ (lane & 1)) == 1

    def swap(v):
        return jnp.where(moved, lax.ppermute(v, ("fsdp", "tensor"), swap_tokens), v)

    def to_local(v):
        parts = []
        for r in range(2):
            for q in range(4):
                parts.append(
                    lax.dynamic_slice_in_dim(v, ((place ^ q) * 2 + r) * shard_rows, shard_rows, 1)
                )
        return jnp.concatenate(parts, axis=1)

    def to_global(v):
        parts = []
        for q in range(4):
            for r in range(2):
                parts.append(
                    lax.dynamic_slice_in_dim(v, (r * 4 + (place ^ q)) * shard_rows, shard_rows, 1)
                )
        return jnp.concatenate(parts, axis=1)

    near = lane ^ 1
    far_a = jnp.where(lane < 2, 2, 1)
    far_b = jnp.where(lane < 2, 3, 0)
    order = [lane, near, far_a, far_b]

    def both_halves(v):
        return jnp.concatenate([v, lax.ppermute(v, "fsdp", CORE_SWAP)], axis=0)

    def core_sum(left, right_t):
        other = times_transposed(left[rows:], right_t)
        other = lax.ppermute(other, "fsdp", CORE_SWAP)
        return times_transposed(left[:rows], right_t) + other

    def half_columns(w, width, which):
        return lax.dynamic_slice_in_dim(w, which * width, width, w.ndim - 1)

    def pack(which):
        return jnp.concatenate(
            [
                half_columns(qkv_weight, hw, which).reshape(shard_rows, 3 * hw),
                half_columns(proj_weight, hw, which),
                half_columns(fc1_weight, fw, which),
                half_columns(fc2_weight, fw, which),
            ],
            axis=1,
        ).astype(LOW)

    theirs = lax.ppermute(pack(1 - core), "fsdp", CORE_SWAP)
    packs = jnp.stack(by_core(core, pack(core), theirs))
    vec = jnp.pad(vectors.astype(LOW).astype(jnp.float32).T, ((0, 2), (0, 0)))
    bias = jnp.concatenate(
        [
            half_columns(qkv_bias, hw, core).reshape(3 * hw),
            lax.dynamic_slice_in_dim(fc1_bias, core * fw, fw, 0),
        ]
    )
    bias = jnp.broadcast_to(
        lax.optimization_barrier(bias.astype(LOW)).astype(jnp.float32), (8, 3 * hw + fw)
    )
    weight_qkv, weight_proj, weight_up, weight_down, vec_all, bias_all = gather_all(
        packs, vec, bias
    )
    vector_rows = vec_all.transpose(1, 0, 2).reshape(8, D)
    gain_one, shift_one, proj_shift, gain_two, shift_two, down_shift = [
        vector_rows[i : i + 1] for i in range(6)
    ]
    bias_rows = bias_all[:, 0]
    bias_qkv = bias_rows[:, : 3 * hw].reshape(1, 12 * hw)
    bias_up = (
        bias_rows[:, 3 * hw :].reshape(4, 2, fw // 2).transpose(1, 0, 2).reshape(1, 4 * fw)
    )

    tables = chip_tables(core)
    inputs = to_local(swap(tokens)).astype(jnp.float32)
    upstream_low = to_local(swap(cotangent))
    grad_out_all = both_halves(upstream_low)

    unit_one, scale_one = norm_parts(inputs)
    normed_one = both_halves((unit_one * gain_one + shift_one).astype(LOW))
    projected = jnp.dot(normed_one, weight_qkv, preferred_element_type=jnp.float32) + bias_qkv
    low, mixed, lse = attend(projected, tables)
    middle = inputs + core_sum(mixed, weight_proj) + proj_shift
    unit_two, scale_two = norm_parts(middle)
    normed_two = both_halves((unit_two * gain_two + shift_two).astype(LOW))
    hidden = jnp.dot(normed_two, weight_up, preferred_element_type=jnp.float32) + bias_up
    active, slope = gelu_parts(hidden)
    active = active.astype(LOW)
    grad_down = contract_rows(grad_out_all, active).astype(LOW)
    layer_local = middle + core_sum(active, weight_down) + down_shift
    grad_active = jnp.dot(grad_out_all, weight_down, preferred_element_type=jnp.float32)
    grad_hidden = (grad_active * slope).astype(LOW)
    grad_up = contract_rows(normed_two, grad_hidden).astype(LOW)
    grad_bias_up = jnp.sum(grad_hidden.astype(jnp.float32), axis=0)
    grad_normed_two = core_sum(grad_hidden, weight_up)
    upstream = upstream_low.astype(jnp.float32)
    grad_middle = upstream + norm_back(grad_normed_two, unit_two, scale_two, gain_two)
    grad_branch = grad_middle.astype(LOW)
    grad_branch_all = both_halves(grad_branch)
    grad_proj = contract_rows(grad_branch_all, mixed).astype(LOW)
    grad_mixed = jnp.dot(
        grad_branch_all, weight_proj, preferred_element_type=jnp.float32
    ).astype(LOW)
    grad_low, grad_bias_qkv = attend_back(low, grad_mixed, lse, tables)
    grad_qkv = contract_rows(normed_one, grad_low).astype(LOW)
    grad_normed_one = core_sum(grad_low, weight_qkv)
    input_local = grad_middle + norm_back(grad_normed_one, unit_one, scale_one, gain_one)
    layer_out = to_global(swap(layer_local))
    input_grad = to_global(swap(input_local))

    late = scatter_all((grad_qkv,), ((0, 0, 3 * hw, 0),), 3)
    half = fw // 2
    early = scatter_all(
        (grad_down, grad_up, grad_proj),
        (
            (0, 0, half, 0),
            (0, half, half, 4 * half),
            (1, fw, half, 0),
            (1, fw + half, half, 4 * half),
            (2, 2 * fw, hw, 0),
        ),
        2,
    )

    def settle(sums):
        mine = jnp.where(core == 0, sums[0], sums[1])
        theirs = lax.ppermute(jnp.where(core == 0, sums[1], sums[0]), "fsdp", CORE_SWAP)
        return by_core(core, mine, theirs)

    def joined(halves, first, width, pieces):
        left, right = (
            half[:, first : first + width].reshape(shard_rows, pieces, -1) for half in halves
        )
        return jnp.concatenate([left, right], axis=2).reshape(shard_rows, -1)

    early = settle(early)
    late = settle(late)
    grad_down = joined(early, 0, fw, 1)
    grad_up = joined(early, fw, fw, 1)
    grad_proj = joined(early, 2 * fw, hw, 1)
    grad_qkv = joined(late, 0, 3 * hw, 3)

    vector_part = to_global(
        jnp.stack(
            [
                jnp.sum(grad_normed_one * unit_one, axis=0),
                jnp.sum(grad_normed_one, axis=0),
                jnp.sum(grad_branch.astype(jnp.float32), axis=0),
                jnp.sum(grad_normed_two * unit_two, axis=0),
                jnp.sum(grad_normed_two, axis=0),
                jnp.sum(upstream, axis=0),
            ]
        )
    ).T
    qkv_placed = jnp.zeros((3, D), jnp.float32)
    up_placed = jnp.zeros((FF,), jnp.float32)
    for position, z in enumerate(order):
        piece = grad_bias_qkv[0, position * 3 * hw : (position + 1) * 3 * hw].reshape(3, hw)
        qkv_placed = lax.dynamic_update_slice(qkv_placed, piece, (0, z * head_width + core * hw))
        piece = grad_bias_up.reshape(2, 4, fw // 2)[:, position].reshape(fw)
        up_placed = lax.dynamic_update_slice(up_placed, piece, (z * hidden_width + core * fw,))
    vector_total, qkv_total, up_total = lax.psum(
        (vector_part, qkv_placed, up_placed), ("fsdp", "tensor")
    )
    return finish(
        (layer_out, input_grad),
        (grad_qkv, grad_proj, grad_up, grad_down),
        (vector_total, qkv_total, up_total),
        (qkv_weight, qkv_bias, proj_weight, fc1_weight, fc1_bias, fc2_weight, vectors),
        (row_state, qkv_cols, proj_cols, fc1_cols, fc2_cols),
        (vector_state, qkv_bias_state, fc1_bias_state),
    )


def finish(block_outs, grads, totals, params, stats, states):
    grad_qkv, grad_proj, grad_up, grad_down = grads
    vector_total, qkv_total, up_total = totals
    qkv_weight, qkv_bias, proj_weight, fc1_weight, fc1_bias, fc2_weight, vectors = params
    row_state, qkv_cols, proj_cols, fc1_cols, fc2_cols = stats
    vector_state, qkv_bias_state, fc1_bias_state = states
    lane_index = lax.axis_index("tensor")
    head_width = qkv_weight.shape[2]
    hidden_width = fc1_weight.shape[1]
    shard_rows = qkv_weight.shape[0]
    grad_vectors = lax.dynamic_slice_in_dim(
        vector_total, lax.axis_index("fsdp") * shard_rows, shard_rows, 0
    )
    grad_qkv_bias = lax.dynamic_slice_in_dim(qkv_total, lane_index * head_width, head_width, 1)
    grad_up_bias = lax.dynamic_slice_in_dim(up_total, lane_index * hidden_width, hidden_width, 0)
    matrices = [
        (
            grad_qkv.reshape(shard_rows, 3 * head_width),
            qkv_weight.reshape(shard_rows, 3 * head_width),
            qkv_cols.reshape(3 * head_width),
        ),
        (grad_proj, proj_weight, proj_cols),
        (grad_up, fc1_weight, fc1_cols),
        (grad_down, fc2_weight, fc2_cols),
    ]
    column_counts = [3 * D, D, FF, FF]
    column_weights = jnp.array(column_counts, jnp.float32)
    qkv_state_new = DECAY * qkv_bias_state + (1.0 - DECAY) * (grad_qkv_bias * grad_qkv_bias + TINY)
    qkv_direction = grad_qkv_bias * lax.rsqrt(qkv_state_new)
    up_state_new = DECAY * fc1_bias_state + (1.0 - DECAY) * (grad_up_bias * grad_up_bias + TINY)
    up_direction = grad_up_bias * lax.rsqrt(up_state_new)
    row_squares = jnp.stack(
        [jnp.sum(matrix_entry[0] * matrix_entry[0], axis=1) for matrix_entry in matrices]
    )
    weight_squares = jnp.stack(
        [jnp.sum(matrix_entry[1] * matrix_entry[1]) for matrix_entry in matrices]
    )
    bias_terms = jnp.stack(
        [
            jnp.sum(qkv_direction * qkv_direction),
            jnp.sum(up_direction * up_direction),
            jnp.sum(qkv_bias * qkv_bias),
            jnp.sum(fc1_bias * fc1_bias),
        ]
    )
    row_total, weight_partial, bias_total = lax.psum(
        (row_squares, weight_squares, bias_terms), "tensor"
    )
    rows_new = DECAY * row_state + (1.0 - DECAY) * (row_total / column_weights[:, None] + TINY)
    vector_state_new = DECAY * vector_state + (1.0 - DECAY) * (grad_vectors * grad_vectors + TINY)
    vector_direction = grad_vectors * lax.rsqrt(vector_state_new)
    vector_terms = jnp.stack(
        [jnp.sum(vector_direction * vector_direction, axis=0), jnp.sum(vectors * vectors, axis=0)]
    )
    col_squares = jnp.concatenate(
        [jnp.sum(matrix_entry[0] * matrix_entry[0], axis=0) for matrix_entry in matrices]
    )
    row_new_sums = jnp.sum(rows_new, axis=1)
    col_total, row_new_total, weight_total, vector_sums = lax.psum(
        (col_squares, row_new_sums, weight_partial, vector_terms), "fsdp"
    )
    mean_rows = row_new_total / D
    offsets = [0]
    for matrix_entry in matrices:
        offsets.append(offsets[-1] + matrix_entry[0].shape[1])
    cols_list = []
    direction_list = []
    square_list = []
    for position, matrix_entry in enumerate(matrices):
        col_slice = col_total[offsets[position] : offsets[position + 1]]
        cols_new = DECAY * matrix_entry[2] + (1.0 - DECAY) * (col_slice / D + TINY)
        direction = matrix_entry[0] * lax.rsqrt(
            rows_new[position][:, None] * cols_new[None, :] / mean_rows[position]
        )
        cols_list.append(cols_new)
        direction_list.append(direction)
        square_list.append(jnp.sum(direction * direction))
    square_total = lax.psum(jnp.stack(square_list), ("fsdp", "tensor"))
    matrix_count = D * column_weights
    update_rms = jnp.sqrt(square_total / matrix_count)
    weight_scale = jnp.sqrt(weight_total / matrix_count)
    new_weights = []
    for position, matrix_entry in enumerate(matrices):
        new_weights.append(
            matrix_entry[1]
            - RATE
            * weight_scale[position]
            * direction_list[position]
            / jnp.maximum(1.0, update_rms[position] / CLIP_LEVEL)
        )
    vector_rms = jnp.sqrt(vector_sums[0] / D)
    vector_scale = jnp.sqrt(vector_sums[1] / D)
    vectors_new = vectors - RATE * vector_scale * vector_direction / jnp.maximum(
        1.0, vector_rms / CLIP_LEVEL
    )
    qkv_rms = jnp.sqrt(bias_total[0] / (3 * D))
    qkv_scale = jnp.sqrt(bias_total[2] / (3 * D))
    qkv_bias_new = qkv_bias - RATE * qkv_scale * qkv_direction / jnp.maximum(
        1.0, qkv_rms / CLIP_LEVEL
    )
    up_rms = jnp.sqrt(bias_total[1] / FF)
    up_scale = jnp.sqrt(bias_total[3] / FF)
    up_bias_new = fc1_bias - RATE * up_scale * up_direction / jnp.maximum(1.0, up_rms / CLIP_LEVEL)
    return (
        *block_outs,
        grad_qkv.reshape(shard_rows, 3, head_width),
        grad_qkv_bias,
        grad_proj,
        grad_up,
        grad_up_bias,
        grad_down,
        grad_vectors,
        rows_new,
        cols_list[0].reshape(3, head_width),
        cols_list[1],
        cols_list[2],
        cols_list[3],
        vector_state_new,
        qkv_state_new,
        up_state_new,
        new_weights[0].reshape(shard_rows, 3, head_width),
        qkv_bias_new,
        new_weights[1],
        new_weights[2],
        up_bias_new,
        new_weights[3],
        vectors_new,
        update_rms,
    )


def solution(mesh):
    chips = mesh.shape["fsdp"] == 8 and mesh.shape["tensor"] == 4
    return jax.shard_map(
        on_chip if chips else on_device,
        mesh=mesh,
        in_specs=(
            P(("fsdp", "tensor"), None),
            P(("fsdp", "tensor"), None),
            P("fsdp", None, "tensor"),
            P(None, "tensor"),
            P("fsdp", "tensor"),
            P("fsdp", "tensor"),
            P("tensor"),
            P("fsdp", "tensor"),
            P("fsdp", None),
            P(None, "fsdp"),
            P(None, "tensor"),
            P("tensor"),
            P("tensor"),
            P("tensor"),
            P("fsdp", None),
            P(None, "tensor"),
            P("tensor"),
        ),
        out_specs=(
            P(("fsdp", "tensor"), None),
            P(("fsdp", "tensor"), None),
            P("fsdp", None, "tensor"),
            P(None, "tensor"),
            P("fsdp", "tensor"),
            P("fsdp", "tensor"),
            P("tensor"),
            P("fsdp", "tensor"),
            P("fsdp", None),
            P(None, "fsdp"),
            P(None, "tensor"),
            P("tensor"),
            P("tensor"),
            P("tensor"),
            P("fsdp", None),
            P(None, "tensor"),
            P("tensor"),
            P("fsdp", None, "tensor"),
            P(None, "tensor"),
            P("fsdp", "tensor"),
            P("fsdp", "tensor"),
            P("tensor"),
            P("fsdp", "tensor"),
            P("fsdp", None),
            P(),
        ),
        check_vma=False,
    )
```

```python
import functools

import jax
import jax.numpy as jnp
from jax import lax
from jax.experimental import pallas as pl
from jax.experimental.pallas import tpu as pltpu
from jax.sharding import PartitionSpec as P

D = 1024
HD = 64
FF = 4096
GT = 4
GH = 16
GW = 16


NORM_EPS = 1e-06
DECAY = 0.5
CLIP_LEVEL = 1.0
RATE = 0.3
TINY = 1e-30
BASE = 10000.0


def layer_norm(values, gain_row, shift_row):
    center = values - jnp.mean(values, axis=-1, keepdims=True)
    variance = jnp.mean(center * center, axis=-1, keepdims=True)
    return center * lax.rsqrt(variance + NORM_EPS) * gain_row + shift_row


def exact_gelu(values):
    return jax.nn.gelu(values, approximate=False)


def rope_tables(length, half_width):
    token_index = jnp.arange(length, dtype=jnp.int32)
    coordinates = jnp.stack(
        [token_index // (GH * GW), token_index // GW % GH, token_index % GW], axis=1
    ).astype(jnp.float32)
    frequency = BASE ** (-jnp.arange(half_width, dtype=jnp.float32) / half_width)
    angles = coordinates[:, :, None] * frequency[None, None, :]
    return (jnp.cos(angles), jnp.sin(angles))


def rotate(values, cosine_table, sine_table):
    half_width = cosine_table.shape[-1]
    rotated_width = 6 * half_width
    leading = values.shape[:-1]
    pair_rows = values[..., :rotated_width].reshape(leading + (3, 2, half_width))
    first_half = pair_rows[..., 0, :]
    second_half = pair_rows[..., 1, :]
    cosine_wide = cosine_table[:, None]
    sine_wide = sine_table[:, None]
    turned = jnp.stack(
        [
            first_half * cosine_wide - second_half * sine_wide,
            second_half * cosine_wide + first_half * sine_wide,
        ],
        axis=-2,
    )
    return jnp.concatenate(
        [turned.reshape(leading + (rotated_width,)), values[..., rotated_width:]], axis=-1
    )


def contract_rows(left, right):
    return lax.dot_general(
        left, right, (((0,), (0,)), ((), ())), preferred_element_type=jnp.float32
    )


def times_transposed(left, right):
    return lax.dot_general(
        left, right, (((1,), (1,)), ((), ())), preferred_element_type=jnp.float32
    )


def forward_block(query_rows, key_rows, value_rows):
    score_scale = query_rows.shape[-1] ** (-0.5)
    scores = (
        jnp.einsum("qhd,khd->hqk", query_rows, key_rows, preferred_element_type=jnp.float32)
        * score_scale
    )
    row_peak = jnp.max(scores, axis=-1, keepdims=True)
    raised = jnp.exp(scores - row_peak)
    totals = jnp.sum(raised, axis=-1, keepdims=True)
    attention = (raised / totals).astype(jnp.bfloat16)
    mixed_rows = jnp.einsum(
        "hqk,khd->qhd", attention, value_rows, preferred_element_type=jnp.float32
    )
    return (mixed_rows, (row_peak + jnp.log(totals))[..., 0])


def backward_block(running, block_item, key_rows, value_rows):
    query_rows, log_totals, grad_mixed = block_item
    score_scale = query_rows.shape[-1] ** (-0.5)
    scores = (
        jnp.einsum("qhd,khd->hqk", query_rows, key_rows, preferred_element_type=jnp.float32)
        * score_scale
    )
    attention = jnp.exp(scores - log_totals[..., None])
    grad_attention = jnp.einsum(
        "qhd,khd->hqk", grad_mixed, value_rows, preferred_element_type=jnp.float32
    )
    grad_scores = attention * (
        grad_attention - jnp.sum(attention * grad_attention, axis=-1, keepdims=True)
    )
    grad_low = grad_scores.astype(jnp.bfloat16)
    grad_queries = (
        jnp.einsum("hqk,khd->qhd", grad_low, key_rows, preferred_element_type=jnp.float32)
        * score_scale
    )
    key_total = (
        running[0]
        + jnp.einsum("hqk,qhd->khd", grad_low, query_rows, preferred_element_type=jnp.float32)
        * score_scale
    )
    value_total = running[1] + jnp.einsum(
        "hqk,qhd->khd",
        attention.astype(jnp.bfloat16),
        grad_mixed,
        preferred_element_type=jnp.float32,
    )
    return ((key_total, value_total), grad_queries)


def on_device(
    tokens,
    cotangent,
    qkv_weight,
    qkv_bias,
    proj_weight,
    fc1_weight,
    fc1_bias,
    fc2_weight,
    vectors,
    row_state,
    qkv_cols,
    proj_cols,
    fc1_cols,
    fc2_cols,
    vector_state,
    qkv_bias_state,
    fc1_bias_state,
):
    low_type = jnp.bfloat16
    lane_count = lax.axis_size("tensor")
    local_rows = tokens.shape[0]
    group_rows = local_rows * lane_count
    length = GT * GH * GW
    clip_count = group_rows // length
    block_rows = min(512, length)
    block_count = length // block_rows
    head_width = qkv_weight.shape[2]
    head_count = head_width // HD
    hidden_width = fc1_weight.shape[1]
    shard_rows = qkv_weight.shape[0]
    cosine_table, sine_table = rope_tables(length, HD // 3 // 2)
    weight_qkv, weight_proj, weight_up, weight_down, vector_low = (
        lax.all_gather(qkv_weight.astype(low_type), "fsdp", axis=0, tiled=True),
        lax.all_gather(proj_weight.astype(low_type), "fsdp", axis=0, tiled=True),
        lax.all_gather(fc1_weight.astype(low_type), "fsdp", axis=0, tiled=True),
        lax.all_gather(fc2_weight.astype(low_type), "fsdp", axis=0, tiled=True),
        lax.all_gather(vectors.astype(low_type), "fsdp", axis=0, tiled=True),
    )
    weight_qkv = weight_qkv.reshape(D, 3 * head_width)
    vector_full = vector_low.astype(jnp.float32)
    gain_one = vector_full[:, 0]
    shift_one = vector_full[:, 1]
    proj_shift = vector_full[:, 2]
    gain_two = vector_full[:, 3]
    shift_two = vector_full[:, 4]
    down_shift = vector_full[:, 5]
    bias_qkv = (
        lax.optimization_barrier(qkv_bias.astype(low_type))
        .astype(jnp.float32)
        .reshape(3 * head_width)
    )
    bias_up = lax.optimization_barrier(fc1_bias.astype(low_type)).astype(jnp.float32)
    inputs = tokens.astype(jnp.float32)
    normed_one = layer_norm(inputs, gain_one, shift_one).astype(low_type)
    gathered_one = lax.all_gather(normed_one, "tensor", axis=0, tiled=True)
    projected = jnp.dot(gathered_one, weight_qkv, preferred_element_type=jnp.float32) + bias_qkv
    projected = projected.reshape(clip_count, length, 3, head_count, HD)
    queries = rotate(projected[:, :, 0], cosine_table, sine_table).astype(low_type)
    key_rows = rotate(projected[:, :, 1], cosine_table, sine_table).astype(low_type)
    value_rows = projected[:, :, 2].astype(low_type)

    def clip_forward(clip_item):
        query_rows, clip_keys, clip_values = clip_item
        blocks = query_rows.reshape(block_count, block_rows, head_count, HD)
        return lax.map(
            lambda query_block: forward_block(query_block, clip_keys, clip_values), blocks
        )

    mixed_rows, log_totals = lax.map(clip_forward, (queries, key_rows, value_rows))
    mixed_low = mixed_rows.reshape(group_rows, head_width).astype(low_type)
    attn_sum = lax.psum_scatter(
        times_transposed(mixed_low, weight_proj), "tensor", scatter_dimension=0, tiled=True
    )
    middle = inputs + attn_sum + proj_shift
    normed_two = layer_norm(middle, gain_two, shift_two).astype(low_type)
    gathered_two = lax.all_gather(normed_two, "tensor", axis=0, tiled=True)
    hidden = jnp.dot(gathered_two, weight_up, preferred_element_type=jnp.float32) + bias_up
    active = exact_gelu(hidden).astype(low_type)
    layer_out = (
        middle
        + lax.psum_scatter(
            times_transposed(active, weight_down), "tensor", scatter_dimension=0, tiled=True
        )
        + down_shift
    )
    upstream = cotangent.astype(jnp.float32)
    grad_out_all, normed_two_all = (
        lax.all_gather(cotangent, "tensor", axis=0, tiled=True),
        lax.all_gather(normed_two, "tensor", axis=0, tiled=True),
    )
    grad_down = contract_rows(grad_out_all, active)
    grad_active = jnp.dot(grad_out_all, weight_down, preferred_element_type=jnp.float32)
    gelu_pull = jax.vjp(exact_gelu, hidden)[1]
    grad_hidden = gelu_pull(grad_active)[0].astype(low_type)
    grad_up = contract_rows(normed_two_all, grad_hidden)
    grad_bias_up = jnp.sum(grad_hidden.astype(jnp.float32), axis=0)
    grad_normed_two = lax.psum_scatter(
        times_transposed(grad_hidden, weight_up), "tensor", scatter_dimension=0, tiled=True
    )
    middle_part, grad_gain_two, grad_shift_two = jax.vjp(layer_norm, middle, gain_two, shift_two)[
        1
    ](grad_normed_two)
    grad_middle = upstream + middle_part
    grad_branch = grad_middle.astype(low_type)
    grad_proj_shift = jnp.sum(grad_branch.astype(jnp.float32), axis=0)
    grad_down_shift = jnp.sum(upstream, axis=0)
    grad_branch_all, normed_one_all = (
        lax.all_gather(grad_branch, "tensor", axis=0, tiled=True),
        lax.all_gather(normed_one, "tensor", axis=0, tiled=True),
    )
    grad_proj = contract_rows(grad_branch_all, mixed_low)
    grad_mixed = jnp.dot(grad_branch_all, weight_proj, preferred_element_type=jnp.float32).astype(
        low_type
    )
    grad_mixed = grad_mixed.reshape(clip_count, length, head_count, HD)

    def clip_backward(clip_item):
        query_rows, clip_keys, clip_values, clip_totals, clip_grads = clip_item
        starts = (jnp.zeros(clip_keys.shape, jnp.float32), jnp.zeros(clip_keys.shape, jnp.float32))
        block_items = (
            query_rows.reshape(block_count, block_rows, head_count, HD),
            clip_totals,
            clip_grads.reshape(block_count, block_rows, head_count, HD),
        )
        sums, grad_queries = lax.scan(
            lambda running, block_item: backward_block(running, block_item, clip_keys, clip_values),
            starts,
            block_items,
        )
        return (grad_queries.reshape(query_rows.shape), sums[0], sums[1])

    grad_queries, grad_keys, grad_values = lax.map(
        clip_backward, (queries, key_rows, value_rows, log_totals, grad_mixed)
    )
    grad_projected = jnp.stack(
        [
            rotate(grad_queries, cosine_table, -sine_table),
            rotate(grad_keys, cosine_table, -sine_table),
            grad_values,
        ],
        axis=2,
    )
    grad_projected = grad_projected.reshape(group_rows, 3 * head_width).astype(low_type)
    grad_qkv = contract_rows(normed_one_all, grad_projected).reshape(D, 3, head_width)
    grad_bias_qkv = jnp.sum(grad_projected.astype(jnp.float32), axis=0)
    grad_normed_one = lax.psum_scatter(
        times_transposed(grad_projected, weight_qkv), "tensor", scatter_dimension=0, tiled=True
    )
    input_part, grad_gain_one, grad_shift_one = jax.vjp(layer_norm, inputs, gain_one, shift_one)[1](
        grad_normed_one
    )
    input_grad = grad_middle + input_part
    grad_qkv, grad_proj, grad_up, grad_down = (
        lax.psum_scatter(grad_qkv, "fsdp", scatter_dimension=0, tiled=True),
        lax.psum_scatter(grad_proj, "fsdp", scatter_dimension=0, tiled=True),
        lax.psum_scatter(grad_up, "fsdp", scatter_dimension=0, tiled=True),
        lax.psum_scatter(grad_down, "fsdp", scatter_dimension=0, tiled=True),
    )
    lane_index = lax.axis_index("tensor")
    vector_part = jnp.stack(
        [
            grad_gain_one,
            grad_shift_one,
            grad_proj_shift,
            grad_gain_two,
            grad_shift_two,
            grad_down_shift,
        ],
        axis=1,
    )
    qkv_placed = lax.dynamic_update_slice(
        jnp.zeros((3, D), jnp.float32),
        grad_bias_qkv.reshape(3, head_width),
        (jnp.int32(0), lane_index * head_width),
    )
    up_placed = lax.dynamic_update_slice(
        jnp.zeros((FF,), jnp.float32), grad_bias_up, (lane_index * hidden_width,)
    )
    vector_total, qkv_total, up_total = lax.psum(
        (vector_part, qkv_placed, up_placed), ("fsdp", "tensor")
    )
    grad_vectors = lax.dynamic_slice_in_dim(
        vector_total, lax.axis_index("fsdp") * shard_rows, shard_rows, 0
    )
    grad_qkv_bias = lax.dynamic_slice_in_dim(qkv_total, lane_index * head_width, head_width, 1)
    grad_up_bias = lax.dynamic_slice_in_dim(up_total, lane_index * hidden_width, hidden_width, 0)
    matrices = [
        (
            grad_qkv.reshape(shard_rows, 3 * head_width),
            qkv_weight.reshape(shard_rows, 3 * head_width),
            qkv_cols.reshape(3 * head_width),
        ),
        (grad_proj, proj_weight, proj_cols),
        (grad_up, fc1_weight, fc1_cols),
        (grad_down, fc2_weight, fc2_cols),
    ]
    column_counts = [3 * D, D, FF, FF]
    column_weights = jnp.array(column_counts, jnp.float32)
    qkv_state_new = DECAY * qkv_bias_state + (1.0 - DECAY) * (grad_qkv_bias * grad_qkv_bias + TINY)
    qkv_direction = grad_qkv_bias * lax.rsqrt(qkv_state_new)
    up_state_new = DECAY * fc1_bias_state + (1.0 - DECAY) * (grad_up_bias * grad_up_bias + TINY)
    up_direction = grad_up_bias * lax.rsqrt(up_state_new)
    row_squares = jnp.stack(
        [jnp.sum(matrix_entry[0] * matrix_entry[0], axis=1) for matrix_entry in matrices]
    )
    weight_squares = jnp.stack(
        [jnp.sum(matrix_entry[1] * matrix_entry[1]) for matrix_entry in matrices]
    )
    bias_terms = jnp.stack(
        [
            jnp.sum(qkv_direction * qkv_direction),
            jnp.sum(up_direction * up_direction),
            jnp.sum(qkv_bias * qkv_bias),
            jnp.sum(fc1_bias * fc1_bias),
        ]
    )
    row_total, weight_partial, bias_total = lax.psum(
        (row_squares, weight_squares, bias_terms), "tensor"
    )
    rows_new = DECAY * row_state + (1.0 - DECAY) * (row_total / column_weights[:, None] + TINY)
    vector_state_new = DECAY * vector_state + (1.0 - DECAY) * (grad_vectors * grad_vectors + TINY)
    vector_direction = grad_vectors * lax.rsqrt(vector_state_new)
    vector_terms = jnp.stack(
        [jnp.sum(vector_direction * vector_direction, axis=0), jnp.sum(vectors * vectors, axis=0)]
    )
    col_squares = jnp.concatenate(
        [jnp.sum(matrix_entry[0] * matrix_entry[0], axis=0) for matrix_entry in matrices]
    )
    row_new_sums = jnp.sum(rows_new, axis=1)
    col_total, row_new_total, weight_total, vector_sums = lax.psum(
        (col_squares, row_new_sums, weight_partial, vector_terms), "fsdp"
    )
    mean_rows = row_new_total / D
    offsets = [0]
    for matrix_entry in matrices:
        offsets.append(offsets[-1] + matrix_entry[0].shape[1])
    cols_list = []
    direction_list = []
    square_list = []
    for position, matrix_entry in enumerate(matrices):
        col_slice = col_total[offsets[position] : offsets[position + 1]]
        cols_new = DECAY * matrix_entry[2] + (1.0 - DECAY) * (col_slice / D + TINY)
        direction = matrix_entry[0] * lax.rsqrt(
            rows_new[position][:, None] * cols_new[None, :] / mean_rows[position]
        )
        cols_list.append(cols_new)
        direction_list.append(direction)
        square_list.append(jnp.sum(direction * direction))
    square_total = lax.psum(jnp.stack(square_list), ("fsdp", "tensor"))
    matrix_count = D * column_weights
    update_rms = jnp.sqrt(square_total / matrix_count)
    weight_scale = jnp.sqrt(weight_total / matrix_count)
    new_weights = []
    for position, matrix_entry in enumerate(matrices):
        new_weights.append(
            matrix_entry[1]
            - RATE
            * weight_scale[position]
            * direction_list[position]
            / jnp.maximum(1.0, update_rms[position] / CLIP_LEVEL)
        )
    vector_rms = jnp.sqrt(vector_sums[0] / D)
    vector_scale = jnp.sqrt(vector_sums[1] / D)
    vectors_new = vectors - RATE * vector_scale * vector_direction / jnp.maximum(
        1.0, vector_rms / CLIP_LEVEL
    )
    qkv_rms = jnp.sqrt(bias_total[0] / (3 * D))
    qkv_scale = jnp.sqrt(bias_total[2] / (3 * D))
    qkv_bias_new = qkv_bias - RATE * qkv_scale * qkv_direction / jnp.maximum(
        1.0, qkv_rms / CLIP_LEVEL
    )
    up_rms = jnp.sqrt(bias_total[1] / FF)
    up_scale = jnp.sqrt(bias_total[3] / FF)
    up_bias_new = fc1_bias - RATE * up_scale * up_direction / jnp.maximum(1.0, up_rms / CLIP_LEVEL)
    return (
        layer_out,
        input_grad,
        grad_qkv,
        grad_qkv_bias,
        grad_proj,
        grad_up,
        grad_up_bias,
        grad_down,
        grad_vectors,
        rows_new,
        cols_list[0].reshape(3, head_width),
        cols_list[1],
        cols_list[2],
        cols_list[3],
        vector_state_new,
        qkv_state_new,
        up_state_new,
        new_weights[0].reshape(shard_rows, 3, head_width),
        qkv_bias_new,
        new_weights[1],
        new_weights[2],
        up_bias_new,
        new_weights[3],
        vectors_new,
        update_rms,
    )


SCALE = HD**-0.5
LENGTH = GT * GH * GW
ROLL = HD // 3 // 2
CORE_SWAP = [(i, i ^ 1) for i in range(8)]
LOW = jnp.bfloat16
QB = 256


def chip_tables(core):
    rows = lax.broadcasted_iota(jnp.int32, (LENGTH, 2 * HD), 0)
    token = (rows + core * (LENGTH // 2)) % LENGTH
    lane = lax.broadcasted_iota(jnp.int32, (LENGTH, 2 * HD), 1) % HD
    axis = lane // (2 * ROLL)
    within = lane % (2 * ROLL)
    coordinate = jnp.where(
        axis == 0, token // (GH * GW), jnp.where(axis == 1, token // GW % GH, token % GW)
    ).astype(jnp.float32)
    step = (within % ROLL).astype(jnp.float32)
    frequency = BASE ** (-step / ROLL)
    live = lane < 6 * ROLL
    angle = jnp.where(live, coordinate * frequency, 0.0)
    cosine = jnp.cos(angle)
    sine = jnp.sin(angle)
    second = within >= ROLL
    from_first = jnp.where(live & second, sine, 0.0)
    from_second = jnp.where(live & ~second, -sine, 0.0)
    return cosine, from_first, from_second


def turn(v, c, s1, s2, sign):
    return v * c + sign * (pltpu.roll(v, ROLL, 1) * s1 + pltpu.roll(v, 2 * HD - ROLL, 1) * s2)


def dot_nt(a, b):
    return lax.dot_general(a, b, (((1,), (1,)), ((), ())), preferred_element_type=jnp.float32)


def dot_tn(a, b):
    return lax.dot_general(a, b, (((0,), (0,)), ((), ())), preferred_element_type=jnp.float32)


def dot_nn(a, b):
    return lax.dot_general(a, b, (((1,), (0,)), ((), ())), preferred_element_type=jnp.float32)


def attend_kernel(x_ref, c_ref, s1_ref, s2_ref, low_ref, o_ref, lse_ref, kh_ref, vh_ref):
    width = 2 * HD
    c, s1, s2 = c_ref[...], s1_ref[...], s2_ref[...]
    lane = lax.broadcasted_iota(jnp.int32, (LENGTH, width), 1)
    low_ref[:, :width] = turn(x_ref[:, :width], c, s1, s2, 1.0).astype(LOW)
    k = turn(x_ref[:, width : 2 * width], c, s1, s2, 1.0)
    v = x_ref[:, 2 * width :]
    low_ref[:, width : 2 * width] = k.astype(LOW)
    low_ref[:, 2 * width :] = v.astype(LOW)
    for h in range(2):
        mine = (lane < HD) if h == 0 else (lane >= HD)
        kh_ref[h] = jnp.where(mine, k, 0.0).astype(LOW)
        vh_ref[h] = jnp.where(mine, v, 0.0).astype(LOW)

    def block(j, carry):
        rows = pl.ds(pl.multiple_of(j * QB, QB), QB)
        q = (low_ref[rows, :width].astype(jnp.float32) * SCALE).astype(LOW)
        total = jnp.zeros((width, QB), jnp.float32)
        for h in range(2):
            s = dot_nt(kh_ref[h], q)
            peak = jnp.max(s, axis=0, keepdims=True)
            e = jnp.exp(s - peak)
            mass = jnp.sum(e, axis=0, keepdims=True)
            p = (e * (1.0 / mass)).astype(LOW)
            total += dot_tn(vh_ref[h], p)
            lse_ref[0, h : h + 1, rows] = peak + jnp.log(mass)
        o_ref[rows, :] = total.T.astype(LOW)
        return carry

    lax.fori_loop(0, LENGTH // QB, block, 0)


def attend(projected, tables):
    lanes = projected.shape[1] // (6 * HD)
    table = pl.BlockSpec((LENGTH, 2 * HD), lambda z: (0, 0))
    return pl.pallas_call(
        attend_kernel,
        grid=(lanes,),
        in_specs=[pl.BlockSpec((LENGTH, 6 * HD), lambda z: (0, z)), table, table, table],
        out_specs=[
            pl.BlockSpec((LENGTH, 6 * HD), lambda z: (0, z)),
            pl.BlockSpec((LENGTH, 2 * HD), lambda z: (0, z)),
            pl.BlockSpec((1, 2, LENGTH), lambda z: (z, 0, 0)),
        ],
        out_shape=[
            jax.ShapeDtypeStruct((LENGTH, lanes * 6 * HD), LOW),
            jax.ShapeDtypeStruct((LENGTH, lanes * 2 * HD), LOW),
            jax.ShapeDtypeStruct((lanes, 2, LENGTH), jnp.float32),
        ],
        scratch_shapes=[pltpu.VMEM((2, LENGTH, 2 * HD), LOW), pltpu.VMEM((2, LENGTH, 2 * HD), LOW)],
        compiler_params=pltpu.CompilerParams(vmem_limit_bytes=40 * 1024 * 1024),
        cost_estimate=pl.CostEstimate(
            flops=16 * LENGTH * LENGTH * HD * lanes,
            bytes_accessed=20 * LENGTH * HD * lanes,
            transcendentals=2 * lanes * LENGTH * LENGTH,
        ),
        name="attend",
    )(projected, *tables)


def attend_back_kernel(
    low_ref, go_ref, lse_ref, c_ref, s1_ref, s2_ref, g_ref, sum_ref, kh_ref, vh_ref, gk_ref, gv_ref
):
    width = 2 * HD
    lane = lax.broadcasted_iota(jnp.int32, (LENGTH, width), 1)
    lane_q = lax.broadcasted_iota(jnp.int32, (QB, width), 1)
    k = low_ref[:, width : 2 * width].astype(jnp.float32)
    v = low_ref[:, 2 * width :].astype(jnp.float32)
    for h in range(2):
        mine = (lane < HD) if h == 0 else (lane >= HD)
        kh_ref[h] = jnp.where(mine, k, 0.0).astype(LOW)
        vh_ref[h] = jnp.where(mine, v, 0.0).astype(LOW)
    gk_ref[...] = jnp.zeros_like(gk_ref)
    gv_ref[...] = jnp.zeros_like(gv_ref)

    def block(j, carry):
        rows = pl.ds(pl.multiple_of(j * QB, QB), QB)
        q = low_ref[rows, :width].astype(jnp.float32) * SCALE
        go = go_ref[rows, :].astype(jnp.float32)
        total = jnp.zeros((width, QB), jnp.float32)
        for h in range(2):
            mine = (lane_q < HD) if h == 0 else (lane_q >= HD)
            qh = jnp.where(mine, q, 0.0).astype(LOW)
            gh = jnp.where(mine, go, 0.0).astype(LOW)
            p = jnp.exp(dot_nt(kh_ref[h], qh) - lse_ref[0, h : h + 1, rows])
            dp = dot_nt(vh_ref[h], gh)
            pd = jnp.sum(p * dp, axis=0, keepdims=True)
            ds = (p * (dp - pd)).astype(LOW)
            gv_ref[...] += dot_nn(p.astype(LOW), gh)
            gk_ref[...] += dot_nn(ds, qh)
            total += dot_tn(kh_ref[h], ds)
        gq = turn(total.T * SCALE, c_ref[rows, :], s1_ref[rows, :], s2_ref[rows, :], -1.0)
        g_ref[rows, :width] = gq.astype(LOW)
        return carry

    lax.fori_loop(0, LENGTH // QB, block, 0)
    gk = turn(gk_ref[...], c_ref[...], s1_ref[...], s2_ref[...], -1.0)
    g_ref[:, width : 2 * width] = gk.astype(LOW)
    g_ref[:, 2 * width :] = gv_ref[...].astype(LOW)
    sum_ref[...] = jnp.sum(g_ref[...].astype(jnp.float32), axis=0, keepdims=True)


def attend_back(low, go, lse, tables):
    lanes = low.shape[1] // (6 * HD)
    table = pl.BlockSpec((LENGTH, 2 * HD), lambda z: (0, 0))
    wide = pl.BlockSpec((LENGTH, 6 * HD), lambda z: (0, z))
    return pl.pallas_call(
        attend_back_kernel,
        grid=(lanes,),
        in_specs=[
            wide,
            pl.BlockSpec((LENGTH, 2 * HD), lambda z: (0, z)),
            pl.BlockSpec((1, 2, LENGTH), lambda z: (z, 0, 0)),
            table,
            table,
            table,
        ],
        out_specs=[wide, pl.BlockSpec((1, 6 * HD), lambda z: (0, z))],
        out_shape=[
            jax.ShapeDtypeStruct((LENGTH, lanes * 6 * HD), LOW),
            jax.ShapeDtypeStruct((1, lanes * 6 * HD), jnp.float32),
        ],
        scratch_shapes=[
            pltpu.VMEM((2, LENGTH, 2 * HD), LOW),
            pltpu.VMEM((2, LENGTH, 2 * HD), LOW),
            pltpu.VMEM((LENGTH, 2 * HD), jnp.float32),
            pltpu.VMEM((LENGTH, 2 * HD), jnp.float32),
        ],
        compiler_params=pltpu.CompilerParams(vmem_limit_bytes=40 * 1024 * 1024),
        cost_estimate=pl.CostEstimate(
            flops=40 * LENGTH * LENGTH * HD * lanes,
            bytes_accessed=26 * LENGTH * HD * lanes,
            transcendentals=2 * lanes * LENGTH * LENGTH,
        ),
        name="attend_back",
    )(low, go, lse, *tables)


MESH = pl.DeviceIdType.MESH
PIECES = ((0, 0, 384, 0), (1, 384, 128, 0), (2, 512, 256, 0), (2, 768, 256, 1024), (3, 1024, 256, 0), (3, 1280, 256, 1024))
SHARD = 128


def remote(src, dst, send, recv, target):
    return pltpu.make_async_remote_copy(
        src_ref=src, dst_ref=dst, send_sem=send, recv_sem=recv, device_id=target, device_id_type=MESH
    )


def flip(index, bit):
    return index + bit - 2 * bit * ((index // bit) % 2)


def peers():
    lane = lax.axis_index("tensor")
    shard = lax.axis_index("fsdp")
    is_mid = (lane == 1) | (lane == 2)
    pair = {"tensor": flip(lane, 1)}
    across = {"tensor": 3 - lane}
    x_peer = {"fsdp": flip(shard, 2)}
    y_peer = {"fsdp": flip(shard, 4)}
    return lane, shard, is_mid, pair, across, x_peer, y_peer


def meet(targets):
    barrier = pltpu.get_barrier_semaphore()
    for target in targets:
        pl.semaphore_signal(barrier, inc=1, device_id=target, device_id_type=MESH)
    pl.semaphore_wait(barrier, len(targets))


def gather_kernel(
    pack_ref, vec_ref, bias_ref, qkv_ref, proj_ref, up_ref, down_ref, vec_all, bias_all,
    local_sem, send_sem, recv_sem, small_send, small_recv,
):
    lane, shard, is_mid, pair, across, x_peer, y_peer = peers()
    core = shard % 2
    outs = (qkv_ref, proj_ref, up_ref, down_ref)
    shard_peers = [
        (q, dc, {"fsdp": flip_place(shard, q, dc)})
        for q in range(4)
        for dc in range(2)
        if (q, dc) != (0, 0)
    ]
    lane_peers = [pair, {"tensor": (lane + 2) % 4}, across]
    meet([t for _, _, t in shard_peers] + lane_peers)

    chunks = [(piece, r) for piece in PIECES for r in range(2)]

    def window(c, row0, row_count, col0, col_count):
        (m, _, width, base), r = chunks[c]
        return outs[m].at[
            pl.ds(r * 4 * SHARD + row0, row_count), pl.ds(base + col0 * width, col_count * width)
        ]

    def own(c):
        (_, first, width, _), r = chunks[c]
        return pack_ref.at[r, :, pl.ds(first, width)]

    def local(c):
        return pltpu.make_async_copy(own(c), window(c, 0, SHARD, 0, 1), local_sem.at[c])

    def hop_pair(c):
        return remote(own(c), window(c, 0, SHARD, 1, 1), send_sem.at[c, 0], recv_sem.at[c, 0], pair)

    def hop_across(c):
        return remote(
            window(c, 0, SHARD, 0, 2), window(c, 0, SHARD, 2, 2), send_sem.at[c, 1], recv_sem.at[c, 1], across
        )

    def hop_out(c):
        far = window(c, 0, SHARD, 2, 2)
        return remote(far, far, send_sem.at[c, 2], recv_sem.at[c, 1], pair)

    def hop_first(c):
        src = window(c, 0, SHARD, 0, 4)
        if chunks[c][1] == 0:
            return remote(src, window(c, SHARD, SHARD, 0, 4), send_sem.at[c, 3], recv_sem.at[c, 2], x_peer)
        return remote(src, window(c, 2 * SHARD, SHARD, 0, 4), send_sem.at[c, 3], recv_sem.at[c, 2], y_peer)

    def hop_second(c):
        if chunks[c][1] == 0:
            return [
                remote(
                    window(c, 0, 2 * SHARD, 0, 4), window(c, 2 * SHARD, 2 * SHARD, 0, 4),
                    send_sem.at[c, 4], recv_sem.at[c, 3], y_peer,
                )
            ]
        return [
            remote(
                window(c, k * 2 * SHARD, SHARD, 0, 4), window(c, (2 * k + 1) * SHARD, SHARD, 0, 4),
                send_sem.at[c, 4 + k], recv_sem.at[c, 3 + k], x_peer,
            )
            for k in range(2)
        ]

    count = len(chunks)
    small = []
    slot = core * 4
    vec_all[pl.ds(slot, 1)] = vec_ref[...][None]
    bias_all[0] = bias_ref[...]
    for i, (q, _, target) in enumerate(shard_peers):
        small.append(remote(vec_ref, vec_all.at[slot + q], small_send.at[i], small_recv.at[i], target))
    far_slot = 3 - is_mid.astype(jnp.int32)
    for i, target in enumerate(lane_peers):
        to = bias_all.at[1] if i == 0 else bias_all.at[far_slot]
        small.append(remote(bias_ref, to, small_send.at[7 + i], small_recv.at[7 + i], target))
    for c in range(count):
        local(c).start()
    hop_pair(0).start()
    hop_pair(1).start()
    for copy in small:
        copy.start()
    for tick in range(count + 5):
        if 2 <= tick < count:
            hop_pair(tick).start()
        c = tick - 1
        if 0 <= c < count:
            local(c).wait()
            hop_pair(c).wait_recv()

            @pl.when(is_mid)
            def _():
                hop_across(c).start()

        c = tick - 2
        if 0 <= c < count:
            hop_across(c).wait_recv()

            @pl.when(is_mid)
            def _():
                hop_out(c).start()

            hop_first(c).start()
        c = tick - 4
        if 0 <= c < count:
            hop_first(c).wait_recv()
            for copy in hop_second(c):
                copy.start()
    for copy in small:
        copy.wait()
    for c in range(count):
        for copy in hop_second(c):
            copy.wait()
        hop_pair(c).wait_send()
        hop_first(c).wait_send()

        @pl.when(is_mid)
        def _():
            hop_across(c).wait_send()
            hop_out(c).wait_send()


def flip_place(shard, q, dc):
    target = shard
    for bit, on in ((1, dc), (2, q & 1), (4, q >> 1)):
        if on:
            target = flip(target, bit)
    return target


def gather_all(pack, vec, bias):
    count = 2 * len(PIECES)
    width = pack.shape[2]
    rows = 8 * SHARD
    any_space = pl.BlockSpec(memory_space=pl.ANY)
    vmem = pl.BlockSpec(memory_space=pltpu.VMEM)
    return pl.pallas_call(
        gather_kernel,
        in_specs=[vmem] * 3,
        out_specs=[any_space] * 4 + [vmem] * 2,
        out_shape=[
            jax.ShapeDtypeStruct((rows, 1536), LOW),
            jax.ShapeDtypeStruct((rows, 512), LOW),
            jax.ShapeDtypeStruct((rows, 2048), LOW),
            jax.ShapeDtypeStruct((rows, 2048), LOW),
            jax.ShapeDtypeStruct((8,) + vec.shape, jnp.float32),
            jax.ShapeDtypeStruct((4,) + bias.shape, jnp.float32),
        ],
        scratch_shapes=[
            pltpu.SemaphoreType.DMA((count,)),
            pltpu.SemaphoreType.DMA((count, 6)),
            pltpu.SemaphoreType.DMA((count, 5)),
            pltpu.SemaphoreType.DMA((10,)),
            pltpu.SemaphoreType.DMA((10,)),
        ],
        compiler_params=pltpu.CompilerParams(collective_id=1, has_side_effects=True),
        name="gather_all",
    )(pack, vec, bias)


def scatter_kernel(arrays, chunks, *refs):
    grads = refs[:arrays]
    out_ref, own_ref, first_ref, second_ref, in_ref, mid_ref, near_ref = refs[arrays : arrays + 7]
    local_sem, send_sem, recv_sem = refs[arrays + 7 :]
    lane, shard, is_mid, pair, across, x_peer, y_peer = peers()
    barrier = pltpu.get_barrier_semaphore()
    for target in (pair, x_peer, y_peer):
        pl.semaphore_signal(barrier, inc=1, device_id=target, device_id_type=MESH)

    @pl.when(is_mid)
    def _():
        pl.semaphore_signal(barrier, inc=1, device_id=across, device_id_type=MESH)

    pl.semaphore_wait(barrier, 3 + is_mid.astype(jnp.int32))

    def source(c, row0, row_count):
        (a, _, width, base), r = chunks[c]
        return grads[a].at[pl.ds(r * 4 * SHARD + row0, row_count), pl.ds(base, 4 * width)]

    def part(ref, c, row0, row_count, lo, hi, each):
        (_, first, width, _), r = chunks[c]
        return ref.at[r, pl.ds(row0, row_count), pl.ds(first * each + lo * width, (hi - lo) * width)]

    def keep(c):
        if chunks[c][1] == 0:
            return [
                pltpu.make_async_copy(
                    source(c, 0, 2 * SHARD), part(own_ref, c, 0, 2 * SHARD, 0, 4, 4), local_sem.at[c, 0]
                )
            ]
        return [
            pltpu.make_async_copy(
                source(c, k * 2 * SHARD, SHARD), part(own_ref, c, k * SHARD, SHARD, 0, 4, 4), local_sem.at[c, k]
            )
            for k in range(2)
        ]

    def hop_first(c):
        if chunks[c][1] == 0:
            return [
                remote(
                    source(c, 2 * SHARD, 2 * SHARD), part(first_ref, c, 0, 2 * SHARD, 0, 4, 4),
                    send_sem.at[c, 0], recv_sem.at[c, 0], y_peer,
                )
            ]
        return [
            remote(
                source(c, (2 * k + 1) * SHARD, SHARD), part(first_ref, c, k * SHARD, SHARD, 0, 4, 4),
                send_sem.at[c, k], recv_sem.at[c, k], x_peer,
            )
            for k in range(2)
        ]

    def hop_second(c):
        return remote(
            part(own_ref, c, SHARD, SHARD, 0, 4, 4), part(second_ref, c, 0, SHARD, 0, 4, 4),
            send_sem.at[c, 2], recv_sem.at[c, 2], x_peer if chunks[c][1] == 0 else y_peer,
        )

    def hop_in(c):
        return remote(
            part(own_ref, c, 0, SHARD, 2, 4, 4), part(in_ref, c, 0, SHARD, 0, 2, 2),
            send_sem.at[c, 3], recv_sem.at[c, 3], pair,
        )

    def hop_across(c):
        return remote(
            part(own_ref, c, 0, SHARD, 2, 4, 4), part(mid_ref, c, 0, SHARD, 0, 2, 2),
            send_sem.at[c, 3], recv_sem.at[c, 4], across,
        )

    def hop_pair(c):
        return remote(
            part(own_ref, c, 0, SHARD, 1, 2, 4), part(near_ref, c, 0, SHARD, 0, 1, 1),
            send_sem.at[c, 4], recv_sem.at[c, 5], pair,
        )

    def add(dst, left, right, rows):
        step = 16

        @pl.loop(0, rows // step)
        def _(i):
            at = pl.ds(pl.multiple_of(i * step, step), step)
            total = left[at, :].astype(jnp.float32) + right[at, :].astype(jnp.float32)
            dst[at, :] = total.astype(dst.dtype)

    count = len(chunks)
    lead = 4
    for c in range(count):
        for copy in keep(c):
            copy.start()
    for c in range(min(lead, count)):
        for copy in hop_first(c):
            copy.start()
    for tick in range(count + 5):
        c = tick
        if c < count:
            for copy in keep(c):
                copy.wait()
            for copy in hop_first(c):
                copy.wait_recv()
            if c + lead < count:
                for copy in hop_first(c + lead):
                    copy.start()
            mine = part(own_ref, c, SHARD, SHARD, 0, 4, 4)
            add(mine, mine, part(first_ref, c, SHARD, SHARD, 0, 4, 4), SHARD)
            hop_second(c).start()
            mine = part(own_ref, c, 0, SHARD, 0, 4, 4)
            add(mine, mine, part(first_ref, c, 0, SHARD, 0, 4, 4), SHARD)
        c = tick - 2
        if 0 <= c < count:
            hop_second(c).wait_recv()
            mine = part(own_ref, c, 0, SHARD, 0, 4, 4)
            add(mine, mine, part(second_ref, c, 0, SHARD, 0, 4, 4), SHARD)

            @pl.when(jnp.logical_not(is_mid))
            def _():
                hop_in(c).start()

        c = tick - 3
        if 0 <= c < count:

            @pl.when(is_mid)
            def _():
                hop_in(c).wait_recv()
                far = part(own_ref, c, 0, SHARD, 2, 4, 4)
                add(far, far, part(in_ref, c, 0, SHARD, 0, 2, 2), SHARD)
                hop_across(c).start()

        c = tick - 4
        if 0 <= c < count:

            @pl.when(is_mid)
            def _():
                hop_across(c).wait_recv()
                near = part(own_ref, c, 0, SHARD, 0, 2, 4)
                add(near, near, part(mid_ref, c, 0, SHARD, 0, 2, 2), SHARD)

            hop_pair(c).start()
        c = tick - 5
        if 0 <= c < count:
            hop_pair(c).wait_recv()
            add(
                part(out_ref, c, 0, SHARD, 0, 1, 1), part(own_ref, c, 0, SHARD, 0, 1, 4),
                part(near_ref, c, 0, SHARD, 0, 1, 1), SHARD,
            )
    for c in range(count):
        for copy in hop_first(c):
            copy.wait_send()
        hop_second(c).wait_send()
        hop_pair(c).wait_send()

        @pl.when(is_mid)
        def _():
            hop_across(c).wait_send()

        @pl.when(jnp.logical_not(is_mid))
        def _():
            hop_in(c).wait_send()


def scatter_all(grads, pieces, collective_id):
    chunks = [(piece, r) for piece in pieces for r in range(2)]
    count = len(chunks)
    width = sum(piece[2] for piece in pieces)
    vmem = pl.BlockSpec(memory_space=pltpu.VMEM)
    return pl.pallas_call(
        functools.partial(scatter_kernel, len(grads), chunks),
        in_specs=[pl.BlockSpec(memory_space=pl.ANY)] * len(grads),
        out_specs=vmem,
        out_shape=jax.ShapeDtypeStruct((2, SHARD, width), jnp.float32),
        scratch_shapes=[
            pltpu.VMEM((2, 2 * SHARD, 4 * width), LOW),
            pltpu.VMEM((2, 2 * SHARD, 4 * width), LOW),
            pltpu.VMEM((2, SHARD, 4 * width), LOW),
            pltpu.VMEM((2, SHARD, 2 * width), LOW),
            pltpu.VMEM((2, SHARD, 2 * width), LOW),
            pltpu.VMEM((2, SHARD, width), LOW),
            pltpu.SemaphoreType.DMA((count, 2)),
            pltpu.SemaphoreType.DMA((count, 5)),
            pltpu.SemaphoreType.DMA((count, 6)),
        ],
        compiler_params=pltpu.CompilerParams(collective_id=collective_id, has_side_effects=True, vmem_limit_bytes=48 * 1024 * 1024),
        name="scatter_all",
    )(*grads)


COUNTS = (3 * D, D, FF, FF)
BLOCKS = (6, 2, 8, 8)


def offsets():
    return [(z * 8 + q * 2 + dc, q, dc, z) for z in range(4) for q in range(4) for dc in range(2)]


def tune_kernel(
    late_ref, early_ref, vec_ref, db_ref, wq_ref, wp_ref, wu_ref, wd_ref, vw_ref, vs_ref, rows_ref,
    cq_ref, cp_ref, cu_ref, cd_ref, bq_ref, bu_ref, bqs_ref, bus_ref,
    gq_out, gp_out, gu_out, gd_out, nq_out, np_out, nu_out, nd_out, vec_out, rows_out,
    cq_out, cp_out, cu_out, cd_out, bq_out, bqs_out, bqn_out, bu_out, bus_out, bun_out, rms_out,
    gq, upb, vec_send, vec_recv, db_recv, lane_send, lane_recv, col_send, col_recv, all_send, all_recv,
    core_send, core_done, a_send, a_recv, b_send, b_recv, c_send, c_recv,
):
    lane = lax.axis_index("tensor")
    shard = lax.axis_index("fsdp")
    core = shard % 2
    is_mid = (lane == 1) | (lane == 2)
    z_of = [lane, flip(lane, 1), 3 - lane, (lane + 2) % 4]

    def device(q, dc, z):
        target = {}
        if q or dc:
            target["fsdp"] = flip_place(shard, q, dc)
        if z:
            target["tensor"] = z_of[z]
        return target

    others = [entry for entry in offsets() if entry[0]]
    meet([device(q, dc, z) for _, q, dc, z in others])
    shard_peers = [(slot, q, dc) for slot, q, dc, z in others if z == 0]

    def core_copies():
        give = 1 - core
        hq = pl.ds(pl.multiple_of(core * 128, 128), 128)
        hf = pl.ds(pl.multiple_of(core * 512, 512), 512)
        pairs = [(late_ref.at[give, :, pl.ds(j * 128, 128)], gq.at[j, :, hq]) for j in range(3)]
        pairs.append((early_ref.at[give, :, pl.ds(1024, 128)], gp_out.at[:, hq]))
        pairs.append((early_ref.at[give, :, pl.ds(512, 512)], gu_out.at[:, hf]))
        pairs.append((early_ref.at[give, :, pl.ds(0, 512)], gd_out.at[:, hf]))
        return [
            remote(src, dst, core_send.at[i], core_done.at[i], {"fsdp": flip(shard, 1)})
            for i, (src, dst) in enumerate(pairs)
        ]

    for copy in core_copies():
        copy.start()

    def round_a():
        copies = [
            remote(vec_send.at[slot], vec_recv.at[slot], a_send.at[slot], a_recv.at[slot], device(q, dc, 0))
            for slot, q, dc in shard_peers
        ]
        for z in range(1, 4):
            position = 1 if z == 1 else (3 - is_mid.astype(jnp.int32) if z == 2 else 2 + is_mid.astype(jnp.int32))
            copies.append(
                remote(db_ref.at[position], db_recv.at[z], a_send.at[7 + z], a_recv.at[7 + z], device(0, 0, z))
            )
        return copies

    for slot in range(8):
        q, dc = slot // 2, slot % 2
        block = (core + dc - 2 * core * dc) * 4 + q
        at = pl.ds(pl.multiple_of(block * 128, 128), 128)
        if slot == 0:
            vec_recv[0] = vec_ref[:, at]
        else:
            vec_send[slot] = vec_ref[:, at]
    for copy in round_a():
        copy.start()
    db_recv[0] = db_ref[0]

    mine_q = pl.ds(pl.multiple_of(core * 128, 128), 128)
    mine_f = pl.ds(pl.multiple_of(core * 512, 512), 512)
    for j in range(3):
        gq[j, :, mine_q] = late_ref[core, :, j * 128 : (j + 1) * 128]
    gp_out[:, mine_q] = early_ref[core, :, 1024:1152]
    gu_out[:, mine_f] = early_ref[core, :, 512:1024]
    gd_out[:, mine_f] = early_ref[core, :, 0:512]

    def weight_block(m, i):
        if m == 0:
            return wq_ref[:, i // 2, (i % 2) * 128 : (i % 2) * 128 + 128]
        return (None, wp_ref, wu_ref, wd_ref)[m][:, i * 128 : (i + 1) * 128]

    def grad_block(m, i):
        if m == 0:
            return gq[i // 2, :, (i % 2) * 128 : (i % 2) * 128 + 128]
        return (None, gp_out, gu_out, gd_out)[m][:, i * 128 : (i + 1) * 128]

    zero = jnp.zeros((128, 128), jnp.float32)

    def total_of(v):
        return jnp.sum(jnp.sum(v, axis=0, keepdims=True), axis=1, keepdims=True)

    weight_squares = []
    for m in range(4):
        acc = zero
        for i in range(BLOCKS[m]):
            w = weight_block(m, i)
            acc += w * w
        weight_squares.append(total_of(acc))

    for copy in core_copies():
        copy.wait()
    for j in range(3):
        gq_out[:, j, :] = gq[j]
    lane_send[...] = jnp.zeros_like(lane_send)
    row = 0
    for m in range(4):
        acc = zero
        for i in range(BLOCKS[m]):
            g = grad_block(m, i)
            square = g * g
            acc += square
            col_send[row : row + 1, :] = jnp.sum(square, axis=0, keepdims=True)
            row += 1
        lane_send[8 + m : 9 + m, :] = jnp.sum(acc.T, axis=0, keepdims=True)

    for copy in round_a():
        copy.wait()
    vec_sum = vec_recv[0]
    for slot in range(1, 8):
        vec_sum += vec_recv[slot]
    lane_send[0:8, :] = vec_sum
    col_send[24:32, :] = db_recv[0] + db_recv[1] + db_recv[2] + db_recv[3]

    def round_b():
        copies = [
            remote(lane_send, lane_recv.at[z], b_send.at[z], b_recv.at[z], device(0, 0, z)) for z in range(1, 4)
        ]
        copies += [
            remote(col_send, col_recv.at[slot], b_send.at[3 + slot], b_recv.at[3 + slot], device(q, dc, 0))
            for slot, q, dc in shard_peers
        ]
        return copies

    for copy in round_b():
        copy.start()
    for copy in round_b():
        copy.wait()
    lane_total = lane_send[...] + lane_recv[1] + lane_recv[2] + lane_recv[3]
    same = col_send[...] + col_recv[2] + col_recv[4] + col_recv[6]
    cross = col_recv[1] + col_recv[3] + col_recv[5] + col_recv[7]
    col_total = same[0:24] + cross[0:24]
    low_half = jnp.where(core == 0, same[24:32], cross[24:32])
    high_half = jnp.where(core == 0, cross[24:32], same[24:32])
    bq_out[:, 0:128] = low_half[0:3]
    bq_out[:, 128:256] = high_half[0:3]
    bu_out[0:4, :] = low_half[3:7]
    bu_out[4:8, :] = high_half[3:7]

    def stepped(g, state):
        new = DECAY * state + (1.0 - DECAY) * (g * g + TINY)
        return new, g * lax.rsqrt(new)

    gvec = lane_total[0:8]
    vs_new, v_dir = stepped(gvec, vs_ref[...])
    bqs_new, bq_dir = stepped(bq_out[...], bqs_ref[...])
    bus_new, bu_dir = stepped(bu_out[...], bus_ref[...])
    bqs_out[...] = bqs_new
    bus_out[...] = bus_new
    vec_out[0:8, :] = gvec
    vec_out[8:16, :] = vs_new

    row_counts = jnp.where(
        lax.broadcasted_iota(jnp.int32, (4, 128), 0) == 0,
        float(COUNTS[0]),
        jnp.where(lax.broadcasted_iota(jnp.int32, (4, 128), 0) == 1, float(COUNTS[1]), float(COUNTS[2])),
    )
    rows_new = DECAY * rows_ref[...] + (1.0 - DECAY) * (lane_total[8:12] / row_counts + TINY)
    rows_out[...] = rows_new
    inverse_rows = lax.rsqrt(rows_new)
    spots = lax.broadcasted_iota(jnp.int32, (8, 128), 1)
    message = jnp.zeros((8, 128), jnp.float32)
    sums = []
    inverse_cols = []
    tall = []
    row = 0
    for m in range(4):
        tall.append(jnp.broadcast_to(inverse_rows[m : m + 1], (128, 128)).T)
        acc = zero
        for i in range(BLOCKS[m]):
            if m == 0:
                old = cq_ref[i // 2 : i // 2 + 1, (i % 2) * 128 : (i % 2) * 128 + 128]
            else:
                old = (None, cp_ref, cu_ref, cd_ref)[m][i : i + 1, :]
            new = DECAY * old + (1.0 - DECAY) * (col_total[row : row + 1] / D + TINY)
            if m == 0:
                cq_out[i // 2 : i // 2 + 1, (i % 2) * 128 : (i % 2) * 128 + 128] = new
            else:
                (None, cp_out, cu_out, cd_out)[m][i : i + 1, :] = new
            inverse_cols.append(lax.rsqrt(new))
            step = grad_block(m, i) * tall[m] * inverse_cols[row]
            acc += step * step
            row += 1
        sums.append(total_of(acc))
    terms = sums
    terms = terms + [0.25 * total_of(rows_new[m : m + 1]) for m in range(4)]
    terms = terms + weight_squares
    vw = vw_ref[...]
    v_squares = jnp.sum(v_dir * v_dir, axis=1, keepdims=True)
    w_squares = jnp.sum(vw * vw, axis=1, keepdims=True)
    terms = terms + [0.25 * v_squares[i : i + 1] for i in range(6)]
    terms = terms + [0.25 * w_squares[i : i + 1] for i in range(6)]
    for value in (bq_dir, bu_dir, bq_ref[...], bu_ref[...]):
        terms = terms + [0.125 * total_of(value * value)]
    for i, term in enumerate(terms):
        message = jnp.where(spots == i, term, message)
    all_send[...] = message

    def round_c():
        return [
            remote(all_send, all_recv.at[slot], c_send.at[slot], c_recv.at[slot], device(q, dc, z))
            for slot, q, dc, z in others
        ]

    for copy in round_c():
        copy.start()
    for copy in round_c():
        copy.wait()
    grand = message
    for slot, _, _, _ in others:
        grand += all_recv[slot]
    line = grand[0:1]
    spot = spots[0:1]

    def pick(i):
        return jnp.sum(jnp.where(spot == i, line, 0.0), axis=1, keepdims=True)

    rms_line = jnp.zeros((1, 128), jnp.float32)
    row = 0
    for m in range(4):
        size = float(D * COUNTS[m])
        mean_rows = pick(4 + m) / D
        rms = jnp.sqrt(pick(m) * mean_rows / size)
        scale = jnp.sqrt(pick(8 + m) / size)
        factor = RATE * scale * jnp.sqrt(mean_rows) / jnp.maximum(1.0, rms / CLIP_LEVEL)
        rms_line = jnp.where(spot == m, rms, rms_line)
        for i in range(BLOCKS[m]):
            new = weight_block(m, i) - factor * (grad_block(m, i) * tall[m] * inverse_cols[row])
            if m == 0:
                nq_out[:, i // 2, (i % 2) * 128 : (i % 2) * 128 + 128] = new
            else:
                (None, np_out, nu_out, nd_out)[m][:, i * 128 : (i + 1) * 128] = new
            row += 1
    rms_out[...] = rms_line
    for i in range(6):
        spread = jnp.sqrt(pick(12 + i) / D)
        factor = RATE * jnp.sqrt(pick(18 + i) / D) / jnp.maximum(1.0, spread / CLIP_LEVEL)
        vec_out[16 + i : 17 + i, :] = vw[i : i + 1] - factor * v_dir[i : i + 1]
    vec_out[22:24, :] = jnp.zeros((2, 128), jnp.float32)
    for direction, weight, out, at, size in (
        (bq_dir, bq_ref, bqn_out, 24, 3 * D),
        (bu_dir, bu_ref, bun_out, 25, FF),
    ):
        spread = jnp.sqrt(pick(at) / size)
        factor = RATE * jnp.sqrt(pick(at + 2) / size) / jnp.maximum(1.0, spread / CLIP_LEVEL)
        out[...] = weight[...] - factor * direction


def tune_all(late, early, vec_part, db_part, params, stats, states):
    qkv_weight, qkv_bias, proj_weight, fc1_weight, fc1_bias, fc2_weight, vectors = params
    row_state, qkv_cols, proj_cols, fc1_cols, fc2_cols = stats
    vector_state, qkv_bias_state, fc1_bias_state = states
    pad = ((0, 2), (0, 0))

    def dense(v):
        return v.reshape(v.shape[0] // 128, 128)

    operands = (
        late, early, vec_part, db_part, qkv_weight, proj_weight, fc1_weight, fc2_weight,
        jnp.pad(vectors.T, pad), jnp.pad(vector_state.T, pad, constant_values=1.0), row_state,
        qkv_cols, dense(proj_cols), dense(fc1_cols), dense(fc2_cols),
        qkv_bias, dense(fc1_bias), qkv_bias_state, dense(fc1_bias_state),
    )
    vmem = pl.BlockSpec(memory_space=pltpu.VMEM)
    shapes = [
        (128, 3, 256), (128, 256), (128, 1024), (128, 1024),
        (128, 3, 256), (128, 256), (128, 1024), (128, 1024),
        (24, 128), (4, 128), (3, 256), (2, 128), (8, 128), (8, 128),
        (3, 256), (3, 256), (3, 256), (8, 128), (8, 128), (8, 128), (1, 128),
    ]
    f32 = jnp.float32
    (
        gq, gp, gu, gd, nq, np_, nu, nd, vec, rows, cq, cp, cu, cd, bq, bqs, bqn, bu, bus, bun, rms
    ) = pl.pallas_call(
        tune_kernel,
        in_specs=[vmem] * len(operands),
        out_specs=[vmem] * len(shapes),
        out_shape=[jax.ShapeDtypeStruct(shape, f32) for shape in shapes],
        scratch_shapes=[
            pltpu.VMEM((3, 128, 256), f32),
            pltpu.VMEM((8, 128), f32),
            pltpu.VMEM((8, 8, 128), f32),
            pltpu.VMEM((8, 8, 128), f32),
            pltpu.VMEM((4, 8, 128), f32),
            pltpu.VMEM((16, 128), f32),
            pltpu.VMEM((4, 16, 128), f32),
            pltpu.VMEM((32, 128), f32),
            pltpu.VMEM((8, 32, 128), f32),
            pltpu.VMEM((8, 128), f32),
            pltpu.VMEM((32, 8, 128), f32),
            pltpu.SemaphoreType.DMA((6,)),
            pltpu.SemaphoreType.DMA((6,)),
            pltpu.SemaphoreType.DMA((11,)),
            pltpu.SemaphoreType.DMA((11,)),
            pltpu.SemaphoreType.DMA((11,)),
            pltpu.SemaphoreType.DMA((11,)),
            pltpu.SemaphoreType.DMA((32,)),
            pltpu.SemaphoreType.DMA((32,)),
        ],
        compiler_params=pltpu.CompilerParams(collective_id=4, has_side_effects=True, vmem_limit_bytes=40 * 1024 * 1024),
        name="tune_all",
    )(*operands)
    vec = vec.T
    return (
        gq, bq, gp, gu, bu.reshape(1024), gd, vec[:, 0:6], rows,
        cq, cp.reshape(256), cu.reshape(1024), cd.reshape(1024),
        vec[:, 8:14], bqs, bus.reshape(1024),
        nq, bqn, np_, nu, bun.reshape(1024), nd, vec[:, 16:22], rms[0, 0:4],
    )


def by_core(core, mine, theirs):
    return jnp.where(core == 0, mine, theirs), jnp.where(core == 0, theirs, mine)


def gelu_parts(u):
    cdf = 0.5 * (1.0 + lax.erf(u * (0.5**0.5)))
    density = jnp.exp(-0.5 * u * u) * ((2.0 * jnp.pi) ** -0.5)
    return u * cdf, cdf + u * density


def norm_parts(values):
    center = values - jnp.mean(values, axis=-1, keepdims=True)
    scale = lax.rsqrt(jnp.mean(center * center, axis=-1, keepdims=True) + NORM_EPS)
    return center * scale, scale


def norm_back(grad, unit, scale, gain):
    c = grad * gain
    return scale * (
        c
        - jnp.mean(c, axis=-1, keepdims=True)
        - unit * jnp.mean(c * unit, axis=-1, keepdims=True)
    )


def on_chip(
    tokens,
    cotangent,
    qkv_weight,
    qkv_bias,
    proj_weight,
    fc1_weight,
    fc1_bias,
    fc2_weight,
    vectors,
    row_state,
    qkv_cols,
    proj_cols,
    fc1_cols,
    fc2_cols,
    vector_state,
    qkv_bias_state,
    fc1_bias_state,
):
    shard = lax.axis_index("fsdp")
    lane = lax.axis_index("tensor")
    core = shard % 2
    place = shard // 2
    rows = tokens.shape[0]
    head_width = qkv_weight.shape[2]
    hidden_width = fc1_weight.shape[1]
    hw, fw = head_width // 2, hidden_width // 2
    shard_rows = qkv_weight.shape[0]
    swap_tokens = []
    for k in range(4):
        for p in range(2):
            a, b = (2 * k + 1) * 4 + 2 * p, 2 * k * 4 + 2 * p + 1
            swap_tokens += [(a, b), (b, a)]
    moved = (core ^ (lane & 1)) == 1

    def swap(v):
        return jnp.where(moved, lax.ppermute(v, ("fsdp", "tensor"), swap_tokens), v)

    def to_local(v):
        parts = []
        for r in range(2):
            for q in range(4):
                parts.append(
                    lax.dynamic_slice_in_dim(v, ((place ^ q) * 2 + r) * shard_rows, shard_rows, 1)
                )
        return jnp.concatenate(parts, axis=1)

    def to_global(v):
        parts = []
        for q in range(4):
            for r in range(2):
                parts.append(
                    lax.dynamic_slice_in_dim(v, (r * 4 + (place ^ q)) * shard_rows, shard_rows, 1)
                )
        return jnp.concatenate(parts, axis=1)

    def both_halves(v):
        return jnp.concatenate([v, lax.ppermute(v, "fsdp", CORE_SWAP)], axis=0)

    def core_sum(left, right_t):
        other = times_transposed(left[rows:], right_t)
        other = lax.ppermute(other, "fsdp", CORE_SWAP)
        return times_transposed(left[:rows], right_t) + other

    def half_columns(w, width, which):
        return lax.dynamic_slice_in_dim(w, which * width, width, w.ndim - 1)

    def pack(which):
        return jnp.concatenate(
            [
                half_columns(qkv_weight, hw, which).reshape(shard_rows, 3 * hw),
                half_columns(proj_weight, hw, which),
                half_columns(fc1_weight, fw, which),
                half_columns(fc2_weight, fw, which),
            ],
            axis=1,
        ).astype(LOW)

    theirs = lax.ppermute(pack(1 - core), "fsdp", CORE_SWAP)
    packs = jnp.stack(by_core(core, pack(core), theirs))
    vec = jnp.pad(vectors.astype(LOW).astype(jnp.float32).T, ((0, 2), (0, 0)))
    bias = jnp.concatenate(
        [
            half_columns(qkv_bias, hw, core).reshape(3 * hw),
            lax.dynamic_slice_in_dim(fc1_bias, core * fw, fw, 0),
        ]
    )
    bias = jnp.broadcast_to(
        lax.optimization_barrier(bias.astype(LOW)).astype(jnp.float32), (8, 3 * hw + fw)
    )
    weight_qkv, weight_proj, weight_up, weight_down, vec_all, bias_all = gather_all(
        packs, vec, bias
    )
    vector_rows = vec_all.transpose(1, 0, 2).reshape(8, D)
    gain_one, shift_one, proj_shift, gain_two, shift_two, down_shift = [
        vector_rows[i : i + 1] for i in range(6)
    ]
    bias_rows = bias_all[:, 0]
    bias_qkv = bias_rows[:, : 3 * hw].reshape(1, 12 * hw)
    bias_up = (
        bias_rows[:, 3 * hw :].reshape(4, 2, fw // 2).transpose(1, 0, 2).reshape(1, 4 * fw)
    )

    tables = chip_tables(core)
    inputs = to_local(swap(tokens)).astype(jnp.float32)
    upstream_low = to_local(swap(cotangent))
    grad_out_all = both_halves(upstream_low)

    unit_one, scale_one = norm_parts(inputs)
    normed_one = both_halves((unit_one * gain_one + shift_one).astype(LOW))
    projected = jnp.dot(normed_one, weight_qkv, preferred_element_type=jnp.float32) + bias_qkv
    low, mixed, lse = attend(projected, tables)
    middle = inputs + core_sum(mixed, weight_proj) + proj_shift
    unit_two, scale_two = norm_parts(middle)
    normed_two = both_halves((unit_two * gain_two + shift_two).astype(LOW))
    hidden = jnp.dot(normed_two, weight_up, preferred_element_type=jnp.float32) + bias_up
    active, slope = gelu_parts(hidden)
    active = active.astype(LOW)
    grad_down = contract_rows(grad_out_all, active).astype(LOW)
    layer_local = middle + core_sum(active, weight_down) + down_shift
    grad_active = jnp.dot(grad_out_all, weight_down, preferred_element_type=jnp.float32)
    grad_hidden = (grad_active * slope).astype(LOW)
    grad_up = contract_rows(normed_two, grad_hidden).astype(LOW)
    grad_bias_up = jnp.sum(grad_hidden.astype(jnp.float32), axis=0)
    grad_normed_two = core_sum(grad_hidden, weight_up)
    upstream = upstream_low.astype(jnp.float32)
    grad_middle = upstream + norm_back(grad_normed_two, unit_two, scale_two, gain_two)
    grad_branch = grad_middle.astype(LOW)
    grad_branch_all = both_halves(grad_branch)
    grad_proj = contract_rows(grad_branch_all, mixed).astype(LOW)
    grad_mixed = jnp.dot(
        grad_branch_all, weight_proj, preferred_element_type=jnp.float32
    ).astype(LOW)
    grad_low, grad_bias_qkv = attend_back(low, grad_mixed, lse, tables)
    grad_qkv = contract_rows(normed_one, grad_low).astype(LOW)
    grad_normed_one = core_sum(grad_low, weight_qkv)
    input_local = grad_middle + norm_back(grad_normed_one, unit_one, scale_one, gain_one)
    layer_out = to_global(swap(layer_local))
    input_grad = to_global(swap(input_local))

    late = scatter_all((grad_qkv,), ((0, 0, 3 * hw, 0),), 3)
    half = fw // 2
    early = scatter_all(
        (grad_down, grad_up, grad_proj),
        (
            (0, 0, half, 0),
            (0, half, half, 4 * half),
            (1, fw, half, 0),
            (1, fw + half, half, 4 * half),
            (2, 2 * fw, hw, 0),
        ),
        2,
    )

    vec_part = jnp.concatenate(
        [
            jnp.sum(grad_normed_one * unit_one, axis=0, keepdims=True),
            jnp.sum(grad_normed_one, axis=0, keepdims=True),
            jnp.sum(grad_branch.astype(jnp.float32), axis=0, keepdims=True),
            jnp.sum(grad_normed_two * unit_two, axis=0, keepdims=True),
            jnp.sum(grad_normed_two, axis=0, keepdims=True),
            jnp.sum(upstream, axis=0, keepdims=True),
            jnp.zeros((2, D), jnp.float32),
        ]
    )
    db_part = jnp.concatenate(
        [
            grad_bias_qkv.reshape(4, 3, hw),
            grad_bias_up.reshape(2, 4, 2, hw).transpose(1, 0, 2, 3).reshape(4, 4, hw),
            jnp.zeros((4, 1, hw), jnp.float32),
        ],
        axis=1,
    )
    return (
        layer_out,
        input_grad,
        *tune_all(
            late,
            early,
            vec_part,
            db_part,
            (qkv_weight, qkv_bias, proj_weight, fc1_weight, fc1_bias, fc2_weight, vectors),
            (row_state, qkv_cols, proj_cols, fc1_cols, fc2_cols),
            (vector_state, qkv_bias_state, fc1_bias_state),
        ),
    )


def solution(mesh):
    chips = mesh.shape["fsdp"] == 8 and mesh.shape["tensor"] == 4
    return jax.shard_map(
        on_chip if chips else on_device,
        mesh=mesh,
        in_specs=(
            P(("fsdp", "tensor"), None),
            P(("fsdp", "tensor"), None),
            P("fsdp", None, "tensor"),
            P(None, "tensor"),
            P("fsdp", "tensor"),
            P("fsdp", "tensor"),
            P("tensor"),
            P("fsdp", "tensor"),
            P("fsdp", None),
            P(None, "fsdp"),
            P(None, "tensor"),
            P("tensor"),
            P("tensor"),
            P("tensor"),
            P("fsdp", None),
            P(None, "tensor"),
            P("tensor"),
        ),
        out_specs=(
            P(("fsdp", "tensor"), None),
            P(("fsdp", "tensor"), None),
            P("fsdp", None, "tensor"),
            P(None, "tensor"),
            P("fsdp", "tensor"),
            P("fsdp", "tensor"),
            P("tensor"),
            P("fsdp", "tensor"),
            P("fsdp", None),
            P(None, "fsdp"),
            P(None, "tensor"),
            P("tensor"),
            P("tensor"),
            P("tensor"),
            P("fsdp", None),
            P(None, "tensor"),
            P("tensor"),
            P("fsdp", None, "tensor"),
            P(None, "tensor"),
            P("fsdp", "tensor"),
            P("fsdp", "tensor"),
            P("tensor"),
            P("fsdp", "tensor"),
            P("fsdp", None),
            P(),
        ),
        check_vma=False,
    )
```

```python
import functools

import jax
import jax.numpy as jnp
from jax import lax
from jax.experimental import pallas as pl
from jax.experimental.pallas import tpu as pltpu
from jax.sharding import PartitionSpec as P

D = 1024
HD = 64
FF = 4096
GT = 4
GH = 16
GW = 16


NORM_EPS = 1e-06
DECAY = 0.5
CLIP_LEVEL = 1.0
RATE = 0.3
TINY = 1e-30
BASE = 10000.0


def layer_norm(values, gain_row, shift_row):
    center = values - jnp.mean(values, axis=-1, keepdims=True)
    variance = jnp.mean(center * center, axis=-1, keepdims=True)
    return center * lax.rsqrt(variance + NORM_EPS) * gain_row + shift_row


def exact_gelu(values):
    return jax.nn.gelu(values, approximate=False)


def rope_tables(length, half_width):
    token_index = jnp.arange(length, dtype=jnp.int32)
    coordinates = jnp.stack(
        [token_index // (GH * GW), token_index // GW % GH, token_index % GW], axis=1
    ).astype(jnp.float32)
    frequency = BASE ** (-jnp.arange(half_width, dtype=jnp.float32) / half_width)
    angles = coordinates[:, :, None] * frequency[None, None, :]
    return (jnp.cos(angles), jnp.sin(angles))


def rotate(values, cosine_table, sine_table):
    half_width = cosine_table.shape[-1]
    rotated_width = 6 * half_width
    leading = values.shape[:-1]
    pair_rows = values[..., :rotated_width].reshape(leading + (3, 2, half_width))
    first_half = pair_rows[..., 0, :]
    second_half = pair_rows[..., 1, :]
    cosine_wide = cosine_table[:, None]
    sine_wide = sine_table[:, None]
    turned = jnp.stack(
        [
            first_half * cosine_wide - second_half * sine_wide,
            second_half * cosine_wide + first_half * sine_wide,
        ],
        axis=-2,
    )
    return jnp.concatenate(
        [turned.reshape(leading + (rotated_width,)), values[..., rotated_width:]], axis=-1
    )


def contract_rows(left, right):
    return lax.dot_general(
        left, right, (((0,), (0,)), ((), ())), preferred_element_type=jnp.float32
    )


def times_transposed(left, right):
    return lax.dot_general(
        left, right, (((1,), (1,)), ((), ())), preferred_element_type=jnp.float32
    )


def forward_block(query_rows, key_rows, value_rows):
    score_scale = query_rows.shape[-1] ** (-0.5)
    scores = (
        jnp.einsum("qhd,khd->hqk", query_rows, key_rows, preferred_element_type=jnp.float32)
        * score_scale
    )
    row_peak = jnp.max(scores, axis=-1, keepdims=True)
    raised = jnp.exp(scores - row_peak)
    totals = jnp.sum(raised, axis=-1, keepdims=True)
    attention = (raised / totals).astype(jnp.bfloat16)
    mixed_rows = jnp.einsum(
        "hqk,khd->qhd", attention, value_rows, preferred_element_type=jnp.float32
    )
    return (mixed_rows, (row_peak + jnp.log(totals))[..., 0])


def backward_block(running, block_item, key_rows, value_rows):
    query_rows, log_totals, grad_mixed = block_item
    score_scale = query_rows.shape[-1] ** (-0.5)
    scores = (
        jnp.einsum("qhd,khd->hqk", query_rows, key_rows, preferred_element_type=jnp.float32)
        * score_scale
    )
    attention = jnp.exp(scores - log_totals[..., None])
    grad_attention = jnp.einsum(
        "qhd,khd->hqk", grad_mixed, value_rows, preferred_element_type=jnp.float32
    )
    grad_scores = attention * (
        grad_attention - jnp.sum(attention * grad_attention, axis=-1, keepdims=True)
    )
    grad_low = grad_scores.astype(jnp.bfloat16)
    grad_queries = (
        jnp.einsum("hqk,khd->qhd", grad_low, key_rows, preferred_element_type=jnp.float32)
        * score_scale
    )
    key_total = (
        running[0]
        + jnp.einsum("hqk,qhd->khd", grad_low, query_rows, preferred_element_type=jnp.float32)
        * score_scale
    )
    value_total = running[1] + jnp.einsum(
        "hqk,qhd->khd",
        attention.astype(jnp.bfloat16),
        grad_mixed,
        preferred_element_type=jnp.float32,
    )
    return ((key_total, value_total), grad_queries)


def on_device(
    tokens,
    cotangent,
    qkv_weight,
    qkv_bias,
    proj_weight,
    fc1_weight,
    fc1_bias,
    fc2_weight,
    vectors,
    row_state,
    qkv_cols,
    proj_cols,
    fc1_cols,
    fc2_cols,
    vector_state,
    qkv_bias_state,
    fc1_bias_state,
):
    low_type = jnp.bfloat16
    lane_count = lax.axis_size("tensor")
    local_rows = tokens.shape[0]
    group_rows = local_rows * lane_count
    length = GT * GH * GW
    clip_count = group_rows // length
    block_rows = min(512, length)
    block_count = length // block_rows
    head_width = qkv_weight.shape[2]
    head_count = head_width // HD
    hidden_width = fc1_weight.shape[1]
    shard_rows = qkv_weight.shape[0]
    cosine_table, sine_table = rope_tables(length, HD // 3 // 2)
    weight_qkv, weight_proj, weight_up, weight_down, vector_low = (
        lax.all_gather(qkv_weight.astype(low_type), "fsdp", axis=0, tiled=True),
        lax.all_gather(proj_weight.astype(low_type), "fsdp", axis=0, tiled=True),
        lax.all_gather(fc1_weight.astype(low_type), "fsdp", axis=0, tiled=True),
        lax.all_gather(fc2_weight.astype(low_type), "fsdp", axis=0, tiled=True),
        lax.all_gather(vectors.astype(low_type), "fsdp", axis=0, tiled=True),
    )
    weight_qkv = weight_qkv.reshape(D, 3 * head_width)
    vector_full = vector_low.astype(jnp.float32)
    gain_one = vector_full[:, 0]
    shift_one = vector_full[:, 1]
    proj_shift = vector_full[:, 2]
    gain_two = vector_full[:, 3]
    shift_two = vector_full[:, 4]
    down_shift = vector_full[:, 5]
    bias_qkv = (
        lax.optimization_barrier(qkv_bias.astype(low_type))
        .astype(jnp.float32)
        .reshape(3 * head_width)
    )
    bias_up = lax.optimization_barrier(fc1_bias.astype(low_type)).astype(jnp.float32)
    inputs = tokens.astype(jnp.float32)
    normed_one = layer_norm(inputs, gain_one, shift_one).astype(low_type)
    gathered_one = lax.all_gather(normed_one, "tensor", axis=0, tiled=True)
    projected = jnp.dot(gathered_one, weight_qkv, preferred_element_type=jnp.float32) + bias_qkv
    projected = projected.reshape(clip_count, length, 3, head_count, HD)
    queries = rotate(projected[:, :, 0], cosine_table, sine_table).astype(low_type)
    key_rows = rotate(projected[:, :, 1], cosine_table, sine_table).astype(low_type)
    value_rows = projected[:, :, 2].astype(low_type)

    def clip_forward(clip_item):
        query_rows, clip_keys, clip_values = clip_item
        blocks = query_rows.reshape(block_count, block_rows, head_count, HD)
        return lax.map(
            lambda query_block: forward_block(query_block, clip_keys, clip_values), blocks
        )

    mixed_rows, log_totals = lax.map(clip_forward, (queries, key_rows, value_rows))
    mixed_low = mixed_rows.reshape(group_rows, head_width).astype(low_type)
    attn_sum = lax.psum_scatter(
        times_transposed(mixed_low, weight_proj), "tensor", scatter_dimension=0, tiled=True
    )
    middle = inputs + attn_sum + proj_shift
    normed_two = layer_norm(middle, gain_two, shift_two).astype(low_type)
    gathered_two = lax.all_gather(normed_two, "tensor", axis=0, tiled=True)
    hidden = jnp.dot(gathered_two, weight_up, preferred_element_type=jnp.float32) + bias_up
    active = exact_gelu(hidden).astype(low_type)
    layer_out = (
        middle
        + lax.psum_scatter(
            times_transposed(active, weight_down), "tensor", scatter_dimension=0, tiled=True
        )
        + down_shift
    )
    upstream = cotangent.astype(jnp.float32)
    grad_out_all, normed_two_all = (
        lax.all_gather(cotangent, "tensor", axis=0, tiled=True),
        lax.all_gather(normed_two, "tensor", axis=0, tiled=True),
    )
    grad_down = contract_rows(grad_out_all, active)
    grad_active = jnp.dot(grad_out_all, weight_down, preferred_element_type=jnp.float32)
    gelu_pull = jax.vjp(exact_gelu, hidden)[1]
    grad_hidden = gelu_pull(grad_active)[0].astype(low_type)
    grad_up = contract_rows(normed_two_all, grad_hidden)
    grad_bias_up = jnp.sum(grad_hidden.astype(jnp.float32), axis=0)
    grad_normed_two = lax.psum_scatter(
        times_transposed(grad_hidden, weight_up), "tensor", scatter_dimension=0, tiled=True
    )
    middle_part, grad_gain_two, grad_shift_two = jax.vjp(layer_norm, middle, gain_two, shift_two)[
        1
    ](grad_normed_two)
    grad_middle = upstream + middle_part
    grad_branch = grad_middle.astype(low_type)
    grad_proj_shift = jnp.sum(grad_branch.astype(jnp.float32), axis=0)
    grad_down_shift = jnp.sum(upstream, axis=0)
    grad_branch_all, normed_one_all = (
        lax.all_gather(grad_branch, "tensor", axis=0, tiled=True),
        lax.all_gather(normed_one, "tensor", axis=0, tiled=True),
    )
    grad_proj = contract_rows(grad_branch_all, mixed_low)
    grad_mixed = jnp.dot(grad_branch_all, weight_proj, preferred_element_type=jnp.float32).astype(
        low_type
    )
    grad_mixed = grad_mixed.reshape(clip_count, length, head_count, HD)

    def clip_backward(clip_item):
        query_rows, clip_keys, clip_values, clip_totals, clip_grads = clip_item
        starts = (jnp.zeros(clip_keys.shape, jnp.float32), jnp.zeros(clip_keys.shape, jnp.float32))
        block_items = (
            query_rows.reshape(block_count, block_rows, head_count, HD),
            clip_totals,
            clip_grads.reshape(block_count, block_rows, head_count, HD),
        )
        sums, grad_queries = lax.scan(
            lambda running, block_item: backward_block(running, block_item, clip_keys, clip_values),
            starts,
            block_items,
        )
        return (grad_queries.reshape(query_rows.shape), sums[0], sums[1])

    grad_queries, grad_keys, grad_values = lax.map(
        clip_backward, (queries, key_rows, value_rows, log_totals, grad_mixed)
    )
    grad_projected = jnp.stack(
        [
            rotate(grad_queries, cosine_table, -sine_table),
            rotate(grad_keys, cosine_table, -sine_table),
            grad_values,
        ],
        axis=2,
    )
    grad_projected = grad_projected.reshape(group_rows, 3 * head_width).astype(low_type)
    grad_qkv = contract_rows(normed_one_all, grad_projected).reshape(D, 3, head_width)
    grad_bias_qkv = jnp.sum(grad_projected.astype(jnp.float32), axis=0)
    grad_normed_one = lax.psum_scatter(
        times_transposed(grad_projected, weight_qkv), "tensor", scatter_dimension=0, tiled=True
    )
    input_part, grad_gain_one, grad_shift_one = jax.vjp(layer_norm, inputs, gain_one, shift_one)[1](
        grad_normed_one
    )
    input_grad = grad_middle + input_part
    grad_qkv, grad_proj, grad_up, grad_down = (
        lax.psum_scatter(grad_qkv, "fsdp", scatter_dimension=0, tiled=True),
        lax.psum_scatter(grad_proj, "fsdp", scatter_dimension=0, tiled=True),
        lax.psum_scatter(grad_up, "fsdp", scatter_dimension=0, tiled=True),
        lax.psum_scatter(grad_down, "fsdp", scatter_dimension=0, tiled=True),
    )
    lane_index = lax.axis_index("tensor")
    vector_part = jnp.stack(
        [
            grad_gain_one,
            grad_shift_one,
            grad_proj_shift,
            grad_gain_two,
            grad_shift_two,
            grad_down_shift,
        ],
        axis=1,
    )
    qkv_placed = lax.dynamic_update_slice(
        jnp.zeros((3, D), jnp.float32),
        grad_bias_qkv.reshape(3, head_width),
        (jnp.int32(0), lane_index * head_width),
    )
    up_placed = lax.dynamic_update_slice(
        jnp.zeros((FF,), jnp.float32), grad_bias_up, (lane_index * hidden_width,)
    )
    vector_total, qkv_total, up_total = lax.psum(
        (vector_part, qkv_placed, up_placed), ("fsdp", "tensor")
    )
    grad_vectors = lax.dynamic_slice_in_dim(
        vector_total, lax.axis_index("fsdp") * shard_rows, shard_rows, 0
    )
    grad_qkv_bias = lax.dynamic_slice_in_dim(qkv_total, lane_index * head_width, head_width, 1)
    grad_up_bias = lax.dynamic_slice_in_dim(up_total, lane_index * hidden_width, hidden_width, 0)
    matrices = [
        (
            grad_qkv.reshape(shard_rows, 3 * head_width),
            qkv_weight.reshape(shard_rows, 3 * head_width),
            qkv_cols.reshape(3 * head_width),
        ),
        (grad_proj, proj_weight, proj_cols),
        (grad_up, fc1_weight, fc1_cols),
        (grad_down, fc2_weight, fc2_cols),
    ]
    column_counts = [3 * D, D, FF, FF]
    column_weights = jnp.array(column_counts, jnp.float32)
    qkv_state_new = DECAY * qkv_bias_state + (1.0 - DECAY) * (grad_qkv_bias * grad_qkv_bias + TINY)
    qkv_direction = grad_qkv_bias * lax.rsqrt(qkv_state_new)
    up_state_new = DECAY * fc1_bias_state + (1.0 - DECAY) * (grad_up_bias * grad_up_bias + TINY)
    up_direction = grad_up_bias * lax.rsqrt(up_state_new)
    row_squares = jnp.stack(
        [jnp.sum(matrix_entry[0] * matrix_entry[0], axis=1) for matrix_entry in matrices]
    )
    weight_squares = jnp.stack(
        [jnp.sum(matrix_entry[1] * matrix_entry[1]) for matrix_entry in matrices]
    )
    bias_terms = jnp.stack(
        [
            jnp.sum(qkv_direction * qkv_direction),
            jnp.sum(up_direction * up_direction),
            jnp.sum(qkv_bias * qkv_bias),
            jnp.sum(fc1_bias * fc1_bias),
        ]
    )
    row_total, weight_partial, bias_total = lax.psum(
        (row_squares, weight_squares, bias_terms), "tensor"
    )
    rows_new = DECAY * row_state + (1.0 - DECAY) * (row_total / column_weights[:, None] + TINY)
    vector_state_new = DECAY * vector_state + (1.0 - DECAY) * (grad_vectors * grad_vectors + TINY)
    vector_direction = grad_vectors * lax.rsqrt(vector_state_new)
    vector_terms = jnp.stack(
        [jnp.sum(vector_direction * vector_direction, axis=0), jnp.sum(vectors * vectors, axis=0)]
    )
    col_squares = jnp.concatenate(
        [jnp.sum(matrix_entry[0] * matrix_entry[0], axis=0) for matrix_entry in matrices]
    )
    row_new_sums = jnp.sum(rows_new, axis=1)
    col_total, row_new_total, weight_total, vector_sums = lax.psum(
        (col_squares, row_new_sums, weight_partial, vector_terms), "fsdp"
    )
    mean_rows = row_new_total / D
    offsets = [0]
    for matrix_entry in matrices:
        offsets.append(offsets[-1] + matrix_entry[0].shape[1])
    cols_list = []
    direction_list = []
    square_list = []
    for position, matrix_entry in enumerate(matrices):
        col_slice = col_total[offsets[position] : offsets[position + 1]]
        cols_new = DECAY * matrix_entry[2] + (1.0 - DECAY) * (col_slice / D + TINY)
        direction = matrix_entry[0] * lax.rsqrt(
            rows_new[position][:, None] * cols_new[None, :] / mean_rows[position]
        )
        cols_list.append(cols_new)
        direction_list.append(direction)
        square_list.append(jnp.sum(direction * direction))
    square_total = lax.psum(jnp.stack(square_list), ("fsdp", "tensor"))
    matrix_count = D * column_weights
    update_rms = jnp.sqrt(square_total / matrix_count)
    weight_scale = jnp.sqrt(weight_total / matrix_count)
    new_weights = []
    for position, matrix_entry in enumerate(matrices):
        new_weights.append(
            matrix_entry[1]
            - RATE
            * weight_scale[position]
            * direction_list[position]
            / jnp.maximum(1.0, update_rms[position] / CLIP_LEVEL)
        )
    vector_rms = jnp.sqrt(vector_sums[0] / D)
    vector_scale = jnp.sqrt(vector_sums[1] / D)
    vectors_new = vectors - RATE * vector_scale * vector_direction / jnp.maximum(
        1.0, vector_rms / CLIP_LEVEL
    )
    qkv_rms = jnp.sqrt(bias_total[0] / (3 * D))
    qkv_scale = jnp.sqrt(bias_total[2] / (3 * D))
    qkv_bias_new = qkv_bias - RATE * qkv_scale * qkv_direction / jnp.maximum(
        1.0, qkv_rms / CLIP_LEVEL
    )
    up_rms = jnp.sqrt(bias_total[1] / FF)
    up_scale = jnp.sqrt(bias_total[3] / FF)
    up_bias_new = fc1_bias - RATE * up_scale * up_direction / jnp.maximum(1.0, up_rms / CLIP_LEVEL)
    return (
        layer_out,
        input_grad,
        grad_qkv,
        grad_qkv_bias,
        grad_proj,
        grad_up,
        grad_up_bias,
        grad_down,
        grad_vectors,
        rows_new,
        cols_list[0].reshape(3, head_width),
        cols_list[1],
        cols_list[2],
        cols_list[3],
        vector_state_new,
        qkv_state_new,
        up_state_new,
        new_weights[0].reshape(shard_rows, 3, head_width),
        qkv_bias_new,
        new_weights[1],
        new_weights[2],
        up_bias_new,
        new_weights[3],
        vectors_new,
        update_rms,
    )


SCALE = HD**-0.5
LENGTH = GT * GH * GW
ROLL = HD // 3 // 2
CORE_SWAP = [(i, i ^ 1) for i in range(8)]
LOW = jnp.bfloat16
QB = 256


def chip_tables(core):
    rows = lax.broadcasted_iota(jnp.int32, (LENGTH, 2 * HD), 0)
    token = (rows + core * (LENGTH // 2)) % LENGTH
    lane = lax.broadcasted_iota(jnp.int32, (LENGTH, 2 * HD), 1) % HD
    axis = lane // (2 * ROLL)
    within = lane % (2 * ROLL)
    coordinate = jnp.where(
        axis == 0, token // (GH * GW), jnp.where(axis == 1, token // GW % GH, token % GW)
    ).astype(jnp.float32)
    step = (within % ROLL).astype(jnp.float32)
    frequency = BASE ** (-step / ROLL)
    live = lane < 6 * ROLL
    angle = jnp.where(live, coordinate * frequency, 0.0)
    cosine = jnp.cos(angle)
    sine = jnp.sin(angle)
    second = within >= ROLL
    from_first = jnp.where(live & second, sine, 0.0)
    from_second = jnp.where(live & ~second, -sine, 0.0)
    return cosine, from_first, from_second


def turn(v, c, s1, s2, sign):
    return v * c + sign * (pltpu.roll(v, ROLL, 1) * s1 + pltpu.roll(v, 2 * HD - ROLL, 1) * s2)


def dot_nt(a, b):
    return lax.dot_general(a, b, (((1,), (1,)), ((), ())), preferred_element_type=jnp.float32)


def dot_tn(a, b):
    return lax.dot_general(a, b, (((0,), (0,)), ((), ())), preferred_element_type=jnp.float32)


def dot_nn(a, b):
    return lax.dot_general(a, b, (((1,), (0,)), ((), ())), preferred_element_type=jnp.float32)


MESH = pl.DeviceIdType.MESH
PIECES = ((0, 0, 384, 0), (1, 384, 128, 0), (2, 512, 256, 0), (2, 768, 256, 1024), (3, 1024, 256, 0), (3, 1280, 256, 1024))
SHARD = 128
HALVES = ((0, 64), (64, 64))
WHOLE = ((0, 128),)
MIB = 1024 * 1024


def split(piece_and_rows):
    return [(piece, r, at, rows) for piece, parts in piece_and_rows for at, rows in parts for r in range(2)]


def remote(src, dst, send, recv, target):
    return pltpu.make_async_remote_copy(
        src_ref=src, dst_ref=dst, send_sem=send, recv_sem=recv, device_id=target, device_id_type=MESH
    )


def flip(index, bit):
    return index + bit - 2 * bit * ((index // bit) % 2)


def peers():
    lane = lax.axis_index("tensor")
    shard = lax.axis_index("fsdp")
    is_mid = (lane == 1) | (lane == 2)
    pair = {"tensor": flip(lane, 1)}
    across = {"tensor": 3 - lane}
    x_peer = {"fsdp": flip(shard, 2)}
    y_peer = {"fsdp": flip(shard, 4)}
    return lane, shard, is_mid, pair, across, x_peer, y_peer


def meet(targets):
    barrier = pltpu.get_barrier_semaphore()
    for target in targets:
        pl.semaphore_signal(barrier, inc=1, device_id=target, device_id_type=MESH)
    pl.semaphore_wait(barrier, len(targets))


GATHER = split([(PIECES[0], HALVES)] + [(piece, WHOLE) for piece in PIECES[1:]])


def gather_kernel(
    pack_ref, vec_ref, bias_ref, x_ref, c_ref, s1_ref, s2_ref,
    qkv_ref, proj_ref, up_ref, down_ref, vec_all, bias_all, h_ref, low_ref, o_ref, lse_ref,
    wq_ref, kh_ref, vh_ref, load_sem, local_sem, send_sem, recv_sem, small_send, small_recv,
):
    lane, shard, is_mid, pair, across, x_peer, y_peer = peers()
    core = shard % 2
    outs = (qkv_ref, proj_ref, up_ref, down_ref)
    shard_peers = [
        (q, dc, {"fsdp": flip_place(shard, q, dc)})
        for q in range(4)
        for dc in range(2)
        if (q, dc) != (0, 0)
    ]
    lane_peers = [pair, {"tensor": (lane + 2) % 4}, across]
    meet([t for _, _, t in shard_peers] + lane_peers)

    def window(c, block, col0, col_count):
        (m, _, width, base), r, at, rows = GATHER[c]
        return outs[m].at[
            pl.ds((r * 4 + block) * SHARD + at, rows), pl.ds(base + col0 * width, col_count * width)
        ]

    def own(c):
        (_, first, width, _), r, at, rows = GATHER[c]
        return pack_ref.at[r, pl.ds(at, rows), pl.ds(first, width)]

    def local(c):
        return pltpu.make_async_copy(own(c), window(c, 0, 0, 1), local_sem.at[c])

    def hop_pair(c):
        return remote(own(c), window(c, 0, 1, 1), send_sem.at[c, 0], recv_sem.at[c, 0], pair)

    def hop_across(c):
        return remote(
            window(c, 0, 0, 2), window(c, 0, 2, 2), send_sem.at[c, 1], recv_sem.at[c, 1], across
        )

    def hop_out(c):
        far = window(c, 0, 2, 2)
        return remote(far, far, send_sem.at[c, 2], recv_sem.at[c, 1], pair)

    def hop_first(c):
        block, target = ((1, x_peer), (2, y_peer))[GATHER[c][1]]
        return remote(
            window(c, 0, 0, 4), window(c, block, 0, 4), send_sem.at[c, 3], recv_sem.at[c, 2], target
        )

    def hop_second(c):
        moves, target = ((((0, 2), (1, 3)), y_peer), (((0, 1), (2, 3)), x_peer))[GATHER[c][1]]
        return [
            remote(
                window(c, src, 0, 4), window(c, dst, 0, 4), send_sem.at[c, 4 + k], recv_sem.at[c, 3 + k], target
            )
            for k, (src, dst) in enumerate(moves)
        ]

    count = len(GATHER)
    small = []
    slot = core * 4
    vec_all[pl.ds(slot, 1)] = vec_ref[...][None]
    bias_all[0] = bias_ref[...]
    for i, (q, _, target) in enumerate(shard_peers):
        small.append(remote(vec_ref, vec_all.at[slot + q], small_send.at[i], small_recv.at[i], target))
    far_slot = 3 - is_mid.astype(jnp.int32)
    for i, target in enumerate(lane_peers):
        to = bias_all.at[1] if i == 0 else bias_all.at[far_slot]
        small.append(remote(bias_ref, to, small_send.at[7 + i], small_recv.at[7 + i], target))

    def tick(now):
        if 2 <= now < count:
            hop_pair(now).start()
        c = now - 1
        if 0 <= c < count:
            local(c).wait()
            hop_pair(c).wait_recv()

            @pl.when(is_mid)
            def _():
                hop_across(c).start()

        c = now - 2
        if 0 <= c < count:
            hop_across(c).wait_recv()

            @pl.when(is_mid)
            def _():
                hop_out(c).start()

            hop_first(c).start()
        c = now - 4
        if 0 <= c < count:
            hop_first(c).wait_recv()
            for copy in hop_second(c):
                copy.start()

    for copy in small:
        copy.start()
    for c in range(count):
        local(c).start()
    hop_pair(0).start()
    hop_pair(1).start()
    for copy in small:
        copy.wait()
    tick(0)
    tick(1)
    gain = jnp.concatenate([vec_all[b, 0:1, :] for b in range(8)], axis=1)
    shift = jnp.concatenate([vec_all[b, 1:2, :] for b in range(8)], axis=1)

    @pl.loop(0, LENGTH // 64)
    def _(i):
        rows = pl.ds(pl.multiple_of(i * 64, 64), 64)
        unit, _ = norm_parts(x_ref[rows, :].astype(jnp.float32))
        h_ref[rows, :] = (unit * gain + shift).astype(LOW)

    first = 4
    for now in range(2, first + 4):
        tick(now)
    for c in range(first):
        for copy in hop_second(c):
            copy.wait_recv()
    load = pltpu.make_async_copy(qkv_ref, wq_ref, load_sem.at[0])
    load.start()
    tick(first + 4)
    load.wait()
    width = 2 * HD
    lane_q = lax.broadcasted_iota(jnp.int32, (QB, width), 1)

    @pl.loop(0, 8)
    def _(t):
        z = t // 2
        base = z * 3 * width

        def columns(part):
            return pl.ds(pl.multiple_of(base + part * width, width), width)

        @pl.when(t % 2 == 0)
        def _():
            bias = bias_all[pl.ds(z, 1), 0:1, 0 : 3 * width][0]

            @pl.loop(0, LENGTH // QB)
            def _(i):
                rows = pl.ds(pl.multiple_of(i * QB, QB), QB)
                weights = wq_ref[:, pl.ds(pl.multiple_of(base, width), 3 * width)]
                qkv = dot_nn(h_ref[rows, :], weights) + bias
                c, s1, s2 = c_ref[rows, :], s1_ref[rows, :], s2_ref[rows, :]
                low_ref[rows, columns(0)] = turn(qkv[:, :width], c, s1, s2, 1.0).astype(LOW)
                k = turn(qkv[:, width : 2 * width], c, s1, s2, 1.0)
                v = qkv[:, 2 * width :]
                low_ref[rows, columns(1)] = k.astype(LOW)
                low_ref[rows, columns(2)] = v.astype(LOW)
                for h in range(2):
                    mine = (lane_q < HD) if h == 0 else (lane_q >= HD)
                    kh_ref[h, rows, :] = jnp.where(mine, k, 0.0).astype(LOW)
                    vh_ref[h, rows, :] = jnp.where(mine, v, 0.0).astype(LOW)

        for k in range(8):

            @pl.when(t == k)
            def _():
                tick(first + 5 + k)

        @pl.loop(0, 2)
        def _(half):
            rows = pl.ds(pl.multiple_of(((t % 2) * 2 + half) * QB, QB), QB)
            q = (low_ref[rows, columns(0)].astype(jnp.float32) * SCALE).astype(LOW)
            total = jnp.zeros((width, QB), jnp.float32)
            for h in range(2):
                s = dot_nt(kh_ref[h], q)
                peak = jnp.max(s, axis=0, keepdims=True)
                e = jnp.exp(s - peak)
                mass = jnp.sum(e, axis=0, keepdims=True)
                p = (e * (1.0 / mass)).astype(LOW)
                total += dot_tn(vh_ref[h], p)
                lse_ref[pl.ds(z, 1), h : h + 1, rows] = (peak + jnp.log(mass))[None]
            o_ref[rows, pl.ds(pl.multiple_of(z * width, width), width)] = total.T.astype(LOW)

    for now in range(first + 13, count + 4):
        tick(now)
    for c in range(count):
        for copy in hop_second(c):
            copy.wait_send()
            if c >= first:
                copy.wait_recv()
        hop_pair(c).wait_send()
        hop_first(c).wait_send()

        @pl.when(is_mid)
        def _():
            hop_across(c).wait_send()
            hop_out(c).wait_send()


def flip_place(shard, q, dc):
    target = shard
    for bit, on in ((1, dc), (2, q & 1), (4, q >> 1)):
        if on:
            target = flip(target, bit)
    return target


def gather_all(pack, vec, bias, x, tables):
    count = len(GATHER)
    rows = 8 * SHARD
    any_space = pl.BlockSpec(memory_space=pl.ANY)
    vmem = pl.BlockSpec(memory_space=pltpu.VMEM)
    width = 2 * HD
    return pl.pallas_call(
        gather_kernel,
        in_specs=[vmem] * 7,
        out_specs=[any_space] * 4 + [vmem] * 6,
        out_shape=[
            jax.ShapeDtypeStruct((rows, 1536), LOW),
            jax.ShapeDtypeStruct((rows, 512), LOW),
            jax.ShapeDtypeStruct((rows, 2048), LOW),
            jax.ShapeDtypeStruct((rows, 2048), LOW),
            jax.ShapeDtypeStruct((8,) + vec.shape, jnp.float32),
            jax.ShapeDtypeStruct((4,) + bias.shape, jnp.float32),
            jax.ShapeDtypeStruct((LENGTH, D), LOW),
            jax.ShapeDtypeStruct((LENGTH, 1536), LOW),
            jax.ShapeDtypeStruct((LENGTH, 512), LOW),
            jax.ShapeDtypeStruct((4, 2, LENGTH), jnp.float32),
        ],
        scratch_shapes=[
            pltpu.VMEM((D, 1536), LOW),
            pltpu.VMEM((2, LENGTH, width), LOW),
            pltpu.VMEM((2, LENGTH, width), LOW),
            pltpu.SemaphoreType.DMA((1,)),
            pltpu.SemaphoreType.DMA((count,)),
            pltpu.SemaphoreType.DMA((count, 6)),
            pltpu.SemaphoreType.DMA((count, 5)),
            pltpu.SemaphoreType.DMA((10,)),
            pltpu.SemaphoreType.DMA((10,)),
        ],
        compiler_params=pltpu.CompilerParams(
            collective_id=1, has_side_effects=True, vmem_limit_bytes=48 * MIB
        ),
        name="gather_attend",
    )(pack, vec, bias, x, *tables)


SUMMED = (
    (0, 0, 256, 0),
    (0, 256, 256, 1024),
    (1, 512, 256, 0),
    (1, 768, 256, 1024),
    (2, 1024, 128, 0),
    (3, 1152, 384, 0),
)
SCATTER = split([(piece, WHOLE) for piece in SUMMED[:5]] + [(SUMMED[5], HALVES)])
SUM_WIDTH = 1536


def scatter_kernel(
    down_ref, up_ref, proj_ref, low_ref, go_ref, lse_ref, c_ref, s1_ref, s2_ref, h_ref, wq_ref,
    out_ref, bias_ref, gh_ref,
    gq_ref, g_ref, kh_ref, vh_ref, gk_ref, gv_ref,
    own_ref, first_ref, second_ref, in_ref, mid_ref, near_ref, local_sem, send_sem, recv_sem,
):
    grads = (down_ref, up_ref, proj_ref, gq_ref)
    lane, shard, is_mid, pair, across, x_peer, y_peer = peers()
    barrier = pltpu.get_barrier_semaphore()
    for target in (pair, x_peer, y_peer):
        pl.semaphore_signal(barrier, inc=1, device_id=target, device_id_type=MESH)

    @pl.when(is_mid)
    def _():
        pl.semaphore_signal(barrier, inc=1, device_id=across, device_id_type=MESH)

    pl.semaphore_wait(barrier, 3 + is_mid.astype(jnp.int32))

    def source(c, block):
        (a, _, width, base), r, at, rows = SCATTER[c]
        return grads[a].at[pl.ds((r * 4 + block) * SHARD + at, rows), pl.ds(base, 4 * width)]

    def part(ref, c, block, lo, hi, each):
        (_, first, width, _), r, at, rows = SCATTER[c]
        return ref.at[
            r, pl.ds(block * SHARD + at, rows), pl.ds(first * each + lo * width, (hi - lo) * width)
        ]

    def keep(c):
        blocks = ((0, 1), (0, 2))[SCATTER[c][1]]
        return [
            pltpu.make_async_copy(source(c, block), part(own_ref, c, k, 0, 4, 4), local_sem.at[c, k])
            for k, block in enumerate(blocks)
        ]

    def hop_first(c):
        blocks, target = (((2, 3), y_peer), ((1, 3), x_peer))[SCATTER[c][1]]
        return [
            remote(
                source(c, block), part(first_ref, c, k, 0, 4, 4), send_sem.at[c, k], recv_sem.at[c, k], target
            )
            for k, block in enumerate(blocks)
        ]

    def hop_second(c):
        return remote(
            part(own_ref, c, 1, 0, 4, 4), part(second_ref, c, 0, 0, 4, 4),
            send_sem.at[c, 2], recv_sem.at[c, 2], (x_peer, y_peer)[SCATTER[c][1]],
        )

    def hop_in(c):
        return remote(
            part(own_ref, c, 0, 2, 4, 4), part(in_ref, c, 0, 0, 2, 2), send_sem.at[c, 3], recv_sem.at[c, 3], pair
        )

    def hop_across(c):
        return remote(
            part(own_ref, c, 0, 2, 4, 4), part(mid_ref, c, 0, 0, 2, 2), send_sem.at[c, 3], recv_sem.at[c, 4], across
        )

    def hop_pair(c):
        return remote(
            part(own_ref, c, 0, 1, 2, 4), part(near_ref, c, 0, 0, 1, 1), send_sem.at[c, 4], recv_sem.at[c, 5], pair
        )

    def add(dst, left, right):
        step = 16

        @pl.loop(0, dst.shape[0] // step)
        def _(i):
            at = pl.ds(pl.multiple_of(i * step, step), step)
            total = left[at, :].astype(jnp.float32) + right[at, :].astype(jnp.float32)
            dst[at, :] = total.astype(dst.dtype)

    count = len(SCATTER)
    lead = 4

    def tick(now):
        c = now
        if c < count:
            if c + lead < count:
                for copy in hop_first(c + lead):
                    copy.start()
                for copy in keep(c + lead):
                    copy.start()
            for copy in keep(c):
                copy.wait()
            for copy in hop_first(c):
                copy.wait_recv()
            mine = part(own_ref, c, 1, 0, 4, 4)
            add(mine, mine, part(first_ref, c, 1, 0, 4, 4))
            hop_second(c).start()
            mine = part(own_ref, c, 0, 0, 4, 4)
            add(mine, mine, part(first_ref, c, 0, 0, 4, 4))
        c = now - 2
        if 0 <= c < count:
            hop_second(c).wait_recv()
            mine = part(own_ref, c, 0, 0, 4, 4)
            add(mine, mine, part(second_ref, c, 0, 0, 4, 4))

            @pl.when(jnp.logical_not(is_mid))
            def _():
                hop_in(c).start()

        c = now - 3
        if 0 <= c < count:

            @pl.when(is_mid)
            def _():
                hop_in(c).wait_recv()
                far = part(own_ref, c, 0, 2, 4, 4)
                add(far, far, part(in_ref, c, 0, 0, 2, 2))
                hop_across(c).start()

        c = now - 4
        if 0 <= c < count:

            @pl.when(is_mid)
            def _():
                hop_across(c).wait_recv()
                near = part(own_ref, c, 0, 0, 2, 4)
                add(near, near, part(mid_ref, c, 0, 0, 2, 2))

            hop_pair(c).start()
        c = now - 5
        if 0 <= c < count:
            hop_pair(c).wait_recv()
            add(part(out_ref, c, 0, 0, 1, 1), part(own_ref, c, 0, 0, 1, 4), part(near_ref, c, 0, 0, 1, 1))

    for c in range(lead):
        for copy in hop_first(c):
            copy.start()
        for copy in keep(c):
            copy.start()

    width = 2 * HD
    lane_q = lax.broadcasted_iota(jnp.int32, (QB, width), 1)

    @pl.loop(0, 8)
    def _(t):
        z = t // 2
        base = z * 3 * width

        def columns(part_index):
            return pl.ds(pl.multiple_of(base + part_index * width, width), width)

        @pl.when(t % 2 == 0)
        def _():
            @pl.loop(0, LENGTH // QB)
            def _(i):
                rows = pl.ds(pl.multiple_of(i * QB, QB), QB)
                k = low_ref[rows, columns(1)].astype(jnp.float32)
                v = low_ref[rows, columns(2)].astype(jnp.float32)
                for h in range(2):
                    mine = (lane_q < HD) if h == 0 else (lane_q >= HD)
                    kh_ref[h, rows, :] = jnp.where(mine, k, 0.0).astype(LOW)
                    vh_ref[h, rows, :] = jnp.where(mine, v, 0.0).astype(LOW)

            gk_ref[...] = jnp.zeros_like(gk_ref)
            gv_ref[...] = jnp.zeros_like(gv_ref)

        for k in range(2, 8):

            @pl.when(t == k)
            def _():
                tick(k - 2)

        @pl.loop(0, 2)
        def _(half):
            rows = pl.ds(pl.multiple_of(((t % 2) * 2 + half) * QB, QB), QB)
            q = low_ref[rows, columns(0)].astype(jnp.float32) * SCALE
            go = go_ref[rows, pl.ds(pl.multiple_of(z * width, width), width)].astype(jnp.float32)
            total = jnp.zeros((width, QB), jnp.float32)
            for h in range(2):
                mine = (lane_q < HD) if h == 0 else (lane_q >= HD)
                qh = jnp.where(mine, q, 0.0).astype(LOW)
                gh = jnp.where(mine, go, 0.0).astype(LOW)
                p = jnp.exp(dot_nt(kh_ref[h], qh) - lse_ref[pl.ds(z, 1), h : h + 1, rows][0])
                dp = dot_nt(vh_ref[h], gh)
                pd = jnp.sum(p * dp, axis=0, keepdims=True)
                ds = (p * (dp - pd)).astype(LOW)
                gv_ref[...] += dot_nn(p.astype(LOW), gh)
                gk_ref[...] += dot_nn(ds, qh)
                total += dot_tn(kh_ref[h], ds)
            gq = turn(total.T * SCALE, c_ref[rows, :], s1_ref[rows, :], s2_ref[rows, :], -1.0)
            g_ref[rows, :width] = gq.astype(LOW)

        @pl.when(t % 2 == 1)
        def _():
            wide = pl.ds(pl.multiple_of(base, width), 3 * width)
            gk = turn(gk_ref[...], c_ref[...], s1_ref[...], s2_ref[...], -1.0)
            g_ref[:, width : 2 * width] = gk.astype(LOW)
            g_ref[:, 2 * width :] = gv_ref[...].astype(LOW)
            bias_ref[:, wide] = jnp.sum(g_ref[...].astype(jnp.float32), axis=0, keepdims=True)

            @pl.loop(0, D // QB)
            def _(i):
                some = pl.ds(pl.multiple_of(i * QB, QB), QB)
                gq_ref[some, wide] = dot_tn(h_ref[:, some], g_ref[...]).astype(LOW)
                product = dot_nt(g_ref[some, :], wq_ref[:, wide])

                @pl.when(z == 0)
                def _():
                    gh_ref[some, :] = product

                @pl.when(z > 0)
                def _():
                    gh_ref[some, :] += product

    for now in range(6, count + 5):
        tick(now)
    for c in range(count):
        for copy in hop_first(c):
            copy.wait_send()
        hop_second(c).wait_send()
        hop_pair(c).wait_send()

        @pl.when(is_mid)
        def _():
            hop_across(c).wait_send()

        @pl.when(jnp.logical_not(is_mid))
        def _():
            hop_in(c).wait_send()


def scatter_all(grad_down, grad_up, grad_proj, low, go, lse, tables, normed, weight_qkv):
    count = len(SCATTER)
    width = SUM_WIDTH
    vmem = pl.BlockSpec(memory_space=pltpu.VMEM)
    any_space = pl.BlockSpec(memory_space=pl.ANY)
    pair_width = 2 * HD
    return pl.pallas_call(
        scatter_kernel,
        in_specs=[any_space] * 3 + [vmem] * 8,
        out_specs=[vmem] * 3,
        out_shape=[
            jax.ShapeDtypeStruct((2, SHARD, width), jnp.float32),
            jax.ShapeDtypeStruct((1, 1536), jnp.float32),
            jax.ShapeDtypeStruct((LENGTH, D), jnp.float32),
        ],
        scratch_shapes=[
            pltpu.VMEM((D, 1536), LOW),
            pltpu.VMEM((LENGTH, 3 * pair_width), LOW),
            pltpu.VMEM((2, LENGTH, pair_width), LOW),
            pltpu.VMEM((2, LENGTH, pair_width), LOW),
            pltpu.VMEM((LENGTH, pair_width), jnp.float32),
            pltpu.VMEM((LENGTH, pair_width), jnp.float32),
            pltpu.VMEM((2, 2 * SHARD, 4 * width), LOW),
            pltpu.VMEM((2, 2 * SHARD, 4 * width), LOW),
            pltpu.VMEM((2, SHARD, 4 * width), LOW),
            pltpu.VMEM((2, SHARD, 2 * width), LOW),
            pltpu.VMEM((2, SHARD, 2 * width), LOW),
            pltpu.VMEM((2, SHARD, width), LOW),
            pltpu.SemaphoreType.DMA((count, 2)),
            pltpu.SemaphoreType.DMA((count, 5)),
            pltpu.SemaphoreType.DMA((count, 6)),
        ],
        compiler_params=pltpu.CompilerParams(
            collective_id=2, has_side_effects=True, vmem_limit_bytes=60 * MIB
        ),
        name="scatter_attend_back",
    )(grad_down, grad_up, grad_proj, low, go, lse, *tables, normed, weight_qkv)


COUNTS = (3 * D, D, FF, FF)
BLOCKS = (6, 2, 8, 8)


def offsets():
    return [(z * 8 + q * 2 + dc, q, dc, z) for z in range(4) for q in range(4) for dc in range(2)]


def tune_kernel(
    sums_ref, vec_ref, db_ref, wq_ref, wp_ref, wu_ref, wd_ref, vw_ref, vs_ref, rows_ref,
    cq_ref, cp_ref, cu_ref, cd_ref, bq_ref, bu_ref, bqs_ref, bus_ref,
    gq_out, gp_out, gu_out, gd_out, nq_out, np_out, nu_out, nd_out, vec_out, rows_out,
    cq_out, cp_out, cu_out, cd_out, bq_out, bqs_out, bqn_out, bu_out, bus_out, bun_out, rms_out,
    gq, vec_send, vec_recv, db_recv, lane_send, lane_recv, col_send, col_recv, all_send, all_recv,
    core_send, core_done, a_send, a_recv, b_send, b_recv, c_send, c_recv,
):
    lane = lax.axis_index("tensor")
    shard = lax.axis_index("fsdp")
    core = shard % 2
    is_mid = (lane == 1) | (lane == 2)
    z_of = [lane, flip(lane, 1), 3 - lane, (lane + 2) % 4]

    def device(q, dc, z):
        target = {}
        if q or dc:
            target["fsdp"] = flip_place(shard, q, dc)
        if z:
            target["tensor"] = z_of[z]
        return target

    others = [entry for entry in offsets() if entry[0]]
    meet([device(q, dc, z) for _, q, dc, z in others])
    shard_peers = [(slot, q, dc) for slot, q, dc, z in others if z == 0]

    def core_copies():
        give = 1 - core
        hq = pl.ds(pl.multiple_of(core * 128, 128), 128)
        hf = pl.ds(pl.multiple_of(core * 512, 512), 512)
        pairs = [(sums_ref.at[give, :, pl.ds(1152 + j * 128, 128)], gq.at[j, :, hq]) for j in range(3)]
        pairs.append((sums_ref.at[give, :, pl.ds(1024, 128)], gp_out.at[:, hq]))
        pairs.append((sums_ref.at[give, :, pl.ds(512, 512)], gu_out.at[:, hf]))
        pairs.append((sums_ref.at[give, :, pl.ds(0, 512)], gd_out.at[:, hf]))
        return [
            remote(src, dst, core_send.at[i], core_done.at[i], {"fsdp": flip(shard, 1)})
            for i, (src, dst) in enumerate(pairs)
        ]

    for copy in core_copies():
        copy.start()

    def round_a():
        copies = [
            remote(vec_send.at[slot], vec_recv.at[slot], a_send.at[slot], a_recv.at[slot], device(q, dc, 0))
            for slot, q, dc in shard_peers
        ]
        for z in range(1, 4):
            position = 1 if z == 1 else (3 - is_mid.astype(jnp.int32) if z == 2 else 2 + is_mid.astype(jnp.int32))
            copies.append(
                remote(db_ref.at[position], db_recv.at[z], a_send.at[7 + z], a_recv.at[7 + z], device(0, 0, z))
            )
        return copies

    for slot in range(8):
        q, dc = slot // 2, slot % 2
        block = (core + dc - 2 * core * dc) * 4 + q
        at = pl.ds(pl.multiple_of(block * 128, 128), 128)
        if slot == 0:
            vec_recv[0] = vec_ref[:, at]
        else:
            vec_send[slot] = vec_ref[:, at]
    for copy in round_a():
        copy.start()
    db_recv[0] = db_ref[0]

    mine_q = pl.ds(pl.multiple_of(core * 128, 128), 128)
    mine_f = pl.ds(pl.multiple_of(core * 512, 512), 512)
    for j in range(3):
        gq[j, :, mine_q] = sums_ref[core, :, 1152 + j * 128 : 1280 + j * 128]
    gp_out[:, mine_q] = sums_ref[core, :, 1024:1152]
    gu_out[:, mine_f] = sums_ref[core, :, 512:1024]
    gd_out[:, mine_f] = sums_ref[core, :, 0:512]

    def weight_block(m, i):
        if m == 0:
            return wq_ref[:, i // 2, (i % 2) * 128 : (i % 2) * 128 + 128]
        return (None, wp_ref, wu_ref, wd_ref)[m][:, i * 128 : (i + 1) * 128]

    def grad_block(m, i):
        if m == 0:
            return gq[i // 2, :, (i % 2) * 128 : (i % 2) * 128 + 128]
        return (None, gp_out, gu_out, gd_out)[m][:, i * 128 : (i + 1) * 128]

    zero = jnp.zeros((128, 128), jnp.float32)

    def total_of(v):
        return jnp.sum(jnp.sum(v, axis=0, keepdims=True), axis=1, keepdims=True)

    weight_squares = []
    for m in range(4):
        acc = zero
        for i in range(BLOCKS[m]):
            w = weight_block(m, i)
            acc += w * w
        weight_squares.append(total_of(acc))

    for copy in core_copies():
        copy.wait()
    for j in range(3):
        gq_out[:, j, :] = gq[j]
    lane_send[...] = jnp.zeros_like(lane_send)
    row = 0
    for m in range(4):
        acc = zero
        for i in range(BLOCKS[m]):
            g = grad_block(m, i)
            square = g * g
            acc += square
            col_send[row : row + 1, :] = jnp.sum(square, axis=0, keepdims=True)
            row += 1
        lane_send[8 + m : 9 + m, :] = jnp.sum(acc.T, axis=0, keepdims=True)

    for copy in round_a():
        copy.wait()
    vec_sum = vec_recv[0]
    for slot in range(1, 8):
        vec_sum += vec_recv[slot]
    lane_send[0:8, :] = vec_sum
    col_send[24:32, :] = db_recv[0] + db_recv[1] + db_recv[2] + db_recv[3]

    def round_b():
        copies = [
            remote(lane_send, lane_recv.at[z], b_send.at[z], b_recv.at[z], device(0, 0, z)) for z in range(1, 4)
        ]
        copies += [
            remote(col_send, col_recv.at[slot], b_send.at[3 + slot], b_recv.at[3 + slot], device(q, dc, 0))
            for slot, q, dc in shard_peers
        ]
        return copies

    for copy in round_b():
        copy.start()
    for copy in round_b():
        copy.wait()
    lane_total = lane_send[...] + lane_recv[1] + lane_recv[2] + lane_recv[3]
    same = col_send[...] + col_recv[2] + col_recv[4] + col_recv[6]
    cross = col_recv[1] + col_recv[3] + col_recv[5] + col_recv[7]
    col_total = same[0:24] + cross[0:24]
    low_half = jnp.where(core == 0, same[24:32], cross[24:32])
    high_half = jnp.where(core == 0, cross[24:32], same[24:32])
    bq_out[:, 0:128] = low_half[0:3]
    bq_out[:, 128:256] = high_half[0:3]
    bu_out[0:4, :] = low_half[3:7]
    bu_out[4:8, :] = high_half[3:7]

    def stepped(g, state):
        new = DECAY * state + (1.0 - DECAY) * (g * g + TINY)
        return new, g * lax.rsqrt(new)

    gvec = lane_total[0:8]
    vs_new, v_dir = stepped(gvec, vs_ref[...])
    bqs_new, bq_dir = stepped(bq_out[...], bqs_ref[...])
    bus_new, bu_dir = stepped(bu_out[...], bus_ref[...])
    bqs_out[...] = bqs_new
    bus_out[...] = bus_new
    vec_out[0:8, :] = gvec
    vec_out[8:16, :] = vs_new

    row_counts = jnp.where(
        lax.broadcasted_iota(jnp.int32, (4, 128), 0) == 0,
        float(COUNTS[0]),
        jnp.where(lax.broadcasted_iota(jnp.int32, (4, 128), 0) == 1, float(COUNTS[1]), float(COUNTS[2])),
    )
    rows_new = DECAY * rows_ref[...] + (1.0 - DECAY) * (lane_total[8:12] / row_counts + TINY)
    rows_out[...] = rows_new
    inverse_rows = lax.rsqrt(rows_new)
    spots = lax.broadcasted_iota(jnp.int32, (8, 128), 1)
    message = jnp.zeros((8, 128), jnp.float32)
    sums = []
    inverse_cols = []
    tall = []
    row = 0
    for m in range(4):
        tall.append(jnp.broadcast_to(inverse_rows[m : m + 1], (128, 128)).T)
        acc = zero
        for i in range(BLOCKS[m]):
            if m == 0:
                old = cq_ref[i // 2 : i // 2 + 1, (i % 2) * 128 : (i % 2) * 128 + 128]
            else:
                old = (None, cp_ref, cu_ref, cd_ref)[m][i : i + 1, :]
            new = DECAY * old + (1.0 - DECAY) * (col_total[row : row + 1] / D + TINY)
            if m == 0:
                cq_out[i // 2 : i // 2 + 1, (i % 2) * 128 : (i % 2) * 128 + 128] = new
            else:
                (None, cp_out, cu_out, cd_out)[m][i : i + 1, :] = new
            inverse_cols.append(lax.rsqrt(new))
            step = grad_block(m, i) * tall[m] * inverse_cols[row]
            acc += step * step
            row += 1
        sums.append(total_of(acc))
    terms = sums
    terms = terms + [0.25 * total_of(rows_new[m : m + 1]) for m in range(4)]
    terms = terms + weight_squares
    vw = vw_ref[...]
    v_squares = jnp.sum(v_dir * v_dir, axis=1, keepdims=True)
    w_squares = jnp.sum(vw * vw, axis=1, keepdims=True)
    terms = terms + [0.25 * v_squares[i : i + 1] for i in range(6)]
    terms = terms + [0.25 * w_squares[i : i + 1] for i in range(6)]
    for value in (bq_dir, bu_dir, bq_ref[...], bu_ref[...]):
        terms = terms + [0.125 * total_of(value * value)]
    for i, term in enumerate(terms):
        message = jnp.where(spots == i, term, message)
    all_send[...] = message

    def round_c():
        return [
            remote(all_send, all_recv.at[slot], c_send.at[slot], c_recv.at[slot], device(q, dc, z))
            for slot, q, dc, z in others
        ]

    for copy in round_c():
        copy.start()
    for copy in round_c():
        copy.wait()
    grand = message
    for slot, _, _, _ in others:
        grand += all_recv[slot]
    line = grand[0:1]
    spot = spots[0:1]

    def pick(i):
        return jnp.sum(jnp.where(spot == i, line, 0.0), axis=1, keepdims=True)

    rms_line = jnp.zeros((1, 128), jnp.float32)
    row = 0
    for m in range(4):
        size = float(D * COUNTS[m])
        mean_rows = pick(4 + m) / D
        rms = jnp.sqrt(pick(m) * mean_rows / size)
        scale = jnp.sqrt(pick(8 + m) / size)
        factor = RATE * scale * jnp.sqrt(mean_rows) / jnp.maximum(1.0, rms / CLIP_LEVEL)
        rms_line = jnp.where(spot == m, rms, rms_line)
        for i in range(BLOCKS[m]):
            new = weight_block(m, i) - factor * (grad_block(m, i) * tall[m] * inverse_cols[row])
            if m == 0:
                nq_out[:, i // 2, (i % 2) * 128 : (i % 2) * 128 + 128] = new
            else:
                (None, np_out, nu_out, nd_out)[m][:, i * 128 : (i + 1) * 128] = new
            row += 1
    rms_out[...] = rms_line
    for i in range(6):
        spread = jnp.sqrt(pick(12 + i) / D)
        factor = RATE * jnp.sqrt(pick(18 + i) / D) / jnp.maximum(1.0, spread / CLIP_LEVEL)
        vec_out[16 + i : 17 + i, :] = vw[i : i + 1] - factor * v_dir[i : i + 1]
    vec_out[22:24, :] = jnp.zeros((2, 128), jnp.float32)
    for direction, weight, out, at, size in (
        (bq_dir, bq_ref, bqn_out, 24, 3 * D),
        (bu_dir, bu_ref, bun_out, 25, FF),
    ):
        spread = jnp.sqrt(pick(at) / size)
        factor = RATE * jnp.sqrt(pick(at + 2) / size) / jnp.maximum(1.0, spread / CLIP_LEVEL)
        out[...] = weight[...] - factor * direction


def tune_all(sums, vec_part, db_part, params, stats, states):
    qkv_weight, qkv_bias, proj_weight, fc1_weight, fc1_bias, fc2_weight, vectors = params
    row_state, qkv_cols, proj_cols, fc1_cols, fc2_cols = stats
    vector_state, qkv_bias_state, fc1_bias_state = states
    pad = ((0, 2), (0, 0))

    def dense(v):
        return v.reshape(v.shape[0] // 128, 128)

    operands = (
        sums, vec_part, db_part, qkv_weight, proj_weight, fc1_weight, fc2_weight,
        jnp.pad(vectors.T, pad), jnp.pad(vector_state.T, pad, constant_values=1.0), row_state,
        qkv_cols, dense(proj_cols), dense(fc1_cols), dense(fc2_cols),
        qkv_bias, dense(fc1_bias), qkv_bias_state, dense(fc1_bias_state),
    )
    vmem = pl.BlockSpec(memory_space=pltpu.VMEM)
    shapes = [
        (128, 3, 256), (128, 256), (128, 1024), (128, 1024),
        (128, 3, 256), (128, 256), (128, 1024), (128, 1024),
        (24, 128), (4, 128), (3, 256), (2, 128), (8, 128), (8, 128),
        (3, 256), (3, 256), (3, 256), (8, 128), (8, 128), (8, 128), (1, 128),
    ]
    f32 = jnp.float32
    (
        gq, gp, gu, gd, nq, np_, nu, nd, vec, rows, cq, cp, cu, cd, bq, bqs, bqn, bu, bus, bun, rms
    ) = pl.pallas_call(
        tune_kernel,
        in_specs=[vmem] * len(operands),
        out_specs=[vmem] * len(shapes),
        out_shape=[jax.ShapeDtypeStruct(shape, f32) for shape in shapes],
        scratch_shapes=[
            pltpu.VMEM((3, 128, 256), f32),
            pltpu.VMEM((8, 8, 128), f32),
            pltpu.VMEM((8, 8, 128), f32),
            pltpu.VMEM((4, 8, 128), f32),
            pltpu.VMEM((16, 128), f32),
            pltpu.VMEM((4, 16, 128), f32),
            pltpu.VMEM((32, 128), f32),
            pltpu.VMEM((8, 32, 128), f32),
            pltpu.VMEM((8, 128), f32),
            pltpu.VMEM((32, 8, 128), f32),
            pltpu.SemaphoreType.DMA((6,)),
            pltpu.SemaphoreType.DMA((6,)),
            pltpu.SemaphoreType.DMA((11,)),
            pltpu.SemaphoreType.DMA((11,)),
            pltpu.SemaphoreType.DMA((11,)),
            pltpu.SemaphoreType.DMA((11,)),
            pltpu.SemaphoreType.DMA((32,)),
            pltpu.SemaphoreType.DMA((32,)),
        ],
        compiler_params=pltpu.CompilerParams(collective_id=4, has_side_effects=True, vmem_limit_bytes=40 * 1024 * 1024),
        name="tune_all",
    )(*operands)
    vec = vec.T
    return (
        gq, bq, gp, gu, bu.reshape(1024), gd, vec[:, 0:6], rows,
        cq, cp.reshape(256), cu.reshape(1024), cd.reshape(1024),
        vec[:, 8:14], bqs, bus.reshape(1024),
        nq, bqn, np_, nu, bun.reshape(1024), nd, vec[:, 16:22], rms[0, 0:4],
    )


def by_core(core, mine, theirs):
    return jnp.where(core == 0, mine, theirs), jnp.where(core == 0, theirs, mine)


def gelu_parts(u):
    cdf = 0.5 * (1.0 + lax.erf(u * (0.5**0.5)))
    density = jnp.exp(-0.5 * u * u) * ((2.0 * jnp.pi) ** -0.5)
    return u * cdf, cdf + u * density


def norm_parts(values):
    center = values - jnp.mean(values, axis=-1, keepdims=True)
    scale = lax.rsqrt(jnp.mean(center * center, axis=-1, keepdims=True) + NORM_EPS)
    return center * scale, scale


def norm_back(grad, unit, scale, gain):
    c = grad * gain
    return scale * (
        c
        - jnp.mean(c, axis=-1, keepdims=True)
        - unit * jnp.mean(c * unit, axis=-1, keepdims=True)
    )


def on_chip(
    tokens,
    cotangent,
    qkv_weight,
    qkv_bias,
    proj_weight,
    fc1_weight,
    fc1_bias,
    fc2_weight,
    vectors,
    row_state,
    qkv_cols,
    proj_cols,
    fc1_cols,
    fc2_cols,
    vector_state,
    qkv_bias_state,
    fc1_bias_state,
):
    shard = lax.axis_index("fsdp")
    lane = lax.axis_index("tensor")
    core = shard % 2
    place = shard // 2
    rows = tokens.shape[0]
    head_width = qkv_weight.shape[2]
    hidden_width = fc1_weight.shape[1]
    hw, fw = head_width // 2, hidden_width // 2
    shard_rows = qkv_weight.shape[0]
    swap_tokens = []
    for k in range(4):
        for p in range(2):
            a, b = (2 * k + 1) * 4 + 2 * p, 2 * k * 4 + 2 * p + 1
            swap_tokens += [(a, b), (b, a)]
    moved = (core ^ (lane & 1)) == 1

    def swap(v):
        return jnp.where(moved, lax.ppermute(v, ("fsdp", "tensor"), swap_tokens), v)

    def to_local(v):
        parts = []
        for r in range(2):
            for q in range(4):
                parts.append(
                    lax.dynamic_slice_in_dim(v, ((place ^ q) * 2 + r) * shard_rows, shard_rows, 1)
                )
        return jnp.concatenate(parts, axis=1)

    def to_global(v):
        parts = []
        for q in range(4):
            for r in range(2):
                parts.append(
                    lax.dynamic_slice_in_dim(v, (r * 4 + (place ^ q)) * shard_rows, shard_rows, 1)
                )
        return jnp.concatenate(parts, axis=1)

    def both_halves(v):
        return jnp.concatenate([v, lax.ppermute(v, "fsdp", CORE_SWAP)], axis=0)

    def core_sum(left, right_t):
        other = times_transposed(left[rows:], right_t)
        other = lax.ppermute(other, "fsdp", CORE_SWAP)
        return times_transposed(left[:rows], right_t) + other

    def half_columns(w, width, which):
        return lax.dynamic_slice_in_dim(w, which * width, width, w.ndim - 1)

    def pack(which):
        return jnp.concatenate(
            [
                half_columns(qkv_weight, hw, which).reshape(shard_rows, 3 * hw),
                half_columns(proj_weight, hw, which),
                half_columns(fc1_weight, fw, which),
                half_columns(fc2_weight, fw, which),
            ],
            axis=1,
        ).astype(LOW)

    theirs = lax.ppermute(pack(1 - core), "fsdp", CORE_SWAP)
    packs = jnp.stack(by_core(core, pack(core), theirs))
    vec = jnp.pad(vectors.astype(LOW).astype(jnp.float32).T, ((0, 2), (0, 0)))
    bias = jnp.concatenate(
        [
            half_columns(qkv_bias, hw, core).reshape(3 * hw),
            lax.dynamic_slice_in_dim(fc1_bias, core * fw, fw, 0),
        ]
    )
    bias = jnp.broadcast_to(
        lax.optimization_barrier(bias.astype(LOW)).astype(jnp.float32), (8, 3 * hw + fw)
    )
    tables = chip_tables(core)
    tokens_local = to_local(swap(tokens))
    (
        weight_qkv, weight_proj, weight_up, weight_down, vec_all, bias_all, normed_one, low, mixed, lse
    ) = gather_all(packs, vec, bias, both_halves(tokens_local), tables)
    vector_rows = vec_all.transpose(1, 0, 2).reshape(8, D)
    gain_one, shift_one, proj_shift, gain_two, shift_two, down_shift = [
        vector_rows[i : i + 1] for i in range(6)
    ]
    bias_rows = bias_all[:, 0]
    bias_up = (
        bias_rows[:, 3 * hw :].reshape(4, 2, fw // 2).transpose(1, 0, 2).reshape(1, 4 * fw)
    )

    inputs = tokens_local.astype(jnp.float32)
    upstream_low = to_local(swap(cotangent))
    grad_out_all = both_halves(upstream_low)
    unit_one, scale_one = norm_parts(inputs)
    middle = inputs + core_sum(mixed, weight_proj) + proj_shift
    unit_two, scale_two = norm_parts(middle)
    normed_two = both_halves((unit_two * gain_two + shift_two).astype(LOW))
    hidden = jnp.dot(normed_two, weight_up, preferred_element_type=jnp.float32) + bias_up
    active, slope = gelu_parts(hidden)
    active = active.astype(LOW)
    grad_down = contract_rows(grad_out_all, active).astype(LOW)
    layer_local = middle + core_sum(active, weight_down) + down_shift
    grad_active = jnp.dot(grad_out_all, weight_down, preferred_element_type=jnp.float32)
    grad_hidden = (grad_active * slope).astype(LOW)
    grad_up = contract_rows(normed_two, grad_hidden).astype(LOW)
    grad_bias_up = jnp.sum(grad_hidden.astype(jnp.float32), axis=0)
    grad_normed_two = core_sum(grad_hidden, weight_up)
    upstream = upstream_low.astype(jnp.float32)
    grad_middle = upstream + norm_back(grad_normed_two, unit_two, scale_two, gain_two)
    grad_branch = grad_middle.astype(LOW)
    grad_branch_all = both_halves(grad_branch)
    grad_proj = contract_rows(grad_branch_all, mixed).astype(LOW)
    grad_mixed = jnp.dot(
        grad_branch_all, weight_proj, preferred_element_type=jnp.float32
    ).astype(LOW)
    sums, grad_bias_qkv, partial_one = scatter_all(
        grad_down, grad_up, grad_proj, low, grad_mixed, lse, tables, normed_one, weight_qkv
    )
    grad_normed_one = partial_one[:rows] + lax.ppermute(partial_one[rows:], "fsdp", CORE_SWAP)
    input_local = grad_middle + norm_back(grad_normed_one, unit_one, scale_one, gain_one)
    layer_out = to_global(swap(layer_local))
    input_grad = to_global(swap(input_local))

    vec_part = jnp.concatenate(
        [
            jnp.sum(grad_normed_one * unit_one, axis=0, keepdims=True),
            jnp.sum(grad_normed_one, axis=0, keepdims=True),
            jnp.sum(grad_branch.astype(jnp.float32), axis=0, keepdims=True),
            jnp.sum(grad_normed_two * unit_two, axis=0, keepdims=True),
            jnp.sum(grad_normed_two, axis=0, keepdims=True),
            jnp.sum(upstream, axis=0, keepdims=True),
            jnp.zeros((2, D), jnp.float32),
        ]
    )
    db_part = jnp.concatenate(
        [
            grad_bias_qkv.reshape(4, 3, hw),
            grad_bias_up.reshape(2, 4, 2, hw).transpose(1, 0, 2, 3).reshape(4, 4, hw),
            jnp.zeros((4, 1, hw), jnp.float32),
        ],
        axis=1,
    )
    return (
        layer_out,
        input_grad,
        *tune_all(
            sums,
            vec_part,
            db_part,
            (qkv_weight, qkv_bias, proj_weight, fc1_weight, fc1_bias, fc2_weight, vectors),
            (row_state, qkv_cols, proj_cols, fc1_cols, fc2_cols),
            (vector_state, qkv_bias_state, fc1_bias_state),
        ),
    )


def solution(mesh):
    chips = mesh.shape["fsdp"] == 8 and mesh.shape["tensor"] == 4
    return jax.shard_map(
        on_chip if chips else on_device,
        mesh=mesh,
        in_specs=(
            P(("fsdp", "tensor"), None),
            P(("fsdp", "tensor"), None),
            P("fsdp", None, "tensor"),
            P(None, "tensor"),
            P("fsdp", "tensor"),
            P("fsdp", "tensor"),
            P("tensor"),
            P("fsdp", "tensor"),
            P("fsdp", None),
            P(None, "fsdp"),
            P(None, "tensor"),
            P("tensor"),
            P("tensor"),
            P("tensor"),
            P("fsdp", None),
            P(None, "tensor"),
            P("tensor"),
        ),
        out_specs=(
            P(("fsdp", "tensor"), None),
            P(("fsdp", "tensor"), None),
            P("fsdp", None, "tensor"),
            P(None, "tensor"),
            P("fsdp", "tensor"),
            P("fsdp", "tensor"),
            P("tensor"),
            P("fsdp", "tensor"),
            P("fsdp", None),
            P(None, "fsdp"),
            P(None, "tensor"),
            P("tensor"),
            P("tensor"),
            P("tensor"),
            P("fsdp", None),
            P(None, "tensor"),
            P("tensor"),
            P("fsdp", None, "tensor"),
            P(None, "tensor"),
            P("fsdp", "tensor"),
            P("fsdp", "tensor"),
            P("tensor"),
            P("fsdp", "tensor"),
            P("fsdp", None),
            P(),
        ),
        check_vma=False,
    )
```

```python
import math

import jax
import jax.numpy as jnp
from jax import lax
from jax.experimental import pallas as pl
from jax.experimental.pallas import tpu as pltpu
from jax.sharding import PartitionSpec as P

D = 1024
HD = 64
FF = 4096
GT = 4
GH = 16
GW = 16


NORM_EPS = 1e-06
DECAY = 0.5
CLIP_LEVEL = 1.0
RATE = 0.3
TINY = 1e-30
BASE = 10000.0


def layer_norm(values, gain_row, shift_row):
    center = values - jnp.mean(values, axis=-1, keepdims=True)
    variance = jnp.mean(center * center, axis=-1, keepdims=True)
    return center * lax.rsqrt(variance + NORM_EPS) * gain_row + shift_row


def exact_gelu(values):
    return jax.nn.gelu(values, approximate=False)


def rope_tables(length, half_width):
    token_index = jnp.arange(length, dtype=jnp.int32)
    coordinates = jnp.stack(
        [token_index // (GH * GW), token_index // GW % GH, token_index % GW], axis=1
    ).astype(jnp.float32)
    frequency = BASE ** (-jnp.arange(half_width, dtype=jnp.float32) / half_width)
    angles = coordinates[:, :, None] * frequency[None, None, :]
    return (jnp.cos(angles), jnp.sin(angles))


def rotate(values, cosine_table, sine_table):
    half_width = cosine_table.shape[-1]
    rotated_width = 6 * half_width
    leading = values.shape[:-1]
    pair_rows = values[..., :rotated_width].reshape(leading + (3, 2, half_width))
    first_half = pair_rows[..., 0, :]
    second_half = pair_rows[..., 1, :]
    cosine_wide = cosine_table[:, None]
    sine_wide = sine_table[:, None]
    turned = jnp.stack(
        [
            first_half * cosine_wide - second_half * sine_wide,
            second_half * cosine_wide + first_half * sine_wide,
        ],
        axis=-2,
    )
    return jnp.concatenate(
        [turned.reshape(leading + (rotated_width,)), values[..., rotated_width:]], axis=-1
    )


def contract_rows(left, right):
    return lax.dot_general(
        left, right, (((0,), (0,)), ((), ())), preferred_element_type=jnp.float32
    )


def times_transposed(left, right):
    return lax.dot_general(
        left, right, (((1,), (1,)), ((), ())), preferred_element_type=jnp.float32
    )


def forward_block(query_rows, key_rows, value_rows):
    score_scale = query_rows.shape[-1] ** (-0.5)
    scores = (
        jnp.einsum("qhd,khd->hqk", query_rows, key_rows, preferred_element_type=jnp.float32)
        * score_scale
    )
    row_peak = jnp.max(scores, axis=-1, keepdims=True)
    raised = jnp.exp(scores - row_peak)
    totals = jnp.sum(raised, axis=-1, keepdims=True)
    attention = (raised / totals).astype(jnp.bfloat16)
    mixed_rows = jnp.einsum(
        "hqk,khd->qhd", attention, value_rows, preferred_element_type=jnp.float32
    )
    return (mixed_rows, (row_peak + jnp.log(totals))[..., 0])


def backward_block(running, block_item, key_rows, value_rows):
    query_rows, log_totals, grad_mixed = block_item
    score_scale = query_rows.shape[-1] ** (-0.5)
    scores = (
        jnp.einsum("qhd,khd->hqk", query_rows, key_rows, preferred_element_type=jnp.float32)
        * score_scale
    )
    attention = jnp.exp(scores - log_totals[..., None])
    grad_attention = jnp.einsum(
        "qhd,khd->hqk", grad_mixed, value_rows, preferred_element_type=jnp.float32
    )
    grad_scores = attention * (
        grad_attention - jnp.sum(attention * grad_attention, axis=-1, keepdims=True)
    )
    grad_low = grad_scores.astype(jnp.bfloat16)
    grad_queries = (
        jnp.einsum("hqk,khd->qhd", grad_low, key_rows, preferred_element_type=jnp.float32)
        * score_scale
    )
    key_total = (
        running[0]
        + jnp.einsum("hqk,qhd->khd", grad_low, query_rows, preferred_element_type=jnp.float32)
        * score_scale
    )
    value_total = running[1] + jnp.einsum(
        "hqk,qhd->khd",
        attention.astype(jnp.bfloat16),
        grad_mixed,
        preferred_element_type=jnp.float32,
    )
    return ((key_total, value_total), grad_queries)


def on_device(
    tokens,
    cotangent,
    qkv_weight,
    qkv_bias,
    proj_weight,
    fc1_weight,
    fc1_bias,
    fc2_weight,
    vectors,
    row_state,
    qkv_cols,
    proj_cols,
    fc1_cols,
    fc2_cols,
    vector_state,
    qkv_bias_state,
    fc1_bias_state,
):
    low_type = jnp.bfloat16
    lane_count = lax.axis_size("tensor")
    local_rows = tokens.shape[0]
    group_rows = local_rows * lane_count
    length = GT * GH * GW
    clip_count = group_rows // length
    block_rows = min(512, length)
    block_count = length // block_rows
    head_width = qkv_weight.shape[2]
    head_count = head_width // HD
    hidden_width = fc1_weight.shape[1]
    shard_rows = qkv_weight.shape[0]
    cosine_table, sine_table = rope_tables(length, HD // 3 // 2)
    weight_qkv, weight_proj, weight_up, weight_down, vector_low = (
        lax.all_gather(qkv_weight.astype(low_type), "fsdp", axis=0, tiled=True),
        lax.all_gather(proj_weight.astype(low_type), "fsdp", axis=0, tiled=True),
        lax.all_gather(fc1_weight.astype(low_type), "fsdp", axis=0, tiled=True),
        lax.all_gather(fc2_weight.astype(low_type), "fsdp", axis=0, tiled=True),
        lax.all_gather(vectors.astype(low_type), "fsdp", axis=0, tiled=True),
    )
    weight_qkv = weight_qkv.reshape(D, 3 * head_width)
    vector_full = vector_low.astype(jnp.float32)
    gain_one = vector_full[:, 0]
    shift_one = vector_full[:, 1]
    proj_shift = vector_full[:, 2]
    gain_two = vector_full[:, 3]
    shift_two = vector_full[:, 4]
    down_shift = vector_full[:, 5]
    bias_qkv = (
        lax.optimization_barrier(qkv_bias.astype(low_type))
        .astype(jnp.float32)
        .reshape(3 * head_width)
    )
    bias_up = lax.optimization_barrier(fc1_bias.astype(low_type)).astype(jnp.float32)
    inputs = tokens.astype(jnp.float32)
    normed_one = layer_norm(inputs, gain_one, shift_one).astype(low_type)
    gathered_one = lax.all_gather(normed_one, "tensor", axis=0, tiled=True)
    projected = jnp.dot(gathered_one, weight_qkv, preferred_element_type=jnp.float32) + bias_qkv
    projected = projected.reshape(clip_count, length, 3, head_count, HD)
    queries = rotate(projected[:, :, 0], cosine_table, sine_table).astype(low_type)
    key_rows = rotate(projected[:, :, 1], cosine_table, sine_table).astype(low_type)
    value_rows = projected[:, :, 2].astype(low_type)

    def clip_forward(clip_item):
        query_rows, clip_keys, clip_values = clip_item
        blocks = query_rows.reshape(block_count, block_rows, head_count, HD)
        return lax.map(
            lambda query_block: forward_block(query_block, clip_keys, clip_values), blocks
        )

    mixed_rows, log_totals = lax.map(clip_forward, (queries, key_rows, value_rows))
    mixed_low = mixed_rows.reshape(group_rows, head_width).astype(low_type)
    attn_sum = lax.psum_scatter(
        times_transposed(mixed_low, weight_proj), "tensor", scatter_dimension=0, tiled=True
    )
    middle = inputs + attn_sum + proj_shift
    normed_two = layer_norm(middle, gain_two, shift_two).astype(low_type)
    gathered_two = lax.all_gather(normed_two, "tensor", axis=0, tiled=True)
    hidden = jnp.dot(gathered_two, weight_up, preferred_element_type=jnp.float32) + bias_up
    active = exact_gelu(hidden).astype(low_type)
    layer_out = (
        middle
        + lax.psum_scatter(
            times_transposed(active, weight_down), "tensor", scatter_dimension=0, tiled=True
        )
        + down_shift
    )
    upstream = cotangent.astype(jnp.float32)
    grad_out_all, normed_two_all = (
        lax.all_gather(cotangent, "tensor", axis=0, tiled=True),
        lax.all_gather(normed_two, "tensor", axis=0, tiled=True),
    )
    grad_down = contract_rows(grad_out_all, active)
    grad_active = jnp.dot(grad_out_all, weight_down, preferred_element_type=jnp.float32)
    gelu_pull = jax.vjp(exact_gelu, hidden)[1]
    grad_hidden = gelu_pull(grad_active)[0].astype(low_type)
    grad_up = contract_rows(normed_two_all, grad_hidden)
    grad_bias_up = jnp.sum(grad_hidden.astype(jnp.float32), axis=0)
    grad_normed_two = lax.psum_scatter(
        times_transposed(grad_hidden, weight_up), "tensor", scatter_dimension=0, tiled=True
    )
    middle_part, grad_gain_two, grad_shift_two = jax.vjp(layer_norm, middle, gain_two, shift_two)[
        1
    ](grad_normed_two)
    grad_middle = upstream + middle_part
    grad_branch = grad_middle.astype(low_type)
    grad_proj_shift = jnp.sum(grad_branch.astype(jnp.float32), axis=0)
    grad_down_shift = jnp.sum(upstream, axis=0)
    grad_branch_all, normed_one_all = (
        lax.all_gather(grad_branch, "tensor", axis=0, tiled=True),
        lax.all_gather(normed_one, "tensor", axis=0, tiled=True),
    )
    grad_proj = contract_rows(grad_branch_all, mixed_low)
    grad_mixed = jnp.dot(grad_branch_all, weight_proj, preferred_element_type=jnp.float32).astype(
        low_type
    )
    grad_mixed = grad_mixed.reshape(clip_count, length, head_count, HD)

    def clip_backward(clip_item):
        query_rows, clip_keys, clip_values, clip_totals, clip_grads = clip_item
        starts = (jnp.zeros(clip_keys.shape, jnp.float32), jnp.zeros(clip_keys.shape, jnp.float32))
        block_items = (
            query_rows.reshape(block_count, block_rows, head_count, HD),
            clip_totals,
            clip_grads.reshape(block_count, block_rows, head_count, HD),
        )
        sums, grad_queries = lax.scan(
            lambda running, block_item: backward_block(running, block_item, clip_keys, clip_values),
            starts,
            block_items,
        )
        return (grad_queries.reshape(query_rows.shape), sums[0], sums[1])

    grad_queries, grad_keys, grad_values = lax.map(
        clip_backward, (queries, key_rows, value_rows, log_totals, grad_mixed)
    )
    grad_projected = jnp.stack(
        [
            rotate(grad_queries, cosine_table, -sine_table),
            rotate(grad_keys, cosine_table, -sine_table),
            grad_values,
        ],
        axis=2,
    )
    grad_projected = grad_projected.reshape(group_rows, 3 * head_width).astype(low_type)
    grad_qkv = contract_rows(normed_one_all, grad_projected).reshape(D, 3, head_width)
    grad_bias_qkv = jnp.sum(grad_projected.astype(jnp.float32), axis=0)
    grad_normed_one = lax.psum_scatter(
        times_transposed(grad_projected, weight_qkv), "tensor", scatter_dimension=0, tiled=True
    )
    input_part, grad_gain_one, grad_shift_one = jax.vjp(layer_norm, inputs, gain_one, shift_one)[1](
        grad_normed_one
    )
    input_grad = grad_middle + input_part
    grad_qkv, grad_proj, grad_up, grad_down = (
        lax.psum_scatter(grad_qkv, "fsdp", scatter_dimension=0, tiled=True),
        lax.psum_scatter(grad_proj, "fsdp", scatter_dimension=0, tiled=True),
        lax.psum_scatter(grad_up, "fsdp", scatter_dimension=0, tiled=True),
        lax.psum_scatter(grad_down, "fsdp", scatter_dimension=0, tiled=True),
    )
    lane_index = lax.axis_index("tensor")
    vector_part = jnp.stack(
        [
            grad_gain_one,
            grad_shift_one,
            grad_proj_shift,
            grad_gain_two,
            grad_shift_two,
            grad_down_shift,
        ],
        axis=1,
    )
    qkv_placed = lax.dynamic_update_slice(
        jnp.zeros((3, D), jnp.float32),
        grad_bias_qkv.reshape(3, head_width),
        (jnp.int32(0), lane_index * head_width),
    )
    up_placed = lax.dynamic_update_slice(
        jnp.zeros((FF,), jnp.float32), grad_bias_up, (lane_index * hidden_width,)
    )
    vector_total, qkv_total, up_total = lax.psum(
        (vector_part, qkv_placed, up_placed), ("fsdp", "tensor")
    )
    grad_vectors = lax.dynamic_slice_in_dim(
        vector_total, lax.axis_index("fsdp") * shard_rows, shard_rows, 0
    )
    grad_qkv_bias = lax.dynamic_slice_in_dim(qkv_total, lane_index * head_width, head_width, 1)
    grad_up_bias = lax.dynamic_slice_in_dim(up_total, lane_index * hidden_width, hidden_width, 0)
    matrices = [
        (
            grad_qkv.reshape(shard_rows, 3 * head_width),
            qkv_weight.reshape(shard_rows, 3 * head_width),
            qkv_cols.reshape(3 * head_width),
        ),
        (grad_proj, proj_weight, proj_cols),
        (grad_up, fc1_weight, fc1_cols),
        (grad_down, fc2_weight, fc2_cols),
    ]
    column_counts = [3 * D, D, FF, FF]
    column_weights = jnp.array(column_counts, jnp.float32)
    qkv_state_new = DECAY * qkv_bias_state + (1.0 - DECAY) * (grad_qkv_bias * grad_qkv_bias + TINY)
    qkv_direction = grad_qkv_bias * lax.rsqrt(qkv_state_new)
    up_state_new = DECAY * fc1_bias_state + (1.0 - DECAY) * (grad_up_bias * grad_up_bias + TINY)
    up_direction = grad_up_bias * lax.rsqrt(up_state_new)
    row_squares = jnp.stack(
        [jnp.sum(matrix_entry[0] * matrix_entry[0], axis=1) for matrix_entry in matrices]
    )
    weight_squares = jnp.stack(
        [jnp.sum(matrix_entry[1] * matrix_entry[1]) for matrix_entry in matrices]
    )
    bias_terms = jnp.stack(
        [
            jnp.sum(qkv_direction * qkv_direction),
            jnp.sum(up_direction * up_direction),
            jnp.sum(qkv_bias * qkv_bias),
            jnp.sum(fc1_bias * fc1_bias),
        ]
    )
    row_total, weight_partial, bias_total = lax.psum(
        (row_squares, weight_squares, bias_terms), "tensor"
    )
    rows_new = DECAY * row_state + (1.0 - DECAY) * (row_total / column_weights[:, None] + TINY)
    vector_state_new = DECAY * vector_state + (1.0 - DECAY) * (grad_vectors * grad_vectors + TINY)
    vector_direction = grad_vectors * lax.rsqrt(vector_state_new)
    vector_terms = jnp.stack(
        [jnp.sum(vector_direction * vector_direction, axis=0), jnp.sum(vectors * vectors, axis=0)]
    )
    col_squares = jnp.concatenate(
        [jnp.sum(matrix_entry[0] * matrix_entry[0], axis=0) for matrix_entry in matrices]
    )
    row_new_sums = jnp.sum(rows_new, axis=1)
    col_total, row_new_total, weight_total, vector_sums = lax.psum(
        (col_squares, row_new_sums, weight_partial, vector_terms), "fsdp"
    )
    mean_rows = row_new_total / D
    offsets = [0]
    for matrix_entry in matrices:
        offsets.append(offsets[-1] + matrix_entry[0].shape[1])
    cols_list = []
    direction_list = []
    square_list = []
    for position, matrix_entry in enumerate(matrices):
        col_slice = col_total[offsets[position] : offsets[position + 1]]
        cols_new = DECAY * matrix_entry[2] + (1.0 - DECAY) * (col_slice / D + TINY)
        direction = matrix_entry[0] * lax.rsqrt(
            rows_new[position][:, None] * cols_new[None, :] / mean_rows[position]
        )
        cols_list.append(cols_new)
        direction_list.append(direction)
        square_list.append(jnp.sum(direction * direction))
    square_total = lax.psum(jnp.stack(square_list), ("fsdp", "tensor"))
    matrix_count = D * column_weights
    update_rms = jnp.sqrt(square_total / matrix_count)
    weight_scale = jnp.sqrt(weight_total / matrix_count)
    new_weights = []
    for position, matrix_entry in enumerate(matrices):
        new_weights.append(
            matrix_entry[1]
            - RATE
            * weight_scale[position]
            * direction_list[position]
            / jnp.maximum(1.0, update_rms[position] / CLIP_LEVEL)
        )
    vector_rms = jnp.sqrt(vector_sums[0] / D)
    vector_scale = jnp.sqrt(vector_sums[1] / D)
    vectors_new = vectors - RATE * vector_scale * vector_direction / jnp.maximum(
        1.0, vector_rms / CLIP_LEVEL
    )
    qkv_rms = jnp.sqrt(bias_total[0] / (3 * D))
    qkv_scale = jnp.sqrt(bias_total[2] / (3 * D))
    qkv_bias_new = qkv_bias - RATE * qkv_scale * qkv_direction / jnp.maximum(
        1.0, qkv_rms / CLIP_LEVEL
    )
    up_rms = jnp.sqrt(bias_total[1] / FF)
    up_scale = jnp.sqrt(bias_total[3] / FF)
    up_bias_new = fc1_bias - RATE * up_scale * up_direction / jnp.maximum(1.0, up_rms / CLIP_LEVEL)
    return (
        layer_out,
        input_grad,
        grad_qkv,
        grad_qkv_bias,
        grad_proj,
        grad_up,
        grad_up_bias,
        grad_down,
        grad_vectors,
        rows_new,
        cols_list[0].reshape(3, head_width),
        cols_list[1],
        cols_list[2],
        cols_list[3],
        vector_state_new,
        qkv_state_new,
        up_state_new,
        new_weights[0].reshape(shard_rows, 3, head_width),
        qkv_bias_new,
        new_weights[1],
        new_weights[2],
        up_bias_new,
        new_weights[3],
        vectors_new,
        update_rms,
    )


SCALE = HD**-0.5
LENGTH = GT * GH * GW
ROLL = HD // 3 // 2
CORE_SWAP = [(i, i ^ 1) for i in range(8)]
LOW = jnp.bfloat16
QB = 256


def rotary_rows(first, core):
    token = (lax.broadcasted_iota(jnp.int32, (128, 2 * HD), 0) + first + core * (LENGTH // 2)) & (
        LENGTH - 1
    )
    lane = lax.broadcasted_iota(jnp.int32, (128, 2 * HD), 1) & (HD - 1)
    past_one, past_two = lane >= 2 * ROLL, lane >= 4 * ROLL
    live = lane < 6 * ROLL
    within = lane - jnp.where(past_two, 4 * ROLL, jnp.where(past_one, 2 * ROLL, 0))
    second = within >= ROLL
    step = jnp.where(second, within - ROLL, within).astype(jnp.float32)
    coordinate = jnp.where(
        past_two, token & (GW - 1), jnp.where(past_one, (token >> 4) & (GH - 1), token >> 8)
    ).astype(jnp.float32)
    angle = jnp.where(live, coordinate * jnp.exp(step * (-math.log(BASE) / ROLL)), 0.0)
    cosine = jnp.cos(angle)
    sine = jnp.sin(angle)
    from_first = jnp.where(live & second, sine, 0.0)
    from_second = jnp.where(live, jnp.where(second, 0.0, -sine), 0.0)
    return cosine, from_first, from_second


def turn(v, c, s1, s2, sign):
    return v * c + sign * (pltpu.roll(v, ROLL, 1) * s1 + pltpu.roll(v, 2 * HD - ROLL, 1) * s2)


def dot_nt(a, b):
    return lax.dot_general(a, b, (((1,), (1,)), ((), ())), preferred_element_type=jnp.float32)


def dot_tn(a, b):
    return lax.dot_general(a, b, (((0,), (0,)), ((), ())), preferred_element_type=jnp.float32)


def dot_nn(a, b):
    return lax.dot_general(a, b, (((1,), (0,)), ((), ())), preferred_element_type=jnp.float32)


MESH = pl.DeviceIdType.MESH
PIECES = ((0, 0, 384, 0), (1, 384, 128, 0), (2, 512, 256, 0), (2, 768, 256, 1024), (3, 1024, 256, 0), (3, 1280, 256, 1024))
SHARD = 128
HALVES = ((0, 64), (64, 64))
WHOLE = ((0, 128),)
MIB = 1024 * 1024


def split(piece_and_rows):
    return [(piece, r, at, rows) for piece, parts in piece_and_rows for at, rows in parts for r in range(2)]


def remote(src, dst, send, recv, target):
    return pltpu.make_async_remote_copy(
        src_ref=src, dst_ref=dst, send_sem=send, recv_sem=recv, device_id=target, device_id_type=MESH
    )


def flip(index, bit):
    return index + bit - 2 * bit * ((index // bit) % 2)


def peers():
    lane = lax.axis_index("tensor")
    shard = lax.axis_index("fsdp")
    is_mid = (lane == 1) | (lane == 2)
    pair = {"tensor": flip(lane, 1)}
    across = {"tensor": 3 - lane}
    x_peer = {"fsdp": flip(shard, 2)}
    y_peer = {"fsdp": flip(shard, 4)}
    return lane, shard, is_mid, pair, across, x_peer, y_peer


def meet(targets):
    barrier = pltpu.get_barrier_semaphore()
    for target in targets:
        pl.semaphore_signal(barrier, inc=1, device_id=target, device_id_type=MESH)
    pl.semaphore_wait(barrier, len(targets))


GATHER = split([(PIECES[0], HALVES)] + [(piece, WHOLE) for piece in PIECES[1:]])


def gather_kernel(
    packs_ref, vec_ref, bias_ref, tokens_ref, cotangent_ref,
    qkv_ref, proj_ref, up_ref, down_ref, vec_all, bias_all, h_ref, low_ref, o_ref, lse_ref,
    x_ref, gy_ref, c_ref, s1_ref, s2_ref,
    pack_ref, stage_ref, wq_ref, kh_ref, vh_ref,
    load_sem, local_sem, send_sem, recv_sem, small_send, small_recv, row_send, row_recv,
):
    lane, shard, is_mid, pair, across, x_peer, y_peer = peers()
    core = shard % 2
    outs = (qkv_ref, proj_ref, up_ref, down_ref)
    shard_peers = [
        (q, dc, {"fsdp": flip_place(shard, q, dc)})
        for q in range(4)
        for dc in range(2)
        if (q, dc) != (0, 0)
    ]
    lane_peers = [pair, {"tensor": (lane + 2) % 4}, across]
    other_core = {"fsdp": flip(shard, 1)}
    cross = {"fsdp": flip(shard, 1), "tensor": flip(lane, 1)}
    meet([t for _, _, t in shard_peers] + lane_peers + [cross])
    moved = (core + lane) % 2 == 1
    half = LENGTH // 2

    def permuted(index, src_ref, dst_ref):
        for r in range(2):
            for q in range(4):
                at = pl.ds(pl.multiple_of(global_block(shard, r, q) * SHARD, SHARD), SHARD)
                block = r * 4 + q
                dst_ref[index, :, block * SHARD : (block + 1) * SHARD] = src_ref[:, at]

    def hop_swap(k, dst_ref):
        return remote(
            stage_ref.at[k], dst_ref.at[pl.ds(0, half)], row_send.at[k, 0], row_recv.at[k, 0], cross
        )

    def hop_core(k, dst_ref):
        return remote(
            dst_ref.at[pl.ds(0, half)], dst_ref.at[pl.ds(half, half)], row_send.at[k, 1], row_recv.at[k, 1], other_core
        )

    def rows_out(k, src_ref, dst_ref):
        permuted(k, src_ref, stage_ref)

        @pl.when(moved)
        def _():
            hop_swap(k, dst_ref).start()

        @pl.when(jnp.logical_not(moved))
        def _():
            dst_ref[0:half, :] = stage_ref[k]
            hop_core(k, dst_ref).start()

    def rows_on(k, dst_ref):
        @pl.when(moved)
        def _():
            hop_swap(k, dst_ref).wait_recv()
            hop_core(k, dst_ref).start()

    def rows_in(k, dst_ref):
        hop_core(k, dst_ref).wait()

        @pl.when(moved)
        def _():
            hop_swap(k, dst_ref).wait_send()

    pack_hop = remote(packs_ref.at[1 - core], pack_ref.at[core], row_send.at[2, 0], row_recv.at[2, 0], other_core)
    pack_hop.start()
    pack_ref[core] = packs_ref[core]

    def window(c, block, col0, col_count):
        (m, _, width, base), r, at, rows = GATHER[c]
        return outs[m].at[
            pl.ds((r * 4 + block) * SHARD + at, rows), pl.ds(base + col0 * width, col_count * width)
        ]

    def own(c):
        (_, first, width, _), r, at, rows = GATHER[c]
        return pack_ref.at[r, pl.ds(at, rows), pl.ds(first, width)]

    def local(c):
        return pltpu.make_async_copy(own(c), window(c, 0, 0, 1), local_sem.at[c])

    def hop_pair(c):
        return remote(own(c), window(c, 0, 1, 1), send_sem.at[c, 0], recv_sem.at[c, 0], pair)

    def hop_across(c):
        return remote(
            window(c, 0, 0, 2), window(c, 0, 2, 2), send_sem.at[c, 1], recv_sem.at[c, 1], across
        )

    def hop_out(c):
        far = window(c, 0, 2, 2)
        return remote(far, far, send_sem.at[c, 2], recv_sem.at[c, 1], pair)

    def hop_first(c):
        block, target = ((1, x_peer), (2, y_peer))[GATHER[c][1]]
        return remote(
            window(c, 0, 0, 4), window(c, block, 0, 4), send_sem.at[c, 3], recv_sem.at[c, 2], target
        )

    def hop_second(c):
        moves, target = ((((0, 2), (1, 3)), y_peer), (((0, 1), (2, 3)), x_peer))[GATHER[c][1]]
        return [
            remote(
                window(c, src, 0, 4), window(c, dst, 0, 4), send_sem.at[c, 4 + k], recv_sem.at[c, 3 + k], target
            )
            for k, (src, dst) in enumerate(moves)
        ]

    count = len(GATHER)
    small = []
    slot = core * 4
    vec_all[pl.ds(slot, 1)] = vec_ref[...][None]
    bias_all[0] = bias_ref[...]
    for i, (q, _, target) in enumerate(shard_peers):
        small.append(remote(vec_ref, vec_all.at[slot + q], small_send.at[i], small_recv.at[i], target))
    far_slot = 3 - is_mid.astype(jnp.int32)
    for i, target in enumerate(lane_peers):
        to = bias_all.at[1] if i == 0 else bias_all.at[far_slot]
        small.append(remote(bias_ref, to, small_send.at[7 + i], small_recv.at[7 + i], target))

    def tick(now):
        if 2 <= now < count:
            hop_pair(now).start()
        c = now - 1
        if 0 <= c < count:
            local(c).wait()
            hop_pair(c).wait_recv()

            @pl.when(is_mid)
            def _():
                hop_across(c).start()

        c = now - 2
        if 0 <= c < count:
            hop_across(c).wait_recv()

            @pl.when(is_mid)
            def _():
                hop_out(c).start()

            hop_first(c).start()
        c = now - 4
        if 0 <= c < count:
            hop_first(c).wait_recv()
            for copy in hop_second(c):
                copy.start()

    for copy in small:
        copy.start()
    pack_hop.wait()
    hop_pair(0).start()
    hop_pair(1).start()
    for c in range(count):
        local(c).start()
    tick(0)
    tick(1)

    @pl.loop(0, LENGTH // 128)
    def _(i):
        rows = pl.ds(pl.multiple_of(i * 128, 128), 128)
        c_ref[rows, :], s1_ref[rows, :], s2_ref[rows, :] = rotary_rows(i * 128, core)

    tick(2)
    tick(3)
    rows_out(0, tokens_ref, x_ref)
    tick(4)
    rows_on(0, x_ref)
    tick(5)
    for copy in small:
        copy.wait()
    rows_in(0, x_ref)
    gain = jnp.concatenate([vec_all[b, 0:1, :] for b in range(8)], axis=1)
    shift = jnp.concatenate([vec_all[b, 1:2, :] for b in range(8)], axis=1)

    @pl.loop(0, LENGTH // 64)
    def _(i):
        rows = pl.ds(pl.multiple_of(i * 64, 64), 64)
        unit, _ = norm_parts(x_ref[rows, :].astype(jnp.float32))
        h_ref[rows, :] = (unit * gain + shift).astype(LOW)

    first = 4
    for now in range(6, first + 4):
        tick(now)
    for c in range(first):
        for copy in hop_second(c):
            copy.wait_recv()
    load = pltpu.make_async_copy(qkv_ref, wq_ref, load_sem.at[0])
    load.start()
    tick(first + 4)
    load.wait()
    width = 2 * HD
    lane_q = lax.broadcasted_iota(jnp.int32, (QB, width), 1)

    @pl.loop(0, 8)
    def _(t):
        z = t // 2
        base = z * 3 * width

        def columns(part):
            return pl.ds(pl.multiple_of(base + part * width, width), width)

        @pl.when(t % 2 == 0)
        def _():
            bias = bias_all[pl.ds(z, 1), 0:1, 0 : 3 * width][0]

            @pl.loop(0, LENGTH // QB)
            def _(i):
                rows = pl.ds(pl.multiple_of(i * QB, QB), QB)
                weights = wq_ref[:, pl.ds(pl.multiple_of(base, width), 3 * width)]
                qkv = dot_nn(h_ref[rows, :], weights) + bias
                c, s1, s2 = c_ref[rows, :], s1_ref[rows, :], s2_ref[rows, :]
                low_ref[rows, columns(0)] = turn(qkv[:, :width], c, s1, s2, 1.0).astype(LOW)
                k = turn(qkv[:, width : 2 * width], c, s1, s2, 1.0)
                v = qkv[:, 2 * width :]
                low_ref[rows, columns(1)] = k.astype(LOW)
                low_ref[rows, columns(2)] = v.astype(LOW)
                for h in range(2):
                    mine = (lane_q < HD) if h == 0 else (lane_q >= HD)
                    kh_ref[h, rows, :] = jnp.where(mine, k, 0.0).astype(LOW)
                    vh_ref[h, rows, :] = jnp.where(mine, v, 0.0).astype(LOW)

        for k in range(8):

            @pl.when(t == k)
            def _():
                tick(first + 5 + k)
                if k == 1:
                    rows_out(1, cotangent_ref, gy_ref)
                if k == 5:
                    rows_on(1, gy_ref)

        @pl.loop(0, 2)
        def _(half):
            rows = pl.ds(pl.multiple_of(((t % 2) * 2 + half) * QB, QB), QB)
            q = (low_ref[rows, columns(0)].astype(jnp.float32) * SCALE).astype(LOW)
            total = jnp.zeros((width, QB), jnp.float32)
            for h in range(2):
                s = dot_nt(kh_ref[h], q)
                peak = jnp.max(s, axis=0, keepdims=True)
                e = jnp.exp(s - peak)
                mass = jnp.sum(e, axis=0, keepdims=True)
                p = (e * (1.0 / mass)).astype(LOW)
                total += dot_tn(vh_ref[h], p)
                lse_ref[pl.ds(z, 1), h : h + 1, rows] = (peak + jnp.log(mass))[None]
            o_ref[rows, pl.ds(pl.multiple_of(z * width, width), width)] = total.T.astype(LOW)

    for now in range(first + 13, count + 4):
        tick(now)
    rows_in(1, gy_ref)
    for c in range(count):
        for copy in hop_second(c):
            copy.wait_send()
            if c >= first:
                copy.wait_recv()
        hop_pair(c).wait_send()
        hop_first(c).wait_send()

        @pl.when(is_mid)
        def _():
            hop_across(c).wait_send()
            hop_out(c).wait_send()


def global_block(shard, r, q):
    return flip_place(shard - shard % 2 + r, q, 0)


def flip_place(shard, q, dc):
    target = shard
    for bit, on in ((1, dc), (2, q & 1), (4, q >> 1)):
        if on:
            target = flip(target, bit)
    return target


def gather_all(packs, vec, bias, tokens, cotangent):
    count = len(GATHER)
    rows = 8 * SHARD
    any_space = pl.BlockSpec(memory_space=pl.ANY)
    vmem = pl.BlockSpec(memory_space=pltpu.VMEM)
    width = 2 * HD
    return pl.pallas_call(
        gather_kernel,
        in_specs=[vmem] * 5,
        out_specs=[any_space] * 4 + [vmem] * 11,
        out_shape=[
            jax.ShapeDtypeStruct((rows, 1536), LOW),
            jax.ShapeDtypeStruct((rows, 512), LOW),
            jax.ShapeDtypeStruct((rows, 2048), LOW),
            jax.ShapeDtypeStruct((rows, 2048), LOW),
            jax.ShapeDtypeStruct((8,) + vec.shape, jnp.float32),
            jax.ShapeDtypeStruct((4,) + bias.shape, jnp.float32),
            jax.ShapeDtypeStruct((LENGTH, D), LOW),
            jax.ShapeDtypeStruct((LENGTH, 1536), LOW),
            jax.ShapeDtypeStruct((LENGTH, 512), LOW),
            jax.ShapeDtypeStruct((4, 2, LENGTH), jnp.float32),
            jax.ShapeDtypeStruct((LENGTH, D), LOW),
            jax.ShapeDtypeStruct((LENGTH, D), LOW),
            jax.ShapeDtypeStruct((LENGTH, width), jnp.float32),
            jax.ShapeDtypeStruct((LENGTH, width), jnp.float32),
            jax.ShapeDtypeStruct((LENGTH, width), jnp.float32),
        ],
        scratch_shapes=[
            pltpu.VMEM((2, SHARD, 1536), LOW),
            pltpu.VMEM((2, LENGTH // 2, D), LOW),
            pltpu.VMEM((D, 1536), LOW),
            pltpu.VMEM((2, LENGTH, width), LOW),
            pltpu.VMEM((2, LENGTH, width), LOW),
            pltpu.SemaphoreType.DMA((1,)),
            pltpu.SemaphoreType.DMA((count,)),
            pltpu.SemaphoreType.DMA((count, 6)),
            pltpu.SemaphoreType.DMA((count, 5)),
            pltpu.SemaphoreType.DMA((10,)),
            pltpu.SemaphoreType.DMA((10,)),
            pltpu.SemaphoreType.DMA((3, 2)),
            pltpu.SemaphoreType.DMA((3, 2)),
        ],
        compiler_params=pltpu.CompilerParams(
            collective_id=1, has_side_effects=True, vmem_limit_bytes=48 * MIB
        ),
        name="gather_attend",
    )(packs, vec, bias, tokens, cotangent)


SUMMED = (
    (0, 0, 256, 0),
    (0, 256, 256, 1024),
    (1, 512, 256, 0),
    (1, 768, 256, 1024),
    (2, 1024, 128, 0),
    (3, 1152, 384, 0),
)
SCATTER = split([(piece, WHOLE) for piece in SUMMED[:5]] + [(SUMMED[5], HALVES)])
SUM_WIDTH = 1536


def scatter_kernel(
    down_ref, up_ref, proj_ref, low_ref, go_ref, lse_ref, c_ref, s1_ref, s2_ref, h_ref, wq_ref,
    vec_ref, x_ref, gx_ref, layer_ref,
    out_ref, bias_ref, norm_ref, layer_out, input_out, gh_ref,
    other_ref, low_stage, gq_ref, g_ref, kh_ref, vh_ref, gk_ref, gv_ref,
    own_ref, first_ref, second_ref, in_ref, mid_ref, near_ref,
    local_sem, send_sem, recv_sem, row_send, row_recv,
):
    grads = (down_ref, up_ref, proj_ref, gq_ref)
    lane, shard, is_mid, pair, across, x_peer, y_peer = peers()
    barrier = pltpu.get_barrier_semaphore()
    other_core = {"fsdp": flip(shard, 1)}
    cross = {"fsdp": flip(shard, 1), "tensor": flip(lane, 1)}
    moved = (shard % 2 + lane) % 2 == 1
    half = LENGTH // 2
    for target in (pair, x_peer, y_peer, other_core, cross):
        pl.semaphore_signal(barrier, inc=1, device_id=target, device_id_type=MESH)

    @pl.when(is_mid)
    def _():
        pl.semaphore_signal(barrier, inc=1, device_id=across, device_id_type=MESH)

    pl.semaphore_wait(barrier, 5 + is_mid.astype(jnp.int32))

    def hop_rows(k, src, dst):
        return remote(src, dst, row_send.at[k], row_recv.at[k], cross)

    hop_sum = remote(gh_ref.at[pl.ds(half, half)], other_ref, row_send.at[2], row_recv.at[2], other_core)

    def source(c, block):
        (a, _, width, base), r, at, rows = SCATTER[c]
        return grads[a].at[pl.ds((r * 4 + block) * SHARD + at, rows), pl.ds(base, 4 * width)]

    def part(ref, c, block, lo, hi, each):
        (_, first, width, _), r, at, rows = SCATTER[c]
        return ref.at[
            r, pl.ds(block * SHARD + at, rows), pl.ds(first * each + lo * width, (hi - lo) * width)
        ]

    def keep(c):
        blocks = ((0, 1), (0, 2))[SCATTER[c][1]]
        return [
            pltpu.make_async_copy(source(c, block), part(own_ref, c, k, 0, 4, 4), local_sem.at[c, k])
            for k, block in enumerate(blocks)
        ]

    def hop_first(c):
        blocks, target = (((2, 3), y_peer), ((1, 3), x_peer))[SCATTER[c][1]]
        return [
            remote(
                source(c, block), part(first_ref, c, k, 0, 4, 4), send_sem.at[c, k], recv_sem.at[c, k], target
            )
            for k, block in enumerate(blocks)
        ]

    def hop_second(c):
        return remote(
            part(own_ref, c, 1, 0, 4, 4), part(second_ref, c, 0, 0, 4, 4),
            send_sem.at[c, 2], recv_sem.at[c, 2], (x_peer, y_peer)[SCATTER[c][1]],
        )

    def hop_in(c):
        return remote(
            part(own_ref, c, 0, 2, 4, 4), part(in_ref, c, 0, 0, 2, 2), send_sem.at[c, 3], recv_sem.at[c, 3], pair
        )

    def hop_across(c):
        return remote(
            part(own_ref, c, 0, 2, 4, 4), part(mid_ref, c, 0, 0, 2, 2), send_sem.at[c, 3], recv_sem.at[c, 4], across
        )

    def hop_pair(c):
        return remote(
            part(own_ref, c, 0, 1, 2, 4), part(near_ref, c, 0, 0, 1, 1), send_sem.at[c, 4], recv_sem.at[c, 5], pair
        )

    def add(dst, left, right):
        step = 16

        @pl.loop(0, dst.shape[0] // step)
        def _(i):
            at = pl.ds(pl.multiple_of(i * step, step), step)
            total = left[at, :].astype(jnp.float32) + right[at, :].astype(jnp.float32)
            dst[at, :] = total.astype(dst.dtype)

    count = len(SCATTER)
    lead = 4

    def tick(now):
        c = now
        if c < count:
            if c + lead < count:
                for copy in hop_first(c + lead):
                    copy.start()
                for copy in keep(c + lead):
                    copy.start()
            for copy in keep(c):
                copy.wait()
            for copy in hop_first(c):
                copy.wait_recv()
            mine = part(own_ref, c, 1, 0, 4, 4)
            add(mine, mine, part(first_ref, c, 1, 0, 4, 4))
            hop_second(c).start()
            mine = part(own_ref, c, 0, 0, 4, 4)
            add(mine, mine, part(first_ref, c, 0, 0, 4, 4))
        c = now - 2
        if 0 <= c < count:
            hop_second(c).wait_recv()
            mine = part(own_ref, c, 0, 0, 4, 4)
            add(mine, mine, part(second_ref, c, 0, 0, 4, 4))

            @pl.when(jnp.logical_not(is_mid))
            def _():
                hop_in(c).start()

        c = now - 3
        if 0 <= c < count:

            @pl.when(is_mid)
            def _():
                hop_in(c).wait_recv()
                far = part(own_ref, c, 0, 2, 4, 4)
                add(far, far, part(in_ref, c, 0, 0, 2, 2))
                hop_across(c).start()

        c = now - 4
        if 0 <= c < count:

            @pl.when(is_mid)
            def _():
                hop_across(c).wait_recv()
                near = part(own_ref, c, 0, 0, 2, 4)
                add(near, near, part(mid_ref, c, 0, 0, 2, 2))

            hop_pair(c).start()
        c = now - 5
        if 0 <= c < count:
            hop_pair(c).wait_recv()
            add(part(out_ref, c, 0, 0, 1, 1), part(own_ref, c, 0, 0, 1, 4), part(near_ref, c, 0, 0, 1, 1))

    for c in range(lead):
        for copy in hop_first(c):
            copy.start()
        for copy in keep(c):
            copy.start()

    @pl.when(moved)
    def _():
        hop_rows(0, layer_ref, layer_out).start()

    width = 2 * HD
    lane_q = lax.broadcasted_iota(jnp.int32, (QB, width), 1)

    @pl.loop(0, 8)
    def _(t):
        z = t // 2
        base = z * 3 * width

        def columns(part_index):
            return pl.ds(pl.multiple_of(base + part_index * width, width), width)

        @pl.when(t % 2 == 0)
        def _():
            @pl.loop(0, LENGTH // QB)
            def _(i):
                rows = pl.ds(pl.multiple_of(i * QB, QB), QB)
                k = low_ref[rows, columns(1)].astype(jnp.float32)
                v = low_ref[rows, columns(2)].astype(jnp.float32)
                for h in range(2):
                    mine = (lane_q < HD) if h == 0 else (lane_q >= HD)
                    kh_ref[h, rows, :] = jnp.where(mine, k, 0.0).astype(LOW)
                    vh_ref[h, rows, :] = jnp.where(mine, v, 0.0).astype(LOW)

            gk_ref[...] = jnp.zeros_like(gk_ref)
            gv_ref[...] = jnp.zeros_like(gv_ref)

        for k in range(2, 8):

            @pl.when(t == k)
            def _():
                tick(k - 2)

        @pl.loop(0, 2)
        def _(half):
            rows = pl.ds(pl.multiple_of(((t % 2) * 2 + half) * QB, QB), QB)
            q = low_ref[rows, columns(0)].astype(jnp.float32) * SCALE
            go = go_ref[rows, pl.ds(pl.multiple_of(z * width, width), width)].astype(jnp.float32)
            total = jnp.zeros((width, QB), jnp.float32)
            for h in range(2):
                mine = (lane_q < HD) if h == 0 else (lane_q >= HD)
                qh = jnp.where(mine, q, 0.0).astype(LOW)
                gh = jnp.where(mine, go, 0.0).astype(LOW)
                p = jnp.exp(dot_nt(kh_ref[h], qh) - lse_ref[pl.ds(z, 1), h : h + 1, rows][0])
                dp = dot_nt(vh_ref[h], gh)
                pd = jnp.sum(p * dp, axis=0, keepdims=True)
                ds = (p * (dp - pd)).astype(LOW)
                gv_ref[...] += dot_nn(p.astype(LOW), gh)
                gk_ref[...] += dot_nn(ds, qh)
                total += dot_tn(kh_ref[h], ds)
            gq = turn(total.T * SCALE, c_ref[rows, :], s1_ref[rows, :], s2_ref[rows, :], -1.0)
            g_ref[rows, :width] = gq.astype(LOW)

        @pl.when(t % 2 == 1)
        def _():
            wide = pl.ds(pl.multiple_of(base, width), 3 * width)
            gk = turn(gk_ref[...], c_ref[...], s1_ref[...], s2_ref[...], -1.0)
            g_ref[:, width : 2 * width] = gk.astype(LOW)
            g_ref[:, 2 * width :] = gv_ref[...].astype(LOW)
            bias_ref[:, wide] = jnp.sum(g_ref[...].astype(jnp.float32), axis=0, keepdims=True)

            @pl.loop(0, D // QB)
            def _(i):
                some = pl.ds(pl.multiple_of(i * QB, QB), QB)
                gq_ref[some, wide] = dot_tn(h_ref[:, some], g_ref[...]).astype(LOW)
                product = dot_nt(g_ref[some, :], wq_ref[:, wide])

                @pl.when(z == 0)
                def _():
                    gh_ref[some, :] = product

                @pl.when(z > 0)
                def _():
                    gh_ref[some, :] += product

    hop_sum.start()
    tick(6)
    gain = jnp.concatenate([vec_ref[b, 0:1, :] for b in range(8)], axis=1)
    norm_ref[...] = jnp.zeros_like(norm_ref)
    hop_sum.wait()

    @pl.loop(0, half // 64)
    def _(i):
        some = pl.ds(pl.multiple_of(i * 64, 64), 64)
        grad = gh_ref[some, :] + other_ref[some, :]
        unit, scale = norm_parts(x_ref[some, :].astype(jnp.float32))
        norm_ref[0:1, :] += jnp.sum(grad * unit, axis=0, keepdims=True)
        norm_ref[1:2, :] += jnp.sum(grad, axis=0, keepdims=True)
        value = gx_ref[some, :] + norm_back(grad, unit, scale, gain)
        gh_ref[some, :] = value
        low_stage[some, :] = value.astype(LOW)

    @pl.when(moved)
    def _():
        hop_rows(1, low_stage, input_out).start()

    for now in range(7, count + 5):
        tick(now)

    @pl.when(moved)
    def _():
        hop_rows(0, layer_ref, layer_out).wait()
        hop_rows(1, low_stage, input_out).wait()

    for c in range(count):
        for copy in hop_first(c):
            copy.wait_send()
        hop_second(c).wait_send()
        hop_pair(c).wait_send()

        @pl.when(is_mid)
        def _():
            hop_across(c).wait_send()

        @pl.when(jnp.logical_not(is_mid))
        def _():
            hop_in(c).wait_send()


def scatter_all(grads, attention, rows):
    count = len(SCATTER)
    width = SUM_WIDTH
    vmem = pl.BlockSpec(memory_space=pltpu.VMEM)
    any_space = pl.BlockSpec(memory_space=pl.ANY)
    pair_width = 2 * HD
    return pl.pallas_call(
        scatter_kernel,
        in_specs=[any_space] * 3 + [vmem] * 11 + [any_space],
        out_specs=[vmem] * 3 + [any_space] * 2 + [vmem],
        out_shape=[
            jax.ShapeDtypeStruct((2, SHARD, width), jnp.float32),
            jax.ShapeDtypeStruct((1, 1536), jnp.float32),
            jax.ShapeDtypeStruct((8, D), jnp.float32),
            jax.ShapeDtypeStruct((LENGTH // 2, D), LOW),
            jax.ShapeDtypeStruct((LENGTH // 2, D), LOW),
            jax.ShapeDtypeStruct((LENGTH, D), jnp.float32),
        ],
        scratch_shapes=[
            pltpu.VMEM((LENGTH // 2, D), jnp.float32),
            pltpu.VMEM((LENGTH // 2, D), LOW),
            pltpu.VMEM((D, 1536), LOW),
            pltpu.VMEM((LENGTH, 3 * pair_width), LOW),
            pltpu.VMEM((2, LENGTH, pair_width), LOW),
            pltpu.VMEM((2, LENGTH, pair_width), LOW),
            pltpu.VMEM((LENGTH, pair_width), jnp.float32),
            pltpu.VMEM((LENGTH, pair_width), jnp.float32),
            pltpu.VMEM((2, 2 * SHARD, 4 * width), LOW),
            pltpu.VMEM((2, 2 * SHARD, 4 * width), LOW),
            pltpu.VMEM((2, SHARD, 4 * width), LOW),
            pltpu.VMEM((2, SHARD, 2 * width), LOW),
            pltpu.VMEM((2, SHARD, 2 * width), LOW),
            pltpu.VMEM((2, SHARD, width), LOW),
            pltpu.SemaphoreType.DMA((count, 2)),
            pltpu.SemaphoreType.DMA((count, 5)),
            pltpu.SemaphoreType.DMA((count, 6)),
            pltpu.SemaphoreType.DMA((3,)),
            pltpu.SemaphoreType.DMA((3,)),
        ],
        compiler_params=pltpu.CompilerParams(
            collective_id=2, has_side_effects=True, vmem_limit_bytes=60 * MIB
        ),
        name="scatter_attend_back",
    )(*grads, *attention, *rows)


def place_kernel(layer_ref, layer_low, input_ref, input_low, layer_out, input_out):
    shard = lax.axis_index("fsdp")
    moved = (shard % 2 + lax.axis_index("tensor")) % 2 == 1
    for own, other, out in ((layer_ref, layer_low, layer_out), (input_ref, input_low, input_out)):
        for r in range(2):
            for q in range(4):
                at = pl.ds(pl.multiple_of(global_block(shard, r, q) * SHARD, SHARD), SHARD)
                here = pl.ds((r * 4 + q) * SHARD, SHARD)

                @pl.when(moved)
                def _():
                    out[:, at] = other[:, here].astype(jnp.float32)

                @pl.when(jnp.logical_not(moved))
                def _():
                    out[:, at] = own[:, here]


def place_rows(layer, layer_low, grad, grad_low):
    block = pl.BlockSpec((128, D), lambda i: (i, 0))
    shape = jax.ShapeDtypeStruct((LENGTH // 2, D), jnp.float32)
    return pl.pallas_call(
        place_kernel,
        grid=(LENGTH // 256,),
        in_specs=[block] * 4,
        out_specs=[block] * 2,
        out_shape=[shape] * 2,
        name="place_rows",
    )(layer, layer_low, grad, grad_low)


COUNTS = (3 * D, D, FF, FF)
BLOCKS = (6, 2, 8, 8)


def offsets():
    return [(z * 8 + q * 2 + dc, q, dc, z) for z in range(4) for q in range(4) for dc in range(2)]


def stepped(g, state):
    new = DECAY * state + (1.0 - DECAY) * (g * g + TINY)
    return new, g * lax.rsqrt(new)


def rows_step(squares, old):
    which = lax.broadcasted_iota(jnp.int32, (4, 128), 0)
    counts = jnp.where(
        which == 0, float(COUNTS[0]), jnp.where(which == 1, float(COUNTS[1]), float(COUNTS[2]))
    )
    return DECAY * old + (1.0 - DECAY) * (squares / counts + TINY)


def tune_kernel(
    sums_ref, vec_ref, db_ref, wq_ref, wp_ref, wu_ref, wd_ref, vw_ref, vs_ref, rows_ref,
    cq_ref, cp_ref, cu_ref, cd_ref, bq_ref, bu_ref, bqs_ref, bus_ref,
    gq, gp_out, gu_out, gd_out, bq_out, bu_out, lane_out, col_out, grand_out,
    vec_send, vec_recv, db_recv, lane_send, lane_recv, col_send, col_recv, all_send, all_recv,
    core_send, core_done, a_send, a_recv, b_send, b_recv, c_send, c_recv,
):
    lane = lax.axis_index("tensor")
    shard = lax.axis_index("fsdp")
    core = shard % 2
    is_mid = (lane == 1) | (lane == 2)
    z_of = [lane, flip(lane, 1), 3 - lane, (lane + 2) % 4]

    def device(q, dc, z):
        target = {}
        if q or dc:
            target["fsdp"] = flip_place(shard, q, dc)
        if z:
            target["tensor"] = z_of[z]
        return target

    others = [entry for entry in offsets() if entry[0]]
    meet([device(q, dc, z) for _, q, dc, z in others])
    shard_peers = [(slot, q, dc) for slot, q, dc, z in others if z == 0]

    def core_copies():
        give = 1 - core
        hq = pl.ds(pl.multiple_of(core * 128, 128), 128)
        hf = pl.ds(pl.multiple_of(core * 512, 512), 512)
        pairs = [(sums_ref.at[give, :, pl.ds(1152 + j * 128, 128)], gq.at[j, :, hq]) for j in range(3)]
        pairs.append((sums_ref.at[give, :, pl.ds(1024, 128)], gp_out.at[:, hq]))
        pairs.append((sums_ref.at[give, :, pl.ds(512, 512)], gu_out.at[:, hf]))
        pairs.append((sums_ref.at[give, :, pl.ds(0, 512)], gd_out.at[:, hf]))
        return [
            remote(src, dst, core_send.at[i], core_done.at[i], {"fsdp": flip(shard, 1)})
            for i, (src, dst) in enumerate(pairs)
        ]

    for copy in core_copies():
        copy.start()

    def round_a():
        copies = [
            remote(vec_send.at[slot], vec_recv.at[slot], a_send.at[slot], a_recv.at[slot], device(q, dc, 0))
            for slot, q, dc in shard_peers
        ]
        for z in range(1, 4):
            position = 1 if z == 1 else (3 - is_mid.astype(jnp.int32) if z == 2 else 2 + is_mid.astype(jnp.int32))
            copies.append(
                remote(db_ref.at[position], db_recv.at[z], a_send.at[7 + z], a_recv.at[7 + z], device(0, 0, z))
            )
        return copies

    for slot in range(8):
        q, dc = slot // 2, slot % 2
        block = (core + dc - 2 * core * dc) * 4 + q
        at = pl.ds(pl.multiple_of(block * 128, 128), 128)
        if slot == 0:
            vec_recv[0] = vec_ref[:, at]
        else:
            vec_send[slot] = vec_ref[:, at]
    for copy in round_a():
        copy.start()
    db_recv[0] = db_ref[0]

    mine_q = pl.ds(pl.multiple_of(core * 128, 128), 128)
    mine_f = pl.ds(pl.multiple_of(core * 512, 512), 512)
    for j in range(3):
        gq[j, :, mine_q] = sums_ref[core, :, 1152 + j * 128 : 1280 + j * 128]
    gp_out[:, mine_q] = sums_ref[core, :, 1024:1152]
    gu_out[:, mine_f] = sums_ref[core, :, 512:1024]
    gd_out[:, mine_f] = sums_ref[core, :, 0:512]

    def weight_block(m, i):
        if m == 0:
            return wq_ref[:, i // 2, (i % 2) * 128 : (i % 2) * 128 + 128]
        return (None, wp_ref, wu_ref, wd_ref)[m][:, i * 128 : (i + 1) * 128]

    def grad_block(m, i):
        if m == 0:
            return gq[i // 2, :, (i % 2) * 128 : (i % 2) * 128 + 128]
        return (None, gp_out, gu_out, gd_out)[m][:, i * 128 : (i + 1) * 128]

    zero = jnp.zeros((128, 128), jnp.float32)

    def total_of(v):
        return jnp.sum(jnp.sum(v, axis=0, keepdims=True), axis=1, keepdims=True)

    weight_squares = []
    for m in range(4):
        acc = zero
        for i in range(BLOCKS[m]):
            w = weight_block(m, i)
            acc += w * w
        weight_squares.append(total_of(acc))

    for copy in core_copies():
        copy.wait()
    lane_send[...] = jnp.zeros_like(lane_send)
    row = 0
    for m in range(4):
        acc = zero
        for i in range(BLOCKS[m]):
            g = grad_block(m, i)
            square = g * g
            acc += square
            col_send[row : row + 1, :] = jnp.sum(square, axis=0, keepdims=True)
            row += 1
        lane_send[8 + m : 9 + m, :] = jnp.sum(acc.T, axis=0, keepdims=True)

    for copy in round_a():
        copy.wait()
    vec_sum = vec_recv[0]
    for slot in range(1, 8):
        vec_sum += vec_recv[slot]
    lane_send[0:8, :] = vec_sum
    col_send[24:32, :] = db_recv[0] + db_recv[1] + db_recv[2] + db_recv[3]

    def round_b():
        copies = [
            remote(lane_send, lane_recv.at[z], b_send.at[z], b_recv.at[z], device(0, 0, z)) for z in range(1, 4)
        ]
        copies += [
            remote(col_send, col_recv.at[slot], b_send.at[3 + slot], b_recv.at[3 + slot], device(q, dc, 0))
            for slot, q, dc in shard_peers
        ]
        return copies

    for copy in round_b():
        copy.start()
    for copy in round_b():
        copy.wait()
    lane_total = lane_send[...] + lane_recv[1] + lane_recv[2] + lane_recv[3]
    same = col_send[...] + col_recv[2] + col_recv[4] + col_recv[6]
    cross = col_recv[1] + col_recv[3] + col_recv[5] + col_recv[7]
    col_total = same[0:24] + cross[0:24]
    low_half = jnp.where(core == 0, same[24:32], cross[24:32])
    high_half = jnp.where(core == 0, cross[24:32], same[24:32])
    bq_out[:, 0:128] = low_half[0:3]
    bq_out[:, 128:256] = high_half[0:3]
    bu_out[0:4, :] = low_half[3:7]
    bu_out[4:8, :] = high_half[3:7]

    lane_out[...] = lane_total
    col_out[...] = col_total
    gvec = lane_total[0:8]
    _, v_dir = stepped(gvec, vs_ref[...])
    _, bq_dir = stepped(bq_out[...], bqs_ref[...])
    _, bu_dir = stepped(bu_out[...], bus_ref[...])
    rows_new = rows_step(lane_total[8:12], rows_ref[...])
    inverse_rows = lax.rsqrt(rows_new)
    spots = lax.broadcasted_iota(jnp.int32, (8, 128), 1)
    message = jnp.zeros((8, 128), jnp.float32)
    sums = []
    inverse_cols = []
    tall = []
    row = 0
    for m in range(4):
        tall.append(jnp.broadcast_to(inverse_rows[m : m + 1], (128, 128)).T)
        acc = zero
        for i in range(BLOCKS[m]):
            if m == 0:
                old = cq_ref[i // 2 : i // 2 + 1, (i % 2) * 128 : (i % 2) * 128 + 128]
            else:
                old = (None, cp_ref, cu_ref, cd_ref)[m][i : i + 1, :]
            new = DECAY * old + (1.0 - DECAY) * (col_total[row : row + 1] / D + TINY)
            inverse_cols.append(lax.rsqrt(new))
            step = grad_block(m, i) * tall[m] * inverse_cols[row]
            acc += step * step
            row += 1
        sums.append(total_of(acc))
    terms = sums
    terms = terms + [0.25 * total_of(rows_new[m : m + 1]) for m in range(4)]
    terms = terms + weight_squares
    vw = vw_ref[...]
    v_squares = jnp.sum(v_dir * v_dir, axis=1, keepdims=True)
    w_squares = jnp.sum(vw * vw, axis=1, keepdims=True)
    terms = terms + [0.25 * v_squares[i : i + 1] for i in range(6)]
    terms = terms + [0.25 * w_squares[i : i + 1] for i in range(6)]
    for value in (bq_dir, bu_dir, bq_ref[...], bu_ref[...]):
        terms = terms + [0.125 * total_of(value * value)]
    for i, term in enumerate(terms):
        message = jnp.where(spots == i, term, message)
    all_send[...] = message

    def round_c():
        return [
            remote(all_send, all_recv.at[slot], c_send.at[slot], c_recv.at[slot], device(q, dc, z))
            for slot, q, dc, z in others
        ]

    for copy in round_c():
        copy.start()
    for copy in round_c():
        copy.wait()
    grand = message
    for slot, _, _, _ in others:
        grand += all_recv[slot]
    grand_out[...] = grand


def apply_kernel(
    gq, gp_ref, gu_ref, gd_ref, bg_ref, ug_ref, lane_ref, col_ref, grand_ref,
    wq_ref, wp_ref, wu_ref, wd_ref, vw_ref, vs_ref, rows_ref,
    cq_ref, cp_ref, cu_ref, cd_ref, bq_ref, bu_ref, bqs_ref, bus_ref,
    gq_out, gp_out, gu_out, gd_out, nq_out, np_out, nu_out, nd_out, vec_out, rows_out,
    cq_out, cp_out, cu_out, cd_out, bq_out, bqs_out, bqn_out, bu_out, bus_out, bun_out, rms_out,
):
    def weight_block(m, i):
        if m == 0:
            return wq_ref[:, i // 2, (i % 2) * 128 : (i % 2) * 128 + 128]
        return (None, wp_ref, wu_ref, wd_ref)[m][:, i * 128 : (i + 1) * 128]

    def grad_block(m, i):
        if m == 0:
            return gq[i // 2, :, (i % 2) * 128 : (i % 2) * 128 + 128]
        return (None, gp_ref, gu_ref, gd_ref)[m][:, i * 128 : (i + 1) * 128]

    for j in range(3):
        gq_out[:, j, :] = gq[j]
    gp_out[...] = gp_ref[...]
    gu_out[...] = gu_ref[...]
    gd_out[...] = gd_ref[...]
    bq_out[...] = bg_ref[...]
    bu_out[...] = ug_ref[...]
    gvec = lane_ref[0:8, :]
    vw = vw_ref[...]
    vs_new, v_dir = stepped(gvec, vs_ref[...])
    bqs_new, bq_dir = stepped(bg_ref[...], bqs_ref[...])
    bus_new, bu_dir = stepped(ug_ref[...], bus_ref[...])
    bqs_out[...] = bqs_new
    bus_out[...] = bus_new
    vec_out[0:8, :] = gvec
    vec_out[8:16, :] = vs_new
    rows_new = rows_step(lane_ref[8:12, :], rows_ref[...])
    rows_out[...] = rows_new
    inverse_rows = lax.rsqrt(rows_new)
    line = grand_ref[0:1, :]
    spot = lax.broadcasted_iota(jnp.int32, (1, 128), 1)

    def pick(i):
        return jnp.sum(jnp.where(spot == i, line, 0.0), axis=1, keepdims=True)

    rms_line = jnp.zeros((1, 128), jnp.float32)
    row = 0
    for m in range(4):
        size = float(D * COUNTS[m])
        mean_rows = pick(4 + m) / D
        rms = jnp.sqrt(pick(m) * mean_rows / size)
        scale = jnp.sqrt(pick(8 + m) / size)
        factor = RATE * scale * jnp.sqrt(mean_rows) / jnp.maximum(1.0, rms / CLIP_LEVEL)
        rms_line = jnp.where(spot == m, rms, rms_line)
        tall = jnp.broadcast_to(inverse_rows[m : m + 1], (128, 128)).T
        for i in range(BLOCKS[m]):
            if m == 0:
                old = cq_ref[i // 2 : i // 2 + 1, (i % 2) * 128 : (i % 2) * 128 + 128]
            else:
                old = (None, cp_ref, cu_ref, cd_ref)[m][i : i + 1, :]
            cols = DECAY * old + (1.0 - DECAY) * (col_ref[row : row + 1, :] / D + TINY)
            if m == 0:
                cq_out[i // 2 : i // 2 + 1, (i % 2) * 128 : (i % 2) * 128 + 128] = cols
            else:
                (None, cp_out, cu_out, cd_out)[m][i : i + 1, :] = cols
            new = weight_block(m, i) - factor * (grad_block(m, i) * tall * lax.rsqrt(cols))
            if m == 0:
                nq_out[:, i // 2, (i % 2) * 128 : (i % 2) * 128 + 128] = new
            else:
                (None, np_out, nu_out, nd_out)[m][:, i * 128 : (i + 1) * 128] = new
            row += 1
    rms_out[...] = rms_line
    for i in range(6):
        spread = jnp.sqrt(pick(12 + i) / D)
        factor = RATE * jnp.sqrt(pick(18 + i) / D) / jnp.maximum(1.0, spread / CLIP_LEVEL)
        vec_out[16 + i : 17 + i, :] = vw[i : i + 1] - factor * v_dir[i : i + 1]
    vec_out[22:24, :] = jnp.zeros((2, 128), jnp.float32)
    for direction, weight, out, at, size in (
        (bq_dir, bq_ref, bqn_out, 24, 3 * D),
        (bu_dir, bu_ref, bun_out, 25, FF),
    ):
        spread = jnp.sqrt(pick(at) / size)
        factor = RATE * jnp.sqrt(pick(at + 2) / size) / jnp.maximum(1.0, spread / CLIP_LEVEL)
        out[...] = weight[...] - factor * direction


def tune_all(sums, vec_part, db_part, params, stats, states):
    qkv_weight, qkv_bias, proj_weight, fc1_weight, fc1_bias, fc2_weight, vectors = params
    row_state, qkv_cols, proj_cols, fc1_cols, fc2_cols = stats
    vector_state, qkv_bias_state, fc1_bias_state = states
    pad = ((0, 2), (0, 0))

    def dense(v):
        return v.reshape(v.shape[0] // 128, 128)

    operands = (
        sums, vec_part, db_part, qkv_weight, proj_weight, fc1_weight, fc2_weight,
        jnp.pad(vectors.T, pad), jnp.pad(vector_state.T, pad, constant_values=1.0), row_state,
        qkv_cols, dense(proj_cols), dense(fc1_cols), dense(fc2_cols),
        qkv_bias, dense(fc1_bias), qkv_bias_state, dense(fc1_bias_state),
    )
    vmem = pl.BlockSpec(memory_space=pltpu.VMEM)
    shapes = [
        (128, 3, 256), (128, 256), (128, 1024), (128, 1024),
        (128, 3, 256), (128, 256), (128, 1024), (128, 1024),
        (24, 128), (4, 128), (3, 256), (2, 128), (8, 128), (8, 128),
        (3, 256), (3, 256), (3, 256), (8, 128), (8, 128), (8, 128), (1, 128),
    ]
    f32 = jnp.float32
    middle = [
        (3, 128, 256), (128, 256), (128, 1024), (128, 1024), (3, 256), (8, 128), (16, 128), (24, 128), (8, 128)
    ]
    reduced = pl.pallas_call(
        tune_kernel,
        in_specs=[vmem] * len(operands),
        out_specs=[vmem] * len(middle),
        out_shape=[jax.ShapeDtypeStruct(shape, f32) for shape in middle],
        scratch_shapes=[
            pltpu.VMEM((8, 8, 128), f32),
            pltpu.VMEM((8, 8, 128), f32),
            pltpu.VMEM((4, 8, 128), f32),
            pltpu.VMEM((16, 128), f32),
            pltpu.VMEM((4, 16, 128), f32),
            pltpu.VMEM((32, 128), f32),
            pltpu.VMEM((8, 32, 128), f32),
            pltpu.VMEM((8, 128), f32),
            pltpu.VMEM((32, 8, 128), f32),
            pltpu.SemaphoreType.DMA((6,)),
            pltpu.SemaphoreType.DMA((6,)),
            pltpu.SemaphoreType.DMA((11,)),
            pltpu.SemaphoreType.DMA((11,)),
            pltpu.SemaphoreType.DMA((11,)),
            pltpu.SemaphoreType.DMA((11,)),
            pltpu.SemaphoreType.DMA((32,)),
            pltpu.SemaphoreType.DMA((32,)),
        ],
        compiler_params=pltpu.CompilerParams(collective_id=4, has_side_effects=True, vmem_limit_bytes=40 * 1024 * 1024),
        name="tune_all",
    )(*operands)
    inputs = (*reduced, *operands[3:])
    (
        gq, gp, gu, gd, nq, np_, nu, nd, vec, rows, cq, cp, cu, cd, bq, bqs, bqn, bu, bus, bun, rms
    ) = pl.pallas_call(
        apply_kernel,
        in_specs=[vmem] * len(inputs),
        out_specs=[vmem] * len(shapes),
        out_shape=[jax.ShapeDtypeStruct(shape, f32) for shape in shapes],
        compiler_params=pltpu.CompilerParams(vmem_limit_bytes=40 * MIB),
        name="apply_all",
    )(*inputs)
    vec = vec.T
    return (
        gq, bq, gp, gu, bu.reshape(1024), gd, vec[:, 0:6], rows,
        cq, cp.reshape(256), cu.reshape(1024), cd.reshape(1024),
        vec[:, 8:14], bqs, bus.reshape(1024),
        nq, bqn, np_, nu, bun.reshape(1024), nd, vec[:, 16:22], rms[0, 0:4],
    )


def gelu_parts(u):
    cdf = 0.5 * (1.0 + lax.erf(u * (0.5**0.5)))
    density = jnp.exp(-0.5 * u * u) * ((2.0 * jnp.pi) ** -0.5)
    return u * cdf, cdf + u * density


def norm_parts(values):
    center = values - jnp.mean(values, axis=-1, keepdims=True)
    scale = lax.rsqrt(jnp.mean(center * center, axis=-1, keepdims=True) + NORM_EPS)
    return center * scale, scale


def norm_back(grad, unit, scale, gain):
    c = grad * gain
    return scale * (
        c
        - jnp.mean(c, axis=-1, keepdims=True)
        - unit * jnp.mean(c * unit, axis=-1, keepdims=True)
    )


def on_chip(
    tokens,
    cotangent,
    qkv_weight,
    qkv_bias,
    proj_weight,
    fc1_weight,
    fc1_bias,
    fc2_weight,
    vectors,
    row_state,
    qkv_cols,
    proj_cols,
    fc1_cols,
    fc2_cols,
    vector_state,
    qkv_bias_state,
    fc1_bias_state,
):
    shard = lax.axis_index("fsdp")
    core = shard % 2
    rows = tokens.shape[0]
    hw, fw = qkv_weight.shape[2] // 2, fc1_weight.shape[1] // 2
    shard_rows = qkv_weight.shape[0]

    def both_halves(v):
        return jnp.concatenate([v, lax.ppermute(v, "fsdp", CORE_SWAP)], axis=0)

    def core_sum(left, right_t):
        other = times_transposed(left[rows:], right_t)
        other = lax.ppermute(other, "fsdp", CORE_SWAP)
        return times_transposed(left[:rows], right_t) + other

    def half_columns(w, width, which):
        return lax.dynamic_slice_in_dim(w, which * width, width, w.ndim - 1)

    def pack(which):
        return jnp.concatenate(
            [
                qkv_weight[:, :, which * hw : (which + 1) * hw].reshape(shard_rows, 3 * hw),
                proj_weight[:, which * hw : (which + 1) * hw],
                fc1_weight[:, which * fw : (which + 1) * fw],
                fc2_weight[:, which * fw : (which + 1) * fw],
            ],
            axis=1,
        ).astype(LOW)

    packs = jnp.stack([pack(0), pack(1)])
    vec = jnp.pad(vectors.astype(LOW).astype(jnp.float32).T, ((0, 2), (0, 0)))
    bias = jnp.concatenate(
        [
            half_columns(qkv_bias, hw, core).reshape(3 * hw),
            lax.dynamic_slice_in_dim(fc1_bias, core * fw, fw, 0),
        ]
    )
    bias = jnp.broadcast_to(
        lax.optimization_barrier(bias.astype(LOW)).astype(jnp.float32), (8, 3 * hw + fw)
    )
    (
        weight_qkv, weight_proj, weight_up, weight_down, vec_all, bias_all, normed_one, low, mixed, lse,
        tokens_all, grad_out_all, *tables,
    ) = gather_all(packs, vec, bias, tokens, cotangent)
    vector_rows = vec_all.transpose(1, 0, 2).reshape(8, D)
    _, _, proj_shift, gain_two, shift_two, down_shift = [
        vector_rows[i : i + 1] for i in range(6)
    ]
    bias_rows = bias_all[:, 0]
    bias_up = (
        bias_rows[:, 3 * hw :].reshape(4, 2, fw // 2).transpose(1, 0, 2).reshape(1, 4 * fw)
    )

    inputs = tokens_all[:rows].astype(jnp.float32)
    upstream = grad_out_all[:rows].astype(jnp.float32)
    middle = inputs + core_sum(mixed, weight_proj) + proj_shift
    unit_two, scale_two = norm_parts(middle)
    normed_two = both_halves((unit_two * gain_two + shift_two).astype(LOW))
    hidden = jnp.dot(normed_two, weight_up, preferred_element_type=jnp.float32) + bias_up
    active, slope = gelu_parts(hidden)
    active = active.astype(LOW)
    grad_down = contract_rows(grad_out_all, active).astype(LOW)
    layer_local = middle + core_sum(active, weight_down) + down_shift
    grad_active = jnp.dot(grad_out_all, weight_down, preferred_element_type=jnp.float32)
    grad_hidden = (grad_active * slope).astype(LOW)
    grad_up = contract_rows(normed_two, grad_hidden).astype(LOW)
    grad_bias_up = jnp.sum(grad_hidden.astype(jnp.float32), axis=0)
    grad_normed_two = core_sum(grad_hidden, weight_up)
    grad_middle = upstream + norm_back(grad_normed_two, unit_two, scale_two, gain_two)
    grad_branch = grad_middle.astype(LOW)
    grad_branch_all = both_halves(grad_branch)
    grad_proj = contract_rows(grad_branch_all, mixed).astype(LOW)
    grad_mixed = jnp.dot(
        grad_branch_all, weight_proj, preferred_element_type=jnp.float32
    ).astype(LOW)
    sums, grad_bias_qkv, norm_sums, layer_low, input_low, input_local = scatter_all(
        (grad_down, grad_up, grad_proj),
        (low, grad_mixed, lse, *tables, normed_one, weight_qkv),
        (vec_all, tokens_all, grad_middle, layer_local.astype(LOW)),
    )
    layer_out, input_grad = place_rows(layer_local, layer_low, input_local, input_low)

    vec_part = jnp.concatenate(
        [
            norm_sums[0:2],
            jnp.sum(grad_branch.astype(jnp.float32), axis=0, keepdims=True),
            jnp.sum(grad_normed_two * unit_two, axis=0, keepdims=True),
            jnp.sum(grad_normed_two, axis=0, keepdims=True),
            jnp.sum(upstream, axis=0, keepdims=True),
            jnp.zeros((2, D), jnp.float32),
        ]
    )
    db_part = jnp.concatenate(
        [
            grad_bias_qkv.reshape(4, 3, hw),
            grad_bias_up.reshape(2, 4, 2, hw).transpose(1, 0, 2, 3).reshape(4, 4, hw),
            jnp.zeros((4, 1, hw), jnp.float32),
        ],
        axis=1,
    )
    return (
        layer_out,
        input_grad,
        *tune_all(
            sums,
            vec_part,
            db_part,
            (qkv_weight, qkv_bias, proj_weight, fc1_weight, fc1_bias, fc2_weight, vectors),
            (row_state, qkv_cols, proj_cols, fc1_cols, fc2_cols),
            (vector_state, qkv_bias_state, fc1_bias_state),
        ),
    )


def solution(mesh):
    chips = mesh.shape["fsdp"] == 8 and mesh.shape["tensor"] == 4
    return jax.shard_map(
        on_chip if chips else on_device,
        mesh=mesh,
        in_specs=(
            P(("fsdp", "tensor"), None),
            P(("fsdp", "tensor"), None),
            P("fsdp", None, "tensor"),
            P(None, "tensor"),
            P("fsdp", "tensor"),
            P("fsdp", "tensor"),
            P("tensor"),
            P("fsdp", "tensor"),
            P("fsdp", None),
            P(None, "fsdp"),
            P(None, "tensor"),
            P("tensor"),
            P("tensor"),
            P("tensor"),
            P("fsdp", None),
            P(None, "tensor"),
            P("tensor"),
        ),
        out_specs=(
            P(("fsdp", "tensor"), None),
            P(("fsdp", "tensor"), None),
            P("fsdp", None, "tensor"),
            P(None, "tensor"),
            P("fsdp", "tensor"),
            P("fsdp", "tensor"),
            P("tensor"),
            P("fsdp", "tensor"),
            P("fsdp", None),
            P(None, "fsdp"),
            P(None, "tensor"),
            P("tensor"),
            P("tensor"),
            P("tensor"),
            P("fsdp", None),
            P(None, "tensor"),
            P("tensor"),
            P("fsdp", None, "tensor"),
            P(None, "tensor"),
            P("fsdp", "tensor"),
            P("fsdp", "tensor"),
            P("tensor"),
            P("fsdp", "tensor"),
            P("fsdp", None),
            P(),
        ),
        check_vma=False,
    )
```

```python
import math

import jax
import jax.numpy as jnp
from jax import lax
from jax.experimental import pallas as pl
from jax.experimental.pallas import tpu as pltpu
from jax.sharding import PartitionSpec as P

D = 1024
HD = 64
FF = 4096
GT = 4
GH = 16
GW = 16


NORM_EPS = 1e-06
DECAY = 0.5
CLIP_LEVEL = 1.0
RATE = 0.3
TINY = 1e-30
BASE = 10000.0


def layer_norm(values, gain_row, shift_row):
    center = values - jnp.mean(values, axis=-1, keepdims=True)
    variance = jnp.mean(center * center, axis=-1, keepdims=True)
    return center * lax.rsqrt(variance + NORM_EPS) * gain_row + shift_row


def exact_gelu(values):
    return jax.nn.gelu(values, approximate=False)


def rope_tables(length, half_width):
    token_index = jnp.arange(length, dtype=jnp.int32)
    coordinates = jnp.stack(
        [token_index // (GH * GW), token_index // GW % GH, token_index % GW], axis=1
    ).astype(jnp.float32)
    frequency = BASE ** (-jnp.arange(half_width, dtype=jnp.float32) / half_width)
    angles = coordinates[:, :, None] * frequency[None, None, :]
    return (jnp.cos(angles), jnp.sin(angles))


def rotate(values, cosine_table, sine_table):
    half_width = cosine_table.shape[-1]
    rotated_width = 6 * half_width
    leading = values.shape[:-1]
    pair_rows = values[..., :rotated_width].reshape(leading + (3, 2, half_width))
    first_half = pair_rows[..., 0, :]
    second_half = pair_rows[..., 1, :]
    cosine_wide = cosine_table[:, None]
    sine_wide = sine_table[:, None]
    turned = jnp.stack(
        [
            first_half * cosine_wide - second_half * sine_wide,
            second_half * cosine_wide + first_half * sine_wide,
        ],
        axis=-2,
    )
    return jnp.concatenate(
        [turned.reshape(leading + (rotated_width,)), values[..., rotated_width:]], axis=-1
    )


def contract_rows(left, right):
    return lax.dot_general(
        left, right, (((0,), (0,)), ((), ())), preferred_element_type=jnp.float32
    )


def times_transposed(left, right):
    return lax.dot_general(
        left, right, (((1,), (1,)), ((), ())), preferred_element_type=jnp.float32
    )


def forward_block(query_rows, key_rows, value_rows):
    score_scale = query_rows.shape[-1] ** (-0.5)
    scores = (
        jnp.einsum("qhd,khd->hqk", query_rows, key_rows, preferred_element_type=jnp.float32)
        * score_scale
    )
    row_peak = jnp.max(scores, axis=-1, keepdims=True)
    raised = jnp.exp(scores - row_peak)
    totals = jnp.sum(raised, axis=-1, keepdims=True)
    attention = (raised / totals).astype(jnp.bfloat16)
    mixed_rows = jnp.einsum(
        "hqk,khd->qhd", attention, value_rows, preferred_element_type=jnp.float32
    )
    return (mixed_rows, (row_peak + jnp.log(totals))[..., 0])


def backward_block(running, block_item, key_rows, value_rows):
    query_rows, log_totals, grad_mixed = block_item
    score_scale = query_rows.shape[-1] ** (-0.5)
    scores = (
        jnp.einsum("qhd,khd->hqk", query_rows, key_rows, preferred_element_type=jnp.float32)
        * score_scale
    )
    attention = jnp.exp(scores - log_totals[..., None])
    grad_attention = jnp.einsum(
        "qhd,khd->hqk", grad_mixed, value_rows, preferred_element_type=jnp.float32
    )
    grad_scores = attention * (
        grad_attention - jnp.sum(attention * grad_attention, axis=-1, keepdims=True)
    )
    grad_low = grad_scores.astype(jnp.bfloat16)
    grad_queries = (
        jnp.einsum("hqk,khd->qhd", grad_low, key_rows, preferred_element_type=jnp.float32)
        * score_scale
    )
    key_total = (
        running[0]
        + jnp.einsum("hqk,qhd->khd", grad_low, query_rows, preferred_element_type=jnp.float32)
        * score_scale
    )
    value_total = running[1] + jnp.einsum(
        "hqk,qhd->khd",
        attention.astype(jnp.bfloat16),
        grad_mixed,
        preferred_element_type=jnp.float32,
    )
    return ((key_total, value_total), grad_queries)


def on_device(
    tokens,
    cotangent,
    qkv_weight,
    qkv_bias,
    proj_weight,
    fc1_weight,
    fc1_bias,
    fc2_weight,
    vectors,
    row_state,
    qkv_cols,
    proj_cols,
    fc1_cols,
    fc2_cols,
    vector_state,
    qkv_bias_state,
    fc1_bias_state,
):
    low_type = jnp.bfloat16
    lane_count = lax.axis_size("tensor")
    local_rows = tokens.shape[0]
    group_rows = local_rows * lane_count
    length = GT * GH * GW
    clip_count = group_rows // length
    block_rows = min(512, length)
    block_count = length // block_rows
    head_width = qkv_weight.shape[2]
    head_count = head_width // HD
    hidden_width = fc1_weight.shape[1]
    shard_rows = qkv_weight.shape[0]
    cosine_table, sine_table = rope_tables(length, HD // 3 // 2)
    weight_qkv, weight_proj, weight_up, weight_down, vector_low = (
        lax.all_gather(qkv_weight.astype(low_type), "fsdp", axis=0, tiled=True),
        lax.all_gather(proj_weight.astype(low_type), "fsdp", axis=0, tiled=True),
        lax.all_gather(fc1_weight.astype(low_type), "fsdp", axis=0, tiled=True),
        lax.all_gather(fc2_weight.astype(low_type), "fsdp", axis=0, tiled=True),
        lax.all_gather(vectors.astype(low_type), "fsdp", axis=0, tiled=True),
    )
    weight_qkv = weight_qkv.reshape(D, 3 * head_width)
    vector_full = vector_low.astype(jnp.float32)
    gain_one = vector_full[:, 0]
    shift_one = vector_full[:, 1]
    proj_shift = vector_full[:, 2]
    gain_two = vector_full[:, 3]
    shift_two = vector_full[:, 4]
    down_shift = vector_full[:, 5]
    bias_qkv = (
        lax.optimization_barrier(qkv_bias.astype(low_type))
        .astype(jnp.float32)
        .reshape(3 * head_width)
    )
    bias_up = lax.optimization_barrier(fc1_bias.astype(low_type)).astype(jnp.float32)
    inputs = tokens.astype(jnp.float32)
    normed_one = layer_norm(inputs, gain_one, shift_one).astype(low_type)
    gathered_one = lax.all_gather(normed_one, "tensor", axis=0, tiled=True)
    projected = jnp.dot(gathered_one, weight_qkv, preferred_element_type=jnp.float32) + bias_qkv
    projected = projected.reshape(clip_count, length, 3, head_count, HD)
    queries = rotate(projected[:, :, 0], cosine_table, sine_table).astype(low_type)
    key_rows = rotate(projected[:, :, 1], cosine_table, sine_table).astype(low_type)
    value_rows = projected[:, :, 2].astype(low_type)

    def clip_forward(clip_item):
        query_rows, clip_keys, clip_values = clip_item
        blocks = query_rows.reshape(block_count, block_rows, head_count, HD)
        return lax.map(
            lambda query_block: forward_block(query_block, clip_keys, clip_values), blocks
        )

    mixed_rows, log_totals = lax.map(clip_forward, (queries, key_rows, value_rows))
    mixed_low = mixed_rows.reshape(group_rows, head_width).astype(low_type)
    attn_sum = lax.psum_scatter(
        times_transposed(mixed_low, weight_proj), "tensor", scatter_dimension=0, tiled=True
    )
    middle = inputs + attn_sum + proj_shift
    normed_two = layer_norm(middle, gain_two, shift_two).astype(low_type)
    gathered_two = lax.all_gather(normed_two, "tensor", axis=0, tiled=True)
    hidden = jnp.dot(gathered_two, weight_up, preferred_element_type=jnp.float32) + bias_up
    active = exact_gelu(hidden).astype(low_type)
    layer_out = (
        middle
        + lax.psum_scatter(
            times_transposed(active, weight_down), "tensor", scatter_dimension=0, tiled=True
        )
        + down_shift
    )
    upstream = cotangent.astype(jnp.float32)
    grad_out_all, normed_two_all = (
        lax.all_gather(cotangent, "tensor", axis=0, tiled=True),
        lax.all_gather(normed_two, "tensor", axis=0, tiled=True),
    )
    grad_down = contract_rows(grad_out_all, active)
    grad_active = jnp.dot(grad_out_all, weight_down, preferred_element_type=jnp.float32)
    gelu_pull = jax.vjp(exact_gelu, hidden)[1]
    grad_hidden = gelu_pull(grad_active)[0].astype(low_type)
    grad_up = contract_rows(normed_two_all, grad_hidden)
    grad_bias_up = jnp.sum(grad_hidden.astype(jnp.float32), axis=0)
    grad_normed_two = lax.psum_scatter(
        times_transposed(grad_hidden, weight_up), "tensor", scatter_dimension=0, tiled=True
    )
    middle_part, grad_gain_two, grad_shift_two = jax.vjp(layer_norm, middle, gain_two, shift_two)[
        1
    ](grad_normed_two)
    grad_middle = upstream + middle_part
    grad_branch = grad_middle.astype(low_type)
    grad_proj_shift = jnp.sum(grad_branch.astype(jnp.float32), axis=0)
    grad_down_shift = jnp.sum(upstream, axis=0)
    grad_branch_all, normed_one_all = (
        lax.all_gather(grad_branch, "tensor", axis=0, tiled=True),
        lax.all_gather(normed_one, "tensor", axis=0, tiled=True),
    )
    grad_proj = contract_rows(grad_branch_all, mixed_low)
    grad_mixed = jnp.dot(grad_branch_all, weight_proj, preferred_element_type=jnp.float32).astype(
        low_type
    )
    grad_mixed = grad_mixed.reshape(clip_count, length, head_count, HD)

    def clip_backward(clip_item):
        query_rows, clip_keys, clip_values, clip_totals, clip_grads = clip_item
        starts = (jnp.zeros(clip_keys.shape, jnp.float32), jnp.zeros(clip_keys.shape, jnp.float32))
        block_items = (
            query_rows.reshape(block_count, block_rows, head_count, HD),
            clip_totals,
            clip_grads.reshape(block_count, block_rows, head_count, HD),
        )
        sums, grad_queries = lax.scan(
            lambda running, block_item: backward_block(running, block_item, clip_keys, clip_values),
            starts,
            block_items,
        )
        return (grad_queries.reshape(query_rows.shape), sums[0], sums[1])

    grad_queries, grad_keys, grad_values = lax.map(
        clip_backward, (queries, key_rows, value_rows, log_totals, grad_mixed)
    )
    grad_projected = jnp.stack(
        [
            rotate(grad_queries, cosine_table, -sine_table),
            rotate(grad_keys, cosine_table, -sine_table),
            grad_values,
        ],
        axis=2,
    )
    grad_projected = grad_projected.reshape(group_rows, 3 * head_width).astype(low_type)
    grad_qkv = contract_rows(normed_one_all, grad_projected).reshape(D, 3, head_width)
    grad_bias_qkv = jnp.sum(grad_projected.astype(jnp.float32), axis=0)
    grad_normed_one = lax.psum_scatter(
        times_transposed(grad_projected, weight_qkv), "tensor", scatter_dimension=0, tiled=True
    )
    input_part, grad_gain_one, grad_shift_one = jax.vjp(layer_norm, inputs, gain_one, shift_one)[1](
        grad_normed_one
    )
    input_grad = grad_middle + input_part
    grad_qkv, grad_proj, grad_up, grad_down = (
        lax.psum_scatter(grad_qkv, "fsdp", scatter_dimension=0, tiled=True),
        lax.psum_scatter(grad_proj, "fsdp", scatter_dimension=0, tiled=True),
        lax.psum_scatter(grad_up, "fsdp", scatter_dimension=0, tiled=True),
        lax.psum_scatter(grad_down, "fsdp", scatter_dimension=0, tiled=True),
    )
    lane_index = lax.axis_index("tensor")
    vector_part = jnp.stack(
        [
            grad_gain_one,
            grad_shift_one,
            grad_proj_shift,
            grad_gain_two,
            grad_shift_two,
            grad_down_shift,
        ],
        axis=1,
    )
    qkv_placed = lax.dynamic_update_slice(
        jnp.zeros((3, D), jnp.float32),
        grad_bias_qkv.reshape(3, head_width),
        (jnp.int32(0), lane_index * head_width),
    )
    up_placed = lax.dynamic_update_slice(
        jnp.zeros((FF,), jnp.float32), grad_bias_up, (lane_index * hidden_width,)
    )
    vector_total, qkv_total, up_total = lax.psum(
        (vector_part, qkv_placed, up_placed), ("fsdp", "tensor")
    )
    grad_vectors = lax.dynamic_slice_in_dim(
        vector_total, lax.axis_index("fsdp") * shard_rows, shard_rows, 0
    )
    grad_qkv_bias = lax.dynamic_slice_in_dim(qkv_total, lane_index * head_width, head_width, 1)
    grad_up_bias = lax.dynamic_slice_in_dim(up_total, lane_index * hidden_width, hidden_width, 0)
    matrices = [
        (
            grad_qkv.reshape(shard_rows, 3 * head_width),
            qkv_weight.reshape(shard_rows, 3 * head_width),
            qkv_cols.reshape(3 * head_width),
        ),
        (grad_proj, proj_weight, proj_cols),
        (grad_up, fc1_weight, fc1_cols),
        (grad_down, fc2_weight, fc2_cols),
    ]
    column_counts = [3 * D, D, FF, FF]
    column_weights = jnp.array(column_counts, jnp.float32)
    qkv_state_new = DECAY * qkv_bias_state + (1.0 - DECAY) * (grad_qkv_bias * grad_qkv_bias + TINY)
    qkv_direction = grad_qkv_bias * lax.rsqrt(qkv_state_new)
    up_state_new = DECAY * fc1_bias_state + (1.0 - DECAY) * (grad_up_bias * grad_up_bias + TINY)
    up_direction = grad_up_bias * lax.rsqrt(up_state_new)
    row_squares = jnp.stack(
        [jnp.sum(matrix_entry[0] * matrix_entry[0], axis=1) for matrix_entry in matrices]
    )
    weight_squares = jnp.stack(
        [jnp.sum(matrix_entry[1] * matrix_entry[1]) for matrix_entry in matrices]
    )
    bias_terms = jnp.stack(
        [
            jnp.sum(qkv_direction * qkv_direction),
            jnp.sum(up_direction * up_direction),
            jnp.sum(qkv_bias * qkv_bias),
            jnp.sum(fc1_bias * fc1_bias),
        ]
    )
    row_total, weight_partial, bias_total = lax.psum(
        (row_squares, weight_squares, bias_terms), "tensor"
    )
    rows_new = DECAY * row_state + (1.0 - DECAY) * (row_total / column_weights[:, None] + TINY)
    vector_state_new = DECAY * vector_state + (1.0 - DECAY) * (grad_vectors * grad_vectors + TINY)
    vector_direction = grad_vectors * lax.rsqrt(vector_state_new)
    vector_terms = jnp.stack(
        [jnp.sum(vector_direction * vector_direction, axis=0), jnp.sum(vectors * vectors, axis=0)]
    )
    col_squares = jnp.concatenate(
        [jnp.sum(matrix_entry[0] * matrix_entry[0], axis=0) for matrix_entry in matrices]
    )
    row_new_sums = jnp.sum(rows_new, axis=1)
    col_total, row_new_total, weight_total, vector_sums = lax.psum(
        (col_squares, row_new_sums, weight_partial, vector_terms), "fsdp"
    )
    mean_rows = row_new_total / D
    offsets = [0]
    for matrix_entry in matrices:
        offsets.append(offsets[-1] + matrix_entry[0].shape[1])
    cols_list = []
    direction_list = []
    square_list = []
    for position, matrix_entry in enumerate(matrices):
        col_slice = col_total[offsets[position] : offsets[position + 1]]
        cols_new = DECAY * matrix_entry[2] + (1.0 - DECAY) * (col_slice / D + TINY)
        direction = matrix_entry[0] * lax.rsqrt(
            rows_new[position][:, None] * cols_new[None, :] / mean_rows[position]
        )
        cols_list.append(cols_new)
        direction_list.append(direction)
        square_list.append(jnp.sum(direction * direction))
    square_total = lax.psum(jnp.stack(square_list), ("fsdp", "tensor"))
    matrix_count = D * column_weights
    update_rms = jnp.sqrt(square_total / matrix_count)
    weight_scale = jnp.sqrt(weight_total / matrix_count)
    new_weights = []
    for position, matrix_entry in enumerate(matrices):
        new_weights.append(
            matrix_entry[1]
            - RATE
            * weight_scale[position]
            * direction_list[position]
            / jnp.maximum(1.0, update_rms[position] / CLIP_LEVEL)
        )
    vector_rms = jnp.sqrt(vector_sums[0] / D)
    vector_scale = jnp.sqrt(vector_sums[1] / D)
    vectors_new = vectors - RATE * vector_scale * vector_direction / jnp.maximum(
        1.0, vector_rms / CLIP_LEVEL
    )
    qkv_rms = jnp.sqrt(bias_total[0] / (3 * D))
    qkv_scale = jnp.sqrt(bias_total[2] / (3 * D))
    qkv_bias_new = qkv_bias - RATE * qkv_scale * qkv_direction / jnp.maximum(
        1.0, qkv_rms / CLIP_LEVEL
    )
    up_rms = jnp.sqrt(bias_total[1] / FF)
    up_scale = jnp.sqrt(bias_total[3] / FF)
    up_bias_new = fc1_bias - RATE * up_scale * up_direction / jnp.maximum(1.0, up_rms / CLIP_LEVEL)
    return (
        layer_out,
        input_grad,
        grad_qkv,
        grad_qkv_bias,
        grad_proj,
        grad_up,
        grad_up_bias,
        grad_down,
        grad_vectors,
        rows_new,
        cols_list[0].reshape(3, head_width),
        cols_list[1],
        cols_list[2],
        cols_list[3],
        vector_state_new,
        qkv_state_new,
        up_state_new,
        new_weights[0].reshape(shard_rows, 3, head_width),
        qkv_bias_new,
        new_weights[1],
        new_weights[2],
        up_bias_new,
        new_weights[3],
        vectors_new,
        update_rms,
    )


SCALE = HD**-0.5
LENGTH = GT * GH * GW
ROLL = HD // 3 // 2
CORE_SWAP = [(i, i ^ 1) for i in range(8)]
LOW = jnp.bfloat16
QB = 256


def rotary_rows(first, core):
    token = (lax.broadcasted_iota(jnp.int32, (128, 2 * HD), 0) + first + core * (LENGTH // 2)) & (
        LENGTH - 1
    )
    lane = lax.broadcasted_iota(jnp.int32, (128, 2 * HD), 1) & (HD - 1)
    past_one, past_two = lane >= 2 * ROLL, lane >= 4 * ROLL
    live = lane < 6 * ROLL
    within = lane - jnp.where(past_two, 4 * ROLL, jnp.where(past_one, 2 * ROLL, 0))
    second = within >= ROLL
    step = jnp.where(second, within - ROLL, within).astype(jnp.float32)
    coordinate = jnp.where(
        past_two, token & (GW - 1), jnp.where(past_one, (token >> 4) & (GH - 1), token >> 8)
    ).astype(jnp.float32)
    angle = jnp.where(live, coordinate * jnp.exp(step * (-math.log(BASE) / ROLL)), 0.0)
    cosine = jnp.cos(angle)
    sine = jnp.sin(angle)
    from_first = jnp.where(live & second, sine, 0.0)
    from_second = jnp.where(live, jnp.where(second, 0.0, -sine), 0.0)
    return cosine, from_first, from_second


def turn(v, c, s1, s2, sign):
    return v * c + sign * (pltpu.roll(v, ROLL, 1) * s1 + pltpu.roll(v, 2 * HD - ROLL, 1) * s2)


def dot_nt(a, b):
    return lax.dot_general(a, b, (((1,), (1,)), ((), ())), preferred_element_type=jnp.float32)


def dot_tn(a, b):
    return lax.dot_general(a, b, (((0,), (0,)), ((), ())), preferred_element_type=jnp.float32)


def dot_nn(a, b):
    return lax.dot_general(a, b, (((1,), (0,)), ((), ())), preferred_element_type=jnp.float32)


MESH = pl.DeviceIdType.MESH
PIECES = ((0, 0, 384, 0), (1, 384, 128, 0), (2, 512, 256, 0), (2, 768, 256, 1024), (3, 1024, 256, 0), (3, 1280, 256, 1024))
SHARD = 128
PLANE_FIRST = (3,)
HALVES = ((0, 64), (64, 64))
WHOLE = ((0, 128),)
MIB = 1024 * 1024


def split(piece_and_rows):
    return [
        (piece, r, at, rows, early)
        for piece, parts, early in piece_and_rows
        for at, rows in parts
        for r in range(2)
    ]


def remote(src, dst, send, recv, target):
    return pltpu.make_async_remote_copy(
        src_ref=src, dst_ref=dst, send_sem=send, recv_sem=recv, device_id=target, device_id_type=MESH
    )


def flip(index, bit):
    return index + bit - 2 * bit * ((index // bit) % 2)


def peers():
    lane = lax.axis_index("tensor")
    shard = lax.axis_index("fsdp")
    is_mid = (lane == 1) | (lane == 2)
    pair = {"tensor": flip(lane, 1)}
    across = {"tensor": 3 - lane}
    x_peer = {"fsdp": flip(shard, 2)}
    y_peer = {"fsdp": flip(shard, 4)}
    return lane, shard, is_mid, pair, across, x_peer, y_peer


def meet(targets):
    barrier = pltpu.get_barrier_semaphore()
    for target in targets:
        pl.semaphore_signal(barrier, inc=1, device_id=target, device_id_type=MESH)
    pl.semaphore_wait(barrier, len(targets))


GATHER = split(
    [(PIECES[0], HALVES, False)] + [(piece, WHOLE, i in PLANE_FIRST) for i, piece in enumerate(PIECES) if i]
)


def gather_kernel(
    packs_ref, vec_ref, bias_ref, tokens_ref, cotangent_ref,
    qkv_ref, proj_ref, up_ref, down_ref, vec_all, bias_all, h_ref, low_ref, o_ref, lse_ref,
    x_ref, gy_ref, c_ref, s1_ref, s2_ref,
    pack_ref, stage_ref, wq_ref, kh_ref, vh_ref,
    load_sem, local_sem, send_sem, recv_sem, small_send, small_recv, row_send, row_recv,
):
    lane, shard, is_mid, pair, across, x_peer, y_peer = peers()
    core = shard % 2
    outs = (qkv_ref, proj_ref, up_ref, down_ref)
    shard_peers = [
        (q, dc, {"fsdp": flip_place(shard, q, dc)})
        for q in range(4)
        for dc in range(2)
        if (q, dc) != (0, 0)
    ]
    lane_peers = [pair, {"tensor": (lane + 2) % 4}, across]
    other_core = {"fsdp": flip(shard, 1)}
    cross = {"fsdp": flip(shard, 1), "tensor": flip(lane, 1)}
    meet([t for _, _, t in shard_peers] + lane_peers + [cross])
    moved = (core + lane) % 2 == 1
    half = LENGTH // 2

    def permuted(index, src_ref, dst_ref):
        for r in range(2):
            for q in range(4):
                at = pl.ds(pl.multiple_of(global_block(shard, r, q) * SHARD, SHARD), SHARD)
                block = r * 4 + q
                dst_ref[index, :, block * SHARD : (block + 1) * SHARD] = src_ref[:, at]

    def hop_swap(k, dst_ref):
        return remote(
            stage_ref.at[k], dst_ref.at[pl.ds(0, half)], row_send.at[k, 0], row_recv.at[k, 0], cross
        )

    def hop_core(k, dst_ref):
        return remote(
            dst_ref.at[pl.ds(0, half)], dst_ref.at[pl.ds(half, half)], row_send.at[k, 1], row_recv.at[k, 1], other_core
        )

    def rows_out(k, src_ref, dst_ref):
        permuted(k, src_ref, stage_ref)

        @pl.when(moved)
        def _():
            hop_swap(k, dst_ref).start()

        @pl.when(jnp.logical_not(moved))
        def _():
            dst_ref[0:half, :] = stage_ref[k]
            hop_core(k, dst_ref).start()

    def rows_on(k, dst_ref):
        @pl.when(moved)
        def _():
            hop_swap(k, dst_ref).wait_recv()
            hop_core(k, dst_ref).start()

    def rows_in(k, dst_ref):
        hop_core(k, dst_ref).wait()

        @pl.when(moved)
        def _():
            hop_swap(k, dst_ref).wait_send()

    pack_hop = remote(packs_ref.at[1 - core], pack_ref.at[core], row_send.at[2, 0], row_recv.at[2, 0], other_core)
    pack_hop.start()
    pack_ref[core] = packs_ref[core]

    def window(c, block, col0, col_count):
        (m, _, width, base), r, at, rows, _ = GATHER[c]
        return outs[m].at[
            pl.ds((r * 4 + block) * SHARD + at, rows), pl.ds(base + col0 * width, col_count * width)
        ]

    def own(c):
        (_, first, width, _), r, at, rows, _ = GATHER[c]
        return pack_ref.at[r, pl.ds(at, rows), pl.ds(first, width)]

    def local(c):
        return pltpu.make_async_copy(own(c), window(c, 0, 0, 1), local_sem.at[c])

    def plane_first(c):
        return GATHER[c][4]

    def plane(c):
        return ((1, x_peer), (2, y_peer))[GATHER[c][1]]

    def blocks(c):
        return (0, plane(c)[0]) if plane_first(c) else (0,)

    def hop_pair(c):
        return [
            remote(
                own(c) if b == 0 else window(c, b, 0, 1), window(c, b, 1, 1),
                send_sem.at[c, 6 * k], recv_sem.at[c, 5 * k], pair,
            )
            for k, b in enumerate(blocks(c))
        ]

    def hop_across(c):
        return [
            remote(
                window(c, b, 0, 2), window(c, b, 2, 2), send_sem.at[c, 1 + 6 * k], recv_sem.at[c, 1 + 5 * k], across
            )
            for k, b in enumerate(blocks(c))
        ]

    def hop_out(c):
        return [
            remote(
                window(c, b, 2, 2), window(c, b, 2, 2), send_sem.at[c, 2 + 6 * k], recv_sem.at[c, 1 + 5 * k], pair
            )
            for k, b in enumerate(blocks(c))
        ]

    def hop_first(c):
        block, target = plane(c)
        if plane_first(c):
            return remote(
                own(c), window(c, block, 0, 1), send_sem.at[c, 3], recv_sem.at[c, 2], target
            )
        return remote(
            window(c, 0, 0, 4), window(c, block, 0, 4), send_sem.at[c, 3], recv_sem.at[c, 2], target
        )

    def hop_second(c):
        moves, target = ((((0, 2), (1, 3)), y_peer), (((0, 1), (2, 3)), x_peer))[GATHER[c][1]]
        return [
            remote(
                window(c, src, 0, 4), window(c, dst, 0, 4), send_sem.at[c, 4 + k], recv_sem.at[c, 3 + k], target
            )
            for k, (src, dst) in enumerate(moves)
        ]

    count = len(GATHER)
    small = []
    slot = core * 4
    vec_all[pl.ds(slot, 1)] = vec_ref[...][None]
    bias_all[0] = bias_ref[...]
    for i, (q, _, target) in enumerate(shard_peers):
        small.append(remote(vec_ref, vec_all.at[slot + q], small_send.at[i], small_recv.at[i], target))
    far_slot = 3 - is_mid.astype(jnp.int32)
    for i, target in enumerate(lane_peers):
        to = bias_all.at[1] if i == 0 else bias_all.at[far_slot]
        small.append(remote(bias_ref, to, small_send.at[7 + i], small_recv.at[7 + i], target))

    def start(copies):
        for copy in copies:
            copy.start()

    def arrive(copies):
        for copy in copies:
            copy.wait_recv()

    def begin(c):
        if plane_first(c):
            hop_first(c).start()
        else:
            start(hop_pair(c))

    def to_far(c):
        local(c).wait()
        arrive(hop_pair(c))

        @pl.when(is_mid)
        def _():
            start(hop_across(c))

    def into_plane(c):
        if plane_first(c):
            start(hop_second(c))
        else:
            hop_first(c).start()

    def on_mid(c):
        @pl.when(is_mid)
        def _():
            arrive(hop_across(c))
            start(hop_out(c))
            into_plane(c)

    def on_end(c):
        @pl.when(jnp.logical_not(is_mid))
        def _():
            arrive(hop_across(c))
            into_plane(c)

    def to_pair(c):
        hop_first(c).wait_recv()
        start(hop_pair(c))

    def finish(c):
        hop_first(c).wait_recv()
        start(hop_second(c))

    def each(step, *chunks):
        for c in chunks:
            step(c)

    for copy in small:
        copy.start()
    pack_hop.wait()
    each(begin, 0, 1, 2, 3, 8, 9, 4, 5, 6, 7)
    for c in range(count):
        local(c).start()
    each(to_far, 0, 1, 2, 3)
    each(on_mid, 0, 1, 2, 3)
    rows_out(0, tokens_ref, x_ref)
    each(on_end, 0, 1, 2, 3)

    @pl.loop(0, LENGTH // 128)
    def _(i):
        rows = pl.ds(pl.multiple_of(i * 128, 128), 128)
        c_ref[rows, :], s1_ref[rows, :], s2_ref[rows, :] = rotary_rows(i * 128, core)

    each(to_far, 4, 5)
    each(finish, 0, 1, 2, 3)
    rows_on(0, x_ref)
    each(on_mid, 4, 5)
    each(to_far, 6, 7)
    for copy in small:
        copy.wait()
    rows_in(0, x_ref)
    gain = jnp.concatenate([vec_all[b, 0:1, :] for b in range(8)], axis=1)
    shift = jnp.concatenate([vec_all[b, 1:2, :] for b in range(8)], axis=1)

    @pl.loop(0, LENGTH // 64)
    def _(i):
        rows = pl.ds(pl.multiple_of(i * 64, 64), 64)
        unit, _ = norm_parts(x_ref[rows, :].astype(jnp.float32))
        h_ref[rows, :] = (unit * gain + shift).astype(LOW)

    first = 4
    each(on_end, 4, 5)
    each(on_mid, 6, 7)
    each(finish, 4, 5)
    each(on_end, 6, 7)
    for c in range(first):
        for copy in hop_second(c):
            copy.wait_recv()
    load = pltpu.make_async_copy(qkv_ref, wq_ref, load_sem.at[0])
    load.start()
    load.wait()
    width = 2 * HD
    lane_q = lax.broadcasted_iota(jnp.int32, (QB, width), 1)

    plan = (
        ((to_pair, (8, 9)),),
        ((to_far, (8, 9)), (begin, (10, 11, 12, 13))),
        ((on_mid, (8, 9)), (finish, (6, 7))),
        ((on_end, (8, 9)), (to_far, (10, 11))),
        ((on_mid, (10, 11)),),
        ((on_end, (10, 11)), (to_far, (12, 13))),
        ((on_mid, (12, 13)),),
        ((on_end, (12, 13)),),
    )

    @pl.loop(0, 8)
    def _(t):
        z = t // 2
        base = z * 3 * width

        def columns(part):
            return pl.ds(pl.multiple_of(base + part * width, width), width)

        @pl.when(t % 2 == 0)
        def _():
            bias = bias_all[pl.ds(z, 1), 0:1, 0 : 3 * width][0]

            @pl.loop(0, LENGTH // QB)
            def _(i):
                rows = pl.ds(pl.multiple_of(i * QB, QB), QB)
                weights = wq_ref[:, pl.ds(pl.multiple_of(base, width), 3 * width)]
                qkv = dot_nn(h_ref[rows, :], weights) + bias
                c, s1, s2 = c_ref[rows, :], s1_ref[rows, :], s2_ref[rows, :]
                low_ref[rows, columns(0)] = turn(qkv[:, :width], c, s1, s2, 1.0).astype(LOW)
                k = turn(qkv[:, width : 2 * width], c, s1, s2, 1.0)
                v = qkv[:, 2 * width :]
                low_ref[rows, columns(1)] = k.astype(LOW)
                low_ref[rows, columns(2)] = v.astype(LOW)
                for h in range(2):
                    mine = (lane_q < HD) if h == 0 else (lane_q >= HD)
                    kh_ref[h, rows, :] = jnp.where(mine, k, 0.0).astype(LOW)
                    vh_ref[h, rows, :] = jnp.where(mine, v, 0.0).astype(LOW)

        for k, steps in enumerate(plan):

            @pl.when(t == k)
            def _():
                for step, chunks in steps:
                    each(step, *chunks)
                if k == 7:
                    rows_out(1, cotangent_ref, gy_ref)

        @pl.loop(0, 2)
        def _(half):
            rows = pl.ds(pl.multiple_of(((t % 2) * 2 + half) * QB, QB), QB)
            q = (low_ref[rows, columns(0)].astype(jnp.float32) * SCALE).astype(LOW)
            total = jnp.zeros((width, QB), jnp.float32)
            for h in range(2):
                s = dot_nt(kh_ref[h], q)
                peak = jnp.max(s, axis=0, keepdims=True)
                e = jnp.exp(s - peak)
                mass = jnp.sum(e, axis=0, keepdims=True)
                p = (e * (1.0 / mass)).astype(LOW)
                total += dot_tn(vh_ref[h], p)
                lse_ref[pl.ds(z, 1), h : h + 1, rows] = (peak + jnp.log(mass))[None]
            o_ref[rows, pl.ds(pl.multiple_of(z * width, width), width)] = total.T.astype(LOW)

    each(finish, 10, 11)
    rows_on(1, gy_ref)
    each(finish, 12, 13)
    rows_in(1, gy_ref)
    for c in range(count):
        for copy in hop_second(c):
            copy.wait_send()
            if c >= first:
                copy.wait_recv()
        for copy in hop_pair(c):
            copy.wait_send()
        hop_first(c).wait_send()

        @pl.when(is_mid)
        def _():
            for copy in hop_across(c) + hop_out(c):
                copy.wait_send()


def global_block(shard, r, q):
    return flip_place(shard - shard % 2 + r, q, 0)


def flip_place(shard, q, dc):
    target = shard
    for bit, on in ((1, dc), (2, q & 1), (4, q >> 1)):
        if on:
            target = flip(target, bit)
    return target


def gather_all(packs, vec, bias, tokens, cotangent):
    count = len(GATHER)
    rows = 8 * SHARD
    any_space = pl.BlockSpec(memory_space=pl.ANY)
    vmem = pl.BlockSpec(memory_space=pltpu.VMEM)
    width = 2 * HD
    return pl.pallas_call(
        gather_kernel,
        in_specs=[vmem] * 5,
        out_specs=[any_space] * 4 + [vmem] * 11,
        out_shape=[
            jax.ShapeDtypeStruct((rows, 1536), LOW),
            jax.ShapeDtypeStruct((rows, 512), LOW),
            jax.ShapeDtypeStruct((rows, 2048), LOW),
            jax.ShapeDtypeStruct((rows, 2048), LOW),
            jax.ShapeDtypeStruct((8,) + vec.shape, jnp.float32),
            jax.ShapeDtypeStruct((4,) + bias.shape, jnp.float32),
            jax.ShapeDtypeStruct((LENGTH, D), LOW),
            jax.ShapeDtypeStruct((LENGTH, 1536), LOW),
            jax.ShapeDtypeStruct((LENGTH, 512), LOW),
            jax.ShapeDtypeStruct((4, 2, LENGTH), jnp.float32),
            jax.ShapeDtypeStruct((LENGTH, D), LOW),
            jax.ShapeDtypeStruct((LENGTH, D), LOW),
            jax.ShapeDtypeStruct((LENGTH, width), jnp.float32),
            jax.ShapeDtypeStruct((LENGTH, width), jnp.float32),
            jax.ShapeDtypeStruct((LENGTH, width), jnp.float32),
        ],
        scratch_shapes=[
            pltpu.VMEM((2, SHARD, 1536), LOW),
            pltpu.VMEM((2, LENGTH // 2, D), LOW),
            pltpu.VMEM((D, 1536), LOW),
            pltpu.VMEM((2, LENGTH, width), LOW),
            pltpu.VMEM((2, LENGTH, width), LOW),
            pltpu.SemaphoreType.DMA((1,)),
            pltpu.SemaphoreType.DMA((count,)),
            pltpu.SemaphoreType.DMA((count, 9)),
            pltpu.SemaphoreType.DMA((count, 7)),
            pltpu.SemaphoreType.DMA((10,)),
            pltpu.SemaphoreType.DMA((10,)),
            pltpu.SemaphoreType.DMA((3, 2)),
            pltpu.SemaphoreType.DMA((3, 2)),
        ],
        compiler_params=pltpu.CompilerParams(
            collective_id=1, has_side_effects=True, vmem_limit_bytes=48 * MIB
        ),
        name="gather_attend",
    )(packs, vec, bias, tokens, cotangent)


SUMMED = (
    (0, 0, 256, 0),
    (0, 256, 256, 1024),
    (1, 512, 256, 0),
    (1, 768, 256, 1024),
    (2, 1024, 128, 0),
    (3, 1152, 384, 0),
)
SUM_PLANE_LAST = (1, 2)
SCATTER = split(
    [(piece, WHOLE, i in SUM_PLANE_LAST) for i, piece in enumerate(SUMMED[:5])] + [(SUMMED[5], HALVES, False)]
)
EXTRA_AT, EXTRA_WIDTH = 256, 512
SUM_WIDTH = 1536


def scatter_kernel(
    down_ref, up_ref, proj_ref, low_ref, go_ref, lse_ref, c_ref, s1_ref, s2_ref, h_ref, wq_ref,
    vec_ref, x_ref, gx_ref, layer_ref,
    out_ref, bias_ref, norm_ref, layer_out, input_out, gh_ref,
    other_ref, low_stage, gq_ref, g_ref, kh_ref, vh_ref, gk_ref, gv_ref,
    own_ref, first_ref, second_ref, in_ref, mid_ref, near_ref, in_more, mid_more, near_more,
    local_sem, send_sem, recv_sem, row_send, row_recv,
):
    grads = (down_ref, up_ref, proj_ref, gq_ref)
    lane, shard, is_mid, pair, across, x_peer, y_peer = peers()
    barrier = pltpu.get_barrier_semaphore()
    other_core = {"fsdp": flip(shard, 1)}
    cross = {"fsdp": flip(shard, 1), "tensor": flip(lane, 1)}
    moved = (shard % 2 + lane) % 2 == 1
    half = LENGTH // 2
    for target in (pair, x_peer, y_peer, other_core, cross):
        pl.semaphore_signal(barrier, inc=1, device_id=target, device_id_type=MESH)

    @pl.when(is_mid)
    def _():
        pl.semaphore_signal(barrier, inc=1, device_id=across, device_id_type=MESH)

    pl.semaphore_wait(barrier, 5 + is_mid.astype(jnp.int32))

    def hop_rows(k, src, dst):
        return remote(src, dst, row_send.at[k], row_recv.at[k], cross)

    hop_sum = remote(gh_ref.at[pl.ds(half, half)], other_ref, row_send.at[2], row_recv.at[2], other_core)

    def source(c, block):
        (a, _, width, base), r, at, rows, _ = SCATTER[c]
        return grads[a].at[pl.ds((r * 4 + block) * SHARD + at, rows), pl.ds(base, 4 * width)]

    def part(ref, c, block, lo, hi, each):
        (_, first, width, _), r, at, rows, _ = SCATTER[c]
        if ref is in_more or ref is mid_more or ref is near_more:
            first -= EXTRA_AT
        return ref.at[
            r, pl.ds(block * SHARD + at, rows), pl.ds(first * each + lo * width, (hi - lo) * width)
        ]

    def plane_last(c):
        return SCATTER[c][4]

    def keep(c):
        blocks = ((0, 1), (0, 2))[SCATTER[c][1]]
        return [
            pltpu.make_async_copy(source(c, block), part(own_ref, c, k, 0, 4, 4), local_sem.at[c, k])
            for k, block in enumerate(blocks)
        ]

    def hop_first(c):
        blocks, target = (((2, 3), y_peer), ((1, 3), x_peer))[SCATTER[c][1]]
        return [
            remote(
                source(c, block), part(first_ref, c, k, 0, 4, 4), send_sem.at[c, k], recv_sem.at[c, k], target
            )
            for k, block in enumerate(blocks)
        ]

    def hop_second(c):
        hi = 1 if plane_last(c) else 4
        return remote(
            part(own_ref, c, 1, 0, hi, 4), part(second_ref, c, 0, 0, hi, 4),
            send_sem.at[c, 2], recv_sem.at[c, 2], (x_peer, y_peer)[SCATTER[c][1]],
        )

    def sides(c, ref, more):
        return (ref, more) if plane_last(c) else (ref,)

    def hop_in(c):
        return [
            remote(
                part(own_ref, c, k, 2, 4, 4), part(ref, c, 0, 0, 2, 2),
                send_sem.at[c, 3 + 2 * k], recv_sem.at[c, 3 + 3 * k], pair,
            )
            for k, ref in enumerate(sides(c, in_ref, in_more))
        ]

    def hop_across(c):
        return [
            remote(
                part(own_ref, c, k, 2, 4, 4), part(ref, c, 0, 0, 2, 2),
                send_sem.at[c, 3 + 2 * k], recv_sem.at[c, 4 + 3 * k], across,
            )
            for k, ref in enumerate(sides(c, mid_ref, mid_more))
        ]

    def hop_pair(c):
        return [
            remote(
                part(own_ref, c, k, 1, 2, 4), part(ref, c, 0, 0, 1, 1),
                send_sem.at[c, 4 + 2 * k], recv_sem.at[c, 5 + 3 * k], pair,
            )
            for k, ref in enumerate(sides(c, near_ref, near_more))
        ]

    def start(copies):
        for copy in copies:
            copy.start()

    def arrive(copies):
        for copy in copies:
            copy.wait_recv()

    def add(dst, left, right):
        step = 16

        @pl.loop(0, dst.shape[0] // step)
        def _(i):
            at = pl.ds(pl.multiple_of(i * step, step), step)
            total = left[at, :].astype(jnp.float32) + right[at, :].astype(jnp.float32)
            dst[at, :] = total.astype(dst.dtype)

    count = len(SCATTER)
    lead = 2

    def inward(c):
        @pl.when(jnp.logical_not(is_mid))
        def _():
            start(hop_in(c))

    def to_middle(c):
        @pl.when(is_mid)
        def _():
            arrive(hop_in(c))
            for k, ref in enumerate(sides(c, in_ref, in_more)):
                far = part(own_ref, c, k, 2, 4, 4)
                add(far, far, part(ref, c, 0, 0, 2, 2))
            start(hop_across(c))

    def from_middle(c):
        @pl.when(is_mid)
        def _():
            arrive(hop_across(c))
            for k, ref in enumerate(sides(c, mid_ref, mid_more)):
                near = part(own_ref, c, k, 0, 2, 4)
                add(near, near, part(ref, c, 0, 0, 2, 2))

        start(hop_pair(c))

    def tick(now):
        c = now
        if c < count:
            if c + lead < count:
                for copy in hop_first(c + lead):
                    copy.start()
                for copy in keep(c + lead):
                    copy.start()
            for copy in keep(c):
                copy.wait()
            for copy in hop_first(c):
                copy.wait_recv()
            mine = part(own_ref, c, 1, 0, 4, 4)
            add(mine, mine, part(first_ref, c, 1, 0, 4, 4))
            if not plane_last(c):
                hop_second(c).start()
            mine = part(own_ref, c, 0, 0, 4, 4)
            add(mine, mine, part(first_ref, c, 0, 0, 4, 4))
            if plane_last(c):
                inward(c)
        c = now - 2
        if 0 <= c < count:
            if plane_last(c):
                to_middle(c)
            else:
                hop_second(c).wait_recv()
                mine = part(own_ref, c, 0, 0, 4, 4)
                add(mine, mine, part(second_ref, c, 0, 0, 4, 4))
                inward(c)
        c = now - 3
        if 0 <= c < count:
            if plane_last(c):
                from_middle(c)
            else:
                to_middle(c)
        c = now - 4
        if 0 <= c < count:
            if plane_last(c):
                arrive(hop_pair(c))
                for k, ref in ((1, near_more), (0, near_ref)):
                    mine = part(own_ref, c, k, 0, 1, 4)
                    add(mine, mine, part(ref, c, 0, 0, 1, 1))
                    if k:
                        hop_second(c).start()
            else:
                from_middle(c)
        c = now - 5
        if 0 <= c < count:
            if plane_last(c):
                hop_second(c).wait_recv()
                last = part(second_ref, c, 0, 0, 1, 4)
            else:
                arrive(hop_pair(c))
                last = part(near_ref, c, 0, 0, 1, 1)
            add(part(out_ref, c, 0, 0, 1, 1), part(own_ref, c, 0, 0, 1, 4), last)

    for c in range(lead):
        for copy in hop_first(c):
            copy.start()
        for copy in keep(c):
            copy.start()

    @pl.when(moved)
    def _():
        hop_rows(0, layer_ref, layer_out).start()

    width = 2 * HD
    lane_q = lax.broadcasted_iota(jnp.int32, (QB, width), 1)

    @pl.loop(0, 8)
    def _(t):
        z = t // 2
        base = z * 3 * width

        def columns(part_index):
            return pl.ds(pl.multiple_of(base + part_index * width, width), width)

        @pl.when(t % 2 == 0)
        def _():
            @pl.loop(0, LENGTH // QB)
            def _(i):
                rows = pl.ds(pl.multiple_of(i * QB, QB), QB)
                k = low_ref[rows, columns(1)].astype(jnp.float32)
                v = low_ref[rows, columns(2)].astype(jnp.float32)
                for h in range(2):
                    mine = (lane_q < HD) if h == 0 else (lane_q >= HD)
                    kh_ref[h, rows, :] = jnp.where(mine, k, 0.0).astype(LOW)
                    vh_ref[h, rows, :] = jnp.where(mine, v, 0.0).astype(LOW)

            gk_ref[...] = jnp.zeros_like(gk_ref)
            gv_ref[...] = jnp.zeros_like(gv_ref)

        for k in range(2, 8):

            @pl.when(t == k)
            def _():
                tick(k - 2)

        @pl.loop(0, 2)
        def _(half):
            rows = pl.ds(pl.multiple_of(((t % 2) * 2 + half) * QB, QB), QB)
            q = low_ref[rows, columns(0)].astype(jnp.float32) * SCALE
            go = go_ref[rows, pl.ds(pl.multiple_of(z * width, width), width)].astype(jnp.float32)
            total = jnp.zeros((width, QB), jnp.float32)
            for h in range(2):
                mine = (lane_q < HD) if h == 0 else (lane_q >= HD)
                qh = jnp.where(mine, q, 0.0).astype(LOW)
                gh = jnp.where(mine, go, 0.0).astype(LOW)
                p = jnp.exp(dot_nt(kh_ref[h], qh) - lse_ref[pl.ds(z, 1), h : h + 1, rows][0])
                dp = dot_nt(vh_ref[h], gh)
                pd = jnp.sum(p * dp, axis=0, keepdims=True)
                ds = (p * (dp - pd)).astype(LOW)
                gv_ref[...] += dot_nn(p.astype(LOW), gh)
                gk_ref[...] += dot_nn(ds, qh)
                total += dot_tn(kh_ref[h], ds)
            gq = turn(total.T * SCALE, c_ref[rows, :], s1_ref[rows, :], s2_ref[rows, :], -1.0)
            g_ref[rows, :width] = gq.astype(LOW)

        @pl.when(t % 2 == 1)
        def _():
            wide = pl.ds(pl.multiple_of(base, width), 3 * width)
            gk = turn(gk_ref[...], c_ref[...], s1_ref[...], s2_ref[...], -1.0)
            g_ref[:, width : 2 * width] = gk.astype(LOW)
            g_ref[:, 2 * width :] = gv_ref[...].astype(LOW)
            bias_ref[:, wide] = jnp.sum(g_ref[...].astype(jnp.float32), axis=0, keepdims=True)

            @pl.loop(0, D // QB)
            def _(i):
                some = pl.ds(pl.multiple_of(i * QB, QB), QB)
                gq_ref[some, wide] = dot_tn(h_ref[:, some], g_ref[...]).astype(LOW)
                product = dot_nt(g_ref[some, :], wq_ref[:, wide])

                @pl.when(z == 0)
                def _():
                    gh_ref[some, :] = product

                @pl.when(z > 0)
                def _():
                    gh_ref[some, :] += product

    hop_sum.start()
    tick(6)
    gain = jnp.concatenate([vec_ref[b, 0:1, :] for b in range(8)], axis=1)
    norm_ref[...] = jnp.zeros_like(norm_ref)
    hop_sum.wait()

    @pl.loop(0, half // 64)
    def _(i):
        some = pl.ds(pl.multiple_of(i * 64, 64), 64)
        grad = gh_ref[some, :] + other_ref[some, :]
        unit, scale = norm_parts(x_ref[some, :].astype(jnp.float32))
        norm_ref[0:1, :] += jnp.sum(grad * unit, axis=0, keepdims=True)
        norm_ref[1:2, :] += jnp.sum(grad, axis=0, keepdims=True)
        value = gx_ref[some, :] + norm_back(grad, unit, scale, gain)
        gh_ref[some, :] = value
        low_stage[some, :] = value.astype(LOW)

    @pl.when(moved)
    def _():
        hop_rows(1, low_stage, input_out).start()

    for now in range(7, count + 5):
        tick(now)

    @pl.when(moved)
    def _():
        hop_rows(0, layer_ref, layer_out).wait()
        hop_rows(1, low_stage, input_out).wait()

    for c in range(count):
        for copy in hop_first(c):
            copy.wait_send()
        hop_second(c).wait_send()
        for copy in hop_pair(c):
            copy.wait_send()

        @pl.when(is_mid)
        def _():
            for copy in hop_across(c):
                copy.wait_send()

        @pl.when(jnp.logical_not(is_mid))
        def _():
            for copy in hop_in(c):
                copy.wait_send()


def scatter_all(grads, attention, rows):
    count = len(SCATTER)
    width = SUM_WIDTH
    vmem = pl.BlockSpec(memory_space=pltpu.VMEM)
    any_space = pl.BlockSpec(memory_space=pl.ANY)
    pair_width = 2 * HD
    return pl.pallas_call(
        scatter_kernel,
        in_specs=[any_space] * 3 + [vmem] * 11 + [any_space],
        out_specs=[vmem] * 3 + [any_space] * 2 + [vmem],
        out_shape=[
            jax.ShapeDtypeStruct((2, SHARD, width), jnp.float32),
            jax.ShapeDtypeStruct((1, 1536), jnp.float32),
            jax.ShapeDtypeStruct((8, D), jnp.float32),
            jax.ShapeDtypeStruct((LENGTH // 2, D), LOW),
            jax.ShapeDtypeStruct((LENGTH // 2, D), LOW),
            jax.ShapeDtypeStruct((LENGTH, D), jnp.float32),
        ],
        scratch_shapes=[
            pltpu.VMEM((LENGTH // 2, D), jnp.float32),
            pltpu.VMEM((LENGTH // 2, D), LOW),
            pltpu.VMEM((D, 1536), LOW),
            pltpu.VMEM((LENGTH, 3 * pair_width), LOW),
            pltpu.VMEM((2, LENGTH, pair_width), LOW),
            pltpu.VMEM((2, LENGTH, pair_width), LOW),
            pltpu.VMEM((LENGTH, pair_width), jnp.float32),
            pltpu.VMEM((LENGTH, pair_width), jnp.float32),
            pltpu.VMEM((2, 2 * SHARD, 4 * width), LOW),
            pltpu.VMEM((2, 2 * SHARD, 4 * width), LOW),
            pltpu.VMEM((2, SHARD, 4 * width), LOW),
            pltpu.VMEM((2, SHARD, 2 * width), LOW),
            pltpu.VMEM((2, SHARD, 2 * width), LOW),
            pltpu.VMEM((2, SHARD, width), LOW),
            pltpu.VMEM((2, SHARD, 2 * EXTRA_WIDTH), LOW),
            pltpu.VMEM((2, SHARD, 2 * EXTRA_WIDTH), LOW),
            pltpu.VMEM((2, SHARD, EXTRA_WIDTH), LOW),
            pltpu.SemaphoreType.DMA((count, 2)),
            pltpu.SemaphoreType.DMA((count, 7)),
            pltpu.SemaphoreType.DMA((count, 9)),
            pltpu.SemaphoreType.DMA((3,)),
            pltpu.SemaphoreType.DMA((3,)),
        ],
        compiler_params=pltpu.CompilerParams(
            collective_id=2, has_side_effects=True, vmem_limit_bytes=60 * MIB
        ),
        name="scatter_attend_back",
    )(*grads, *attention, *rows)


def place_kernel(layer_ref, layer_low, input_ref, input_low, layer_out, input_out):
    shard = lax.axis_index("fsdp")
    moved = (shard % 2 + lax.axis_index("tensor")) % 2 == 1
    for own, other, out in ((layer_ref, layer_low, layer_out), (input_ref, input_low, input_out)):
        for r in range(2):
            for q in range(4):
                at = pl.ds(pl.multiple_of(global_block(shard, r, q) * SHARD, SHARD), SHARD)
                here = pl.ds((r * 4 + q) * SHARD, SHARD)

                @pl.when(moved)
                def _():
                    out[:, at] = other[:, here].astype(jnp.float32)

                @pl.when(jnp.logical_not(moved))
                def _():
                    out[:, at] = own[:, here]


def place_rows(layer, layer_low, grad, grad_low):
    block = pl.BlockSpec((128, D), lambda i: (i, 0))
    shape = jax.ShapeDtypeStruct((LENGTH // 2, D), jnp.float32)
    return pl.pallas_call(
        place_kernel,
        grid=(LENGTH // 256,),
        in_specs=[block] * 4,
        out_specs=[block] * 2,
        out_shape=[shape] * 2,
        name="place_rows",
    )(layer, layer_low, grad, grad_low)


COUNTS = (3 * D, D, FF, FF)
BLOCKS = (6, 2, 8, 8)


def offsets():
    return [(z * 8 + q * 2 + dc, q, dc, z) for z in range(4) for q in range(4) for dc in range(2)]


def stepped(g, state):
    new = DECAY * state + (1.0 - DECAY) * (g * g + TINY)
    return new, g * lax.rsqrt(new)


def rows_step(squares, old):
    which = lax.broadcasted_iota(jnp.int32, (4, 128), 0)
    counts = jnp.where(
        which == 0, float(COUNTS[0]), jnp.where(which == 1, float(COUNTS[1]), float(COUNTS[2]))
    )
    return DECAY * old + (1.0 - DECAY) * (squares / counts + TINY)


def tune_kernel(
    sums_ref, vec_ref, db_ref, wq_ref, wp_ref, wu_ref, wd_ref, vw_ref, vs_ref, rows_ref,
    cq_ref, cp_ref, cu_ref, cd_ref, bq_ref, bu_ref, bqs_ref, bus_ref,
    gq, gp_out, gu_out, gd_out, bq_out, bu_out, lane_out, col_out, grand_out,
    vec_send, vec_recv, db_recv, lane_send, lane_recv, col_send, col_recv, all_send, all_recv,
    core_send, core_done, a_send, a_recv, b_send, b_recv, c_send, c_recv,
):
    lane = lax.axis_index("tensor")
    shard = lax.axis_index("fsdp")
    core = shard % 2
    is_mid = (lane == 1) | (lane == 2)
    z_of = [lane, flip(lane, 1), 3 - lane, (lane + 2) % 4]

    def device(q, dc, z):
        target = {}
        if q or dc:
            target["fsdp"] = flip_place(shard, q, dc)
        if z:
            target["tensor"] = z_of[z]
        return target

    others = [entry for entry in offsets() if entry[0]]
    meet([device(q, dc, z) for _, q, dc, z in others])
    shard_peers = [(slot, q, dc) for slot, q, dc, z in others if z == 0]

    def core_copies():
        give = 1 - core
        hq = pl.ds(pl.multiple_of(core * 128, 128), 128)
        hf = pl.ds(pl.multiple_of(core * 512, 512), 512)
        pairs = [(sums_ref.at[give, :, pl.ds(1152 + j * 128, 128)], gq.at[j, :, hq]) for j in range(3)]
        pairs.append((sums_ref.at[give, :, pl.ds(1024, 128)], gp_out.at[:, hq]))
        pairs.append((sums_ref.at[give, :, pl.ds(512, 512)], gu_out.at[:, hf]))
        pairs.append((sums_ref.at[give, :, pl.ds(0, 512)], gd_out.at[:, hf]))
        return [
            remote(src, dst, core_send.at[i], core_done.at[i], {"fsdp": flip(shard, 1)})
            for i, (src, dst) in enumerate(pairs)
        ]

    for copy in core_copies():
        copy.start()

    def round_a():
        copies = [
            remote(vec_send.at[slot], vec_recv.at[slot], a_send.at[slot], a_recv.at[slot], device(q, dc, 0))
            for slot, q, dc in shard_peers
        ]
        for z in range(1, 4):
            position = 1 if z == 1 else (3 - is_mid.astype(jnp.int32) if z == 2 else 2 + is_mid.astype(jnp.int32))
            copies.append(
                remote(db_ref.at[position], db_recv.at[z], a_send.at[7 + z], a_recv.at[7 + z], device(0, 0, z))
            )
        return copies

    for slot in range(8):
        q, dc = slot // 2, slot % 2
        block = (core + dc - 2 * core * dc) * 4 + q
        at = pl.ds(pl.multiple_of(block * 128, 128), 128)
        if slot == 0:
            vec_recv[0] = vec_ref[:, at]
        else:
            vec_send[slot] = vec_ref[:, at]
    for copy in round_a():
        copy.start()
    db_recv[0] = db_ref[0]

    mine_q = pl.ds(pl.multiple_of(core * 128, 128), 128)
    mine_f = pl.ds(pl.multiple_of(core * 512, 512), 512)
    for j in range(3):
        gq[j, :, mine_q] = sums_ref[core, :, 1152 + j * 128 : 1280 + j * 128]
    gp_out[:, mine_q] = sums_ref[core, :, 1024:1152]
    gu_out[:, mine_f] = sums_ref[core, :, 512:1024]
    gd_out[:, mine_f] = sums_ref[core, :, 0:512]

    def weight_block(m, i):
        if m == 0:
            return wq_ref[:, i // 2, (i % 2) * 128 : (i % 2) * 128 + 128]
        return (None, wp_ref, wu_ref, wd_ref)[m][:, i * 128 : (i + 1) * 128]

    def grad_block(m, i):
        if m == 0:
            return gq[i // 2, :, (i % 2) * 128 : (i % 2) * 128 + 128]
        return (None, gp_out, gu_out, gd_out)[m][:, i * 128 : (i + 1) * 128]

    zero = jnp.zeros((128, 128), jnp.float32)

    def total_of(v):
        return jnp.sum(jnp.sum(v, axis=0, keepdims=True), axis=1, keepdims=True)

    weight_squares = []
    for m in range(4):
        acc = zero
        for i in range(BLOCKS[m]):
            w = weight_block(m, i)
            acc += w * w
        weight_squares.append(total_of(acc))

    for copy in core_copies():
        copy.wait()
    lane_send[...] = jnp.zeros_like(lane_send)
    row = 0
    for m in range(4):
        acc = zero
        for i in range(BLOCKS[m]):
            g = grad_block(m, i)
            square = g * g
            acc += square
            col_send[row : row + 1, :] = jnp.sum(square, axis=0, keepdims=True)
            row += 1
        lane_send[8 + m : 9 + m, :] = jnp.sum(acc.T, axis=0, keepdims=True)

    for copy in round_a():
        copy.wait()
    vec_sum = vec_recv[0]
    for slot in range(1, 8):
        vec_sum += vec_recv[slot]
    lane_send[0:8, :] = vec_sum
    col_send[24:32, :] = db_recv[0] + db_recv[1] + db_recv[2] + db_recv[3]

    def round_b():
        copies = [
            remote(lane_send, lane_recv.at[z], b_send.at[z], b_recv.at[z], device(0, 0, z)) for z in range(1, 4)
        ]
        copies += [
            remote(col_send, col_recv.at[slot], b_send.at[3 + slot], b_recv.at[3 + slot], device(q, dc, 0))
            for slot, q, dc in shard_peers
        ]
        return copies

    for copy in round_b():
        copy.start()
    for copy in round_b():
        copy.wait()
    lane_total = lane_send[...] + lane_recv[1] + lane_recv[2] + lane_recv[3]
    same = col_send[...] + col_recv[2] + col_recv[4] + col_recv[6]
    cross = col_recv[1] + col_recv[3] + col_recv[5] + col_recv[7]
    col_total = same[0:24] + cross[0:24]
    low_half = jnp.where(core == 0, same[24:32], cross[24:32])
    high_half = jnp.where(core == 0, cross[24:32], same[24:32])
    bq_out[:, 0:128] = low_half[0:3]
    bq_out[:, 128:256] = high_half[0:3]
    bu_out[0:4, :] = low_half[3:7]
    bu_out[4:8, :] = high_half[3:7]

    lane_out[...] = lane_total
    col_out[...] = col_total
    gvec = lane_total[0:8]
    _, v_dir = stepped(gvec, vs_ref[...])
    _, bq_dir = stepped(bq_out[...], bqs_ref[...])
    _, bu_dir = stepped(bu_out[...], bus_ref[...])
    rows_new = rows_step(lane_total[8:12], rows_ref[...])
    inverse_rows = lax.rsqrt(rows_new)
    spots = lax.broadcasted_iota(jnp.int32, (8, 128), 1)
    message = jnp.zeros((8, 128), jnp.float32)
    sums = []
    inverse_cols = []
    tall = []
    row = 0
    for m in range(4):
        tall.append(jnp.broadcast_to(inverse_rows[m : m + 1], (128, 128)).T)
        acc = zero
        for i in range(BLOCKS[m]):
            if m == 0:
                old = cq_ref[i // 2 : i // 2 + 1, (i % 2) * 128 : (i % 2) * 128 + 128]
            else:
                old = (None, cp_ref, cu_ref, cd_ref)[m][i : i + 1, :]
            new = DECAY * old + (1.0 - DECAY) * (col_total[row : row + 1] / D + TINY)
            inverse_cols.append(lax.rsqrt(new))
            step = grad_block(m, i) * tall[m] * inverse_cols[row]
            acc += step * step
            row += 1
        sums.append(total_of(acc))
    terms = sums
    terms = terms + [0.25 * total_of(rows_new[m : m + 1]) for m in range(4)]
    terms = terms + weight_squares
    vw = vw_ref[...]
    v_squares = jnp.sum(v_dir * v_dir, axis=1, keepdims=True)
    w_squares = jnp.sum(vw * vw, axis=1, keepdims=True)
    terms = terms + [0.25 * v_squares[i : i + 1] for i in range(6)]
    terms = terms + [0.25 * w_squares[i : i + 1] for i in range(6)]
    for value in (bq_dir, bu_dir, bq_ref[...], bu_ref[...]):
        terms = terms + [0.125 * total_of(value * value)]
    for i, term in enumerate(terms):
        message = jnp.where(spots == i, term, message)
    all_send[...] = message

    def round_c():
        return [
            remote(all_send, all_recv.at[slot], c_send.at[slot], c_recv.at[slot], device(q, dc, z))
            for slot, q, dc, z in others
        ]

    for copy in round_c():
        copy.start()
    for copy in round_c():
        copy.wait()
    grand = message
    for slot, _, _, _ in others:
        grand += all_recv[slot]
    grand_out[...] = grand


def apply_kernel(
    gq, gp_ref, gu_ref, gd_ref, bg_ref, ug_ref, lane_ref, col_ref, grand_ref,
    wq_ref, wp_ref, wu_ref, wd_ref, vw_ref, vs_ref, rows_ref,
    cq_ref, cp_ref, cu_ref, cd_ref, bq_ref, bu_ref, bqs_ref, bus_ref,
    gq_out, gp_out, gu_out, gd_out, nq_out, np_out, nu_out, nd_out, vec_out, rows_out,
    cq_out, cp_out, cu_out, cd_out, bq_out, bqs_out, bqn_out, bu_out, bus_out, bun_out, rms_out,
):
    def weight_block(m, i):
        if m == 0:
            return wq_ref[:, i // 2, (i % 2) * 128 : (i % 2) * 128 + 128]
        return (None, wp_ref, wu_ref, wd_ref)[m][:, i * 128 : (i + 1) * 128]

    def grad_block(m, i):
        if m == 0:
            return gq[i // 2, :, (i % 2) * 128 : (i % 2) * 128 + 128]
        return (None, gp_ref, gu_ref, gd_ref)[m][:, i * 128 : (i + 1) * 128]

    for j in range(3):
        gq_out[:, j, :] = gq[j]
    gp_out[...] = gp_ref[...]
    gu_out[...] = gu_ref[...]
    gd_out[...] = gd_ref[...]
    bq_out[...] = bg_ref[...]
    bu_out[...] = ug_ref[...]
    gvec = lane_ref[0:8, :]
    vw = vw_ref[...]
    vs_new, v_dir = stepped(gvec, vs_ref[...])
    bqs_new, bq_dir = stepped(bg_ref[...], bqs_ref[...])
    bus_new, bu_dir = stepped(ug_ref[...], bus_ref[...])
    bqs_out[...] = bqs_new
    bus_out[...] = bus_new
    vec_out[0:8, :] = gvec
    vec_out[8:16, :] = vs_new
    rows_new = rows_step(lane_ref[8:12, :], rows_ref[...])
    rows_out[...] = rows_new
    inverse_rows = lax.rsqrt(rows_new)
    line = grand_ref[0:1, :]
    spot = lax.broadcasted_iota(jnp.int32, (1, 128), 1)

    def pick(i):
        return jnp.sum(jnp.where(spot == i, line, 0.0), axis=1, keepdims=True)

    rms_line = jnp.zeros((1, 128), jnp.float32)
    row = 0
    for m in range(4):
        size = float(D * COUNTS[m])
        mean_rows = pick(4 + m) / D
        rms = jnp.sqrt(pick(m) * mean_rows / size)
        scale = jnp.sqrt(pick(8 + m) / size)
        factor = RATE * scale * jnp.sqrt(mean_rows) / jnp.maximum(1.0, rms / CLIP_LEVEL)
        rms_line = jnp.where(spot == m, rms, rms_line)
        tall = jnp.broadcast_to(inverse_rows[m : m + 1], (128, 128)).T
        for i in range(BLOCKS[m]):
            if m == 0:
                old = cq_ref[i // 2 : i // 2 + 1, (i % 2) * 128 : (i % 2) * 128 + 128]
            else:
                old = (None, cp_ref, cu_ref, cd_ref)[m][i : i + 1, :]
            cols = DECAY * old + (1.0 - DECAY) * (col_ref[row : row + 1, :] / D + TINY)
            if m == 0:
                cq_out[i // 2 : i // 2 + 1, (i % 2) * 128 : (i % 2) * 128 + 128] = cols
            else:
                (None, cp_out, cu_out, cd_out)[m][i : i + 1, :] = cols
            new = weight_block(m, i) - factor * (grad_block(m, i) * tall * lax.rsqrt(cols))
            if m == 0:
                nq_out[:, i // 2, (i % 2) * 128 : (i % 2) * 128 + 128] = new
            else:
                (None, np_out, nu_out, nd_out)[m][:, i * 128 : (i + 1) * 128] = new
            row += 1
    rms_out[...] = rms_line
    for i in range(6):
        spread = jnp.sqrt(pick(12 + i) / D)
        factor = RATE * jnp.sqrt(pick(18 + i) / D) / jnp.maximum(1.0, spread / CLIP_LEVEL)
        vec_out[16 + i : 17 + i, :] = vw[i : i + 1] - factor * v_dir[i : i + 1]
    vec_out[22:24, :] = jnp.zeros((2, 128), jnp.float32)
    for direction, weight, out, at, size in (
        (bq_dir, bq_ref, bqn_out, 24, 3 * D),
        (bu_dir, bu_ref, bun_out, 25, FF),
    ):
        spread = jnp.sqrt(pick(at) / size)
        factor = RATE * jnp.sqrt(pick(at + 2) / size) / jnp.maximum(1.0, spread / CLIP_LEVEL)
        out[...] = weight[...] - factor * direction


def tune_all(sums, vec_part, db_part, params, stats, states):
    qkv_weight, qkv_bias, proj_weight, fc1_weight, fc1_bias, fc2_weight, vectors = params
    row_state, qkv_cols, proj_cols, fc1_cols, fc2_cols = stats
    vector_state, qkv_bias_state, fc1_bias_state = states
    pad = ((0, 2), (0, 0))

    def dense(v):
        return v.reshape(v.shape[0] // 128, 128)

    operands = (
        sums, vec_part, db_part, qkv_weight, proj_weight, fc1_weight, fc2_weight,
        jnp.pad(vectors.T, pad), jnp.pad(vector_state.T, pad, constant_values=1.0), row_state,
        qkv_cols, dense(proj_cols), dense(fc1_cols), dense(fc2_cols),
        qkv_bias, dense(fc1_bias), qkv_bias_state, dense(fc1_bias_state),
    )
    vmem = pl.BlockSpec(memory_space=pltpu.VMEM)
    shapes = [
        (128, 3, 256), (128, 256), (128, 1024), (128, 1024),
        (128, 3, 256), (128, 256), (128, 1024), (128, 1024),
        (24, 128), (4, 128), (3, 256), (2, 128), (8, 128), (8, 128),
        (3, 256), (3, 256), (3, 256), (8, 128), (8, 128), (8, 128), (1, 128),
    ]
    f32 = jnp.float32
    middle = [
        (3, 128, 256), (128, 256), (128, 1024), (128, 1024), (3, 256), (8, 128), (16, 128), (24, 128), (8, 128)
    ]
    reduced = pl.pallas_call(
        tune_kernel,
        in_specs=[vmem] * len(operands),
        out_specs=[vmem] * len(middle),
        out_shape=[jax.ShapeDtypeStruct(shape, f32) for shape in middle],
        scratch_shapes=[
            pltpu.VMEM((8, 8, 128), f32),
            pltpu.VMEM((8, 8, 128), f32),
            pltpu.VMEM((4, 8, 128), f32),
            pltpu.VMEM((16, 128), f32),
            pltpu.VMEM((4, 16, 128), f32),
            pltpu.VMEM((32, 128), f32),
            pltpu.VMEM((8, 32, 128), f32),
            pltpu.VMEM((8, 128), f32),
            pltpu.VMEM((32, 8, 128), f32),
            pltpu.SemaphoreType.DMA((6,)),
            pltpu.SemaphoreType.DMA((6,)),
            pltpu.SemaphoreType.DMA((11,)),
            pltpu.SemaphoreType.DMA((11,)),
            pltpu.SemaphoreType.DMA((11,)),
            pltpu.SemaphoreType.DMA((11,)),
            pltpu.SemaphoreType.DMA((32,)),
            pltpu.SemaphoreType.DMA((32,)),
        ],
        compiler_params=pltpu.CompilerParams(collective_id=4, has_side_effects=True, vmem_limit_bytes=40 * 1024 * 1024),
        name="tune_all",
    )(*operands)
    inputs = (*reduced, *operands[3:])
    (
        gq, gp, gu, gd, nq, np_, nu, nd, vec, rows, cq, cp, cu, cd, bq, bqs, bqn, bu, bus, bun, rms
    ) = pl.pallas_call(
        apply_kernel,
        in_specs=[vmem] * len(inputs),
        out_specs=[vmem] * len(shapes),
        out_shape=[jax.ShapeDtypeStruct(shape, f32) for shape in shapes],
        compiler_params=pltpu.CompilerParams(vmem_limit_bytes=40 * MIB),
        name="apply_all",
    )(*inputs)
    vec = vec.T
    return (
        gq, bq, gp, gu, bu.reshape(1024), gd, vec[:, 0:6], rows,
        cq, cp.reshape(256), cu.reshape(1024), cd.reshape(1024),
        vec[:, 8:14], bqs, bus.reshape(1024),
        nq, bqn, np_, nu, bun.reshape(1024), nd, vec[:, 16:22], rms[0, 0:4],
    )


def gelu_parts(u):
    cdf = 0.5 * (1.0 + lax.erf(u * (0.5**0.5)))
    density = jnp.exp(-0.5 * u * u) * ((2.0 * jnp.pi) ** -0.5)
    return u * cdf, cdf + u * density


def norm_parts(values):
    center = values - jnp.mean(values, axis=-1, keepdims=True)
    scale = lax.rsqrt(jnp.mean(center * center, axis=-1, keepdims=True) + NORM_EPS)
    return center * scale, scale


def norm_back(grad, unit, scale, gain):
    c = grad * gain
    return scale * (
        c
        - jnp.mean(c, axis=-1, keepdims=True)
        - unit * jnp.mean(c * unit, axis=-1, keepdims=True)
    )


def on_chip(
    tokens,
    cotangent,
    qkv_weight,
    qkv_bias,
    proj_weight,
    fc1_weight,
    fc1_bias,
    fc2_weight,
    vectors,
    row_state,
    qkv_cols,
    proj_cols,
    fc1_cols,
    fc2_cols,
    vector_state,
    qkv_bias_state,
    fc1_bias_state,
):
    shard = lax.axis_index("fsdp")
    core = shard % 2
    rows = tokens.shape[0]
    hw, fw = qkv_weight.shape[2] // 2, fc1_weight.shape[1] // 2
    shard_rows = qkv_weight.shape[0]

    def both_halves(v):
        return jnp.concatenate([v, lax.ppermute(v, "fsdp", CORE_SWAP)], axis=0)

    def core_sum(left, right_t):
        other = times_transposed(left[rows:], right_t)
        other = lax.ppermute(other, "fsdp", CORE_SWAP)
        return times_transposed(left[:rows], right_t) + other

    def half_columns(w, width, which):
        return lax.dynamic_slice_in_dim(w, which * width, width, w.ndim - 1)

    def pack(which):
        return jnp.concatenate(
            [
                qkv_weight[:, :, which * hw : (which + 1) * hw].reshape(shard_rows, 3 * hw),
                proj_weight[:, which * hw : (which + 1) * hw],
                fc1_weight[:, which * fw : (which + 1) * fw],
                fc2_weight[:, which * fw : (which + 1) * fw],
            ],
            axis=1,
        ).astype(LOW)

    packs = jnp.stack([pack(0), pack(1)])
    vec = jnp.pad(vectors.astype(LOW).astype(jnp.float32).T, ((0, 2), (0, 0)))
    bias = jnp.concatenate(
        [
            half_columns(qkv_bias, hw, core).reshape(3 * hw),
            lax.dynamic_slice_in_dim(fc1_bias, core * fw, fw, 0),
        ]
    )
    bias = jnp.broadcast_to(
        lax.optimization_barrier(bias.astype(LOW)).astype(jnp.float32), (8, 3 * hw + fw)
    )
    (
        weight_qkv, weight_proj, weight_up, weight_down, vec_all, bias_all, normed_one, low, mixed, lse,
        tokens_all, grad_out_all, *tables,
    ) = gather_all(packs, vec, bias, tokens, cotangent)
    vector_rows = vec_all.transpose(1, 0, 2).reshape(8, D)
    _, _, proj_shift, gain_two, shift_two, down_shift = [
        vector_rows[i : i + 1] for i in range(6)
    ]
    bias_rows = bias_all[:, 0]
    bias_up = (
        bias_rows[:, 3 * hw :].reshape(4, 2, fw // 2).transpose(1, 0, 2).reshape(1, 4 * fw)
    )

    inputs = tokens_all[:rows].astype(jnp.float32)
    upstream = grad_out_all[:rows].astype(jnp.float32)
    middle = inputs + core_sum(mixed, weight_proj) + proj_shift
    unit_two, scale_two = norm_parts(middle)
    normed_two = both_halves((unit_two * gain_two + shift_two).astype(LOW))
    hidden = jnp.dot(normed_two, weight_up, preferred_element_type=jnp.float32) + bias_up
    active, slope = gelu_parts(hidden)
    active = active.astype(LOW)
    grad_down = contract_rows(grad_out_all, active).astype(LOW)
    layer_local = middle + core_sum(active, weight_down) + down_shift
    grad_active = jnp.dot(grad_out_all, weight_down, preferred_element_type=jnp.float32)
    grad_hidden = (grad_active * slope).astype(LOW)
    grad_up = contract_rows(normed_two, grad_hidden).astype(LOW)
    grad_bias_up = jnp.sum(grad_hidden.astype(jnp.float32), axis=0)
    grad_normed_two = core_sum(grad_hidden, weight_up)
    grad_middle = upstream + norm_back(grad_normed_two, unit_two, scale_two, gain_two)
    grad_branch = grad_middle.astype(LOW)
    grad_branch_all = both_halves(grad_branch)
    grad_proj = contract_rows(grad_branch_all, mixed).astype(LOW)
    grad_mixed = jnp.dot(
        grad_branch_all, weight_proj, preferred_element_type=jnp.float32
    ).astype(LOW)
    sums, grad_bias_qkv, norm_sums, layer_low, input_low, input_local = scatter_all(
        (grad_down, grad_up, grad_proj),
        (low, grad_mixed, lse, *tables, normed_one, weight_qkv),
        (vec_all, tokens_all, grad_middle, layer_local.astype(LOW)),
    )
    layer_out, input_grad = place_rows(layer_local, layer_low, input_local, input_low)

    vec_part = jnp.concatenate(
        [
            norm_sums[0:2],
            jnp.sum(grad_branch.astype(jnp.float32), axis=0, keepdims=True),
            jnp.sum(grad_normed_two * unit_two, axis=0, keepdims=True),
            jnp.sum(grad_normed_two, axis=0, keepdims=True),
            jnp.sum(upstream, axis=0, keepdims=True),
            jnp.zeros((2, D), jnp.float32),
        ]
    )
    db_part = jnp.concatenate(
        [
            grad_bias_qkv.reshape(4, 3, hw),
            grad_bias_up.reshape(2, 4, 2, hw).transpose(1, 0, 2, 3).reshape(4, 4, hw),
            jnp.zeros((4, 1, hw), jnp.float32),
        ],
        axis=1,
    )
    return (
        layer_out,
        input_grad,
        *tune_all(
            sums,
            vec_part,
            db_part,
            (qkv_weight, qkv_bias, proj_weight, fc1_weight, fc1_bias, fc2_weight, vectors),
            (row_state, qkv_cols, proj_cols, fc1_cols, fc2_cols),
            (vector_state, qkv_bias_state, fc1_bias_state),
        ),
    )


def solution(mesh):
    chips = mesh.shape["fsdp"] == 8 and mesh.shape["tensor"] == 4
    return jax.shard_map(
        on_chip if chips else on_device,
        mesh=mesh,
        in_specs=(
            P(("fsdp", "tensor"), None),
            P(("fsdp", "tensor"), None),
            P("fsdp", None, "tensor"),
            P(None, "tensor"),
            P("fsdp", "tensor"),
            P("fsdp", "tensor"),
            P("tensor"),
            P("fsdp", "tensor"),
            P("fsdp", None),
            P(None, "fsdp"),
            P(None, "tensor"),
            P("tensor"),
            P("tensor"),
            P("tensor"),
            P("fsdp", None),
            P(None, "tensor"),
            P("tensor"),
        ),
        out_specs=(
            P(("fsdp", "tensor"), None),
            P(("fsdp", "tensor"), None),
            P("fsdp", None, "tensor"),
            P(None, "tensor"),
            P("fsdp", "tensor"),
            P("fsdp", "tensor"),
            P("tensor"),
            P("fsdp", "tensor"),
            P("fsdp", None),
            P(None, "fsdp"),
            P(None, "tensor"),
            P("tensor"),
            P("tensor"),
            P("tensor"),
            P("fsdp", None),
            P(None, "tensor"),
            P("tensor"),
            P("fsdp", None, "tensor"),
            P(None, "tensor"),
            P("fsdp", "tensor"),
            P("fsdp", "tensor"),
            P("tensor"),
            P("fsdp", "tensor"),
            P("fsdp", None),
            P(),
        ),
        check_vma=False,
    )
```

```python
import math

import jax
import jax.numpy as jnp
from jax import lax
from jax.experimental import pallas as pl
from jax.experimental.pallas import tpu as pltpu
from jax.sharding import PartitionSpec as P

D = 1024
HD = 64
FF = 4096
GT = 4
GH = 16
GW = 16


NORM_EPS = 1e-06
DECAY = 0.5
CLIP_LEVEL = 1.0
RATE = 0.3
TINY = 1e-30
BASE = 10000.0


def layer_norm(values, gain_row, shift_row):
    center = values - jnp.mean(values, axis=-1, keepdims=True)
    variance = jnp.mean(center * center, axis=-1, keepdims=True)
    return center * lax.rsqrt(variance + NORM_EPS) * gain_row + shift_row


def exact_gelu(values):
    return jax.nn.gelu(values, approximate=False)


def rope_tables(length, half_width):
    token_index = jnp.arange(length, dtype=jnp.int32)
    coordinates = jnp.stack(
        [token_index // (GH * GW), token_index // GW % GH, token_index % GW], axis=1
    ).astype(jnp.float32)
    frequency = BASE ** (-jnp.arange(half_width, dtype=jnp.float32) / half_width)
    angles = coordinates[:, :, None] * frequency[None, None, :]
    return (jnp.cos(angles), jnp.sin(angles))


def rotate(values, cosine_table, sine_table):
    half_width = cosine_table.shape[-1]
    rotated_width = 6 * half_width
    leading = values.shape[:-1]
    pair_rows = values[..., :rotated_width].reshape(leading + (3, 2, half_width))
    first_half = pair_rows[..., 0, :]
    second_half = pair_rows[..., 1, :]
    cosine_wide = cosine_table[:, None]
    sine_wide = sine_table[:, None]
    turned = jnp.stack(
        [
            first_half * cosine_wide - second_half * sine_wide,
            second_half * cosine_wide + first_half * sine_wide,
        ],
        axis=-2,
    )
    return jnp.concatenate(
        [turned.reshape(leading + (rotated_width,)), values[..., rotated_width:]], axis=-1
    )


def contract_rows(left, right):
    return lax.dot_general(
        left, right, (((0,), (0,)), ((), ())), preferred_element_type=jnp.float32
    )


def times_transposed(left, right):
    return lax.dot_general(
        left, right, (((1,), (1,)), ((), ())), preferred_element_type=jnp.float32
    )


def forward_block(query_rows, key_rows, value_rows):
    score_scale = query_rows.shape[-1] ** (-0.5)
    scores = (
        jnp.einsum("qhd,khd->hqk", query_rows, key_rows, preferred_element_type=jnp.float32)
        * score_scale
    )
    row_peak = jnp.max(scores, axis=-1, keepdims=True)
    raised = jnp.exp(scores - row_peak)
    totals = jnp.sum(raised, axis=-1, keepdims=True)
    attention = (raised / totals).astype(jnp.bfloat16)
    mixed_rows = jnp.einsum(
        "hqk,khd->qhd", attention, value_rows, preferred_element_type=jnp.float32
    )
    return (mixed_rows, (row_peak + jnp.log(totals))[..., 0])


def backward_block(running, block_item, key_rows, value_rows):
    query_rows, log_totals, grad_mixed = block_item
    score_scale = query_rows.shape[-1] ** (-0.5)
    scores = (
        jnp.einsum("qhd,khd->hqk", query_rows, key_rows, preferred_element_type=jnp.float32)
        * score_scale
    )
    attention = jnp.exp(scores - log_totals[..., None])
    grad_attention = jnp.einsum(
        "qhd,khd->hqk", grad_mixed, value_rows, preferred_element_type=jnp.float32
    )
    grad_scores = attention * (
        grad_attention - jnp.sum(attention * grad_attention, axis=-1, keepdims=True)
    )
    grad_low = grad_scores.astype(jnp.bfloat16)
    grad_queries = (
        jnp.einsum("hqk,khd->qhd", grad_low, key_rows, preferred_element_type=jnp.float32)
        * score_scale
    )
    key_total = (
        running[0]
        + jnp.einsum("hqk,qhd->khd", grad_low, query_rows, preferred_element_type=jnp.float32)
        * score_scale
    )
    value_total = running[1] + jnp.einsum(
        "hqk,qhd->khd",
        attention.astype(jnp.bfloat16),
        grad_mixed,
        preferred_element_type=jnp.float32,
    )
    return ((key_total, value_total), grad_queries)


def on_device(
    tokens,
    cotangent,
    qkv_weight,
    qkv_bias,
    proj_weight,
    fc1_weight,
    fc1_bias,
    fc2_weight,
    vectors,
    row_state,
    qkv_cols,
    proj_cols,
    fc1_cols,
    fc2_cols,
    vector_state,
    qkv_bias_state,
    fc1_bias_state,
):
    low_type = jnp.bfloat16
    lane_count = lax.axis_size("tensor")
    local_rows = tokens.shape[0]
    group_rows = local_rows * lane_count
    length = GT * GH * GW
    clip_count = group_rows // length
    block_rows = min(512, length)
    block_count = length // block_rows
    head_width = qkv_weight.shape[2]
    head_count = head_width // HD
    hidden_width = fc1_weight.shape[1]
    shard_rows = qkv_weight.shape[0]
    cosine_table, sine_table = rope_tables(length, HD // 3 // 2)
    weight_qkv, weight_proj, weight_up, weight_down, vector_low = (
        lax.all_gather(qkv_weight.astype(low_type), "fsdp", axis=0, tiled=True),
        lax.all_gather(proj_weight.astype(low_type), "fsdp", axis=0, tiled=True),
        lax.all_gather(fc1_weight.astype(low_type), "fsdp", axis=0, tiled=True),
        lax.all_gather(fc2_weight.astype(low_type), "fsdp", axis=0, tiled=True),
        lax.all_gather(vectors.astype(low_type), "fsdp", axis=0, tiled=True),
    )
    weight_qkv = weight_qkv.reshape(D, 3 * head_width)
    vector_full = vector_low.astype(jnp.float32)
    gain_one = vector_full[:, 0]
    shift_one = vector_full[:, 1]
    proj_shift = vector_full[:, 2]
    gain_two = vector_full[:, 3]
    shift_two = vector_full[:, 4]
    down_shift = vector_full[:, 5]
    bias_qkv = (
        lax.optimization_barrier(qkv_bias.astype(low_type))
        .astype(jnp.float32)
        .reshape(3 * head_width)
    )
    bias_up = lax.optimization_barrier(fc1_bias.astype(low_type)).astype(jnp.float32)
    inputs = tokens.astype(jnp.float32)
    normed_one = layer_norm(inputs, gain_one, shift_one).astype(low_type)
    gathered_one = lax.all_gather(normed_one, "tensor", axis=0, tiled=True)
    projected = jnp.dot(gathered_one, weight_qkv, preferred_element_type=jnp.float32) + bias_qkv
    projected = projected.reshape(clip_count, length, 3, head_count, HD)
    queries = rotate(projected[:, :, 0], cosine_table, sine_table).astype(low_type)
    key_rows = rotate(projected[:, :, 1], cosine_table, sine_table).astype(low_type)
    value_rows = projected[:, :, 2].astype(low_type)

    def clip_forward(clip_item):
        query_rows, clip_keys, clip_values = clip_item
        blocks = query_rows.reshape(block_count, block_rows, head_count, HD)
        return lax.map(
            lambda query_block: forward_block(query_block, clip_keys, clip_values), blocks
        )

    mixed_rows, log_totals = lax.map(clip_forward, (queries, key_rows, value_rows))
    mixed_low = mixed_rows.reshape(group_rows, head_width).astype(low_type)
    attn_sum = lax.psum_scatter(
        times_transposed(mixed_low, weight_proj), "tensor", scatter_dimension=0, tiled=True
    )
    middle = inputs + attn_sum + proj_shift
    normed_two = layer_norm(middle, gain_two, shift_two).astype(low_type)
    gathered_two = lax.all_gather(normed_two, "tensor", axis=0, tiled=True)
    hidden = jnp.dot(gathered_two, weight_up, preferred_element_type=jnp.float32) + bias_up
    active = exact_gelu(hidden).astype(low_type)
    layer_out = (
        middle
        + lax.psum_scatter(
            times_transposed(active, weight_down), "tensor", scatter_dimension=0, tiled=True
        )
        + down_shift
    )
    upstream = cotangent.astype(jnp.float32)
    grad_out_all, normed_two_all = (
        lax.all_gather(cotangent, "tensor", axis=0, tiled=True),
        lax.all_gather(normed_two, "tensor", axis=0, tiled=True),
    )
    grad_down = contract_rows(grad_out_all, active)
    grad_active = jnp.dot(grad_out_all, weight_down, preferred_element_type=jnp.float32)
    gelu_pull = jax.vjp(exact_gelu, hidden)[1]
    grad_hidden = gelu_pull(grad_active)[0].astype(low_type)
    grad_up = contract_rows(normed_two_all, grad_hidden)
    grad_bias_up = jnp.sum(grad_hidden.astype(jnp.float32), axis=0)
    grad_normed_two = lax.psum_scatter(
        times_transposed(grad_hidden, weight_up), "tensor", scatter_dimension=0, tiled=True
    )
    middle_part, grad_gain_two, grad_shift_two = jax.vjp(layer_norm, middle, gain_two, shift_two)[
        1
    ](grad_normed_two)
    grad_middle = upstream + middle_part
    grad_branch = grad_middle.astype(low_type)
    grad_proj_shift = jnp.sum(grad_branch.astype(jnp.float32), axis=0)
    grad_down_shift = jnp.sum(upstream, axis=0)
    grad_branch_all, normed_one_all = (
        lax.all_gather(grad_branch, "tensor", axis=0, tiled=True),
        lax.all_gather(normed_one, "tensor", axis=0, tiled=True),
    )
    grad_proj = contract_rows(grad_branch_all, mixed_low)
    grad_mixed = jnp.dot(grad_branch_all, weight_proj, preferred_element_type=jnp.float32).astype(
        low_type
    )
    grad_mixed = grad_mixed.reshape(clip_count, length, head_count, HD)

    def clip_backward(clip_item):
        query_rows, clip_keys, clip_values, clip_totals, clip_grads = clip_item
        starts = (jnp.zeros(clip_keys.shape, jnp.float32), jnp.zeros(clip_keys.shape, jnp.float32))
        block_items = (
            query_rows.reshape(block_count, block_rows, head_count, HD),
            clip_totals,
            clip_grads.reshape(block_count, block_rows, head_count, HD),
        )
        sums, grad_queries = lax.scan(
            lambda running, block_item: backward_block(running, block_item, clip_keys, clip_values),
            starts,
            block_items,
        )
        return (grad_queries.reshape(query_rows.shape), sums[0], sums[1])

    grad_queries, grad_keys, grad_values = lax.map(
        clip_backward, (queries, key_rows, value_rows, log_totals, grad_mixed)
    )
    grad_projected = jnp.stack(
        [
            rotate(grad_queries, cosine_table, -sine_table),
            rotate(grad_keys, cosine_table, -sine_table),
            grad_values,
        ],
        axis=2,
    )
    grad_projected = grad_projected.reshape(group_rows, 3 * head_width).astype(low_type)
    grad_qkv = contract_rows(normed_one_all, grad_projected).reshape(D, 3, head_width)
    grad_bias_qkv = jnp.sum(grad_projected.astype(jnp.float32), axis=0)
    grad_normed_one = lax.psum_scatter(
        times_transposed(grad_projected, weight_qkv), "tensor", scatter_dimension=0, tiled=True
    )
    input_part, grad_gain_one, grad_shift_one = jax.vjp(layer_norm, inputs, gain_one, shift_one)[1](
        grad_normed_one
    )
    input_grad = grad_middle + input_part
    grad_qkv, grad_proj, grad_up, grad_down = (
        lax.psum_scatter(grad_qkv, "fsdp", scatter_dimension=0, tiled=True),
        lax.psum_scatter(grad_proj, "fsdp", scatter_dimension=0, tiled=True),
        lax.psum_scatter(grad_up, "fsdp", scatter_dimension=0, tiled=True),
        lax.psum_scatter(grad_down, "fsdp", scatter_dimension=0, tiled=True),
    )
    lane_index = lax.axis_index("tensor")
    vector_part = jnp.stack(
        [
            grad_gain_one,
            grad_shift_one,
            grad_proj_shift,
            grad_gain_two,
            grad_shift_two,
            grad_down_shift,
        ],
        axis=1,
    )
    qkv_placed = lax.dynamic_update_slice(
        jnp.zeros((3, D), jnp.float32),
        grad_bias_qkv.reshape(3, head_width),
        (jnp.int32(0), lane_index * head_width),
    )
    up_placed = lax.dynamic_update_slice(
        jnp.zeros((FF,), jnp.float32), grad_bias_up, (lane_index * hidden_width,)
    )
    vector_total, qkv_total, up_total = lax.psum(
        (vector_part, qkv_placed, up_placed), ("fsdp", "tensor")
    )
    grad_vectors = lax.dynamic_slice_in_dim(
        vector_total, lax.axis_index("fsdp") * shard_rows, shard_rows, 0
    )
    grad_qkv_bias = lax.dynamic_slice_in_dim(qkv_total, lane_index * head_width, head_width, 1)
    grad_up_bias = lax.dynamic_slice_in_dim(up_total, lane_index * hidden_width, hidden_width, 0)
    matrices = [
        (
            grad_qkv.reshape(shard_rows, 3 * head_width),
            qkv_weight.reshape(shard_rows, 3 * head_width),
            qkv_cols.reshape(3 * head_width),
        ),
        (grad_proj, proj_weight, proj_cols),
        (grad_up, fc1_weight, fc1_cols),
        (grad_down, fc2_weight, fc2_cols),
    ]
    column_counts = [3 * D, D, FF, FF]
    column_weights = jnp.array(column_counts, jnp.float32)
    qkv_state_new = DECAY * qkv_bias_state + (1.0 - DECAY) * (grad_qkv_bias * grad_qkv_bias + TINY)
    qkv_direction = grad_qkv_bias * lax.rsqrt(qkv_state_new)
    up_state_new = DECAY * fc1_bias_state + (1.0 - DECAY) * (grad_up_bias * grad_up_bias + TINY)
    up_direction = grad_up_bias * lax.rsqrt(up_state_new)
    row_squares = jnp.stack(
        [jnp.sum(matrix_entry[0] * matrix_entry[0], axis=1) for matrix_entry in matrices]
    )
    weight_squares = jnp.stack(
        [jnp.sum(matrix_entry[1] * matrix_entry[1]) for matrix_entry in matrices]
    )
    bias_terms = jnp.stack(
        [
            jnp.sum(qkv_direction * qkv_direction),
            jnp.sum(up_direction * up_direction),
            jnp.sum(qkv_bias * qkv_bias),
            jnp.sum(fc1_bias * fc1_bias),
        ]
    )
    row_total, weight_partial, bias_total = lax.psum(
        (row_squares, weight_squares, bias_terms), "tensor"
    )
    rows_new = DECAY * row_state + (1.0 - DECAY) * (row_total / column_weights[:, None] + TINY)
    vector_state_new = DECAY * vector_state + (1.0 - DECAY) * (grad_vectors * grad_vectors + TINY)
    vector_direction = grad_vectors * lax.rsqrt(vector_state_new)
    vector_terms = jnp.stack(
        [jnp.sum(vector_direction * vector_direction, axis=0), jnp.sum(vectors * vectors, axis=0)]
    )
    col_squares = jnp.concatenate(
        [jnp.sum(matrix_entry[0] * matrix_entry[0], axis=0) for matrix_entry in matrices]
    )
    row_new_sums = jnp.sum(rows_new, axis=1)
    col_total, row_new_total, weight_total, vector_sums = lax.psum(
        (col_squares, row_new_sums, weight_partial, vector_terms), "fsdp"
    )
    mean_rows = row_new_total / D
    offsets = [0]
    for matrix_entry in matrices:
        offsets.append(offsets[-1] + matrix_entry[0].shape[1])
    cols_list = []
    direction_list = []
    square_list = []
    for position, matrix_entry in enumerate(matrices):
        col_slice = col_total[offsets[position] : offsets[position + 1]]
        cols_new = DECAY * matrix_entry[2] + (1.0 - DECAY) * (col_slice / D + TINY)
        direction = matrix_entry[0] * lax.rsqrt(
            rows_new[position][:, None] * cols_new[None, :] / mean_rows[position]
        )
        cols_list.append(cols_new)
        direction_list.append(direction)
        square_list.append(jnp.sum(direction * direction))
    square_total = lax.psum(jnp.stack(square_list), ("fsdp", "tensor"))
    matrix_count = D * column_weights
    update_rms = jnp.sqrt(square_total / matrix_count)
    weight_scale = jnp.sqrt(weight_total / matrix_count)
    new_weights = []
    for position, matrix_entry in enumerate(matrices):
        new_weights.append(
            matrix_entry[1]
            - RATE
            * weight_scale[position]
            * direction_list[position]
            / jnp.maximum(1.0, update_rms[position] / CLIP_LEVEL)
        )
    vector_rms = jnp.sqrt(vector_sums[0] / D)
    vector_scale = jnp.sqrt(vector_sums[1] / D)
    vectors_new = vectors - RATE * vector_scale * vector_direction / jnp.maximum(
        1.0, vector_rms / CLIP_LEVEL
    )
    qkv_rms = jnp.sqrt(bias_total[0] / (3 * D))
    qkv_scale = jnp.sqrt(bias_total[2] / (3 * D))
    qkv_bias_new = qkv_bias - RATE * qkv_scale * qkv_direction / jnp.maximum(
        1.0, qkv_rms / CLIP_LEVEL
    )
    up_rms = jnp.sqrt(bias_total[1] / FF)
    up_scale = jnp.sqrt(bias_total[3] / FF)
    up_bias_new = fc1_bias - RATE * up_scale * up_direction / jnp.maximum(1.0, up_rms / CLIP_LEVEL)
    return (
        layer_out,
        input_grad,
        grad_qkv,
        grad_qkv_bias,
        grad_proj,
        grad_up,
        grad_up_bias,
        grad_down,
        grad_vectors,
        rows_new,
        cols_list[0].reshape(3, head_width),
        cols_list[1],
        cols_list[2],
        cols_list[3],
        vector_state_new,
        qkv_state_new,
        up_state_new,
        new_weights[0].reshape(shard_rows, 3, head_width),
        qkv_bias_new,
        new_weights[1],
        new_weights[2],
        up_bias_new,
        new_weights[3],
        vectors_new,
        update_rms,
    )


SCALE = HD**-0.5
LENGTH = GT * GH * GW
ROLL = HD // 3 // 2
CORE_SWAP = [(i, i ^ 1) for i in range(8)]
LOW = jnp.bfloat16
QB = 256


def rotary_rows(first, core):
    token = (lax.broadcasted_iota(jnp.int32, (128, 2 * HD), 0) + first + core * (LENGTH // 2)) & (
        LENGTH - 1
    )
    lane = lax.broadcasted_iota(jnp.int32, (128, 2 * HD), 1) & (HD - 1)
    past_one, past_two = lane >= 2 * ROLL, lane >= 4 * ROLL
    live = lane < 6 * ROLL
    within = lane - jnp.where(past_two, 4 * ROLL, jnp.where(past_one, 2 * ROLL, 0))
    second = within >= ROLL
    step = jnp.where(second, within - ROLL, within).astype(jnp.float32)
    coordinate = jnp.where(
        past_two, token & (GW - 1), jnp.where(past_one, (token >> 4) & (GH - 1), token >> 8)
    ).astype(jnp.float32)
    angle = jnp.where(live, coordinate * jnp.exp(step * (-math.log(BASE) / ROLL)), 0.0)
    cosine = jnp.cos(angle)
    sine = jnp.sin(angle)
    from_first = jnp.where(live & second, sine, 0.0)
    from_second = jnp.where(live, jnp.where(second, 0.0, -sine), 0.0)
    return cosine, from_first, from_second


def turn(v, c, s1, s2, sign):
    return v * c + sign * (pltpu.roll(v, ROLL, 1) * s1 + pltpu.roll(v, 2 * HD - ROLL, 1) * s2)


def dot_nt(a, b):
    return lax.dot_general(a, b, (((1,), (1,)), ((), ())), preferred_element_type=jnp.float32)


def dot_tn(a, b):
    return lax.dot_general(a, b, (((0,), (0,)), ((), ())), preferred_element_type=jnp.float32)


def dot_nn(a, b):
    return lax.dot_general(a, b, (((1,), (0,)), ((), ())), preferred_element_type=jnp.float32)


MESH = pl.DeviceIdType.MESH
PIECES = ((0, 0, 384, 0), (1, 384, 128, 0), (2, 512, 256, 0), (2, 768, 256, 1024), (3, 1024, 256, 0), (3, 1280, 256, 1024))
SHARD = 128
PLANE_FIRST = (3,)
HALVES = ((0, 64), (64, 64))
WHOLE = ((0, 128),)
MIB = 1024 * 1024


def split(piece_and_rows):
    return [
        (piece, r, at, rows, early)
        for piece, parts, early in piece_and_rows
        for at, rows in parts
        for r in range(2)
    ]


def remote(src, dst, send, recv, target):
    return pltpu.make_async_remote_copy(
        src_ref=src, dst_ref=dst, send_sem=send, recv_sem=recv, device_id=target, device_id_type=MESH
    )


def flip(index, bit):
    return index + bit - 2 * bit * ((index // bit) % 2)


def peers():
    lane = lax.axis_index("tensor")
    shard = lax.axis_index("fsdp")
    is_mid = (lane == 1) | (lane == 2)
    pair = {"tensor": flip(lane, 1)}
    across = {"tensor": 3 - lane}
    x_peer = {"fsdp": flip(shard, 2)}
    y_peer = {"fsdp": flip(shard, 4)}
    return lane, shard, is_mid, pair, across, x_peer, y_peer


def meet(targets):
    barrier = pltpu.get_barrier_semaphore()
    for target in targets:
        pl.semaphore_signal(barrier, inc=1, device_id=target, device_id_type=MESH)
    pl.semaphore_wait(barrier, len(targets))


GATHER = split(
    [(PIECES[0], HALVES, False)] + [(piece, WHOLE, i in PLANE_FIRST) for i, piece in enumerate(PIECES) if i]
)


def gather_kernel(
    packs_ref, vec_ref, bias_ref, tokens_ref, cotangent_ref,
    qkv_ref, proj_ref, up_ref, down_ref, vec_all, bias_all, h_ref, low_ref, o_ref, lse_ref,
    x_ref, gy_ref, c_ref, s1_ref, s2_ref,
    pack_ref, stage_ref, wq_ref, kh_ref, vh_ref,
    load_sem, local_sem, send_sem, recv_sem, small_send, small_recv, row_send, row_recv,
):
    lane, shard, is_mid, pair, across, x_peer, y_peer = peers()
    core = shard % 2
    outs = (qkv_ref, proj_ref, up_ref, down_ref)
    shard_peers = [
        (q, dc, {"fsdp": flip_place(shard, q, dc)})
        for q in range(4)
        for dc in range(2)
        if (q, dc) != (0, 0)
    ]
    lane_peers = [pair, {"tensor": (lane + 2) % 4}, across]
    other_core = {"fsdp": flip(shard, 1)}
    cross = {"fsdp": flip(shard, 1), "tensor": flip(lane, 1)}
    meet([t for _, _, t in shard_peers] + lane_peers + [cross])
    moved = (core + lane) % 2 == 1
    half = LENGTH // 2

    def permuted(index, src_ref, dst_ref):
        for r in range(2):
            for q in range(4):
                at = pl.ds(pl.multiple_of(global_block(shard, r, q) * SHARD, SHARD), SHARD)
                block = r * 4 + q
                dst_ref[index, :, block * SHARD : (block + 1) * SHARD] = src_ref[:, at]

    def hop_swap(k, dst_ref):
        return remote(
            stage_ref.at[k], dst_ref.at[pl.ds(0, half)], row_send.at[k, 0], row_recv.at[k, 0], cross
        )

    def hop_core(k, dst_ref):
        return remote(
            dst_ref.at[pl.ds(0, half)], dst_ref.at[pl.ds(half, half)], row_send.at[k, 1], row_recv.at[k, 1], other_core
        )

    def rows_out(k, src_ref, dst_ref):
        permuted(k, src_ref, stage_ref)

        @pl.when(moved)
        def _():
            hop_swap(k, dst_ref).start()

        @pl.when(jnp.logical_not(moved))
        def _():
            dst_ref[0:half, :] = stage_ref[k]
            hop_core(k, dst_ref).start()

    def rows_on(k, dst_ref):
        @pl.when(moved)
        def _():
            hop_swap(k, dst_ref).wait_recv()
            hop_core(k, dst_ref).start()

    def rows_in(k, dst_ref):
        hop_core(k, dst_ref).wait()

        @pl.when(moved)
        def _():
            hop_swap(k, dst_ref).wait_send()

    pack_hop = remote(packs_ref.at[1 - core], pack_ref.at[core], row_send.at[2, 0], row_recv.at[2, 0], other_core)
    pack_hop.start()
    pack_ref[core] = packs_ref[core]

    def window(c, block, col0, col_count):
        (m, _, width, base), r, at, rows, _ = GATHER[c]
        return outs[m].at[
            pl.ds((r * 4 + block) * SHARD + at, rows), pl.ds(base + col0 * width, col_count * width)
        ]

    def own(c):
        (_, first, width, _), r, at, rows, _ = GATHER[c]
        return pack_ref.at[r, pl.ds(at, rows), pl.ds(first, width)]

    def local(c):
        return pltpu.make_async_copy(own(c), window(c, 0, 0, 1), local_sem.at[c])

    def plane_first(c):
        return GATHER[c][4]

    def plane(c):
        return ((1, x_peer), (2, y_peer))[GATHER[c][1]]

    def blocks(c):
        return (0, plane(c)[0]) if plane_first(c) else (0,)

    def hop_pair(c):
        return [
            remote(
                own(c) if b == 0 else window(c, b, 0, 1), window(c, b, 1, 1),
                send_sem.at[c, 6 * k], recv_sem.at[c, 5 * k], pair,
            )
            for k, b in enumerate(blocks(c))
        ]

    def hop_across(c):
        return [
            remote(
                window(c, b, 0, 2), window(c, b, 2, 2), send_sem.at[c, 1 + 6 * k], recv_sem.at[c, 1 + 5 * k], across
            )
            for k, b in enumerate(blocks(c))
        ]

    def hop_out(c):
        return [
            remote(
                window(c, b, 2, 2), window(c, b, 2, 2), send_sem.at[c, 2 + 6 * k], recv_sem.at[c, 1 + 5 * k], pair
            )
            for k, b in enumerate(blocks(c))
        ]

    def hop_first(c):
        block, target = plane(c)
        if plane_first(c):
            return remote(
                own(c), window(c, block, 0, 1), send_sem.at[c, 3], recv_sem.at[c, 2], target
            )
        return remote(
            window(c, 0, 0, 4), window(c, block, 0, 4), send_sem.at[c, 3], recv_sem.at[c, 2], target
        )

    def hop_second(c):
        moves, target = ((((0, 2), (1, 3)), y_peer), (((0, 1), (2, 3)), x_peer))[GATHER[c][1]]
        return [
            remote(
                window(c, src, 0, 4), window(c, dst, 0, 4), send_sem.at[c, 4 + k], recv_sem.at[c, 3 + k], target
            )
            for k, (src, dst) in enumerate(moves)
        ]

    count = len(GATHER)
    small = []
    slot = core * 4
    vec_all[pl.ds(slot, 1)] = vec_ref[...][None]
    bias_all[0] = bias_ref[...]
    for i, (q, _, target) in enumerate(shard_peers):
        small.append(remote(vec_ref, vec_all.at[slot + q], small_send.at[i], small_recv.at[i], target))
    far_slot = 3 - is_mid.astype(jnp.int32)
    for i, target in enumerate(lane_peers):
        to = bias_all.at[1] if i == 0 else bias_all.at[far_slot]
        small.append(remote(bias_ref, to, small_send.at[7 + i], small_recv.at[7 + i], target))

    def start(copies):
        for copy in copies:
            copy.start()

    def arrive(copies):
        for copy in copies:
            copy.wait_recv()

    def begin(c):
        if plane_first(c):
            hop_first(c).start()
        else:
            start(hop_pair(c))

    def to_far(c):
        local(c).wait()
        arrive(hop_pair(c))

        @pl.when(is_mid)
        def _():
            start(hop_across(c))

    def into_plane(c):
        if plane_first(c):
            start(hop_second(c))
        else:
            hop_first(c).start()

    def on_mid(c):
        @pl.when(is_mid)
        def _():
            arrive(hop_across(c))
            start(hop_out(c))
            into_plane(c)

    def on_end(c):
        @pl.when(jnp.logical_not(is_mid))
        def _():
            arrive(hop_across(c))
            into_plane(c)

    def to_pair(c):
        hop_first(c).wait_recv()
        start(hop_pair(c))

    def finish(c):
        hop_first(c).wait_recv()
        start(hop_second(c))

    def each(step, *chunks):
        for c in chunks:
            step(c)

    for copy in small:
        copy.start()
    pack_hop.wait()
    each(begin, 0, 1, 2, 3, 8, 9, 4, 5, 6, 7)
    for c in range(count):
        local(c).start()
    each(to_far, 0, 1, 2, 3)
    each(on_mid, 0, 1, 2, 3)
    rows_out(0, tokens_ref, x_ref)
    each(on_end, 0, 1, 2, 3)

    @pl.loop(0, LENGTH // 128)
    def _(i):
        rows = pl.ds(pl.multiple_of(i * 128, 128), 128)
        c_ref[rows, :], s1_ref[rows, :], s2_ref[rows, :] = rotary_rows(i * 128, core)

    each(to_far, 4, 5)
    each(finish, 0, 1, 2, 3)
    rows_on(0, x_ref)
    each(on_mid, 4, 5)
    each(to_far, 6, 7)
    for copy in small:
        copy.wait()
    rows_in(0, x_ref)
    gain = jnp.concatenate([vec_all[b, 0:1, :] for b in range(8)], axis=1)
    shift = jnp.concatenate([vec_all[b, 1:2, :] for b in range(8)], axis=1)

    @pl.loop(0, LENGTH // 64)
    def _(i):
        rows = pl.ds(pl.multiple_of(i * 64, 64), 64)
        unit, _ = norm_parts(x_ref[rows, :].astype(jnp.float32))
        h_ref[rows, :] = (unit * gain + shift).astype(LOW)

    first = 4
    each(on_end, 4, 5)
    each(on_mid, 6, 7)
    each(finish, 4, 5)
    each(on_end, 6, 7)
    for c in range(first):
        for copy in hop_second(c):
            copy.wait_recv()
    load = pltpu.make_async_copy(qkv_ref, wq_ref, load_sem.at[0])
    load.start()
    load.wait()
    width = 2 * HD
    lane_q = lax.broadcasted_iota(jnp.int32, (QB, width), 1)

    plan = (
        ((to_pair, (8, 9)),),
        ((to_far, (8, 9)), (begin, (10, 11, 12, 13))),
        ((on_mid, (8, 9)), (finish, (6, 7))),
        ((on_end, (8, 9)), (to_far, (10, 11))),
        ((on_mid, (10, 11)),),
        ((on_end, (10, 11)), (to_far, (12, 13))),
        ((on_mid, (12, 13)),),
        ((on_end, (12, 13)),),
    )

    @pl.loop(0, 8)
    def _(t):
        z = t // 2
        base = z * 3 * width

        def columns(part):
            return pl.ds(pl.multiple_of(base + part * width, width), width)

        @pl.when(t % 2 == 0)
        def _():
            bias = bias_all[pl.ds(z, 1), 0:1, 0 : 3 * width][0]

            @pl.loop(0, LENGTH // QB)
            def _(i):
                rows = pl.ds(pl.multiple_of(i * QB, QB), QB)
                weights = wq_ref[:, pl.ds(pl.multiple_of(base, width), 3 * width)]
                qkv = dot_nn(h_ref[rows, :], weights) + bias
                c, s1, s2 = c_ref[rows, :], s1_ref[rows, :], s2_ref[rows, :]
                low_ref[rows, columns(0)] = turn(qkv[:, :width], c, s1, s2, 1.0).astype(LOW)
                k = turn(qkv[:, width : 2 * width], c, s1, s2, 1.0)
                v = qkv[:, 2 * width :]
                low_ref[rows, columns(1)] = k.astype(LOW)
                low_ref[rows, columns(2)] = v.astype(LOW)
                for h in range(2):
                    mine = (lane_q < HD) if h == 0 else (lane_q >= HD)
                    kh_ref[h, rows, :] = jnp.where(mine, k, 0.0).astype(LOW)
                    vh_ref[h, rows, :] = jnp.where(mine, v, 0.0).astype(LOW)

        for k, steps in enumerate(plan):

            @pl.when(t == k)
            def _():
                for step, chunks in steps:
                    each(step, *chunks)
                if k == 7:
                    rows_out(1, cotangent_ref, gy_ref)

        @pl.loop(0, 2)
        def _(half):
            rows = pl.ds(pl.multiple_of(((t % 2) * 2 + half) * QB, QB), QB)
            q = (low_ref[rows, columns(0)].astype(jnp.float32) * SCALE).astype(LOW)
            total = jnp.zeros((width, QB), jnp.float32)
            for h in range(2):
                s = dot_nt(kh_ref[h], q)
                peak = jnp.max(s, axis=0, keepdims=True)
                e = jnp.exp(s - peak)
                mass = jnp.sum(e, axis=0, keepdims=True)
                p = (e * (1.0 / mass)).astype(LOW)
                total += dot_tn(vh_ref[h], p)
                lse_ref[pl.ds(z, 1), h : h + 1, rows] = (peak + jnp.log(mass))[None]
            o_ref[rows, pl.ds(pl.multiple_of(z * width, width), width)] = total.T.astype(LOW)

    each(finish, 10, 11)
    rows_on(1, gy_ref)
    each(finish, 12, 13)
    rows_in(1, gy_ref)
    for c in range(count):
        for copy in hop_second(c):
            copy.wait_send()
            if c >= first:
                copy.wait_recv()
        for copy in hop_pair(c):
            copy.wait_send()
        hop_first(c).wait_send()

        @pl.when(is_mid)
        def _():
            for copy in hop_across(c) + hop_out(c):
                copy.wait_send()


def global_block(shard, r, q):
    return flip_place(shard - shard % 2 + r, q, 0)


def flip_place(shard, q, dc):
    target = shard
    for bit, on in ((1, dc), (2, q & 1), (4, q >> 1)):
        if on:
            target = flip(target, bit)
    return target


def gather_all(packs, vec, bias, tokens, cotangent):
    count = len(GATHER)
    rows = 8 * SHARD
    any_space = pl.BlockSpec(memory_space=pl.ANY)
    vmem = pl.BlockSpec(memory_space=pltpu.VMEM)
    width = 2 * HD
    return pl.pallas_call(
        gather_kernel,
        in_specs=[vmem] * 5,
        out_specs=[any_space] * 4 + [vmem] * 11,
        out_shape=[
            jax.ShapeDtypeStruct((rows, 1536), LOW),
            jax.ShapeDtypeStruct((rows, 512), LOW),
            jax.ShapeDtypeStruct((rows, 2048), LOW),
            jax.ShapeDtypeStruct((rows, 2048), LOW),
            jax.ShapeDtypeStruct((8,) + vec.shape, jnp.float32),
            jax.ShapeDtypeStruct((4,) + bias.shape, jnp.float32),
            jax.ShapeDtypeStruct((LENGTH, D), LOW),
            jax.ShapeDtypeStruct((LENGTH, 1536), LOW),
            jax.ShapeDtypeStruct((LENGTH, 512), LOW),
            jax.ShapeDtypeStruct((4, 2, LENGTH), jnp.float32),
            jax.ShapeDtypeStruct((LENGTH, D), LOW),
            jax.ShapeDtypeStruct((LENGTH, D), LOW),
            jax.ShapeDtypeStruct((LENGTH, width), jnp.float32),
            jax.ShapeDtypeStruct((LENGTH, width), jnp.float32),
            jax.ShapeDtypeStruct((LENGTH, width), jnp.float32),
        ],
        scratch_shapes=[
            pltpu.VMEM((2, SHARD, 1536), LOW),
            pltpu.VMEM((2, LENGTH // 2, D), LOW),
            pltpu.VMEM((D, 1536), LOW),
            pltpu.VMEM((2, LENGTH, width), LOW),
            pltpu.VMEM((2, LENGTH, width), LOW),
            pltpu.SemaphoreType.DMA((1,)),
            pltpu.SemaphoreType.DMA((count,)),
            pltpu.SemaphoreType.DMA((count, 9)),
            pltpu.SemaphoreType.DMA((count, 7)),
            pltpu.SemaphoreType.DMA((10,)),
            pltpu.SemaphoreType.DMA((10,)),
            pltpu.SemaphoreType.DMA((3, 2)),
            pltpu.SemaphoreType.DMA((3, 2)),
        ],
        compiler_params=pltpu.CompilerParams(
            collective_id=1, has_side_effects=True, vmem_limit_bytes=48 * MIB
        ),
        name="gather_attend",
    )(packs, vec, bias, tokens, cotangent)


SUMMED = (
    (0, 0, 256, 0),
    (0, 256, 256, 1024),
    (1, 512, 256, 0),
    (1, 768, 256, 1024),
    (2, 1024, 128, 0),
    (3, 1152, 384, 0),
)
SUM_PLANE_LAST = (1, 2)
SCATTER = split(
    [(piece, WHOLE, i in SUM_PLANE_LAST) for i, piece in enumerate(SUMMED[:5])] + [(SUMMED[5], HALVES, False)]
)
EXTRA_AT, EXTRA_WIDTH = 256, 512
SUM_WIDTH = 1536


def scatter_kernel(
    down_ref, up_ref, proj_ref, low_ref, go_ref, lse_ref, c_ref, s1_ref, s2_ref, h_ref, wq_ref,
    vec_ref, x_ref, gx_ref, layer_ref,
    out_ref, bias_ref, norm_ref, layer_out, input_out, gh_ref,
    other_ref, low_stage, gq_ref, g_ref, kh_ref, vh_ref, gk_ref, gv_ref,
    own_ref, first_ref, second_ref, in_ref, mid_ref, near_ref, in_more, mid_more, near_more,
    local_sem, send_sem, recv_sem, row_send, row_recv,
):
    grads = (down_ref, up_ref, proj_ref, gq_ref)
    lane, shard, is_mid, pair, across, x_peer, y_peer = peers()
    barrier = pltpu.get_barrier_semaphore()
    other_core = {"fsdp": flip(shard, 1)}
    cross = {"fsdp": flip(shard, 1), "tensor": flip(lane, 1)}
    moved = (shard % 2 + lane) % 2 == 1
    half = LENGTH // 2
    for target in (pair, x_peer, y_peer, other_core, cross):
        pl.semaphore_signal(barrier, inc=1, device_id=target, device_id_type=MESH)

    @pl.when(is_mid)
    def _():
        pl.semaphore_signal(barrier, inc=1, device_id=across, device_id_type=MESH)

    pl.semaphore_wait(barrier, 5 + is_mid.astype(jnp.int32))

    def hop_rows(k, src, dst):
        return remote(src, dst, row_send.at[k], row_recv.at[k], cross)

    hop_sum = remote(gh_ref.at[pl.ds(half, half)], other_ref, row_send.at[2], row_recv.at[2], other_core)

    def source(c, block):
        (a, _, width, base), r, at, rows, _ = SCATTER[c]
        return grads[a].at[pl.ds((r * 4 + block) * SHARD + at, rows), pl.ds(base, 4 * width)]

    def part(ref, c, block, lo, hi, each):
        (_, first, width, _), r, at, rows, _ = SCATTER[c]
        if ref is in_more or ref is mid_more or ref is near_more:
            first -= EXTRA_AT
        return ref.at[
            r, pl.ds(block * SHARD + at, rows), pl.ds(first * each + lo * width, (hi - lo) * width)
        ]

    def plane_last(c):
        return SCATTER[c][4]

    def keep(c):
        blocks = ((0, 1), (0, 2))[SCATTER[c][1]]
        return [
            pltpu.make_async_copy(source(c, block), part(own_ref, c, k, 0, 4, 4), local_sem.at[c, k])
            for k, block in enumerate(blocks)
        ]

    def hop_first(c):
        blocks, target = (((2, 3), y_peer), ((1, 3), x_peer))[SCATTER[c][1]]
        return [
            remote(
                source(c, block), part(first_ref, c, k, 0, 4, 4), send_sem.at[c, k], recv_sem.at[c, k], target
            )
            for k, block in enumerate(blocks)
        ]

    def hop_second(c):
        hi = 1 if plane_last(c) else 4
        return remote(
            part(own_ref, c, 1, 0, hi, 4), part(second_ref, c, 0, 0, hi, 4),
            send_sem.at[c, 2], recv_sem.at[c, 2], (x_peer, y_peer)[SCATTER[c][1]],
        )

    def sides(c, ref, more):
        return (ref, more) if plane_last(c) else (ref,)

    def hop_in(c):
        return [
            remote(
                part(own_ref, c, k, 2, 4, 4), part(ref, c, 0, 0, 2, 2),
                send_sem.at[c, 3 + 2 * k], recv_sem.at[c, 3 + 3 * k], pair,
            )
            for k, ref in enumerate(sides(c, in_ref, in_more))
        ]

    def hop_across(c):
        return [
            remote(
                part(own_ref, c, k, 2, 4, 4), part(ref, c, 0, 0, 2, 2),
                send_sem.at[c, 3 + 2 * k], recv_sem.at[c, 4 + 3 * k], across,
            )
            for k, ref in enumerate(sides(c, mid_ref, mid_more))
        ]

    def hop_pair(c):
        return [
            remote(
                part(own_ref, c, k, 1, 2, 4), part(ref, c, 0, 0, 1, 1),
                send_sem.at[c, 4 + 2 * k], recv_sem.at[c, 5 + 3 * k], pair,
            )
            for k, ref in enumerate(sides(c, near_ref, near_more))
        ]

    def start(copies):
        for copy in copies:
            copy.start()

    def arrive(copies):
        for copy in copies:
            copy.wait_recv()

    def add(dst, left, right):
        step = 16

        @pl.loop(0, dst.shape[0] // step)
        def _(i):
            at = pl.ds(pl.multiple_of(i * step, step), step)
            total = left[at, :].astype(jnp.float32) + right[at, :].astype(jnp.float32)
            dst[at, :] = total.astype(dst.dtype)

    count = len(SCATTER)
    lead = 4

    def inward(c):
        @pl.when(jnp.logical_not(is_mid))
        def _():
            start(hop_in(c))

    def to_middle(c):
        @pl.when(is_mid)
        def _():
            arrive(hop_in(c))
            for k, ref in enumerate(sides(c, in_ref, in_more)):
                far = part(own_ref, c, k, 2, 4, 4)
                add(far, far, part(ref, c, 0, 0, 2, 2))
            start(hop_across(c))

    def from_middle(c):
        @pl.when(is_mid)
        def _():
            arrive(hop_across(c))
            for k, ref in enumerate(sides(c, mid_ref, mid_more)):
                near = part(own_ref, c, k, 0, 2, 4)
                add(near, near, part(ref, c, 0, 0, 2, 2))

        start(hop_pair(c))

    def send(c):
        start(hop_first(c))
        start(keep(c))

    def fold_first(c):
        for copy in keep(c):
            copy.wait()
        arrive(hop_first(c))
        mine = part(own_ref, c, 1, 0, 4, 4)
        add(mine, mine, part(first_ref, c, 1, 0, 4, 4))
        if not plane_last(c):
            hop_second(c).start()
        mine = part(own_ref, c, 0, 0, 4, 4)
        add(mine, mine, part(first_ref, c, 0, 0, 4, 4))
        if plane_last(c):
            inward(c)

    def fold_second(c):
        if plane_last(c):
            to_middle(c)
        else:
            hop_second(c).wait_recv()
            mine = part(own_ref, c, 0, 0, 4, 4)
            add(mine, mine, part(second_ref, c, 0, 0, 4, 4))
            inward(c)

    def fold_third(c):
        if plane_last(c):
            from_middle(c)
        else:
            to_middle(c)

    def fold_fourth(c):
        if plane_last(c):
            arrive(hop_pair(c))
            for k, ref in ((1, near_more), (0, near_ref)):
                mine = part(own_ref, c, k, 0, 1, 4)
                add(mine, mine, part(ref, c, 0, 0, 1, 1))
                if k:
                    hop_second(c).start()
        else:
            from_middle(c)

    def fold_last(c):
        if plane_last(c):
            hop_second(c).wait_recv()
            last = part(second_ref, c, 0, 0, 1, 4)
        else:
            arrive(hop_pair(c))
            last = part(near_ref, c, 0, 0, 1, 1)
        add(part(out_ref, c, 0, 0, 1, 1), part(own_ref, c, 0, 0, 1, 4), last)

    def tick(now):
        for step, late in (
            (fold_first, 0), (send, -2), (fold_second, 1), (fold_third, 2), (fold_fourth, 3), (fold_last, 4)
        ):
            group = now - late
            if 0 <= group < count // 2:
                step(2 * group)
                step(2 * group + 1)

    for c in range(lead):
        for copy in hop_first(c):
            copy.start()
        for copy in keep(c):
            copy.start()

    @pl.when(moved)
    def _():
        hop_rows(0, layer_ref, layer_out).start()

    width = 2 * HD
    lane_q = lax.broadcasted_iota(jnp.int32, (QB, width), 1)

    @pl.loop(0, 8)
    def _(t):
        z = t // 2
        base = z * 3 * width

        def columns(part_index):
            return pl.ds(pl.multiple_of(base + part_index * width, width), width)

        @pl.when(t % 2 == 0)
        def _():
            @pl.loop(0, LENGTH // QB)
            def _(i):
                rows = pl.ds(pl.multiple_of(i * QB, QB), QB)
                k = low_ref[rows, columns(1)].astype(jnp.float32)
                v = low_ref[rows, columns(2)].astype(jnp.float32)
                for h in range(2):
                    mine = (lane_q < HD) if h == 0 else (lane_q >= HD)
                    kh_ref[h, rows, :] = jnp.where(mine, k, 0.0).astype(LOW)
                    vh_ref[h, rows, :] = jnp.where(mine, v, 0.0).astype(LOW)

            gk_ref[...] = jnp.zeros_like(gk_ref)
            gv_ref[...] = jnp.zeros_like(gv_ref)

        for k in range(3):

            @pl.when(t == 2 * k + 2)
            def _():
                tick(k)

        @pl.loop(0, 2)
        def _(half):
            rows = pl.ds(pl.multiple_of(((t % 2) * 2 + half) * QB, QB), QB)
            q = low_ref[rows, columns(0)].astype(jnp.float32) * SCALE
            go = go_ref[rows, pl.ds(pl.multiple_of(z * width, width), width)].astype(jnp.float32)
            total = jnp.zeros((width, QB), jnp.float32)
            for h in range(2):
                mine = (lane_q < HD) if h == 0 else (lane_q >= HD)
                qh = jnp.where(mine, q, 0.0).astype(LOW)
                gh = jnp.where(mine, go, 0.0).astype(LOW)
                p = jnp.exp(dot_nt(kh_ref[h], qh) - lse_ref[pl.ds(z, 1), h : h + 1, rows][0])
                dp = dot_nt(vh_ref[h], gh)
                pd = jnp.sum(p * dp, axis=0, keepdims=True)
                ds = (p * (dp - pd)).astype(LOW)
                gv_ref[...] += dot_nn(p.astype(LOW), gh)
                gk_ref[...] += dot_nn(ds, qh)
                total += dot_tn(kh_ref[h], ds)
            gq = turn(total.T * SCALE, c_ref[rows, :], s1_ref[rows, :], s2_ref[rows, :], -1.0)
            g_ref[rows, :width] = gq.astype(LOW)

        @pl.when(t % 2 == 1)
        def _():
            wide = pl.ds(pl.multiple_of(base, width), 3 * width)
            gk = turn(gk_ref[...], c_ref[...], s1_ref[...], s2_ref[...], -1.0)
            g_ref[:, width : 2 * width] = gk.astype(LOW)
            g_ref[:, 2 * width :] = gv_ref[...].astype(LOW)
            bias_ref[:, wide] = jnp.sum(g_ref[...].astype(jnp.float32), axis=0, keepdims=True)

            @pl.loop(0, D // QB)
            def _(i):
                some = pl.ds(pl.multiple_of(i * QB, QB), QB)
                gq_ref[some, wide] = dot_tn(h_ref[:, some], g_ref[...]).astype(LOW)
                product = dot_nt(g_ref[some, :], wq_ref[:, wide])

                @pl.when(z == 0)
                def _():
                    gh_ref[some, :] = product

                @pl.when(z > 0)
                def _():
                    gh_ref[some, :] += product

    hop_sum.start()
    tick(3)
    gain = jnp.concatenate([vec_ref[b, 0:1, :] for b in range(8)], axis=1)
    norm_ref[...] = jnp.zeros_like(norm_ref)
    hop_sum.wait()

    @pl.loop(0, half // 64)
    def _(i):
        some = pl.ds(pl.multiple_of(i * 64, 64), 64)
        grad = gh_ref[some, :] + other_ref[some, :]
        unit, scale = norm_parts(x_ref[some, :].astype(jnp.float32))
        norm_ref[0:1, :] += jnp.sum(grad * unit, axis=0, keepdims=True)
        norm_ref[1:2, :] += jnp.sum(grad, axis=0, keepdims=True)
        value = gx_ref[some, :] + norm_back(grad, unit, scale, gain)
        gh_ref[some, :] = value
        low_stage[some, :] = value.astype(LOW)

    @pl.when(moved)
    def _():
        hop_rows(1, low_stage, input_out).start()

    for now in range(4, count // 2 + 4):
        tick(now)

    @pl.when(moved)
    def _():
        hop_rows(0, layer_ref, layer_out).wait()
        hop_rows(1, low_stage, input_out).wait()

    for c in range(count):
        for copy in hop_first(c):
            copy.wait_send()
        hop_second(c).wait_send()
        for copy in hop_pair(c):
            copy.wait_send()

        @pl.when(is_mid)
        def _():
            for copy in hop_across(c):
                copy.wait_send()

        @pl.when(jnp.logical_not(is_mid))
        def _():
            for copy in hop_in(c):
                copy.wait_send()


def scatter_all(grads, attention, rows):
    count = len(SCATTER)
    width = SUM_WIDTH
    vmem = pl.BlockSpec(memory_space=pltpu.VMEM)
    any_space = pl.BlockSpec(memory_space=pl.ANY)
    pair_width = 2 * HD
    return pl.pallas_call(
        scatter_kernel,
        in_specs=[any_space] * 3 + [vmem] * 11 + [any_space],
        out_specs=[vmem] * 3 + [any_space] * 2 + [vmem],
        out_shape=[
            jax.ShapeDtypeStruct((2, SHARD, width), jnp.float32),
            jax.ShapeDtypeStruct((1, 1536), jnp.float32),
            jax.ShapeDtypeStruct((8, D), jnp.float32),
            jax.ShapeDtypeStruct((LENGTH // 2, D), LOW),
            jax.ShapeDtypeStruct((LENGTH // 2, D), LOW),
            jax.ShapeDtypeStruct((LENGTH, D), jnp.float32),
        ],
        scratch_shapes=[
            pltpu.VMEM((LENGTH // 2, D), jnp.float32),
            pltpu.VMEM((LENGTH // 2, D), LOW),
            pltpu.VMEM((D, 1536), LOW),
            pltpu.VMEM((LENGTH, 3 * pair_width), LOW),
            pltpu.VMEM((2, LENGTH, pair_width), LOW),
            pltpu.VMEM((2, LENGTH, pair_width), LOW),
            pltpu.VMEM((LENGTH, pair_width), jnp.float32),
            pltpu.VMEM((LENGTH, pair_width), jnp.float32),
            pltpu.VMEM((2, 2 * SHARD, 4 * width), LOW),
            pltpu.VMEM((2, 2 * SHARD, 4 * width), LOW),
            pltpu.VMEM((2, SHARD, 4 * width), LOW),
            pltpu.VMEM((2, SHARD, 2 * width), LOW),
            pltpu.VMEM((2, SHARD, 2 * width), LOW),
            pltpu.VMEM((2, SHARD, width), LOW),
            pltpu.VMEM((2, SHARD, 2 * EXTRA_WIDTH), LOW),
            pltpu.VMEM((2, SHARD, 2 * EXTRA_WIDTH), LOW),
            pltpu.VMEM((2, SHARD, EXTRA_WIDTH), LOW),
            pltpu.SemaphoreType.DMA((count, 2)),
            pltpu.SemaphoreType.DMA((count, 7)),
            pltpu.SemaphoreType.DMA((count, 9)),
            pltpu.SemaphoreType.DMA((3,)),
            pltpu.SemaphoreType.DMA((3,)),
        ],
        compiler_params=pltpu.CompilerParams(
            collective_id=2, has_side_effects=True, vmem_limit_bytes=60 * MIB
        ),
        name="scatter_attend_back",
    )(*grads, *attention, *rows)


def place_kernel(layer_ref, layer_low, input_ref, input_low, layer_out, input_out):
    shard = lax.axis_index("fsdp")
    moved = (shard % 2 + lax.axis_index("tensor")) % 2 == 1
    for own, other, out in ((layer_ref, layer_low, layer_out), (input_ref, input_low, input_out)):
        for r in range(2):
            for q in range(4):
                at = pl.ds(pl.multiple_of(global_block(shard, r, q) * SHARD, SHARD), SHARD)
                here = pl.ds((r * 4 + q) * SHARD, SHARD)

                @pl.when(moved)
                def _():
                    out[:, at] = other[:, here].astype(jnp.float32)

                @pl.when(jnp.logical_not(moved))
                def _():
                    out[:, at] = own[:, here]


def place_rows(layer, layer_low, grad, grad_low):
    block = pl.BlockSpec((128, D), lambda i: (i, 0))
    shape = jax.ShapeDtypeStruct((LENGTH // 2, D), jnp.float32)
    return pl.pallas_call(
        place_kernel,
        grid=(LENGTH // 256,),
        in_specs=[block] * 4,
        out_specs=[block] * 2,
        out_shape=[shape] * 2,
        name="place_rows",
    )(layer, layer_low, grad, grad_low)


COUNTS = (3 * D, D, FF, FF)
BLOCKS = (6, 2, 8, 8)


def offsets():
    return [(z * 8 + q * 2 + dc, q, dc, z) for z in range(4) for q in range(4) for dc in range(2)]


def stepped(g, state):
    new = DECAY * state + (1.0 - DECAY) * (g * g + TINY)
    return new, g * lax.rsqrt(new)


def rows_step(squares, old):
    which = lax.broadcasted_iota(jnp.int32, (4, 128), 0)
    counts = jnp.where(
        which == 0, float(COUNTS[0]), jnp.where(which == 1, float(COUNTS[1]), float(COUNTS[2]))
    )
    return DECAY * old + (1.0 - DECAY) * (squares / counts + TINY)


def tune_kernel(
    sums_ref, vec_ref, db_ref, wq_ref, wp_ref, wu_ref, wd_ref, vw_ref, vs_ref, rows_ref,
    cq_ref, cp_ref, cu_ref, cd_ref, bq_ref, bu_ref, bqs_ref, bus_ref,
    gq, gp_out, gu_out, gd_out, bq_out, bu_out, lane_out, col_out, grand_out,
    vec_send, vec_recv, db_recv, lane_send, lane_recv, col_send, col_recv, all_send, all_recv,
    core_send, core_done, a_send, a_recv, b_send, b_recv, c_send, c_recv,
):
    lane = lax.axis_index("tensor")
    shard = lax.axis_index("fsdp")
    core = shard % 2
    is_mid = (lane == 1) | (lane == 2)
    z_of = [lane, flip(lane, 1), 3 - lane, (lane + 2) % 4]

    def device(q, dc, z):
        target = {}
        if q or dc:
            target["fsdp"] = flip_place(shard, q, dc)
        if z:
            target["tensor"] = z_of[z]
        return target

    others = [entry for entry in offsets() if entry[0]]
    meet([device(q, dc, z) for _, q, dc, z in others])
    shard_peers = [(slot, q, dc) for slot, q, dc, z in others if z == 0]

    def core_copies():
        give = 1 - core
        hq = pl.ds(pl.multiple_of(core * 128, 128), 128)
        hf = pl.ds(pl.multiple_of(core * 512, 512), 512)
        pairs = [(sums_ref.at[give, :, pl.ds(1152 + j * 128, 128)], gq.at[j, :, hq]) for j in range(3)]
        pairs.append((sums_ref.at[give, :, pl.ds(1024, 128)], gp_out.at[:, hq]))
        pairs.append((sums_ref.at[give, :, pl.ds(512, 512)], gu_out.at[:, hf]))
        pairs.append((sums_ref.at[give, :, pl.ds(0, 512)], gd_out.at[:, hf]))
        return [
            remote(src, dst, core_send.at[i], core_done.at[i], {"fsdp": flip(shard, 1)})
            for i, (src, dst) in enumerate(pairs)
        ]

    for copy in core_copies():
        copy.start()

    def round_a():
        copies = [
            remote(vec_send.at[slot], vec_recv.at[slot], a_send.at[slot], a_recv.at[slot], device(q, dc, 0))
            for slot, q, dc in shard_peers
        ]
        for z in range(1, 4):
            position = 1 if z == 1 else (3 - is_mid.astype(jnp.int32) if z == 2 else 2 + is_mid.astype(jnp.int32))
            copies.append(
                remote(db_ref.at[position], db_recv.at[z], a_send.at[7 + z], a_recv.at[7 + z], device(0, 0, z))
            )
        return copies

    for slot in range(8):
        q, dc = slot // 2, slot % 2
        block = (core + dc - 2 * core * dc) * 4 + q
        at = pl.ds(pl.multiple_of(block * 128, 128), 128)
        if slot == 0:
            vec_recv[0] = vec_ref[:, at]
        else:
            vec_send[slot] = vec_ref[:, at]
    for copy in round_a():
        copy.start()
    db_recv[0] = db_ref[0]

    mine_q = pl.ds(pl.multiple_of(core * 128, 128), 128)
    mine_f = pl.ds(pl.multiple_of(core * 512, 512), 512)
    for j in range(3):
        gq[j, :, mine_q] = sums_ref[core, :, 1152 + j * 128 : 1280 + j * 128]
    gp_out[:, mine_q] = sums_ref[core, :, 1024:1152]
    gu_out[:, mine_f] = sums_ref[core, :, 512:1024]
    gd_out[:, mine_f] = sums_ref[core, :, 0:512]

    def weight_block(m, i):
        if m == 0:
            return wq_ref[:, i // 2, (i % 2) * 128 : (i % 2) * 128 + 128]
        return (None, wp_ref, wu_ref, wd_ref)[m][:, i * 128 : (i + 1) * 128]

    def grad_block(m, i):
        if m == 0:
            return gq[i // 2, :, (i % 2) * 128 : (i % 2) * 128 + 128]
        return (None, gp_out, gu_out, gd_out)[m][:, i * 128 : (i + 1) * 128]

    zero = jnp.zeros((128, 128), jnp.float32)

    def total_of(v):
        return jnp.sum(jnp.sum(v, axis=0, keepdims=True), axis=1, keepdims=True)

    weight_squares = []
    for m in range(4):
        acc = zero
        for i in range(BLOCKS[m]):
            w = weight_block(m, i)
            acc += w * w
        weight_squares.append(total_of(acc))

    for copy in core_copies():
        copy.wait()
    lane_send[...] = jnp.zeros_like(lane_send)
    row = 0
    for m in range(4):
        acc = zero
        for i in range(BLOCKS[m]):
            g = grad_block(m, i)
            square = g * g
            acc += square
            col_send[row : row + 1, :] = jnp.sum(square, axis=0, keepdims=True)
            row += 1
        lane_send[8 + m : 9 + m, :] = jnp.sum(acc.T, axis=0, keepdims=True)

    for copy in round_a():
        copy.wait()
    vec_sum = vec_recv[0]
    for slot in range(1, 8):
        vec_sum += vec_recv[slot]
    lane_send[0:8, :] = vec_sum
    col_send[24:32, :] = db_recv[0] + db_recv[1] + db_recv[2] + db_recv[3]

    def round_b():
        copies = [
            remote(lane_send, lane_recv.at[z], b_send.at[z], b_recv.at[z], device(0, 0, z)) for z in range(1, 4)
        ]
        copies += [
            remote(col_send, col_recv.at[slot], b_send.at[3 + slot], b_recv.at[3 + slot], device(q, dc, 0))
            for slot, q, dc in shard_peers
        ]
        return copies

    for copy in round_b():
        copy.start()
    for copy in round_b():
        copy.wait()
    lane_total = lane_send[...] + lane_recv[1] + lane_recv[2] + lane_recv[3]
    same = col_send[...] + col_recv[2] + col_recv[4] + col_recv[6]
    cross = col_recv[1] + col_recv[3] + col_recv[5] + col_recv[7]
    col_total = same[0:24] + cross[0:24]
    low_half = jnp.where(core == 0, same[24:32], cross[24:32])
    high_half = jnp.where(core == 0, cross[24:32], same[24:32])
    bq_out[:, 0:128] = low_half[0:3]
    bq_out[:, 128:256] = high_half[0:3]
    bu_out[0:4, :] = low_half[3:7]
    bu_out[4:8, :] = high_half[3:7]

    lane_out[...] = lane_total
    col_out[...] = col_total
    gvec = lane_total[0:8]
    _, v_dir = stepped(gvec, vs_ref[...])
    _, bq_dir = stepped(bq_out[...], bqs_ref[...])
    _, bu_dir = stepped(bu_out[...], bus_ref[...])
    rows_new = rows_step(lane_total[8:12], rows_ref[...])
    inverse_rows = lax.rsqrt(rows_new)
    spots = lax.broadcasted_iota(jnp.int32, (8, 128), 1)
    message = jnp.zeros((8, 128), jnp.float32)
    sums = []
    inverse_cols = []
    tall = []
    row = 0
    for m in range(4):
        tall.append(jnp.broadcast_to(inverse_rows[m : m + 1], (128, 128)).T)
        acc = zero
        for i in range(BLOCKS[m]):
            if m == 0:
                old = cq_ref[i // 2 : i // 2 + 1, (i % 2) * 128 : (i % 2) * 128 + 128]
            else:
                old = (None, cp_ref, cu_ref, cd_ref)[m][i : i + 1, :]
            new = DECAY * old + (1.0 - DECAY) * (col_total[row : row + 1] / D + TINY)
            inverse_cols.append(lax.rsqrt(new))
            step = grad_block(m, i) * tall[m] * inverse_cols[row]
            acc += step * step
            row += 1
        sums.append(total_of(acc))
    terms = sums
    terms = terms + [0.25 * total_of(rows_new[m : m + 1]) for m in range(4)]
    terms = terms + weight_squares
    vw = vw_ref[...]
    v_squares = jnp.sum(v_dir * v_dir, axis=1, keepdims=True)
    w_squares = jnp.sum(vw * vw, axis=1, keepdims=True)
    terms = terms + [0.25 * v_squares[i : i + 1] for i in range(6)]
    terms = terms + [0.25 * w_squares[i : i + 1] for i in range(6)]
    for value in (bq_dir, bu_dir, bq_ref[...], bu_ref[...]):
        terms = terms + [0.125 * total_of(value * value)]
    for i, term in enumerate(terms):
        message = jnp.where(spots == i, term, message)
    all_send[...] = message

    def round_c():
        return [
            remote(all_send, all_recv.at[slot], c_send.at[slot], c_recv.at[slot], device(q, dc, z))
            for slot, q, dc, z in others
        ]

    for copy in round_c():
        copy.start()
    for copy in round_c():
        copy.wait()
    grand = message
    for slot, _, _, _ in others:
        grand += all_recv[slot]
    grand_out[...] = grand


def apply_kernel(
    gq, gp_ref, gu_ref, gd_ref, bg_ref, ug_ref, lane_ref, col_ref, grand_ref,
    wq_ref, wp_ref, wu_ref, wd_ref, vw_ref, vs_ref, rows_ref,
    cq_ref, cp_ref, cu_ref, cd_ref, bq_ref, bu_ref, bqs_ref, bus_ref,
    gq_out, gp_out, gu_out, gd_out, nq_out, np_out, nu_out, nd_out, vec_out, rows_out,
    cq_out, cp_out, cu_out, cd_out, bq_out, bqs_out, bqn_out, bu_out, bus_out, bun_out, rms_out,
):
    def weight_block(m, i):
        if m == 0:
            return wq_ref[:, i // 2, (i % 2) * 128 : (i % 2) * 128 + 128]
        return (None, wp_ref, wu_ref, wd_ref)[m][:, i * 128 : (i + 1) * 128]

    def grad_block(m, i):
        if m == 0:
            return gq[i // 2, :, (i % 2) * 128 : (i % 2) * 128 + 128]
        return (None, gp_ref, gu_ref, gd_ref)[m][:, i * 128 : (i + 1) * 128]

    for j in range(3):
        gq_out[:, j, :] = gq[j]
    gp_out[...] = gp_ref[...]
    gu_out[...] = gu_ref[...]
    gd_out[...] = gd_ref[...]
    bq_out[...] = bg_ref[...]
    bu_out[...] = ug_ref[...]
    gvec = lane_ref[0:8, :]
    vw = vw_ref[...]
    vs_new, v_dir = stepped(gvec, vs_ref[...])
    bqs_new, bq_dir = stepped(bg_ref[...], bqs_ref[...])
    bus_new, bu_dir = stepped(ug_ref[...], bus_ref[...])
    bqs_out[...] = bqs_new
    bus_out[...] = bus_new
    vec_out[0:8, :] = gvec
    vec_out[8:16, :] = vs_new
    rows_new = rows_step(lane_ref[8:12, :], rows_ref[...])
    rows_out[...] = rows_new
    inverse_rows = lax.rsqrt(rows_new)
    line = grand_ref[0:1, :]
    spot = lax.broadcasted_iota(jnp.int32, (1, 128), 1)

    def pick(i):
        return jnp.sum(jnp.where(spot == i, line, 0.0), axis=1, keepdims=True)

    rms_line = jnp.zeros((1, 128), jnp.float32)
    row = 0
    for m in range(4):
        size = float(D * COUNTS[m])
        mean_rows = pick(4 + m) / D
        rms = jnp.sqrt(pick(m) * mean_rows / size)
        scale = jnp.sqrt(pick(8 + m) / size)
        factor = RATE * scale * jnp.sqrt(mean_rows) / jnp.maximum(1.0, rms / CLIP_LEVEL)
        rms_line = jnp.where(spot == m, rms, rms_line)
        tall = jnp.broadcast_to(inverse_rows[m : m + 1], (128, 128)).T
        for i in range(BLOCKS[m]):
            if m == 0:
                old = cq_ref[i // 2 : i // 2 + 1, (i % 2) * 128 : (i % 2) * 128 + 128]
            else:
                old = (None, cp_ref, cu_ref, cd_ref)[m][i : i + 1, :]
            cols = DECAY * old + (1.0 - DECAY) * (col_ref[row : row + 1, :] / D + TINY)
            if m == 0:
                cq_out[i // 2 : i // 2 + 1, (i % 2) * 128 : (i % 2) * 128 + 128] = cols
            else:
                (None, cp_out, cu_out, cd_out)[m][i : i + 1, :] = cols
            new = weight_block(m, i) - factor * (grad_block(m, i) * tall * lax.rsqrt(cols))
            if m == 0:
                nq_out[:, i // 2, (i % 2) * 128 : (i % 2) * 128 + 128] = new
            else:
                (None, np_out, nu_out, nd_out)[m][:, i * 128 : (i + 1) * 128] = new
            row += 1
    rms_out[...] = rms_line
    for i in range(6):
        spread = jnp.sqrt(pick(12 + i) / D)
        factor = RATE * jnp.sqrt(pick(18 + i) / D) / jnp.maximum(1.0, spread / CLIP_LEVEL)
        vec_out[16 + i : 17 + i, :] = vw[i : i + 1] - factor * v_dir[i : i + 1]
    vec_out[22:24, :] = jnp.zeros((2, 128), jnp.float32)
    for direction, weight, out, at, size in (
        (bq_dir, bq_ref, bqn_out, 24, 3 * D),
        (bu_dir, bu_ref, bun_out, 25, FF),
    ):
        spread = jnp.sqrt(pick(at) / size)
        factor = RATE * jnp.sqrt(pick(at + 2) / size) / jnp.maximum(1.0, spread / CLIP_LEVEL)
        out[...] = weight[...] - factor * direction


def tune_all(sums, vec_part, db_part, params, stats, states):
    qkv_weight, qkv_bias, proj_weight, fc1_weight, fc1_bias, fc2_weight, vectors = params
    row_state, qkv_cols, proj_cols, fc1_cols, fc2_cols = stats
    vector_state, qkv_bias_state, fc1_bias_state = states
    pad = ((0, 2), (0, 0))

    def dense(v):
        return v.reshape(v.shape[0] // 128, 128)

    operands = (
        sums, vec_part, db_part, qkv_weight, proj_weight, fc1_weight, fc2_weight,
        jnp.pad(vectors.T, pad), jnp.pad(vector_state.T, pad, constant_values=1.0), row_state,
        qkv_cols, dense(proj_cols), dense(fc1_cols), dense(fc2_cols),
        qkv_bias, dense(fc1_bias), qkv_bias_state, dense(fc1_bias_state),
    )
    vmem = pl.BlockSpec(memory_space=pltpu.VMEM)
    shapes = [
        (128, 3, 256), (128, 256), (128, 1024), (128, 1024),
        (128, 3, 256), (128, 256), (128, 1024), (128, 1024),
        (24, 128), (4, 128), (3, 256), (2, 128), (8, 128), (8, 128),
        (3, 256), (3, 256), (3, 256), (8, 128), (8, 128), (8, 128), (1, 128),
    ]
    f32 = jnp.float32
    middle = [
        (3, 128, 256), (128, 256), (128, 1024), (128, 1024), (3, 256), (8, 128), (16, 128), (24, 128), (8, 128)
    ]
    reduced = pl.pallas_call(
        tune_kernel,
        in_specs=[vmem] * len(operands),
        out_specs=[vmem] * len(middle),
        out_shape=[jax.ShapeDtypeStruct(shape, f32) for shape in middle],
        scratch_shapes=[
            pltpu.VMEM((8, 8, 128), f32),
            pltpu.VMEM((8, 8, 128), f32),
            pltpu.VMEM((4, 8, 128), f32),
            pltpu.VMEM((16, 128), f32),
            pltpu.VMEM((4, 16, 128), f32),
            pltpu.VMEM((32, 128), f32),
            pltpu.VMEM((8, 32, 128), f32),
            pltpu.VMEM((8, 128), f32),
            pltpu.VMEM((32, 8, 128), f32),
            pltpu.SemaphoreType.DMA((6,)),
            pltpu.SemaphoreType.DMA((6,)),
            pltpu.SemaphoreType.DMA((11,)),
            pltpu.SemaphoreType.DMA((11,)),
            pltpu.SemaphoreType.DMA((11,)),
            pltpu.SemaphoreType.DMA((11,)),
            pltpu.SemaphoreType.DMA((32,)),
            pltpu.SemaphoreType.DMA((32,)),
        ],
        compiler_params=pltpu.CompilerParams(collective_id=4, has_side_effects=True, vmem_limit_bytes=40 * 1024 * 1024),
        name="tune_all",
    )(*operands)
    inputs = (*reduced, *operands[3:])
    (
        gq, gp, gu, gd, nq, np_, nu, nd, vec, rows, cq, cp, cu, cd, bq, bqs, bqn, bu, bus, bun, rms
    ) = pl.pallas_call(
        apply_kernel,
        in_specs=[vmem] * len(inputs),
        out_specs=[vmem] * len(shapes),
        out_shape=[jax.ShapeDtypeStruct(shape, f32) for shape in shapes],
        compiler_params=pltpu.CompilerParams(vmem_limit_bytes=40 * MIB),
        name="apply_all",
    )(*inputs)
    vec = vec.T
    return (
        gq, bq, gp, gu, bu.reshape(1024), gd, vec[:, 0:6], rows,
        cq, cp.reshape(256), cu.reshape(1024), cd.reshape(1024),
        vec[:, 8:14], bqs, bus.reshape(1024),
        nq, bqn, np_, nu, bun.reshape(1024), nd, vec[:, 16:22], rms[0, 0:4],
    )


def gelu_parts(u):
    cdf = 0.5 * (1.0 + lax.erf(u * (0.5**0.5)))
    density = jnp.exp(-0.5 * u * u) * ((2.0 * jnp.pi) ** -0.5)
    return u * cdf, cdf + u * density


def norm_parts(values):
    center = values - jnp.mean(values, axis=-1, keepdims=True)
    scale = lax.rsqrt(jnp.mean(center * center, axis=-1, keepdims=True) + NORM_EPS)
    return center * scale, scale


def norm_back(grad, unit, scale, gain):
    c = grad * gain
    return scale * (
        c
        - jnp.mean(c, axis=-1, keepdims=True)
        - unit * jnp.mean(c * unit, axis=-1, keepdims=True)
    )


def on_chip(
    tokens,
    cotangent,
    qkv_weight,
    qkv_bias,
    proj_weight,
    fc1_weight,
    fc1_bias,
    fc2_weight,
    vectors,
    row_state,
    qkv_cols,
    proj_cols,
    fc1_cols,
    fc2_cols,
    vector_state,
    qkv_bias_state,
    fc1_bias_state,
):
    shard = lax.axis_index("fsdp")
    core = shard % 2
    rows = tokens.shape[0]
    hw, fw = qkv_weight.shape[2] // 2, fc1_weight.shape[1] // 2
    shard_rows = qkv_weight.shape[0]

    def both_halves(v):
        return jnp.concatenate([v, lax.ppermute(v, "fsdp", CORE_SWAP)], axis=0)

    def core_sum(left, right_t):
        other = times_transposed(left[rows:], right_t)
        other = lax.ppermute(other, "fsdp", CORE_SWAP)
        return times_transposed(left[:rows], right_t) + other

    def half_columns(w, width, which):
        return lax.dynamic_slice_in_dim(w, which * width, width, w.ndim - 1)

    def pack(which):
        return jnp.concatenate(
            [
                qkv_weight[:, :, which * hw : (which + 1) * hw].reshape(shard_rows, 3 * hw),
                proj_weight[:, which * hw : (which + 1) * hw],
                fc1_weight[:, which * fw : (which + 1) * fw],
                fc2_weight[:, which * fw : (which + 1) * fw],
            ],
            axis=1,
        ).astype(LOW)

    packs = jnp.stack([pack(0), pack(1)])
    vec = jnp.pad(vectors.astype(LOW).astype(jnp.float32).T, ((0, 2), (0, 0)))
    bias = jnp.concatenate(
        [
            half_columns(qkv_bias, hw, core).reshape(3 * hw),
            lax.dynamic_slice_in_dim(fc1_bias, core * fw, fw, 0),
        ]
    )
    bias = jnp.broadcast_to(
        lax.optimization_barrier(bias.astype(LOW)).astype(jnp.float32), (8, 3 * hw + fw)
    )
    (
        weight_qkv, weight_proj, weight_up, weight_down, vec_all, bias_all, normed_one, low, mixed, lse,
        tokens_all, grad_out_all, *tables,
    ) = gather_all(packs, vec, bias, tokens, cotangent)
    vector_rows = vec_all.transpose(1, 0, 2).reshape(8, D)
    _, _, proj_shift, gain_two, shift_two, down_shift = [
        vector_rows[i : i + 1] for i in range(6)
    ]
    bias_rows = bias_all[:, 0]
    bias_up = (
        bias_rows[:, 3 * hw :].reshape(4, 2, fw // 2).transpose(1, 0, 2).reshape(1, 4 * fw)
    )

    inputs = tokens_all[:rows].astype(jnp.float32)
    upstream = grad_out_all[:rows].astype(jnp.float32)
    middle = inputs + core_sum(mixed, weight_proj) + proj_shift
    unit_two, scale_two = norm_parts(middle)
    normed_two = both_halves((unit_two * gain_two + shift_two).astype(LOW))
    hidden = jnp.dot(normed_two, weight_up, preferred_element_type=jnp.float32) + bias_up
    active, slope = gelu_parts(hidden)
    active = active.astype(LOW)
    grad_down = contract_rows(grad_out_all, active).astype(LOW)
    layer_local = middle + core_sum(active, weight_down) + down_shift
    grad_active = jnp.dot(grad_out_all, weight_down, preferred_element_type=jnp.float32)
    grad_hidden = (grad_active * slope).astype(LOW)
    grad_up = contract_rows(normed_two, grad_hidden).astype(LOW)
    grad_bias_up = jnp.sum(grad_hidden.astype(jnp.float32), axis=0)
    grad_normed_two = core_sum(grad_hidden, weight_up)
    grad_middle = upstream + norm_back(grad_normed_two, unit_two, scale_two, gain_two)
    grad_branch = grad_middle.astype(LOW)
    grad_branch_all = both_halves(grad_branch)
    grad_proj = contract_rows(grad_branch_all, mixed).astype(LOW)
    grad_mixed = jnp.dot(
        grad_branch_all, weight_proj, preferred_element_type=jnp.float32
    ).astype(LOW)
    sums, grad_bias_qkv, norm_sums, layer_low, input_low, input_local = scatter_all(
        (grad_down, grad_up, grad_proj),
        (low, grad_mixed, lse, *tables, normed_one, weight_qkv),
        (vec_all, tokens_all, grad_middle, layer_local.astype(LOW)),
    )
    layer_out, input_grad = place_rows(layer_local, layer_low, input_local, input_low)

    vec_part = jnp.concatenate(
        [
            norm_sums[0:2],
            jnp.sum(grad_branch.astype(jnp.float32), axis=0, keepdims=True),
            jnp.sum(grad_normed_two * unit_two, axis=0, keepdims=True),
            jnp.sum(grad_normed_two, axis=0, keepdims=True),
            jnp.sum(upstream, axis=0, keepdims=True),
            jnp.zeros((2, D), jnp.float32),
        ]
    )
    db_part = jnp.concatenate(
        [
            grad_bias_qkv.reshape(4, 3, hw),
            grad_bias_up.reshape(2, 4, 2, hw).transpose(1, 0, 2, 3).reshape(4, 4, hw),
            jnp.zeros((4, 1, hw), jnp.float32),
        ],
        axis=1,
    )
    return (
        layer_out,
        input_grad,
        *tune_all(
            sums,
            vec_part,
            db_part,
            (qkv_weight, qkv_bias, proj_weight, fc1_weight, fc1_bias, fc2_weight, vectors),
            (row_state, qkv_cols, proj_cols, fc1_cols, fc2_cols),
            (vector_state, qkv_bias_state, fc1_bias_state),
        ),
    )


def solution(mesh):
    chips = mesh.shape["fsdp"] == 8 and mesh.shape["tensor"] == 4
    return jax.shard_map(
        on_chip if chips else on_device,
        mesh=mesh,
        in_specs=(
            P(("fsdp", "tensor"), None),
            P(("fsdp", "tensor"), None),
            P("fsdp", None, "tensor"),
            P(None, "tensor"),
            P("fsdp", "tensor"),
            P("fsdp", "tensor"),
            P("tensor"),
            P("fsdp", "tensor"),
            P("fsdp", None),
            P(None, "fsdp"),
            P(None, "tensor"),
            P("tensor"),
            P("tensor"),
            P("tensor"),
            P("fsdp", None),
            P(None, "tensor"),
            P("tensor"),
        ),
        out_specs=(
            P(("fsdp", "tensor"), None),
            P(("fsdp", "tensor"), None),
            P("fsdp", None, "tensor"),
            P(None, "tensor"),
            P("fsdp", "tensor"),
            P("fsdp", "tensor"),
            P("tensor"),
            P("fsdp", "tensor"),
            P("fsdp", None),
            P(None, "fsdp"),
            P(None, "tensor"),
            P("tensor"),
            P("tensor"),
            P("tensor"),
            P("fsdp", None),
            P(None, "tensor"),
            P("tensor"),
            P("fsdp", None, "tensor"),
            P(None, "tensor"),
            P("fsdp", "tensor"),
            P("fsdp", "tensor"),
            P("tensor"),
            P("fsdp", "tensor"),
            P("fsdp", None),
            P(),
        ),
        check_vma=False,
    )
```
